32 devices in a mesh: section: 4 (over z), dp: 2 (over x), mp: 4 (over y, core).
Axes of the slice: x: 2, y: 2, z: 4, core: 2. Of those that a mesh axis runs over, the one named last changes fastest.
Arguments:
- entrance: bfloat16 [2, 2, 96, 4096], P('dp'), may hold values from -6 to 6
- lengths: int32 [2, 2], P('dp'), may hold values from 24 to 96
- positives: int32 [2], replicated, may hold values from 0 to 1, each once
- norm_gains: float32 [4, 4096], P('section'), may hold values from 0.5 to 1.5
- query_proj: bfloat16 [4, 4096, 2048], P('section', None, 'mp'), may hold values from -0.09375 to 0.09375
- key_proj: bfloat16 [4, 4096, 512], P('section', None, 'mp'), may hold values from -0.09375 to 0.09375
- value_proj: bfloat16 [4, 4096, 512], P('section', None, 'mp'), may hold values from -0.09375 to 0.09375
- out_proj: bfloat16 [4, 2048, 4096], P('section', 'mp'), may hold values from -0.125 to 0.125
Outputs:
- losses: float32 [4, 7], P('section')
- norm_gain_grad: float32 [4, 4096], P('section', ('dp', 'mp'))
- query_proj_grad: float32 [4, 4096, 2048], P('section', 'dp', 'mp')
- key_proj_grad: float32 [4, 4096, 512], P('section', 'dp', 'mp')
- value_proj_grad: float32 [4, 4096, 512], P('section', 'dp', 'mp')
- out_proj_grad: float32 [4, 2048, 4096], P('section', 'mp', 'dp')
The draws below stay inside these ranges and needn't reach their ends.
Inputs may be any that keep to these rules, and one draw needn't show every extreme that they name: positives is a permutation of the pair indices. `lengths`: tokens at or past a sequence's length are padding.
All inputs are finite; a program needn't handle non-finite values.
Results may differ from the reference program's by a relative error of at most 0.039.
Values may be sent and summed in bfloat16 or wider, within the bound.
A program may use at most 128 MiB of HBM per device.

```python
import jax
import jax.numpy as jnp
from jax import lax

D = 4096
HQ = 16
HK = 4
HEAD = 128
WIDTHS = 7
LEN = 96
PAIRS = 2
N_SECTION = 4
N_MP = 4


def with_ends(entries, stream_key, low, high):
    longest = entries.shape.index(max(entries.shape))
    spots = []
    for shift in (0, 1):
        where = [jax.random.randint(jax.random.fold_in(stream_key, axis), (), 0, length) for axis, length in enumerate(entries.shape)]
        where[longest] = (where[longest] + shift) % entries.shape[longest]
        spots.append(tuple(where))
    return entries.at[spots[0]].set(low).at[spots[1]].set(high)


def block_levels(rng, shape, split, low, largest):
    loudness = 1.0
    for axis_at, shards_of in split:
        heights = jax.random.uniform(jax.random.fold_in(jax.random.fold_in(rng, 6), axis_at), (shards_of,), jnp.float32, low / len(split), largest / len(split))
        loudness = loudness * jnp.repeat(jnp.exp(heights), shape[axis_at] // shards_of).reshape((-1,) + (1,) * (len(shape) - 1 - axis_at))
    return loudness


def gaussian(stream_key, dims, spread, limit, split=(), held_as=jnp.bfloat16):
    loudness = block_levels(stream_key, dims, split, -0.22, 0.18) if split else 1.0
    values = jax.random.normal(stream_key, dims, jnp.float32) * spread * loudness
    return jnp.minimum(jnp.maximum(values, -limit), limit).astype(held_as)


def setup_inputs(seed: int = 0) -> dict:
    seeds = jax.random.split(jax.random.key(seed), 9)
    entrance = gaussian(seeds[0], (PAIRS, 2, LEN, D), 1.0, 6.0, ((0, 2),))
    lengths = with_ends(jax.random.randint(seeds[1], (PAIRS, 2), LEN // 4, LEN + 1), jax.random.fold_in(seeds[1], 1), LEN // 4, LEN).astype(jnp.int32)
    positives = jax.random.permutation(seeds[2], PAIRS).astype(jnp.int32)
    norm_gains = jnp.clip(1.0 + 0.1 * jax.random.normal(seeds[3], (N_SECTION, D), jnp.float32), 0.5, 1.5)
    query_proj = gaussian(seeds[4], (N_SECTION, D, HQ * HEAD), D ** -0.5, 0.09375, ((0, 4), (2, 4)))
    key_proj = gaussian(seeds[5], (N_SECTION, D, HK * HEAD), D ** -0.5, 0.09375, ((0, 4), (2, 4)))
    value_proj = gaussian(seeds[6], (N_SECTION, D, HK * HEAD), D ** -0.5, 0.09375, ((0, 4), (2, 4)))
    out_proj = gaussian(seeds[7], (N_SECTION, HQ * HEAD, D), (HQ * HEAD) ** -0.5, 0.125, ((0, 4), (1, 4)))
    return dict(entrance=entrance, lengths=lengths, positives=positives, norm_gains=norm_gains, query_proj=query_proj, key_proj=key_proj, value_proj=value_proj, out_proj=out_proj)


EPSILON = 1e-05
SOFTMAX_TEMPER = 0.05
ROPE_BASE = 500000.0

def rope_tables(length, head_size):
    half_size = head_size // 2
    inverse_freq = ROPE_BASE ** (-jnp.arange(half_size, dtype=jnp.float32) * 2.0 / head_size)
    angles = jnp.arange(length, dtype=jnp.float32)[:, None] * inverse_freq[None, :]
    return (jnp.cos(angles), jnp.sin(angles))

def rotate(values, cosine, sine_table):
    half_size = values.shape[-1] // 2
    first_half = values[..., :half_size]
    second = values[..., half_size:]
    cosine = cosine[None, :, None, :]
    sine_table = sine_table[None, :, None, :]
    return jnp.concatenate([first_half * cosine - second * sine_table, second * cosine + first_half * sine_table], axis=-1)

def attend(query_pre, key_pre, value_pre):
    seq_count, length, query_width = query_pre.shape
    query_heads = query_width // HEAD
    kv_heads = key_pre.shape[-1] // HEAD
    group_size = query_heads // kv_heads
    cosine, sine_table = rope_tables(length, HEAD)
    query_vectors = rotate(query_pre.reshape(seq_count, length, query_heads, HEAD), cosine, sine_table).astype(jnp.bfloat16)
    key_rows = rotate(key_pre.reshape(seq_count, length, kv_heads, HEAD), cosine, sine_table).astype(jnp.bfloat16)
    values = value_pre.reshape(seq_count, length, kv_heads, HEAD).astype(jnp.bfloat16)
    query_vectors = query_vectors.reshape(seq_count, length, kv_heads, group_size, HEAD)
    scores = jnp.einsum('sikge,sjke->skgij', query_vectors.astype(jnp.float32), key_rows.astype(jnp.float32)) * HEAD ** (-0.5)
    causal = jnp.arange(length, dtype=jnp.int32)[:, None] >= jnp.arange(length, dtype=jnp.int32)[None, :]
    scores = jnp.where(causal, scores, -1e+30)
    weights = jax.nn.softmax(scores, axis=-1).astype(jnp.bfloat16)
    mixture = jnp.einsum('skgij,sjke->sikge', weights.astype(jnp.float32), values.astype(jnp.float32))
    return mixture.reshape(seq_count, length, query_heads * HEAD)

def normalize(hidden_f, gain_vector):
    inv_rms = lax.rsqrt(lax.optimization_barrier(jnp.mean(hidden_f * hidden_f, axis=-1, keepdims=True)) + EPSILON)
    return hidden_f * inv_rms * gain_vector

def contract_rows(left, right):
    return lax.dot_general(left, right, (((0,), (0,)), ((), ())), preferred_element_type=jnp.float32)

def contract_last(left, right):
    return lax.dot_general(left, right, (((left.ndim - 1,), (1,)), ((), ())), preferred_element_type=jnp.float32)

def pool_exits(batch_rows, mask_of_valid, counts):
    total_value = jnp.einsum('ki,kiu->ku', mask_of_valid, batch_rows.astype(jnp.float32))
    return total_value / counts[:, None]

def spread_grad(exit_grad, mask_of_valid, counts):
    return mask_of_valid[:, :, None] * (exit_grad / counts[:, None])[:, None, :]

def matryoshka_losses(pooled, positives):
    pair_total = pooled.shape[0]
    target = (jnp.arange(pair_total, dtype=jnp.int32)[None, :] == positives[:, None]).astype(jnp.float32)
    losses = []
    for level_index in range(WIDTHS):
        leading_width = pooled.shape[-1] // 2 ** level_index
        query_vectors = pooled[:, 0, :leading_width]
        passage_rows = pooled[:, 1, :leading_width]
        query_vectors = query_vectors * lax.rsqrt(lax.optimization_barrier(jnp.mean(query_vectors * query_vectors, axis=-1, keepdims=True)) + 1e-06)
        passage_rows = passage_rows * lax.rsqrt(lax.optimization_barrier(jnp.mean(passage_rows * passage_rows, axis=-1, keepdims=True)) + 1e-06)
        score_matrix = jnp.dot(query_vectors, passage_rows.T, precision=lax.Precision.HIGHEST) / (leading_width * SOFTMAX_TEMPER)
        picked = lax.optimization_barrier(jnp.sum(score_matrix * target, axis=-1))
        losses.append(jnp.mean(jax.nn.logsumexp(score_matrix, axis=-1) - picked))
    return jnp.stack(losses)

def section_forward(hidden, gain_vector, query_weight, key_weight, value_weight, out_weight):
    hidden_f = hidden.astype(jnp.float32)
    normed = normalize(hidden_f, gain_vector).astype(jnp.bfloat16)
    query_cols = query_weight.shape[1] // N_MP
    kv_cols = key_weight.shape[1] // N_MP
    total_value = jnp.zeros(hidden_f.shape, jnp.float32)
    for member in range(N_MP):
        query_slice = query_weight[:, member * query_cols:(member + 1) * query_cols]
        key_slice = key_weight[:, member * kv_cols:(member + 1) * kv_cols]
        value_slice = value_weight[:, member * kv_cols:(member + 1) * kv_cols]
        out_slice = out_weight[member * query_cols:(member + 1) * query_cols]
        mixture = attend(jnp.dot(normed, query_slice, preferred_element_type=jnp.float32), jnp.dot(normed, key_slice, preferred_element_type=jnp.float32), jnp.dot(normed, value_slice, preferred_element_type=jnp.float32)).astype(jnp.bfloat16)
        partial_value = jnp.dot(mixture, out_slice, preferred_element_type=jnp.float32).astype(jnp.bfloat16)
        total_value = total_value + partial_value.astype(jnp.float32)
    return (hidden_f + total_value).astype(jnp.bfloat16)

def section_backward(hidden, upstream, gain_vector, query_weight, key_weight, value_weight, out_weight):
    hidden_f = hidden.astype(jnp.float32)
    inv_rms = lax.rsqrt(lax.optimization_barrier(jnp.mean(hidden_f * hidden_f, axis=-1, keepdims=True)) + EPSILON)
    normed = normalize(hidden_f, gain_vector).astype(jnp.bfloat16)
    out_grad = upstream.astype(jnp.bfloat16)
    query_cols = query_weight.shape[1] // N_MP
    kv_cols = key_weight.shape[1] // N_MP
    width_all = hidden.shape[-1]
    normed_rows = normed.reshape(-1, width_all)
    out_rows = out_grad.reshape(-1, width_all)
    normed_grad = jnp.zeros(hidden_f.shape, jnp.float32)
    query_parts, key_parts, value_parts, out_parts = ([], [], [], [])
    for member in range(N_MP):
        query_slice = query_weight[:, member * query_cols:(member + 1) * query_cols]
        key_slice = key_weight[:, member * kv_cols:(member + 1) * kv_cols]
        value_slice = value_weight[:, member * kv_cols:(member + 1) * kv_cols]
        out_slice = out_weight[member * query_cols:(member + 1) * query_cols]
        mixture_f, pullback = jax.vjp(attend, jnp.dot(normed, query_slice, preferred_element_type=jnp.float32), jnp.dot(normed, key_slice, preferred_element_type=jnp.float32), jnp.dot(normed, value_slice, preferred_element_type=jnp.float32))
        mixture = mixture_f.astype(jnp.bfloat16)
        mixture_grad = contract_last(out_grad, out_slice).astype(jnp.bfloat16)
        pulled = pullback(lax.optimization_barrier(mixture_grad).astype(jnp.float32))
        query_grad, key_grad, value_grad = [piece_grad.astype(jnp.bfloat16) for piece_grad in pulled]
        member_grad = contract_last(query_grad, query_slice) + contract_last(key_grad, key_slice) + contract_last(value_grad, value_slice)
        normed_grad = normed_grad + lax.optimization_barrier(member_grad.astype(jnp.bfloat16)).astype(jnp.float32)
        query_parts.append(contract_rows(normed_rows, query_grad.reshape(-1, query_cols)))
        key_parts.append(contract_rows(normed_rows, key_grad.reshape(-1, kv_cols)))
        value_parts.append(contract_rows(normed_rows, value_grad.reshape(-1, kv_cols)))
        out_parts.append(contract_rows(mixture.reshape(-1, query_cols), out_rows))
    gain_grad = lax.optimization_barrier(jnp.sum(normed_grad * hidden_f * inv_rms, axis=(0, 1)))
    _, norm_pull = jax.vjp(lambda values: normalize(values, gain_vector), hidden_f)
    input_grad = (upstream + norm_pull(normed_grad)[0]).astype(jnp.bfloat16)
    return (input_grad, (gain_grad, jnp.concatenate(query_parts, axis=1), jnp.concatenate(key_parts, axis=1), jnp.concatenate(value_parts, axis=1), jnp.concatenate(out_parts, axis=0)))

def reference(entrance, lengths, positives, norm_gains, query_proj, key_proj, value_proj, out_proj):
    seq_count = 2 * PAIRS
    hidden = entrance.reshape(seq_count, LEN, D)
    mask_of_valid = (jnp.arange(LEN, dtype=jnp.int32)[None, :] < lengths.reshape(seq_count, 1)).astype(jnp.float32)
    counts = lax.optimization_barrier(jnp.sum(mask_of_valid, axis=1))
    section_inputs = []
    loss_rows = []
    token_grads = []
    for section_index in range(N_SECTION):
        section_inputs.append(hidden)
        hidden = section_forward(hidden, norm_gains[section_index], query_proj[section_index], key_proj[section_index], value_proj[section_index], out_proj[section_index])
        pooled = pool_exits(hidden, mask_of_valid, counts).reshape(PAIRS, 2, D)
        losses_now, pullback = jax.vjp(lambda embedded: matryoshka_losses(embedded, positives), pooled)
        exit_grad = pullback(jnp.ones((WIDTHS,), jnp.float32))[0]
        loss_rows.append(losses_now)
        token_grads.append(spread_grad(exit_grad.reshape(seq_count, D), mask_of_valid, counts))
    incoming = jnp.zeros((seq_count, LEN, D), jnp.bfloat16)
    results = [None] * N_SECTION
    for section_index in reversed(range(N_SECTION)):
        upstream = token_grads[section_index] + incoming.astype(jnp.float32)
        incoming, grads_now = section_backward(section_inputs[section_index], upstream, norm_gains[section_index], query_proj[section_index], key_proj[section_index], value_proj[section_index], out_proj[section_index])
        results[section_index] = grads_now
    return (jnp.stack(loss_rows), jnp.stack([entry[0] for entry in results]), jnp.stack([entry[1] for entry in results]), jnp.stack([entry[2] for entry in results]), jnp.stack([entry[3] for entry in results]), jnp.stack([entry[4] for entry in results]))
```

```python
import functools

import jax
import jax.numpy as jnp
import numpy as np
from jax import lax
from jax.experimental import pallas as pl
from jax.experimental.pallas import tpu as pltpu
from jax.sharding import PartitionSpec as P

HEAD = 128
WIDTHS = 7


EPSILON = 1e-05
SOFTMAX_TEMPER = 0.05
ROPE_BASE = 500000.0
MESH = pl.DeviceIdType.MESH
ROW_TILE = 16
SUB = 4
F32 = jnp.float32
BF16 = jnp.bfloat16


def rope_tables(length, head_size):
    half_size = head_size // 2
    inverse_freq = ROPE_BASE ** (-jnp.arange(half_size, dtype=jnp.float32) * 2.0 / head_size)
    angles = jnp.arange(length, dtype=jnp.float32)[:, None] * inverse_freq[None, :]
    return (jnp.cos(angles), jnp.sin(angles))


def rotate(values, cosine, sine_table):
    half_size = values.shape[-1] // 2
    first_half = values[..., :half_size]
    second = values[..., half_size:]
    cosine = cosine[None, :, None, :]
    sine_table = sine_table[None, :, None, :]
    return jnp.concatenate(
        [first_half * cosine - second * sine_table, second * cosine + first_half * sine_table],
        axis=-1,
    )


def attend(query_pre, key_pre, value_pre):
    seq_count, length, query_width = query_pre.shape
    query_heads = query_width // HEAD
    kv_heads = key_pre.shape[-1] // HEAD
    group_size = query_heads // kv_heads
    cosine, sine_table = rope_tables(length, HEAD)
    query_vectors = rotate(
        query_pre.reshape(seq_count, length, query_heads, HEAD), cosine, sine_table
    ).astype(jnp.bfloat16)
    key_rows = rotate(
        key_pre.reshape(seq_count, length, kv_heads, HEAD), cosine, sine_table
    ).astype(jnp.bfloat16)
    values = value_pre.reshape(seq_count, length, kv_heads, HEAD).astype(jnp.bfloat16)
    query_vectors = query_vectors.reshape(seq_count, length, kv_heads, group_size, HEAD)
    scores = jnp.einsum(
        "sikge,sjke->skgij", query_vectors.astype(jnp.float32), key_rows.astype(jnp.float32)
    ) * HEAD ** (-0.5)
    causal = (
        jnp.arange(length, dtype=jnp.int32)[:, None] >= jnp.arange(length, dtype=jnp.int32)[None, :]
    )
    scores = jnp.where(causal, scores, -1e30)
    weights = jax.nn.softmax(scores, axis=-1).astype(jnp.bfloat16)
    mixture = jnp.einsum(
        "skgij,sjke->sikge", weights.astype(jnp.float32), values.astype(jnp.float32)
    )
    return mixture.reshape(seq_count, length, query_heads * HEAD)


def normalize(hidden_f, gain_vector):
    inv_rms = lax.rsqrt(jnp.mean(hidden_f * hidden_f, axis=-1, keepdims=True) + EPSILON)
    return hidden_f * inv_rms * gain_vector


def contract_rows(left, right):
    return lax.dot_general(
        left, right, (((0,), (0,)), ((), ())), preferred_element_type=jnp.float32
    )


def contract_last(left, right):
    return lax.dot_general(
        left, right, (((left.ndim - 1,), (1,)), ((), ())), preferred_element_type=jnp.float32
    )


def spread_grad(exit_grad, mask_of_valid, counts):
    return mask_of_valid[:, :, None] * (exit_grad / counts[:, None])[:, None, :]


def matryoshka_losses(pooled, positives):
    pair_total = pooled.shape[0]
    target = (jnp.arange(pair_total, dtype=jnp.int32)[None, :] == positives[:, None]).astype(
        jnp.float32
    )
    losses = []
    for level_index in range(WIDTHS):
        leading_width = pooled.shape[-1] // 2**level_index
        query_vectors = pooled[:, 0, :leading_width]
        passage_rows = pooled[:, 1, :leading_width]
        query_vectors = query_vectors * lax.rsqrt(
            jnp.mean(query_vectors * query_vectors, axis=-1, keepdims=True) + 1e-06
        )
        passage_rows = passage_rows * lax.rsqrt(
            jnp.mean(passage_rows * passage_rows, axis=-1, keepdims=True) + 1e-06
        )
        score_matrix = jnp.dot(query_vectors, passage_rows.T, precision=lax.Precision.HIGHEST) / (
            leading_width * SOFTMAX_TEMPER
        )
        picked = jnp.sum(score_matrix * target, axis=-1)
        losses.append(jnp.mean(jax.nn.logsumexp(score_matrix, axis=-1) - picked))
    return jnp.stack(losses)


def rotary_constants(length):
    half_size = HEAD // 2
    frequencies = ROPE_BASE ** (-np.arange(half_size, dtype=np.float64) * 2.0 / HEAD)
    angles = np.arange(length, dtype=np.float64)[:, None] * frequencies[None, :]
    cosine = np.concatenate([np.cos(angles), np.cos(angles)], axis=1)
    sine = np.concatenate([-np.sin(angles), np.sin(angles)], axis=1)
    return np.stack([cosine, sine]).astype(np.float32)


def mp_place(me, levels):
    bits = [(me // (1 << level)) % 2 for level in range(levels)]
    partners = [me + (1 - 2 * bits[level]) * (1 << level) for level in range(levels)]
    return bits, partners


def shard_offset(bits, rows, flips=0):
    offset = 0
    for level, bit in enumerate(bits):
        bit = 1 - bit if (flips >> level) & 1 else bit
        offset = offset + bit * (rows >> (level + 1))
    return offset


def rows_at(start, size):
    return pl.ds(pl.multiple_of(start, ROW_TILE), size)


def lanes_at(start, size):
    return pl.ds(pl.multiple_of(start, 128), size)


class Place:
    def __init__(self, direction):
        self.here = lax.axis_index("section")
        self.count = lax.axis_size("section")
        (self.low, self.high), (self.near, self.far) = mp_place(lax.axis_index("mp"), 2)
        self.direction = direction
        if direction > 0:
            self.has_source, self.has_target = self.here > 0, self.here < self.count - 1
        else:
            self.has_source, self.has_target = self.here < self.count - 1, self.here > 0

    def quarter(self, flip_low, flip_high):
        low = 1 - self.low if flip_low else self.low
        high = 1 - self.high if flip_high else self.high
        return (low * 2 + high) * SUB


def send(source, target, sems, slot, **device):
    return pltpu.make_async_remote_copy(
        src_ref=source,
        dst_ref=target,
        send_sem=sems[0].at[slot],
        recv_sem=sems[1].at[slot],
        device_id=device,
        device_id_type=MESH,
    )


def stream_in(place, buf, relay, far, near, consume):
    def near_copy(slot, block):
        return send(buf.at[block], buf.at[block], near, slot, mp=place.near)

    def far_copy(slot, block):
        return send(buf.at[block], buf.at[block], far, slot, mp=place.far)

    own, other = place.quarter(0, 0), place.quarter(0, 1)
    near_own, near_other = place.quarter(1, 0), place.quarter(1, 1)
    for tick in range(SUB + 2):
        if tick < SUB:
            block = own + tick
            send(buf.at[block], buf.at[block], relay, tick, section=place.here).wait_recv()
            far_copy(tick, block).start()
            near_copy(tick, block).start()
        if 1 <= tick <= SUB:
            block = other + tick - 1
            far_copy(tick - 1, block).wait_recv()
            near_copy(SUB + tick - 1, block).start()
        if tick >= 2:
            step = tick - 2
            near_copy(step, near_own + step).wait_recv()
            near_copy(SUB + step, near_other + step).wait_recv()

            def body(part, carry, step=step):
                consume(part * SUB + step)
                return carry

            lax.fori_loop(0, 4, body, 0)
    for step in range(SUB):
        far_copy(step, own + step).wait_send()
        near_copy(step, own + step).wait_send()
        near_copy(SUB + step, other + step).wait_send()


def stream_out(place, part, finish, dest, bufs, relay, far, near):
    near_send, near_got, far_send, far_got, relay_send = bufs

    def near_copy(slot):
        return send(near_send.at[slot], near_got.at[slot], near, slot, mp=place.near)

    def far_copy(step):
        return send(far_send.at[step], far_got.at[step], far, step, mp=place.far)

    def relay_copy(step):
        return send(
            relay_send.at[step],
            dest.at[place.quarter(0, 0) + step],
            relay,
            step,
            section=place.here + place.direction,
        )

    for flip in (1, 0):
        base = (1 - place.high if flip else place.high) * SUB
        for step in range(SUB):
            near_send[base + step] = part(place.quarter(1, flip) + step).astype(BF16)
            near_copy(base + step).start()
    base = (1 - place.high) * SUB
    for step in range(SUB):
        value = part(place.quarter(0, 1) + step)
        near_copy(base + step).wait_recv()
        far_send[step] = (value + near_got[base + step].astype(F32)).astype(BF16)
        far_copy(step).start()
    base = place.high * SUB
    for step in range(SUB):
        value = part(place.quarter(0, 0) + step)
        near_copy(base + step).wait_recv()
        value = value + near_got[base + step].astype(F32)
        far_copy(step).wait_recv()
        value = value + far_got[step].astype(F32)
        relay_send[step] = finish(place.quarter(0, 0) + step, value)
        relay_copy(step).start()
    for step in range(SUB):
        far_copy(step).wait_send()
        relay_copy(step).wait_send()
    for slot in range(2 * SUB):
        near_copy(slot).wait_send()


def rotary(values, table, sign):
    turned = pltpu.roll(values, HEAD // 2, axis=1)
    return values * table[0] + turned * (table[1] * sign)


def forward_kernel(
    seq_count,
    entrance,
    gain,
    table,
    wq,
    wk,
    wv,
    wo,
    hidden,
    heads,
    head_w,
    out_w,
    acc,
    squares,
    mixture,
    near_send,
    near_got,
    far_send,
    far_got,
    relay_send,
    load_sem,
    relay_s,
    relay_r,
    in_far_s,
    in_far_r,
    in_near_s,
    in_near_r,
    out_far_s,
    out_far_r,
    out_near_s,
    out_near_r,
):
    place = Place(1)
    blocks, rows, width = hidden.shape
    width_all = blocks * width
    length = rows // seq_count
    query_cols = wq.shape[1]
    kv_cols = wk.shape[1]
    loads = [
        pltpu.make_async_copy(wq, head_w.at[:, :query_cols], load_sem.at[0]),
        pltpu.make_async_copy(wk, head_w.at[:, query_cols : query_cols + kv_cols], load_sem.at[1]),
        pltpu.make_async_copy(wv, head_w.at[:, query_cols + kv_cols :], load_sem.at[2]),
        pltpu.make_async_copy(wo, out_w, load_sem.at[3]),
    ]
    for load in loads:
        load.start()
    barrier = pltpu.get_barrier_semaphore()
    for partner in (place.near, place.far):
        pl.semaphore_signal(barrier, inc=1, device_id={"mp": partner}, device_id_type=MESH)

    @pl.when(place.has_source)
    def _():
        pl.semaphore_signal(
            barrier, inc=1, device_id={"section": place.here - 1}, device_id_type=MESH
        )

    @pl.when(place.has_target)
    def _():
        pl.semaphore_signal(
            barrier, inc=1, device_id={"section": place.here + 1}, device_id_type=MESH
        )

    expected = 2 + place.has_source.astype(jnp.int32) + place.has_target.astype(jnp.int32)
    pl.semaphore_wait(barrier, expected)

    acc[...] = jnp.zeros_like(acc)
    squares[...] = jnp.zeros_like(squares)

    def consume(block):
        value = hidden[block].astype(F32)
        square = value * value
        total = square[:, :128]
        for lane in range(1, width // 128):
            total = total + square[:, lane * 128 : (lane + 1) * 128]
        squares[...] += total
        scaled = (value * gain[:, lanes_at(block * width, width)]).astype(BF16)
        acc[...] += jnp.dot(
            scaled, head_w[rows_at(block * width, width), :], preferred_element_type=F32
        )

    for load in loads[:3]:
        load.wait()

    @pl.when(place.has_source)
    def _():
        stream_in(
            place, hidden, (relay_s, relay_r), (in_far_s, in_far_r), (in_near_s, in_near_r), consume
        )

    @pl.when(jnp.logical_not(place.has_source))
    def _():
        def body(block, carry):
            hidden[block] = entrance[:, lanes_at(block * width, width)]
            consume(block)
            return carry

        lax.fori_loop(0, blocks, body, 0)

    inv_rms = lax.rsqrt(
        jnp.sum(squares[...], axis=1, keepdims=True) * (1.0 / width_all) + EPSILON
    )
    heads[...] = acc[...] * inv_rms
    loads[3].wait()

    @pl.when(place.has_target)
    def _():
        groups = query_cols // HEAD
        for seq in range(seq_count):
            span = slice(seq * length, (seq + 1) * length)
            query = jnp.concatenate(
                [
                    rotary(heads[span, g * HEAD : (g + 1) * HEAD], table, 1.0)
                    for g in range(groups)
                ],
                axis=0,
            ).astype(BF16)
            key = rotary(heads[span, query_cols : query_cols + kv_cols], table, 1.0).astype(BF16)
            value = heads[span, query_cols + kv_cols :].astype(BF16)
            scores = contract_last(query, key) * HEAD ** (-0.5)
            spot = lax.broadcasted_iota(jnp.int32, scores.shape, 0) % length
            scores = jnp.where(
                spot >= lax.broadcasted_iota(jnp.int32, scores.shape, 1), scores, -1e30
            )
            weights = jnp.exp(scores - jnp.max(scores, axis=1, keepdims=True))
            weights = weights / jnp.sum(weights, axis=1, keepdims=True)
            mixed = jnp.dot(weights.astype(BF16), value, preferred_element_type=F32).astype(BF16)
            for g in range(groups):
                mixture[span, g * HEAD : (g + 1) * HEAD] = mixed[g * length : (g + 1) * length]

        def part(block):
            return jnp.dot(
                mixture[...],
                out_w[:, lanes_at(block * width, width)],
                preferred_element_type=F32,
            )

        def finish(block, total):
            return (hidden[block].astype(F32) + total).astype(BF16)

        stream_out(
            place,
            part,
            finish,
            hidden,
            (near_send, near_got, far_send, far_got, relay_send),
            (relay_s, relay_r),
            (out_far_s, out_far_r),
            (out_near_s, out_near_r),
        )


def forward_pass(entrance, gain, table, wq, wk, wv, wo, seq_count):
    rows, width_all = entrance.shape
    blocks = lax.axis_size("mp") * SUB
    width = width_all // blocks
    head_cols = wq.shape[1] + wk.shape[1] + wv.shape[1]
    dma = pltpu.SemaphoreType.DMA
    vmem = pl.BlockSpec(memory_space=pltpu.VMEM)
    anywhere = pl.BlockSpec(memory_space=pl.ANY)
    return pl.pallas_call(
        functools.partial(forward_kernel, seq_count),
        out_shape=(
            jax.ShapeDtypeStruct((blocks, rows, width), BF16),
            jax.ShapeDtypeStruct((rows, head_cols), F32),
        ),
        in_specs=[vmem, vmem, vmem, anywhere, anywhere, anywhere, anywhere],
        out_specs=(vmem, vmem),
        scratch_shapes=[
            pltpu.VMEM((width_all, head_cols), BF16),
            pltpu.VMEM(wo.shape, BF16),
            pltpu.VMEM((rows, head_cols), F32),
            pltpu.VMEM((rows, 128), F32),
            pltpu.VMEM((rows, wq.shape[1]), BF16),
            pltpu.VMEM((2 * SUB, rows, width), BF16),
            pltpu.VMEM((2 * SUB, rows, width), BF16),
            pltpu.VMEM((SUB, rows, width), BF16),
            pltpu.VMEM((SUB, rows, width), BF16),
            pltpu.VMEM((SUB, rows, width), BF16),
            dma((4,)),
            dma((SUB,)),
            dma((SUB,)),
            dma((SUB,)),
            dma((SUB,)),
            dma((2 * SUB,)),
            dma((2 * SUB,)),
            dma((SUB,)),
            dma((SUB,)),
            dma((2 * SUB,)),
            dma((2 * SUB,)),
        ],
        compiler_params=pltpu.CompilerParams(
            collective_id=3, has_side_effects=True, vmem_limit_bytes=48 * 1024 * 1024
        ),
        name="forward_pass",
    )(entrance, gain, table, wq, wk, wv, wo)


def scatter_kernel(levels, part_ref, out_ref, *scratch):
    arrived, kept = scratch[:levels], scratch[levels : 2 * levels - 1]
    send_sem, recv_sem = scratch[2 * levels - 1 :]
    bits, partners = mp_place(lax.axis_index("mp"), levels)
    barrier = pltpu.get_barrier_semaphore()
    for partner in partners:
        pl.semaphore_signal(barrier, inc=1, device_id={"mp": partner}, device_id_type=MESH)
    pl.semaphore_wait(barrier, levels)
    held = part_ref
    for level in range(levels):
        half = held.shape[0] // 2
        copy = pltpu.make_async_remote_copy(
            src_ref=held.at[rows_at((1 - bits[level]) * half, half)],
            dst_ref=arrived[level],
            send_sem=send_sem.at[level],
            recv_sem=recv_sem.at[level],
            device_id={"mp": partners[level]},
            device_id_type=MESH,
        )
        copy.start()
        copy.wait()
        target = out_ref if level == levels - 1 else kept[level]

        def add(step, carry, held=held, half=half, target=target, level=level):
            own = held[rows_at(bits[level] * half + step * ROW_TILE, ROW_TILE), :]
            other = arrived[level][rows_at(step * ROW_TILE, ROW_TILE), :]
            total = own.astype(jnp.float32) + other.astype(jnp.float32)
            target[rows_at(step * ROW_TILE, ROW_TILE), :] = total.astype(target.dtype)
            return carry

        lax.fori_loop(0, half // ROW_TILE, add, 0)
        held = target


def scatter_rows(partial_value):
    rows, width = partial_value.shape
    members = lax.axis_size("mp")
    levels = members.bit_length() - 1
    arrived = [pltpu.VMEM((rows >> (level + 1), width), jnp.bfloat16) for level in range(levels)]
    return pl.pallas_call(
        functools.partial(scatter_kernel, levels),
        out_shape=jax.ShapeDtypeStruct((rows // members, width), jnp.float32),
        in_specs=[pl.BlockSpec(memory_space=pltpu.VMEM)],
        out_specs=pl.BlockSpec(memory_space=pltpu.VMEM),
        scratch_shapes=arrived
        + arrived[:-1]
        + [pltpu.SemaphoreType.DMA((levels,)), pltpu.SemaphoreType.DMA((levels,))],
        compiler_params=pltpu.CompilerParams(collective_id=0, has_side_effects=True),
        name="scatter_rows",
    )(partial_value)


def relay_kernel(levels, direction, shard_ref, out_ref, relay_send, relay_recv, send_sem, recv_sem):
    members = 1 << levels
    shard_rows = shard_ref.shape[0]
    rows = out_ref.shape[0]
    chunks = shard_rows // ROW_TILE
    here = lax.axis_index("section")
    count = lax.axis_size("section")
    if direction > 0:
        has_source, has_target = here > 0, here < count - 1
    else:
        has_source, has_target = here < count - 1, here > 0
    bits, partners = mp_place(lax.axis_index("mp"), levels)
    barrier = pltpu.get_barrier_semaphore()

    @pl.when(has_source)
    def _():
        pl.semaphore_signal(
            barrier, inc=1, device_id={"section": here - direction}, device_id_type=MESH
        )
        for partner in partners:
            pl.semaphore_signal(barrier, inc=1, device_id={"mp": partner}, device_id_type=MESH)

    @pl.when(jnp.logical_and(has_source, has_target))
    def _():
        pl.semaphore_wait(barrier, levels + 1)

    @pl.when(jnp.logical_and(has_source, jnp.logical_not(has_target)))
    def _():
        pl.semaphore_wait(barrier, levels)

    @pl.when(jnp.logical_and(has_target, jnp.logical_not(has_source)))
    def _():
        pl.semaphore_wait(barrier, 1)

    def piece(chunk, flips):
        return out_ref.at[rows_at(shard_offset(bits, rows, flips) + chunk * ROW_TILE, ROW_TILE)]

    def relay(chunk):
        return pltpu.make_async_remote_copy(
            src_ref=shard_ref.at[pl.ds(chunk * ROW_TILE, ROW_TILE)],
            dst_ref=piece(chunk, 0),
            send_sem=relay_send.at[chunk],
            recv_sem=relay_recv.at[chunk],
            device_id={"section": here + direction},
            device_id_type=MESH,
        )

    def spread(chunk, flips, level):
        slot = (flips | (1 << level)) - 1
        return pltpu.make_async_remote_copy(
            src_ref=piece(chunk, flips),
            dst_ref=piece(chunk, flips),
            send_sem=send_sem.at[chunk, slot],
            recv_sem=recv_sem.at[chunk, slot],
            device_id={"mp": partners[level]},
            device_id_type=MESH,
        )

    def incoming(chunk, flips):
        level = (flips & -flips).bit_length() - 1
        return pltpu.make_async_remote_copy(
            src_ref=piece(chunk, flips),
            dst_ref=piece(chunk, flips),
            send_sem=send_sem.at[chunk, flips - 1],
            recv_sem=recv_sem.at[chunk, flips - 1],
            device_id={"mp": partners[level]},
            device_id_type=MESH,
        )

    @pl.when(has_target)
    def _():
        for chunk in range(chunks):
            relay(chunk).start()

    @pl.when(has_source)
    def _():
        sent = []
        order = sorted(range(1, members), key=lambda flips: -(flips & -flips))
        for chunk in range(chunks):
            relay(chunk).wait_recv()
            for level in reversed(range(levels)):
                copy = spread(chunk, 0, level)
                copy.start()
                sent.append(copy)
        for chunk in range(chunks):
            for flips in order:
                incoming(chunk, flips).wait_recv()
                lowest = (flips & -flips).bit_length() - 1
                for level in reversed(range(lowest)):
                    copy = spread(chunk, flips, level)
                    copy.start()
                    sent.append(copy)
        for copy in sent:
            copy.wait_send()

    @pl.when(jnp.logical_not(has_source))
    def _():
        def clear(step, carry):
            out_ref[rows_at(step * ROW_TILE, ROW_TILE), :] = jnp.zeros(
                (ROW_TILE, out_ref.shape[1]), out_ref.dtype
            )
            return carry

        lax.fori_loop(0, rows // ROW_TILE, clear, 0)

    @pl.when(has_target)
    def _():
        for chunk in range(chunks):
            relay(chunk).wait_send()


def relay_rows(shard, direction):
    shard_rows, width = shard.shape
    members = lax.axis_size("mp")
    levels = members.bit_length() - 1
    chunks = shard_rows // ROW_TILE
    return pl.pallas_call(
        functools.partial(relay_kernel, levels, direction),
        out_shape=jax.ShapeDtypeStruct((shard_rows * members, width), jnp.bfloat16),
        in_specs=[pl.BlockSpec(memory_space=pltpu.VMEM)],
        out_specs=pl.BlockSpec(memory_space=pltpu.VMEM),
        scratch_shapes=[
            pltpu.SemaphoreType.DMA((chunks,)),
            pltpu.SemaphoreType.DMA((chunks,)),
            pltpu.SemaphoreType.DMA((chunks, members - 1)),
            pltpu.SemaphoreType.DMA((chunks, members - 1)),
        ],
        compiler_params=pltpu.CompilerParams(
            collective_id=1 if direction > 0 else 2, has_side_effects=True
        ),
        name="relay_forward" if direction > 0 else "relay_backward",
    )(shard)


def local(entrance, lengths, positives, norm_gains, query_proj, key_proj, value_proj, out_proj):
    section_count = lax.axis_size("section")
    section_index = lax.axis_index("section")
    member_count = lax.axis_size("mp")
    dp_count = lax.axis_size("dp")
    pair_count = entrance.shape[0]
    seq_count = 2 * pair_count
    length = entrance.shape[2]
    width_all = entrance.shape[3]
    rows = seq_count * length
    shard_rows = rows // member_count
    bits, _ = mp_place(lax.axis_index("mp"), member_count.bit_length() - 1)
    offset = shard_offset(bits, rows)
    start_hidden = entrance.reshape(rows, width_all)
    mask_of_valid = (
        jnp.arange(length, dtype=jnp.int32)[None, :] < lengths.reshape(seq_count, 1)
    ).astype(jnp.float32)
    counts = jnp.sum(mask_of_valid, axis=1)
    gain_vector = norm_gains[0]
    head_weight = jnp.concatenate([query_proj[0], key_proj[0], value_proj[0]], axis=1)
    out_weight = out_proj[0]
    query_cols = query_proj.shape[2]
    kv_cols = key_proj.shape[2]

    def own_rows(values):
        return lax.dynamic_slice_in_dim(values, offset, shard_rows, 0)

    def attend_heads(heads):
        heads = heads.reshape(seq_count, length, -1)
        mixed = attend(
            heads[..., :query_cols],
            heads[..., query_cols : query_cols + kv_cols],
            heads[..., query_cols + kv_cols :],
        )
        return mixed.reshape(rows, -1)

    hidden_blocks, heads = forward_pass(
        start_hidden,
        norm_gains,
        jnp.asarray(rotary_constants(length)),
        query_proj[0],
        key_proj[0],
        value_proj[0],
        out_weight,
        seq_count,
    )
    current = hidden_blocks.transpose(1, 0, 2).reshape(rows, width_all)
    normed = normalize(current.astype(jnp.float32), gain_vector).astype(jnp.bfloat16)
    mixture_f, attend_pull = jax.vjp(attend_heads, heads)
    mixture = mixture_f.astype(jnp.bfloat16)
    hidden_f = current.astype(jnp.float32)
    inv_rms = lax.rsqrt(jnp.mean(hidden_f * hidden_f, axis=-1, keepdims=True) + EPSILON)

    token_mask = mask_of_valid[:, :, None]
    mixture_sum = jnp.sum(
        mixture.astype(jnp.float32).reshape(seq_count, length, -1) * token_mask, axis=1
    )
    coarse = mixture_sum.astype(jnp.bfloat16)
    fine = (mixture_sum - coarse.astype(jnp.float32)).astype(jnp.bfloat16)
    both = jnp.dot(
        jnp.concatenate([coarse, fine], axis=0), out_weight, preferred_element_type=jnp.float32
    )
    hidden_sum = jnp.sum(hidden_f.reshape(seq_count, length, -1) * token_mask, axis=1)
    pooled = both[:seq_count] + both[seq_count:]
    pooled = pooled + jnp.where(lax.axis_index("mp") == 0, hidden_sum, 0.0)
    pooled = pooled / counts[:, None]
    gathered = lax.all_gather(pooled, ("dp", "mp"), axis=0)
    gathered = jnp.sum(gathered.reshape(dp_count, member_count, seq_count, width_all), axis=1)
    gathered = gathered.reshape(dp_count * pair_count, 2, width_all)
    losses_now, pullback = jax.vjp(
        lambda embedded: matryoshka_losses(embedded, positives), gathered
    )
    pair_grads = pullback(jnp.ones((WIDTHS,), jnp.float32))[0]
    own_grad = lax.dynamic_slice_in_dim(
        pair_grads, lax.axis_index("dp") * pair_count, pair_count, 0
    )
    token_grad = spread_grad(own_grad.reshape(seq_count, width_all), mask_of_valid, counts)
    token_grad = token_grad.reshape(rows, width_all)

    normed_cols = lax.all_to_all(normed, "dp", split_axis=1, concat_axis=0, tiled=True)
    mixture_piece = lax.all_gather(mixture, "dp", axis=0, tiled=True)
    shard_hidden = own_rows(current).astype(jnp.float32)
    _, norm_pull = jax.vjp(lambda values: normalize(values, gain_vector), shard_hidden)
    upstream = token_grad
    for section_turn in range(section_count):
        out_grad = upstream.astype(jnp.bfloat16)
        mixture_grad = contract_last(out_grad, out_weight).astype(jnp.bfloat16)
        pulled = attend_pull(lax.optimization_barrier(mixture_grad).astype(jnp.float32))[0]
        head_grads = pulled.astype(jnp.bfloat16)
        member_grad = contract_last(head_grads, head_weight).astype(jnp.bfloat16)
        if section_turn + 1 == section_count:
            break
        normed_grad = scatter_rows(member_grad)
        input_grad = (own_rows(upstream) + norm_pull(normed_grad)[0]).astype(jnp.bfloat16)
        arrived = relay_rows(input_grad, -1).astype(jnp.float32)
        upstream = token_grad + jnp.where(section_index == section_count - 1, 0.0, arrived)
    out_cols = lax.all_to_all(out_grad, "dp", split_axis=1, concat_axis=0, tiled=True)
    head_piece = lax.all_gather(head_grads, "dp", axis=0, tiled=True)
    gain_term = jnp.sum(member_grad.astype(jnp.float32) * hidden_f * inv_rms, axis=0)
    gain_parts = lax.all_to_all(
        gain_term.reshape(dp_count * member_count, -1),
        ("dp", "mp"),
        split_axis=0,
        concat_axis=0,
        tiled=True,
    )
    gain_share = jnp.sum(gain_parts, axis=0)
    return (
        losses_now[None],
        gain_share[None],
        contract_rows(normed_cols, head_piece[:, :query_cols])[None],
        contract_rows(normed_cols, head_piece[:, query_cols : query_cols + kv_cols])[None],
        contract_rows(normed_cols, head_piece[:, query_cols + kv_cols :])[None],
        contract_rows(mixture_piece, out_cols)[None],
    )


def solution(mesh):
    in_specs = (
        P("dp", None, None, None),
        P("dp", None),
        P(),
        P("section", None),
        P("section", None, "mp"),
        P("section", None, "mp"),
        P("section", None, "mp"),
        P("section", "mp", None),
    )
    out_specs = (
        P("section", None),
        P("section", ("dp", "mp")),
        P("section", "dp", "mp"),
        P("section", "dp", "mp"),
        P("section", "dp", "mp"),
        P("section", "mp", "dp"),
    )
    return jax.shard_map(local, mesh=mesh, in_specs=in_specs, out_specs=out_specs, check_vma=False)
```

```python
import functools

import jax
import jax.numpy as jnp
import numpy as np
from jax import lax
from jax.experimental import pallas as pl
from jax.experimental.pallas import tpu as pltpu
from jax.sharding import PartitionSpec as P

HEAD = 128
WIDTHS = 7


EPSILON = 1e-05
SOFTMAX_TEMPER = 0.05
ROPE_BASE = 500000.0
MESH = pl.DeviceIdType.MESH
ROW_TILE = 16
SUB = 4
F32 = jnp.float32
BF16 = jnp.bfloat16


def contract_rows(left, right):
    return lax.dot_general(
        left, right, (((0,), (0,)), ((), ())), preferred_element_type=jnp.float32
    )


def contract_last(left, right):
    return lax.dot_general(
        left, right, (((left.ndim - 1,), (1,)), ((), ())), preferred_element_type=jnp.float32
    )


def rotary_constants(length):
    half_size = HEAD // 2
    frequencies = ROPE_BASE ** (-np.arange(half_size, dtype=np.float64) * 2.0 / HEAD)
    angles = np.arange(length, dtype=np.float64)[:, None] * frequencies[None, :]
    cosine = np.concatenate([np.cos(angles), np.cos(angles)], axis=1)
    sine = np.concatenate([-np.sin(angles), np.sin(angles)], axis=1)
    return np.stack([cosine, sine]).astype(np.float32)


def mp_place(me, levels):
    bits = [(me // (1 << level)) % 2 for level in range(levels)]
    partners = [me + (1 - 2 * bits[level]) * (1 << level) for level in range(levels)]
    return bits, partners


def rows_at(start, size):
    return pl.ds(pl.multiple_of(start, ROW_TILE), size)


def lanes_at(start, size):
    return pl.ds(pl.multiple_of(start, 128), size)


class Place:
    def __init__(self, direction):
        self.here = lax.axis_index("section")
        self.count = lax.axis_size("section")
        (self.low, self.high), (self.near, self.far) = mp_place(lax.axis_index("mp"), 2)
        self.direction = direction
        if direction > 0:
            self.has_source, self.has_target = self.here > 0, self.here < self.count - 1
        else:
            self.has_source, self.has_target = self.here < self.count - 1, self.here > 0

    def quarter(self, flip_low, flip_high):
        low = 1 - self.low if flip_low else self.low
        high = 1 - self.high if flip_high else self.high
        return (low * 2 + high) * SUB


def send(source, target, sems, slot, **device):
    return pltpu.make_async_remote_copy(
        src_ref=source,
        dst_ref=target,
        send_sem=sems[0].at[slot],
        recv_sem=sems[1].at[slot],
        device_id=device,
        device_id_type=MESH,
    )


def stream_in(place, buf, relay, far, near, consume):
    def near_copy(slot, block):
        return send(buf.at[block], buf.at[block], near, slot, mp=place.near)

    def far_copy(slot, block):
        return send(buf.at[block], buf.at[block], far, slot, mp=place.far)

    own, other = place.quarter(0, 0), place.quarter(0, 1)
    near_own, near_other = place.quarter(1, 0), place.quarter(1, 1)
    for tick in range(SUB + 2):
        if tick < SUB:
            block = own + tick
            send(buf.at[block], buf.at[block], relay, tick, section=place.here).wait_recv()
            far_copy(tick, block).start()
            near_copy(tick, block).start()
        if 1 <= tick <= SUB:
            block = other + tick - 1
            far_copy(tick - 1, block).wait_recv()
            near_copy(SUB + tick - 1, block).start()
        if tick >= 2:
            step = tick - 2
            near_copy(step, near_own + step).wait_recv()
            near_copy(SUB + step, near_other + step).wait_recv()

            def body(part, carry, step=step):
                consume(part * SUB + step)
                return carry

            lax.fori_loop(0, 4, body, 0)
    for step in range(SUB):
        far_copy(step, own + step).wait_send()
        near_copy(step, own + step).wait_send()
        near_copy(SUB + step, other + step).wait_send()


def stream_out(place, part, finish, dest, bufs, relay, far, near):
    near_send, near_got, far_send, far_got, relay_send, prepare = bufs

    def near_copy(slot):
        return send(near_send.at[slot], near_got.at[slot], near, slot, mp=place.near)

    def far_copy(step):
        return send(far_send.at[step], far_got.at[step], far, step, mp=place.far)

    def relay_copy(step):
        return send(
            relay_send.at[step],
            dest.at[place.quarter(0, 0) + step],
            relay,
            step,
            section=place.here + place.direction,
        )

    for flip in (1, 0):
        base = (1 - place.high if flip else place.high) * SUB
        for step in range(SUB):
            near_send[base + step] = part(place.quarter(1, flip) + step).astype(BF16)
            near_copy(base + step).start()
    base = (1 - place.high) * SUB
    for step in range(SUB):
        value = part(place.quarter(0, 1) + step)
        near_copy(base + step).wait_recv()
        far_send[step] = (value + near_got[base + step].astype(F32)).astype(BF16)
        far_copy(step).start()
    base = place.high * SUB
    if prepare is not None:
        prepare()
    for step in range(SUB):
        value = part(place.quarter(0, 0) + step)
        near_copy(base + step).wait_recv()
        value = value + near_got[base + step].astype(F32)
        far_copy(step).wait_recv()
        value = value + far_got[step].astype(F32)
        relay_send[step] = finish(place.quarter(0, 0) + step, value)
        relay_copy(step).start()
    for step in range(SUB):
        far_copy(step).wait_send()
        relay_copy(step).wait_send()
    for slot in range(2 * SUB):
        near_copy(slot).wait_send()


def rotary(values, table, sign):
    turned = pltpu.roll(values, HEAD // 2, axis=1)
    return values * table[0] + turned * (table[1] * sign)


def fold_lanes(values):
    total = values[:, :128]
    for lane in range(1, values.shape[1] // 128):
        total = total + values[:, lane * 128 : (lane + 1) * 128]
    return total


def lane_sum(values):
    return jnp.sum(fold_lanes(values), axis=1, keepdims=True)


def matryoshka(queries, passages, target):
    pairs, width_all = queries.shape
    widths = [width_all >> level for level in range(WIDTHS)]
    bounds = [0] + widths[::-1]
    lane = lax.broadcasted_iota(jnp.int32, (pairs, 128), 1)

    def segment_sums(product):
        sums = []
        for low, high in zip(bounds[:-1], bounds[1:]):
            if high <= 128:
                inside = jnp.logical_and(lane >= low, lane < high)
                piece = jnp.where(inside, product[:, :128], 0.0)
            else:
                piece = fold_lanes(product[:, low:high])
            sums.append(jnp.sum(piece, axis=1, keepdims=True))
        for index in range(1, len(sums)):
            sums[index] = sums[index] + sums[index - 1]
        return sums[::-1]

    query_squares = segment_sums(queries * queries)
    passage_squares = segment_sums(passages * passages)
    dots = [segment_sums(queries * passages[j : j + 1]) for j in range(pairs)]
    losses = []
    mixed = [[] for _ in range(pairs)]
    query_own, passage_own = [], []
    for level, width in enumerate(widths):
        query_inv = lax.rsqrt(query_squares[level] * (1.0 / width) + 1e-06)
        passage_inv = lax.rsqrt(passage_squares[level] * (1.0 / width) + 1e-06)
        factors = [
            query_inv * passage_inv[j : j + 1] * (1.0 / (width * SOFTMAX_TEMPER))
            for j in range(pairs)
        ]
        logits = [dots[j][level] * factors[j] for j in range(pairs)]
        highest = logits[0]
        for j in range(1, pairs):
            highest = jnp.maximum(highest, logits[j])
        powers = [jnp.exp(logits[j] - highest) for j in range(pairs)]
        total = powers[0]
        picked = logits[0] * target[:, 0:1]
        for j in range(1, pairs):
            total = total + powers[j]
            picked = picked + logits[j] * target[:, j : j + 1]
        gap = jnp.log(total) + highest - picked
        losses.append(jnp.sum(gap, axis=0, keepdims=True) * (1.0 / pairs))
        slopes = [
            (powers[j] / total - target[:, j : j + 1]) * (1.0 / pairs) for j in range(pairs)
        ]
        pulls = [slopes[j] * logits[j] for j in range(pairs)]
        row_pull = pulls[0]
        for j in range(1, pairs):
            row_pull = row_pull + pulls[j]
        column_pull = jnp.concatenate(
            [jnp.sum(pulls[j], axis=0, keepdims=True) for j in range(pairs)], axis=0
        )
        for j in range(pairs):
            mixed[j].append(slopes[j] * factors[j])
        query_own.append(row_pull * query_inv * query_inv * (-1.0 / width))
        passage_own.append(column_pull * passage_inv * passage_inv * (-1.0 / width))
    for series in mixed + [query_own, passage_own]:
        for level in range(1, WIDTHS):
            series[level] = series[level] + series[level - 1]
    turned = [
        [
            jnp.concatenate([mixed[j][level][p : p + 1] for j in range(pairs)], axis=0)
            for level in range(WIDTHS)
        ]
        for p in range(pairs)
    ]

    def spread(own, own_rows, weights, rows):
        pieces = []
        low = 0
        while low < width_all:
            inside = [k for k in range(WIDTHS) if low < bounds[k + 1] and low + 128 > bounds[k]]
            high = max(low + 128, bounds[inside[-1] + 1])

            def coefficient(series, inside=inside):
                value = series[WIDTHS - 1 - inside[-1]]
                for k in reversed(inside[:-1]):
                    value = jnp.where(lane < bounds[k + 1], series[WIDTHS - 1 - k], value)
                return value

            def columns(values, low=low, high=high):
                return values[:, low:high]

            piece = coefficient(own) * columns(own_rows)
            for j in range(pairs):
                piece = piece + coefficient(weights[j]) * columns(rows[j : j + 1])
            pieces.append(piece)
            low = high
        return jnp.concatenate(pieces, axis=1)

    return (
        losses,
        spread(query_own, queries, mixed, passages),
        spread(passage_own, passages, turned, queries),
    )


SCRATCH = (
    "head_w", "out_w", "acc", "squares", "inv_ref", "query_ref", "key_ref", "value_ref",
    "prob_ref", "pooled", "slopes", "normed_out", "grad_in", "mix_grad", "row_dots", "gain_part",
    "gain_got", "pool_ref", "near_send", "near_got", "far_send", "far_got", "relay_send",
    "near_send_b", "near_got_b", "far_send_b", "far_got_b", "relay_send_b", "load_sem",
    "enter_sem", "relay_s", "relay_r", "in_far_s", "in_far_r", "in_near_s", "in_near_r",
    "out_far_s", "out_far_r", "out_near_s", "out_near_r", "relay_sb", "relay_rb", "in_far_sb",
    "in_far_rb", "in_near_sb", "in_near_rb", "out_far_sb", "out_far_rb", "out_near_sb",
    "out_near_rb", "pool_s", "pool_r", "normed_s", "normed_r", "mixture_s", "mixture_r",
    "outer_s", "outer_r", "heads_s", "heads_r", "dots_s", "dots_r", "gain_s", "gain_r",
)


def step_kernel(
    lengths,
    positives,
    entrance,
    gain,
    table,
    wq,
    wk,
    wv,
    wo,
    losses_out,
    gain_out,
    normed_all,
    mixture_all,
    outer_all,
    heads_all,
    hidden,
    *scratch,
):
    r = dict(zip(SCRATCH, scratch, strict=True))
    head_w, out_w, acc, squares = r["head_w"], r["out_w"], r["acc"], r["squares"]
    forth, back = Place(1), Place(-1)
    blocks, rows, width = hidden.shape
    width_all = blocks * width
    pair_count = lengths.shape[0]
    seq_count = 2 * pair_count
    length = rows // seq_count
    query_cols, kv_cols = wq.shape[1], wk.shape[1]
    groups = query_cols // HEAD
    dp_me, mp_me = lax.axis_index("dp"), lax.axis_index("mp")
    dp_count, mp_count = lax.axis_size("dp"), lax.axis_size("mp")
    members = dp_count * mp_count
    me = dp_me * mp_count + mp_me
    share = blocks // dp_count
    row_pad = r["row_dots"].shape[2]

    def peer(shift):
        spot = lax.rem(me + shift, members)
        return spot // mp_count, lax.rem(spot, mp_count), spot

    loads = [
        pltpu.make_async_copy(wq, head_w.at[:, :query_cols], r["load_sem"].at[0]),
        pltpu.make_async_copy(
            wk, head_w.at[:, query_cols : query_cols + kv_cols], r["load_sem"].at[1]
        ),
        pltpu.make_async_copy(wv, head_w.at[:, query_cols + kv_cols :], r["load_sem"].at[2]),
        pltpu.make_async_copy(wo, out_w, r["load_sem"].at[3]),
    ]

    def enter(block):
        return pltpu.make_async_copy(
            entrance.at[:, lanes_at(block * width, width)],
            hidden.at[block],
            r["enter_sem"].at[block],
        )

    @pl.when(jnp.logical_not(forth.has_source))
    def _():
        for block in range(blocks):
            enter(block).start()

    for load in loads:
        load.start()
    barrier = pltpu.get_barrier_semaphore()
    for shift in range(1, members):
        to_dp, to_mp, _ = peer(shift)
        pl.semaphore_signal(
            barrier, inc=1, device_id={"dp": to_dp, "mp": to_mp}, device_id_type=MESH
        )

    @pl.when(forth.has_source)
    def _():
        pl.semaphore_signal(
            barrier, inc=1, device_id={"section": forth.here - 1}, device_id_type=MESH
        )

    @pl.when(forth.has_target)
    def _():
        pl.semaphore_signal(
            barrier, inc=1, device_id={"section": forth.here + 1}, device_id_type=MESH
        )

    acc[...] = jnp.zeros_like(acc)
    squares[...] = jnp.zeros_like(squares)
    r["mix_grad"][...] = jnp.zeros_like(r["mix_grad"])
    pool_shape = r["pool_ref"].shape
    column = lax.broadcasted_iota(jnp.int32, pool_shape, 1)
    line = lax.broadcasted_iota(jnp.int32, pool_shape, 0)
    picks = jnp.zeros(pool_shape, F32)
    for seq in range(seq_count):
        inside = jnp.logical_and(
            column >= seq * length, column < seq * length + lengths[seq // 2, seq % 2]
        )
        picks = jnp.where(jnp.logical_and(line == seq, inside), 1.0, picks)
    r["pool_ref"][...] = picks.astype(BF16)
    expected = (
        members - 1 + forth.has_source.astype(jnp.int32) + forth.has_target.astype(jnp.int32)
    )
    pl.semaphore_wait(barrier, expected)

    def gain_at(block):
        return gain[:, lanes_at(block * width, width)]

    def consume(block):
        value = hidden[block].astype(F32)
        squares[...] += fold_lanes(value * value)
        acc[...] += jnp.dot(
            (value * gain_at(block)).astype(BF16),
            head_w[rows_at(block * width, width), :],
            preferred_element_type=F32,
        )

    for load in loads[:3]:
        load.wait()

    @pl.when(forth.has_source)
    def _():
        stream_in(
            forth,
            hidden,
            (r["relay_s"], r["relay_r"]),
            (r["in_far_s"], r["in_far_r"]),
            (r["in_near_s"], r["in_near_r"]),
            consume,
        )

    @pl.when(jnp.logical_not(forth.has_source))
    def _():
        def body(block, carry):
            enter(block).wait()
            consume(block)
            return carry

        lax.fori_loop(0, blocks, body, 0)

    inv_rms = lax.rsqrt(
        jnp.sum(squares[...], axis=1, keepdims=True) * (1.0 / width_all) + EPSILON
    )
    r["inv_ref"][...] = inv_rms
    mixture = mixture_all.at[dp_me]
    for seq in range(seq_count):
        span = slice(seq * length, (seq + 1) * length)
        inverse = inv_rms[span]
        query = jnp.concatenate(
            [
                rotary(acc[span, g * HEAD : (g + 1) * HEAD] * inverse, table, 1.0)
                for g in range(groups)
            ],
            axis=0,
        ).astype(BF16)
        key = rotary(acc[span, query_cols : query_cols + kv_cols] * inverse, table, 1.0)
        key = key.astype(BF16)
        value = (acc[span, query_cols + kv_cols :] * inverse).astype(BF16)
        r["query_ref"][seq] = query
        r["key_ref"][seq] = key
        r["value_ref"][seq] = value
        scores = contract_last(query, key) * HEAD ** (-0.5)
        spot = lax.broadcasted_iota(jnp.int32, scores.shape, 0) % length
        scores = jnp.where(spot >= lax.broadcasted_iota(jnp.int32, scores.shape, 1), scores, -1e30)
        weights = jnp.exp(scores - jnp.max(scores, axis=1, keepdims=True))
        weights = weights / jnp.sum(weights, axis=1, keepdims=True)
        r["prob_ref"][seq] = weights
        mixed = jnp.dot(weights.astype(BF16), value, preferred_element_type=F32).astype(BF16)
        for g in range(groups):
            mixture[span, g * HEAD : (g + 1) * HEAD] = mixed[g * length : (g + 1) * length]
    loads[3].wait()

    def out_columns(block):
        return out_w[:, lanes_at(block * width, width)]

    @pl.when(forth.has_target)
    def _():
        def part(block):
            return jnp.dot(mixture[...], out_columns(block), preferred_element_type=F32)

        def finish(block, total):
            return (hidden[block].astype(F32) + total).astype(BF16)

        stream_out(
            forth,
            part,
            finish,
            hidden,
            (r["near_send"], r["near_got"], r["far_send"], r["far_got"], r["relay_send"], None),
            (r["relay_s"], r["relay_r"]),
            (r["out_far_s"], r["out_far_r"]),
            (r["out_near_s"], r["out_near_r"]),
        )

    pool = r["pool_ref"][...]
    mixture_sum = jnp.dot(pool, mixture[...], preferred_element_type=F32)
    coarse = mixture_sum.astype(BF16)
    fine = (mixture_sum - coarse.astype(F32)).astype(BF16)
    both = jnp.concatenate([coarse, fine], axis=0)
    first = (mp_me == 0).astype(F32)
    pooled = r["pooled"]

    def pool_block(block, carry):
        sums = jnp.dot(both, out_columns(block), preferred_element_type=F32)
        sums = sums[: pool_shape[0]] + sums[pool_shape[0] :]
        sums = sums + first * jnp.dot(pool, hidden[block], preferred_element_type=F32)
        lines = [
            sums[seq : seq + 1] / lengths[seq // 2, seq % 2].astype(F32)
            for seq in range(seq_count)
        ]
        pooled[me, :, lanes_at(block * width, width)] = jnp.concatenate(lines, axis=0)
        return carry

    lax.fori_loop(0, blocks, pool_block, 0)

    def pool_copy(shift):
        to_dp, to_mp, _ = peer(shift)
        return pltpu.make_async_remote_copy(
            src_ref=pooled.at[me],
            dst_ref=pooled.at[me],
            send_sem=r["pool_s"].at[shift],
            recv_sem=r["pool_r"].at[me],
            device_id={"dp": to_dp, "mp": to_mp},
            device_id_type=MESH,
        )

    def pool_arrival(shift):
        from_dp, from_mp, spot = peer(shift)
        return pltpu.make_async_remote_copy(
            src_ref=pooled.at[spot],
            dst_ref=pooled.at[spot],
            send_sem=r["pool_s"].at[shift],
            recv_sem=r["pool_r"].at[spot],
            device_id={"dp": from_dp, "mp": from_mp},
            device_id_type=MESH,
        )

    for shift in range(1, members):
        pool_copy(shift).start()

    def to_owner(source, kind, block):
        return pltpu.make_async_remote_copy(
            src_ref=source.at[block],
            dst_ref=(normed_all if kind == "normed" else outer_all).at[dp_me, lax.rem(block, share)],
            send_sem=r[kind + "_s"].at[block],
            recv_sem=r[kind + "_r"].at[dp_me, lax.rem(block, share)],
            device_id={"dp": block // share},
            device_id_type=MESH,
        )

    def from_member(target, kind, member, step):
        return pltpu.make_async_remote_copy(
            src_ref=target.at[member, step],
            dst_ref=target.at[member, step],
            send_sem=r[kind + "_s"].at[0],
            recv_sem=r[kind + "_r"].at[member, step],
            device_id={"dp": member},
            device_id_type=MESH,
        )

    def whole_copy(target, kind, shift):
        return pltpu.make_async_remote_copy(
            src_ref=target.at[dp_me],
            dst_ref=target.at[dp_me],
            send_sem=r[kind + "_s"].at[shift],
            recv_sem=r[kind + "_r"].at[dp_me],
            device_id={"dp": lax.rem(dp_me + shift, dp_count)},
            device_id_type=MESH,
        )

    def whole_arrival(target, kind, shift):
        member = lax.rem(dp_me + shift, dp_count)
        return pltpu.make_async_remote_copy(
            src_ref=target.at[member],
            dst_ref=target.at[member],
            send_sem=r[kind + "_s"].at[shift],
            recv_sem=r[kind + "_r"].at[member],
            device_id={"dp": member},
            device_id_type=MESH,
        )

    def normed_block(block, carry):
        value = hidden[block].astype(F32) * r["inv_ref"][...] * gain_at(block)
        value = value.astype(BF16)
        mine = block // share == dp_me

        @pl.when(mine)
        def _():
            normed_all[dp_me, lax.rem(block, share)] = value

        @pl.when(jnp.logical_not(mine))
        def _():
            r["normed_out"][block] = value
            to_owner(r["normed_out"], "normed", block).start()

        return carry

    lax.fori_loop(0, blocks, normed_block, 0)
    for shift in range(1, dp_count):
        whole_copy(mixture_all, "mixture", shift).start()

    for shift in range(1, members):
        pool_arrival(shift).wait_recv()
    embedded = []
    for member in range(dp_count):
        total = pooled[member * mp_count]
        for other in range(1, mp_count):
            total = total + pooled[member * mp_count + other]
        embedded.append(total)
    pairs = dp_count * pair_count
    queries = jnp.concatenate(
        [embedded[p // pair_count][2 * (p % pair_count) :][:1] for p in range(pairs)], axis=0
    )
    passages = jnp.concatenate(
        [embedded[p // pair_count][2 * (p % pair_count) + 1 :][:1] for p in range(pairs)], axis=0
    )
    partner = lax.broadcasted_iota(jnp.int32, (pairs, pairs), 1)
    line = lax.broadcasted_iota(jnp.int32, (pairs, pairs), 0)
    target = jnp.zeros((pairs, pairs), F32)
    for p in range(pairs):
        target = jnp.where(jnp.logical_and(line == p, partner == positives[p]), 1.0, target)
    losses, query_slopes, passage_slopes = matryoshka(queries, passages, target)
    lane = lax.broadcasted_iota(jnp.int32, (1, 128), 1)
    packed = jnp.zeros((1, 128), F32)
    for level in range(WIDTHS):
        packed = jnp.where(lane == level, losses[level], packed)
    losses_out[...] = packed[:, :WIDTHS]
    slopes = r["slopes"]
    for p in range(pairs):
        slopes[2 * p] = query_slopes[p : p + 1]
        slopes[2 * p + 1] = passage_slopes[p : p + 1]

    grad_in, mix_grad = r["grad_in"], r["mix_grad"]
    spot = lax.broadcasted_iota(jnp.int32, (length, 1), 0)
    shares = []
    for seq in range(seq_count):
        count = lengths[seq // 2, seq % 2]
        shares.append(jnp.where(spot < count, 1.0, 0.0) / count.astype(F32))

    def upstream(block):
        tokens = jnp.concatenate(
            [
                shares[seq] * slopes[dp_me * seq_count + seq, :, lanes_at(block * width, width)]
                for seq in range(seq_count)
            ],
            axis=0,
        )
        return tokens + grad_in[block].astype(F32)

    def consume_back(block):
        outer = upstream(block).astype(BF16)
        mine = block // share == dp_me

        @pl.when(mine)
        def _():
            outer_all[dp_me, lax.rem(block, share)] = outer

        @pl.when(jnp.logical_not(mine))
        def _():
            r["normed_out"][blocks + block] = outer
            to_owner(r["normed_out"].at[pl.ds(blocks, blocks)], "outer", block).start()

        mix_grad[...] += contract_last(outer, out_columns(block))

    @pl.when(back.has_source)
    def _():
        stream_in(
            back,
            grad_in,
            (r["relay_sb"], r["relay_rb"]),
            (r["in_far_sb"], r["in_far_rb"]),
            (r["in_near_sb"], r["in_near_rb"]),
            consume_back,
        )

    @pl.when(jnp.logical_not(back.has_source))
    def _():
        def body(block, carry):
            grad_in[block] = jnp.zeros((rows, width), BF16)
            consume_back(block)
            return carry

        lax.fori_loop(0, blocks, body, 0)

    head_grads = heads_all.at[dp_me]
    row_dot = []
    for seq in range(seq_count):
        span = slice(seq * length, (seq + 1) * length)
        mixed = jnp.concatenate(
            [mix_grad[span, g * HEAD : (g + 1) * HEAD] for g in range(groups)], axis=0
        ).astype(BF16)
        weights = r["prob_ref"][seq]
        value_grad = contract_rows(weights.astype(BF16), mixed).astype(BF16)
        pulled = contract_last(mixed, r["value_ref"][seq]).astype(BF16).astype(F32)
        score_grad = weights * (pulled - jnp.sum(weights * pulled, axis=1, keepdims=True))
        score_grad = (score_grad * HEAD ** (-0.5)).astype(BF16)
        query_grad = jnp.dot(score_grad, r["key_ref"][seq], preferred_element_type=F32)
        query_grad = query_grad.astype(BF16).astype(F32)
        key_grad = contract_rows(score_grad, r["query_ref"][seq]).astype(BF16).astype(F32)
        pieces = [
            rotary(query_grad[g * length : (g + 1) * length], table, -1.0).astype(BF16)
            for g in range(groups)
        ]
        pieces = pieces + [rotary(key_grad, table, -1.0).astype(BF16), value_grad]
        joined = jnp.concatenate(pieces, axis=1)
        head_grads[span, :] = joined
        row_dot.append(lane_sum(joined.astype(F32) * acc[span, :]))
    for shift in range(1, dp_count):
        whole_copy(heads_all, "heads", shift).start()
    row_dot = jnp.concatenate(row_dot, axis=0)

    def part_back(block):
        value = contract_last(head_grads[...], head_w[rows_at(block * width, width), :])
        scaled = value * (hidden[block].astype(F32) * r["inv_ref"][...])
        r["gain_part"][:, lanes_at(block * width, width)] = jnp.sum(scaled, axis=0, keepdims=True)
        return value

    row_dots = r["row_dots"]

    def dots_copy(shift):
        return pltpu.make_async_remote_copy(
            src_ref=row_dots.at[mp_me],
            dst_ref=row_dots.at[mp_me],
            send_sem=r["dots_s"].at[shift],
            recv_sem=r["dots_r"].at[mp_me],
            device_id={"mp": lax.rem(mp_me + shift, mp_count)},
            device_id_type=MESH,
        )

    def dots_arrival(shift):
        member = lax.rem(mp_me + shift, mp_count)
        return pltpu.make_async_remote_copy(
            src_ref=row_dots.at[member],
            dst_ref=row_dots.at[member],
            send_sem=r["dots_s"].at[shift],
            recv_sem=r["dots_r"].at[member],
            device_id={"mp": member},
            device_id_type=MESH,
        )

    @pl.when(back.has_target)
    def _():
        diagonal = lax.broadcasted_iota(jnp.int32, (rows, row_pad), 0) == lax.broadcasted_iota(
            jnp.int32, (rows, row_pad), 1
        )
        row_dots[mp_me] = jnp.sum(jnp.where(diagonal, row_dot, 0.0), axis=0, keepdims=True)
        for shift in range(1, mp_count):
            dots_copy(shift).start()

        def prepare():
            for shift in range(1, mp_count):
                dots_arrival(shift).wait_recv()
            total = row_dots[0]
            for member in range(1, mp_count):
                total = total + row_dots[member]
            column = lane_sum(jnp.where(diagonal, total, 0.0))
            inverse = r["inv_ref"][...]
            squares[:, :1] = column * inverse * inverse * inverse * (1.0 / width_all)

        def finish(block, total):
            value = upstream(block) + total * gain_at(block) * r["inv_ref"][...]
            return (value - hidden[block].astype(F32) * squares[:, :1]).astype(BF16)

        stream_out(
            back,
            part_back,
            finish,
            grad_in,
            (
                r["near_send_b"],
                r["near_got_b"],
                r["far_send_b"],
                r["far_got_b"],
                r["relay_send_b"],
                prepare,
            ),
            (r["relay_sb"], r["relay_rb"]),
            (r["out_far_sb"], r["out_far_rb"]),
            (r["out_near_sb"], r["out_near_rb"]),
        )
        for shift in range(1, mp_count):
            dots_copy(shift).wait_send()

    @pl.when(jnp.logical_not(back.has_target))
    def _():
        def body(block, carry):
            part_back(block)
            return carry

        lax.fori_loop(0, blocks, body, 0)

    gain_got = r["gain_got"]
    gain_cols = gain_got.shape[2]

    def gain_copy(shift):
        to_dp, to_mp, spot = peer(shift)
        return pltpu.make_async_remote_copy(
            src_ref=r["gain_part"].at[:, lanes_at(spot * gain_cols, gain_cols)],
            dst_ref=gain_got.at[me],
            send_sem=r["gain_s"].at[shift],
            recv_sem=r["gain_r"].at[me],
            device_id={"dp": to_dp, "mp": to_mp},
            device_id_type=MESH,
        )

    def gain_arrival(shift):
        from_dp, from_mp, spot = peer(shift)
        return pltpu.make_async_remote_copy(
            src_ref=gain_got.at[spot],
            dst_ref=gain_got.at[spot],
            send_sem=r["gain_s"].at[shift],
            recv_sem=r["gain_r"].at[spot],
            device_id={"dp": from_dp, "mp": from_mp},
            device_id_type=MESH,
        )

    for shift in range(1, members):
        gain_copy(shift).start()
    total = r["gain_part"][:, lanes_at(me * gain_cols, gain_cols)]
    for shift in range(1, members):
        gain_arrival(shift).wait_recv()
        total = total + gain_got[lax.rem(me + shift, members)]
    gain_out[...] = total

    for shift in range(1, members):
        pool_copy(shift).wait_send()
        gain_copy(shift).wait_send()
    for shift in range(1, dp_count):
        whole_copy(mixture_all, "mixture", shift).wait_send()
        whole_copy(heads_all, "heads", shift).wait_send()
        whole_arrival(mixture_all, "mixture", shift).wait_recv()
        whole_arrival(heads_all, "heads", shift).wait_recv()

    def drain(block, carry):
        @pl.when(block // share != dp_me)
        def _():
            to_owner(r["normed_out"], "normed", block).wait_send()
            to_owner(r["normed_out"].at[pl.ds(blocks, blocks)], "outer", block).wait_send()

        return carry

    lax.fori_loop(0, blocks, drain, 0)
    for shift in range(1, dp_count):
        member = lax.rem(dp_me + shift, dp_count)
        for step in range(share):
            from_member(normed_all, "normed", member, step).wait_recv()
            from_member(outer_all, "outer", member, step).wait_recv()


def step_pass(lengths, positives, entrance, gain, table, wq, wk, wv, wo):
    rows, width_all = entrance.shape
    dp_count, mp_count = lax.axis_size("dp"), lax.axis_size("mp")
    members = dp_count * mp_count
    blocks = mp_count * SUB
    width = width_all // blocks
    share = blocks // dp_count
    seq_count = 2 * lengths.shape[0]
    length = rows // seq_count
    query_cols = wq.shape[1]
    head_cols = query_cols + wk.shape[1] + wv.shape[1]
    stacked = query_cols // HEAD * length
    row_pad = -(-rows // 128) * 128
    pool_rows = -(-seq_count // 16) * 16
    dma = pltpu.SemaphoreType.DMA
    block = (rows, width)
    shapes = dict(
        head_w=((width_all, head_cols), BF16),
        out_w=(wo.shape, BF16),
        acc=((rows, head_cols), F32),
        squares=((rows, 128), F32),
        inv_ref=((rows, 1), F32),
        query_ref=((seq_count, stacked, HEAD), BF16),
        key_ref=((seq_count, length, HEAD), BF16),
        value_ref=((seq_count, length, HEAD), BF16),
        prob_ref=((seq_count, stacked, length), F32),
        pooled=((members, seq_count, width_all), F32),
        slopes=((dp_count * seq_count, 1, width_all), F32),
        normed_out=((2 * blocks, *block), BF16),
        grad_in=((blocks, *block), BF16),
        mix_grad=((rows, query_cols), F32),
        row_dots=((mp_count, 1, row_pad), F32),
        gain_part=((1, width_all), F32),
        gain_got=((members, 1, width_all // members), F32),
        pool_ref=((pool_rows, rows), BF16),
    )
    counts = dict(
        load_sem=(4,),
        enter_sem=(blocks,),
        pool_s=(members,),
        pool_r=(members,),
        normed_s=(blocks,),
        normed_r=(dp_count, share),
        outer_s=(blocks,),
        outer_r=(dp_count, share),
        mixture_s=(dp_count,),
        mixture_r=(dp_count,),
        heads_s=(dp_count,),
        heads_r=(dp_count,),
        dots_s=(mp_count,),
        dots_r=(mp_count,),
        gain_s=(members,),
        gain_r=(members,),
    )
    for tail in ("", "_b"):
        shapes["near_send" + tail] = shapes["near_got" + tail] = ((2 * SUB, *block), BF16)
        shapes["far_send" + tail] = shapes["far_got" + tail] = ((SUB, *block), BF16)
        shapes["relay_send" + tail] = ((SUB, *block), BF16)
    for side in ("s", "r", "sb", "rb"):
        counts["relay_" + side] = counts["in_far_" + side] = counts["out_far_" + side] = (SUB,)
        counts["in_near_" + side] = counts["out_near_" + side] = (2 * SUB,)
    scratch = [
        pltpu.VMEM(*shapes[name]) if name in shapes else dma(counts[name]) for name in SCRATCH
    ]
    vmem = pl.BlockSpec(memory_space=pltpu.VMEM)
    smem = pl.BlockSpec(memory_space=pltpu.SMEM)
    hbm = pl.BlockSpec(memory_space=pltpu.HBM)
    return pl.pallas_call(
        step_kernel,
        out_shape=(
            jax.ShapeDtypeStruct((1, WIDTHS), F32),
            jax.ShapeDtypeStruct((1, width_all // members), F32),
            jax.ShapeDtypeStruct((dp_count, share, *block), BF16),
            jax.ShapeDtypeStruct((dp_count, rows, query_cols), BF16),
            jax.ShapeDtypeStruct((dp_count, share, *block), BF16),
            jax.ShapeDtypeStruct((dp_count, rows, head_cols), BF16),
        ),
        in_specs=[smem, smem, hbm, vmem, vmem, hbm, hbm, hbm, hbm],
        out_specs=(vmem,) * 6,
        scratch_shapes=[pltpu.VMEM((blocks, *block), BF16)] + scratch,
        compiler_params=pltpu.CompilerParams(
            collective_id=0, has_side_effects=True, vmem_limit_bytes=56 * 1024 * 1024
        ),
        name="step_pass",
    )(lengths, positives, entrance, gain, table, wq, wk, wv, wo)


def local(entrance, lengths, positives, norm_gains, query_proj, key_proj, value_proj, out_proj):
    length = entrance.shape[2]
    width_all = entrance.shape[3]
    query_cols = query_proj.shape[2]
    kv_cols = key_proj.shape[2]
    losses, gain_share, normed, mixture, outer, heads = step_pass(
        lengths,
        positives,
        entrance.reshape(-1, width_all),
        norm_gains,
        jnp.asarray(rotary_constants(length)),
        query_proj[0],
        key_proj[0],
        value_proj[0],
        out_proj[0],
    )
    normed = normed.transpose(0, 2, 1, 3).reshape(heads.shape[0] * heads.shape[1], -1)
    outer = outer.transpose(0, 2, 1, 3).reshape(heads.shape[0] * heads.shape[1], -1)
    heads = heads.reshape(normed.shape[0], -1)
    mixture = mixture.reshape(normed.shape[0], -1)
    return (
        losses,
        gain_share,
        contract_rows(normed, heads[:, :query_cols])[None],
        contract_rows(normed, heads[:, query_cols : query_cols + kv_cols])[None],
        contract_rows(normed, heads[:, query_cols + kv_cols :])[None],
        contract_rows(mixture, outer)[None],
    )


def solution(mesh):
    in_specs = (
        P("dp", None, None, None),
        P("dp", None),
        P(),
        P("section", None),
        P("section", None, "mp"),
        P("section", None, "mp"),
        P("section", None, "mp"),
        P("section", "mp", None),
    )
    out_specs = (
        P("section", None),
        P("section", ("dp", "mp")),
        P("section", "dp", "mp"),
        P("section", "dp", "mp"),
        P("section", "dp", "mp"),
        P("section", "mp", "dp"),
    )
    return jax.shard_map(local, mesh=mesh, in_specs=in_specs, out_specs=out_specs, check_vma=False)
```

```python
from typing import NamedTuple

import jax
import jax.numpy as jnp
import numpy as np
from jax import lax
from jax.experimental import pallas as pl
from jax.experimental.pallas import tpu as pltpu
from jax.sharding import PartitionSpec as P

HEAD = 128
WIDTHS = 7


EPSILON = 1e-05
SOFTMAX_TEMPER = 0.05
ROPE_BASE = 500000.0
MESH = pl.DeviceIdType.MESH
ROW_TILE = 16
SUB = 4
F32 = jnp.float32
BF16 = jnp.bfloat16


def contract_rows(left, right):
    return lax.dot_general(
        left, right, (((0,), (0,)), ((), ())), preferred_element_type=jnp.float32
    )


def contract_last(left, right):
    return lax.dot_general(
        left, right, (((left.ndim - 1,), (1,)), ((), ())), preferred_element_type=jnp.float32
    )


def rotary_constants(length):
    half_size = HEAD // 2
    frequencies = ROPE_BASE ** (-np.arange(half_size, dtype=np.float64) * 2.0 / HEAD)
    angles = np.arange(length, dtype=np.float64)[:, None] * frequencies[None, :]
    cosine = np.concatenate([np.cos(angles), np.cos(angles)], axis=1)
    sine = np.concatenate([-np.sin(angles), np.sin(angles)], axis=1)
    return np.stack([cosine, sine]).astype(np.float32)


def mp_place(me, levels):
    bits = [(me // (1 << level)) % 2 for level in range(levels)]
    partners = [me + (1 - 2 * bits[level]) * (1 << level) for level in range(levels)]
    return bits, partners


def rows_at(start, size):
    return pl.ds(pl.multiple_of(start, ROW_TILE), size)


def lanes_at(start, size):
    return pl.ds(pl.multiple_of(start, 128), size)


class Place:
    def __init__(self, direction):
        self.here = lax.axis_index("section")
        self.count = lax.axis_size("section")
        (self.low, self.high), (self.near, self.far) = mp_place(lax.axis_index("mp"), 2)
        self.direction = direction
        if direction > 0:
            self.has_source, self.has_target = self.here > 0, self.here < self.count - 1
        else:
            self.has_source, self.has_target = self.here < self.count - 1, self.here > 0

    def quarter(self, flip_low, flip_high):
        low = 1 - self.low if flip_low else self.low
        high = 1 - self.high if flip_high else self.high
        return (low * 2 + high) * SUB


def send(source, target, sems, slot, **device):
    return pltpu.make_async_remote_copy(
        src_ref=source,
        dst_ref=target,
        send_sem=sems[0].at[slot],
        recv_sem=sems[1].at[slot],
        device_id=device,
        device_id_type=MESH,
    )


def stream_in(place, buf, relay, far, near, consume):
    def near_copy(slot, block):
        return send(buf.at[block], buf.at[block], near, slot, mp=place.near)

    def far_copy(slot, block):
        return send(buf.at[block], buf.at[block], far, slot, mp=place.far)

    own, other = place.quarter(0, 0), place.quarter(0, 1)
    near_own, near_other = place.quarter(1, 0), place.quarter(1, 1)
    for tick in range(SUB + 2):
        if tick < SUB:
            block = own + tick
            send(buf.at[block], buf.at[block], relay, tick, section=place.here).wait_recv()
            far_copy(tick, block).start()
            near_copy(tick, block).start()
        if 1 <= tick <= SUB:
            block = other + tick - 1
            far_copy(tick - 1, block).wait_recv()
            near_copy(SUB + tick - 1, block).start()
        if tick >= 2:
            step = tick - 2
            near_copy(step, near_own + step).wait_recv()
            near_copy(SUB + step, near_other + step).wait_recv()

            def body(part, carry, step=step):
                consume(part * SUB + step)
                return carry

            lax.fori_loop(0, 4, body, 0)
    for step in range(SUB):
        far_copy(step, own + step).wait_send()
        near_copy(step, own + step).wait_send()
        near_copy(SUB + step, other + step).wait_send()


def stream_out(place, part, finish, dest, bufs, relay, far, near):
    near_send, near_got, far_send, far_got, relay_send, prepare = bufs

    def near_copy(slot):
        return send(near_send.at[slot], near_got.at[slot], near, slot, mp=place.near)

    def far_copy(step):
        return send(far_send.at[step], far_got.at[step], far, step, mp=place.far)

    def relay_copy(step):
        return send(
            relay_send.at[step],
            dest.at[place.quarter(0, 0) + step],
            relay,
            step,
            section=place.here + place.direction,
        )

    for flip in (1, 0):
        base = (1 - place.high if flip else place.high) * SUB
        for step in range(SUB):
            near_send[base + step] = part(place.quarter(1, flip) + step).astype(BF16)
            near_copy(base + step).start()
    base = (1 - place.high) * SUB
    for step in range(SUB):
        value = part(place.quarter(0, 1) + step)
        near_copy(base + step).wait_recv()
        far_send[step] = (value + near_got[base + step].astype(F32)).astype(BF16)
        far_copy(step).start()
    base = place.high * SUB
    if prepare is not None:
        prepare()
    for step in range(SUB):
        value = part(place.quarter(0, 0) + step)
        near_copy(base + step).wait_recv()
        value = value + near_got[base + step].astype(F32)
        far_copy(step).wait_recv()
        value = value + far_got[step].astype(F32)
        relay_send[step] = finish(place.quarter(0, 0) + step, value)
        relay_copy(step).start()
    for step in range(SUB):
        far_copy(step).wait_send()
        relay_copy(step).wait_send()
    for slot in range(2 * SUB):
        near_copy(slot).wait_send()


def rotary(values, table, sign):
    turned = pltpu.roll(values, HEAD // 2, axis=1)
    return values * table[0] + turned * (table[1] * sign)


def fold_lanes(values):
    total = values[:, :128]
    for lane in range(1, values.shape[1] // 128):
        total = total + values[:, lane * 128 : (lane + 1) * 128]
    return total


def lane_sum(values):
    return jnp.sum(fold_lanes(values), axis=1, keepdims=True)


def matryoshka(queries, passages, target):
    pairs, width_all = queries.shape
    widths = [width_all >> level for level in range(WIDTHS)]
    bounds = [0] + widths[::-1]
    lane = lax.broadcasted_iota(jnp.int32, (pairs, 128), 1)

    def segment_sums(product):
        sums = []
        for low, high in zip(bounds[:-1], bounds[1:]):
            if high <= 128:
                inside = jnp.logical_and(lane >= low, lane < high)
                piece = jnp.where(inside, product[:, :128], 0.0)
            else:
                piece = fold_lanes(product[:, low:high])
            sums.append(jnp.sum(piece, axis=1, keepdims=True))
        for index in range(1, len(sums)):
            sums[index] = sums[index] + sums[index - 1]
        return sums[::-1]

    query_squares = segment_sums(queries * queries)
    passage_squares = segment_sums(passages * passages)
    dots = [segment_sums(queries * passages[j : j + 1]) for j in range(pairs)]
    losses = []
    mixed = [[] for _ in range(pairs)]
    query_own, passage_own = [], []
    for level, width in enumerate(widths):
        query_inv = lax.rsqrt(query_squares[level] * (1.0 / width) + 1e-06)
        passage_inv = lax.rsqrt(passage_squares[level] * (1.0 / width) + 1e-06)
        factors = [
            query_inv * passage_inv[j : j + 1] * (1.0 / (width * SOFTMAX_TEMPER))
            for j in range(pairs)
        ]
        logits = [dots[j][level] * factors[j] for j in range(pairs)]
        highest = logits[0]
        for j in range(1, pairs):
            highest = jnp.maximum(highest, logits[j])
        powers = [jnp.exp(logits[j] - highest) for j in range(pairs)]
        total = powers[0]
        picked = logits[0] * target[:, 0:1]
        for j in range(1, pairs):
            total = total + powers[j]
            picked = picked + logits[j] * target[:, j : j + 1]
        gap = jnp.log(total) + highest - picked
        losses.append(jnp.sum(gap, axis=0, keepdims=True) * (1.0 / pairs))
        slopes = [
            (powers[j] / total - target[:, j : j + 1]) * (1.0 / pairs) for j in range(pairs)
        ]
        pulls = [slopes[j] * logits[j] for j in range(pairs)]
        row_pull = pulls[0]
        for j in range(1, pairs):
            row_pull = row_pull + pulls[j]
        column_pull = jnp.concatenate(
            [jnp.sum(pulls[j], axis=0, keepdims=True) for j in range(pairs)], axis=0
        )
        for j in range(pairs):
            mixed[j].append(slopes[j] * factors[j])
        query_own.append(row_pull * query_inv * query_inv * (-1.0 / width))
        passage_own.append(column_pull * passage_inv * passage_inv * (-1.0 / width))
    for series in mixed + [query_own, passage_own]:
        for level in range(1, WIDTHS):
            series[level] = series[level] + series[level - 1]
    turned = [
        [
            jnp.concatenate([mixed[j][level][p : p + 1] for j in range(pairs)], axis=0)
            for level in range(WIDTHS)
        ]
        for p in range(pairs)
    ]

    def spread(own, own_rows, weights, rows):
        pieces = []
        low = 0
        while low < width_all:
            inside = [k for k in range(WIDTHS) if low < bounds[k + 1] and low + 128 > bounds[k]]
            high = max(low + 128, bounds[inside[-1] + 1])

            def coefficient(series, inside=inside):
                value = series[WIDTHS - 1 - inside[-1]]
                for k in reversed(inside[:-1]):
                    value = jnp.where(lane < bounds[k + 1], series[WIDTHS - 1 - k], value)
                return value

            def columns(values, low=low, high=high):
                return values[:, low:high]

            piece = coefficient(own) * columns(own_rows)
            for j in range(pairs):
                piece = piece + coefficient(weights[j]) * columns(rows[j : j + 1])
            pieces.append(piece)
            low = high
        return jnp.concatenate(pieces, axis=1)

    return (
        losses,
        spread(query_own, queries, mixed, passages),
        spread(passage_own, passages, turned, queries),
    )


class Scratch(NamedTuple):
    head_w: object
    out_w: object
    acc: object
    squares: object
    inv_ref: object
    query_ref: object
    key_ref: object
    value_ref: object
    prob_ref: object
    pooled: object
    slopes: object
    normed_out: object
    outer_out: object
    grad_in: object
    mix_grad: object
    row_dots: object
    gain_part: object
    gain_got: object
    pool_ref: object
    near_send: object
    near_got: object
    far_send: object
    far_got: object
    relay_send: object
    near_send_b: object
    near_got_b: object
    far_send_b: object
    far_got_b: object
    relay_send_b: object
    load_sem: object
    enter_sem: object
    relay_s: object
    relay_r: object
    in_far_s: object
    in_far_r: object
    in_near_s: object
    in_near_r: object
    out_far_s: object
    out_far_r: object
    out_near_s: object
    out_near_r: object
    relay_sb: object
    relay_rb: object
    in_far_sb: object
    in_far_rb: object
    in_near_sb: object
    in_near_rb: object
    out_far_sb: object
    out_far_rb: object
    out_near_sb: object
    out_near_rb: object
    pool_s: object
    pool_r: object
    normed_s: object
    normed_r: object
    mixture_s: object
    mixture_r: object
    outer_s: object
    outer_r: object
    heads_s: object
    heads_r: object
    dots_s: object
    dots_r: object
    gain_s: object
    gain_r: object


def step_kernel(
    lengths,
    positives,
    entrance,
    gain,
    table,
    wq,
    wk,
    wv,
    wo,
    losses_out,
    gain_out,
    normed_all,
    mixture_all,
    outer_all,
    heads_all,
    hidden,
    *scratch,
):
    r = Scratch(*scratch)
    head_w, out_w, acc, squares = r.head_w, r.out_w, r.acc, r.squares
    forth, back = Place(1), Place(-1)
    blocks, rows, width = hidden.shape
    width_all = blocks * width
    pair_count = lengths.shape[0]
    seq_count = 2 * pair_count
    length = rows // seq_count
    query_cols, kv_cols = wq.shape[1], wk.shape[1]
    groups = query_cols // HEAD
    dp_me, mp_me = lax.axis_index("dp"), lax.axis_index("mp")
    dp_count, mp_count = lax.axis_size("dp"), lax.axis_size("mp")
    members = dp_count * mp_count
    me = dp_me * mp_count + mp_me
    share = blocks // dp_count
    row_pad = r.row_dots.shape[2]
    normed_sems, outer_sems = (r.normed_s, r.normed_r), (r.outer_s, r.outer_r)
    mixture_sems, heads_sems = (r.mixture_s, r.mixture_r), (r.heads_s, r.heads_r)
    outer_out = r.outer_out

    def peer(shift):
        spot = lax.rem(me + shift, members)
        return spot // mp_count, lax.rem(spot, mp_count), spot

    loads = [
        pltpu.make_async_copy(wq, head_w.at[:, :query_cols], r.load_sem.at[0]),
        pltpu.make_async_copy(
            wk, head_w.at[:, query_cols : query_cols + kv_cols], r.load_sem.at[1]
        ),
        pltpu.make_async_copy(wv, head_w.at[:, query_cols + kv_cols :], r.load_sem.at[2]),
        pltpu.make_async_copy(wo, out_w, r.load_sem.at[3]),
    ]

    def enter(block):
        return pltpu.make_async_copy(
            entrance.at[:, lanes_at(block * width, width)],
            hidden.at[block],
            r.enter_sem.at[block],
        )

    @pl.when(jnp.logical_not(forth.has_source))
    def _():
        for block in range(blocks):
            enter(block).start()

    for load in loads:
        load.start()
    barrier = pltpu.get_barrier_semaphore()
    for shift in range(1, members):
        to_dp, to_mp, _ = peer(shift)
        pl.semaphore_signal(
            barrier, inc=1, device_id={"dp": to_dp, "mp": to_mp}, device_id_type=MESH
        )

    @pl.when(forth.has_source)
    def _():
        pl.semaphore_signal(
            barrier, inc=1, device_id={"section": forth.here - 1}, device_id_type=MESH
        )

    @pl.when(forth.has_target)
    def _():
        pl.semaphore_signal(
            barrier, inc=1, device_id={"section": forth.here + 1}, device_id_type=MESH
        )

    acc[...] = jnp.zeros_like(acc)
    squares[...] = jnp.zeros_like(squares)
    r.mix_grad[...] = jnp.zeros_like(r.mix_grad)
    pool_shape = r.pool_ref.shape
    column = lax.broadcasted_iota(jnp.int32, pool_shape, 1)
    line = lax.broadcasted_iota(jnp.int32, pool_shape, 0)
    picks = jnp.zeros(pool_shape, F32)
    for seq in range(seq_count):
        inside = jnp.logical_and(
            column >= seq * length, column < seq * length + lengths[seq // 2, seq % 2]
        )
        picks = jnp.where(jnp.logical_and(line == seq, inside), 1.0, picks)
    r.pool_ref[...] = picks.astype(BF16)
    expected = (
        members - 1 + forth.has_source.astype(jnp.int32) + forth.has_target.astype(jnp.int32)
    )
    pl.semaphore_wait(barrier, expected)

    def gain_at(block):
        return gain[:, lanes_at(block * width, width)]

    def consume(block):
        value = hidden[block].astype(F32)
        squares[...] += fold_lanes(value * value)
        acc[...] += jnp.dot(
            (value * gain_at(block)).astype(BF16),
            head_w[rows_at(block * width, width), :],
            preferred_element_type=F32,
        )

    for load in loads[:3]:
        load.wait()

    @pl.when(forth.has_source)
    def _():
        stream_in(
            forth,
            hidden,
            (r.relay_s, r.relay_r),
            (r.in_far_s, r.in_far_r),
            (r.in_near_s, r.in_near_r),
            consume,
        )

    @pl.when(jnp.logical_not(forth.has_source))
    def _():
        def body(block, carry):
            enter(block).wait()
            consume(block)
            return carry

        lax.fori_loop(0, blocks, body, 0)

    inv_rms = lax.rsqrt(
        jnp.sum(squares[...], axis=1, keepdims=True) * (1.0 / width_all) + EPSILON
    )
    r.inv_ref[...] = inv_rms
    mixture = mixture_all.at[dp_me]
    for seq in range(seq_count):
        span = slice(seq * length, (seq + 1) * length)
        inverse = inv_rms[span]
        query = jnp.concatenate(
            [
                rotary(acc[span, g * HEAD : (g + 1) * HEAD] * inverse, table, 1.0)
                for g in range(groups)
            ],
            axis=0,
        ).astype(BF16)
        key = rotary(acc[span, query_cols : query_cols + kv_cols] * inverse, table, 1.0)
        key = key.astype(BF16)
        value = (acc[span, query_cols + kv_cols :] * inverse).astype(BF16)
        r.query_ref[seq] = query
        r.key_ref[seq] = key
        r.value_ref[seq] = value
        scores = contract_last(query, key) * HEAD ** (-0.5)
        spot = lax.broadcasted_iota(jnp.int32, scores.shape, 0) % length
        scores = jnp.where(spot >= lax.broadcasted_iota(jnp.int32, scores.shape, 1), scores, -1e30)
        weights = jnp.exp(scores - jnp.max(scores, axis=1, keepdims=True))
        weights = weights / jnp.sum(weights, axis=1, keepdims=True)
        r.prob_ref[seq] = weights
        mixed = jnp.dot(weights.astype(BF16), value, preferred_element_type=F32).astype(BF16)
        for g in range(groups):
            mixture[span, g * HEAD : (g + 1) * HEAD] = mixed[g * length : (g + 1) * length]
    loads[3].wait()

    def out_columns(block):
        return out_w[:, lanes_at(block * width, width)]

    @pl.when(forth.has_target)
    def _():
        def part(block):
            return jnp.dot(mixture[...], out_columns(block), preferred_element_type=F32)

        def finish(block, total):
            return (hidden[block].astype(F32) + total).astype(BF16)

        stream_out(
            forth,
            part,
            finish,
            hidden,
            (r.near_send, r.near_got, r.far_send, r.far_got, r.relay_send, None),
            (r.relay_s, r.relay_r),
            (r.out_far_s, r.out_far_r),
            (r.out_near_s, r.out_near_r),
        )

    pool = r.pool_ref[...]
    mixture_sum = jnp.dot(pool, mixture[...], preferred_element_type=F32)
    coarse = mixture_sum.astype(BF16)
    fine = (mixture_sum - coarse.astype(F32)).astype(BF16)
    both = jnp.concatenate([coarse, fine], axis=0)
    first = (mp_me == 0).astype(F32)
    pooled = r.pooled

    def pool_block(block, carry):
        sums = jnp.dot(both, out_columns(block), preferred_element_type=F32)
        sums = sums[: pool_shape[0]] + sums[pool_shape[0] :]
        sums = sums + first * jnp.dot(pool, hidden[block], preferred_element_type=F32)
        lines = [
            sums[seq : seq + 1] / lengths[seq // 2, seq % 2].astype(F32)
            for seq in range(seq_count)
        ]
        pooled[me, :, lanes_at(block * width, width)] = jnp.concatenate(lines, axis=0)
        return carry

    lax.fori_loop(0, blocks, pool_block, 0)

    def pool_copy(shift):
        to_dp, to_mp, _ = peer(shift)
        return pltpu.make_async_remote_copy(
            src_ref=pooled.at[me],
            dst_ref=pooled.at[me],
            send_sem=r.pool_s.at[shift],
            recv_sem=r.pool_r.at[me],
            device_id={"dp": to_dp, "mp": to_mp},
            device_id_type=MESH,
        )

    def pool_arrival(shift):
        from_dp, from_mp, spot = peer(shift)
        return pltpu.make_async_remote_copy(
            src_ref=pooled.at[spot],
            dst_ref=pooled.at[spot],
            send_sem=r.pool_s.at[shift],
            recv_sem=r.pool_r.at[spot],
            device_id={"dp": from_dp, "mp": from_mp},
            device_id_type=MESH,
        )

    for shift in range(1, members):
        pool_copy(shift).start()

    def to_owner(source, target, sems, block):
        return pltpu.make_async_remote_copy(
            src_ref=source.at[block],
            dst_ref=target.at[dp_me, lax.rem(block, share)],
            send_sem=sems[0].at[block],
            recv_sem=sems[1].at[dp_me, lax.rem(block, share)],
            device_id={"dp": block // share},
            device_id_type=MESH,
        )

    def from_member(target, sems, member, step):
        return pltpu.make_async_remote_copy(
            src_ref=target.at[member, step],
            dst_ref=target.at[member, step],
            send_sem=sems[0].at[0],
            recv_sem=sems[1].at[member, step],
            device_id={"dp": member},
            device_id_type=MESH,
        )

    def whole_copy(target, sems, shift):
        return pltpu.make_async_remote_copy(
            src_ref=target.at[dp_me],
            dst_ref=target.at[dp_me],
            send_sem=sems[0].at[shift],
            recv_sem=sems[1].at[dp_me],
            device_id={"dp": lax.rem(dp_me + shift, dp_count)},
            device_id_type=MESH,
        )

    def whole_arrival(target, sems, shift):
        member = lax.rem(dp_me + shift, dp_count)
        return pltpu.make_async_remote_copy(
            src_ref=target.at[member],
            dst_ref=target.at[member],
            send_sem=sems[0].at[shift],
            recv_sem=sems[1].at[member],
            device_id={"dp": member},
            device_id_type=MESH,
        )

    def normed_block(block, carry):
        value = hidden[block].astype(F32) * r.inv_ref[...] * gain_at(block)
        value = value.astype(BF16)
        mine = block // share == dp_me

        @pl.when(mine)
        def _():
            normed_all[dp_me, lax.rem(block, share)] = value

        @pl.when(jnp.logical_not(mine))
        def _():
            r.normed_out[block] = value
            to_owner(r.normed_out, normed_all, normed_sems, block).start()

        return carry

    lax.fori_loop(0, blocks, normed_block, 0)
    for shift in range(1, dp_count):
        whole_copy(mixture_all, mixture_sems, shift).start()

    for shift in range(1, members):
        pool_arrival(shift).wait_recv()
    embedded = []
    for member in range(dp_count):
        total = pooled[member * mp_count]
        for other in range(1, mp_count):
            total = total + pooled[member * mp_count + other]
        embedded.append(total)
    pairs = dp_count * pair_count
    queries = jnp.concatenate(
        [embedded[p // pair_count][2 * (p % pair_count) :][:1] for p in range(pairs)], axis=0
    )
    passages = jnp.concatenate(
        [embedded[p // pair_count][2 * (p % pair_count) + 1 :][:1] for p in range(pairs)], axis=0
    )
    partner = lax.broadcasted_iota(jnp.int32, (pairs, pairs), 1)
    line = lax.broadcasted_iota(jnp.int32, (pairs, pairs), 0)
    target = jnp.zeros((pairs, pairs), F32)
    for p in range(pairs):
        target = jnp.where(jnp.logical_and(line == p, partner == positives[p]), 1.0, target)
    losses, query_slopes, passage_slopes = matryoshka(queries, passages, target)
    lane = lax.broadcasted_iota(jnp.int32, (1, 128), 1)
    packed = jnp.zeros((1, 128), F32)
    for level in range(WIDTHS):
        packed = jnp.where(lane == level, losses[level], packed)
    losses_out[...] = packed[:, :WIDTHS]
    slopes = r.slopes
    for p in range(pairs):
        slopes[2 * p] = query_slopes[p : p + 1]
        slopes[2 * p + 1] = passage_slopes[p : p + 1]

    grad_in, mix_grad = r.grad_in, r.mix_grad
    spot = lax.broadcasted_iota(jnp.int32, (length, 1), 0)
    shares = []
    for seq in range(seq_count):
        count = lengths[seq // 2, seq % 2]
        shares.append(jnp.where(spot < count, 1.0, 0.0) / count.astype(F32))

    def upstream(block):
        tokens = jnp.concatenate(
            [
                shares[seq] * slopes[dp_me * seq_count + seq, :, lanes_at(block * width, width)]
                for seq in range(seq_count)
            ],
            axis=0,
        )
        return tokens + grad_in[block].astype(F32)

    def consume_back(block):
        outer = upstream(block).astype(BF16)
        mine = block // share == dp_me

        @pl.when(mine)
        def _():
            outer_all[dp_me, lax.rem(block, share)] = outer

        @pl.when(jnp.logical_not(mine))
        def _():
            outer_out[block] = outer
            to_owner(outer_out, outer_all, outer_sems, block).start()

        mix_grad[...] += contract_last(outer, out_columns(block))

    @pl.when(back.has_source)
    def _():
        stream_in(
            back,
            grad_in,
            (r.relay_sb, r.relay_rb),
            (r.in_far_sb, r.in_far_rb),
            (r.in_near_sb, r.in_near_rb),
            consume_back,
        )

    @pl.when(jnp.logical_not(back.has_source))
    def _():
        def body(block, carry):
            grad_in[block] = jnp.zeros((rows, width), BF16)
            consume_back(block)
            return carry

        lax.fori_loop(0, blocks, body, 0)

    head_grads = heads_all.at[dp_me]
    row_dot = []
    for seq in range(seq_count):
        span = slice(seq * length, (seq + 1) * length)
        mixed = jnp.concatenate(
            [mix_grad[span, g * HEAD : (g + 1) * HEAD] for g in range(groups)], axis=0
        ).astype(BF16)
        weights = r.prob_ref[seq]
        value_grad = contract_rows(weights.astype(BF16), mixed).astype(BF16)
        pulled = contract_last(mixed, r.value_ref[seq]).astype(BF16).astype(F32)
        score_grad = weights * (pulled - jnp.sum(weights * pulled, axis=1, keepdims=True))
        score_grad = (score_grad * HEAD ** (-0.5)).astype(BF16)
        query_grad = jnp.dot(score_grad, r.key_ref[seq], preferred_element_type=F32)
        query_grad = query_grad.astype(BF16).astype(F32)
        key_grad = contract_rows(score_grad, r.query_ref[seq]).astype(BF16).astype(F32)
        pieces = [
            rotary(query_grad[g * length : (g + 1) * length], table, -1.0).astype(BF16)
            for g in range(groups)
        ]
        pieces = pieces + [rotary(key_grad, table, -1.0).astype(BF16), value_grad]
        joined = jnp.concatenate(pieces, axis=1)
        head_grads[span, :] = joined
        row_dot.append(lane_sum(joined.astype(F32) * acc[span, :]))
    for shift in range(1, dp_count):
        whole_copy(heads_all, heads_sems, shift).start()
    row_dot = jnp.concatenate(row_dot, axis=0)

    def part_back(block):
        value = contract_last(head_grads[...], head_w[rows_at(block * width, width), :])
        scaled = value * (hidden[block].astype(F32) * r.inv_ref[...])
        r.gain_part[:, lanes_at(block * width, width)] = jnp.sum(scaled, axis=0, keepdims=True)
        return value

    row_dots = r.row_dots

    def dots_copy(shift):
        return pltpu.make_async_remote_copy(
            src_ref=row_dots.at[mp_me],
            dst_ref=row_dots.at[mp_me],
            send_sem=r.dots_s.at[shift],
            recv_sem=r.dots_r.at[mp_me],
            device_id={"mp": lax.rem(mp_me + shift, mp_count)},
            device_id_type=MESH,
        )

    def dots_arrival(shift):
        member = lax.rem(mp_me + shift, mp_count)
        return pltpu.make_async_remote_copy(
            src_ref=row_dots.at[member],
            dst_ref=row_dots.at[member],
            send_sem=r.dots_s.at[shift],
            recv_sem=r.dots_r.at[member],
            device_id={"mp": member},
            device_id_type=MESH,
        )

    @pl.when(back.has_target)
    def _():
        diagonal = lax.broadcasted_iota(jnp.int32, (rows, row_pad), 0) == lax.broadcasted_iota(
            jnp.int32, (rows, row_pad), 1
        )
        row_dots[mp_me] = jnp.sum(jnp.where(diagonal, row_dot, 0.0), axis=0, keepdims=True)
        for shift in range(1, mp_count):
            dots_copy(shift).start()

        def prepare():
            for shift in range(1, mp_count):
                dots_arrival(shift).wait_recv()
            total = row_dots[0]
            for member in range(1, mp_count):
                total = total + row_dots[member]
            column = lane_sum(jnp.where(diagonal, total, 0.0))
            inverse = r.inv_ref[...]
            squares[:, :1] = column * inverse * inverse * inverse * (1.0 / width_all)

        def finish(block, total):
            value = upstream(block) + total * gain_at(block) * r.inv_ref[...]
            return (value - hidden[block].astype(F32) * squares[:, :1]).astype(BF16)

        stream_out(
            back,
            part_back,
            finish,
            grad_in,
            (
                r.near_send_b,
                r.near_got_b,
                r.far_send_b,
                r.far_got_b,
                r.relay_send_b,
                prepare,
            ),
            (r.relay_sb, r.relay_rb),
            (r.out_far_sb, r.out_far_rb),
            (r.out_near_sb, r.out_near_rb),
        )
        for shift in range(1, mp_count):
            dots_copy(shift).wait_send()

    @pl.when(jnp.logical_not(back.has_target))
    def _():
        def body(block, carry):
            part_back(block)
            return carry

        lax.fori_loop(0, blocks, body, 0)

    gain_got = r.gain_got
    gain_cols = gain_got.shape[2]

    def gain_copy(shift):
        to_dp, to_mp, spot = peer(shift)
        return pltpu.make_async_remote_copy(
            src_ref=r.gain_part.at[:, lanes_at(spot * gain_cols, gain_cols)],
            dst_ref=gain_got.at[me],
            send_sem=r.gain_s.at[shift],
            recv_sem=r.gain_r.at[me],
            device_id={"dp": to_dp, "mp": to_mp},
            device_id_type=MESH,
        )

    def gain_arrival(shift):
        from_dp, from_mp, spot = peer(shift)
        return pltpu.make_async_remote_copy(
            src_ref=gain_got.at[spot],
            dst_ref=gain_got.at[spot],
            send_sem=r.gain_s.at[shift],
            recv_sem=r.gain_r.at[spot],
            device_id={"dp": from_dp, "mp": from_mp},
            device_id_type=MESH,
        )

    for shift in range(1, members):
        gain_copy(shift).start()
    total = r.gain_part[:, lanes_at(me * gain_cols, gain_cols)]
    for shift in range(1, members):
        gain_arrival(shift).wait_recv()
        total = total + gain_got[lax.rem(me + shift, members)]
    gain_out[...] = total

    for shift in range(1, members):
        pool_copy(shift).wait_send()
        gain_copy(shift).wait_send()
    for shift in range(1, dp_count):
        whole_copy(mixture_all, mixture_sems, shift).wait_send()
        whole_copy(heads_all, heads_sems, shift).wait_send()
        whole_arrival(mixture_all, mixture_sems, shift).wait_recv()
        whole_arrival(heads_all, heads_sems, shift).wait_recv()

    def drain(block, carry):
        @pl.when(block // share != dp_me)
        def _():
            to_owner(r.normed_out, normed_all, normed_sems, block).wait_send()
            to_owner(outer_out, outer_all, outer_sems, block).wait_send()

        return carry

    lax.fori_loop(0, blocks, drain, 0)
    for shift in range(1, dp_count):
        member = lax.rem(dp_me + shift, dp_count)
        for step in range(share):
            from_member(normed_all, normed_sems, member, step).wait_recv()
            from_member(outer_all, outer_sems, member, step).wait_recv()


def step_pass(lengths, positives, entrance, gain, table, wq, wk, wv, wo):
    rows, width_all = entrance.shape
    dp_count, mp_count = lax.axis_size("dp"), lax.axis_size("mp")
    members = dp_count * mp_count
    blocks = mp_count * SUB
    width = width_all // blocks
    share = blocks // dp_count
    seq_count = 2 * lengths.shape[0]
    length = rows // seq_count
    query_cols = wq.shape[1]
    head_cols = query_cols + wk.shape[1] + wv.shape[1]
    stacked = query_cols // HEAD * length
    row_pad = -(-rows // 128) * 128
    pool_rows = -(-seq_count // 16) * 16
    dma = pltpu.SemaphoreType.DMA
    block = (rows, width)
    shapes = dict(
        head_w=((width_all, head_cols), BF16),
        out_w=(wo.shape, BF16),
        acc=((rows, head_cols), F32),
        squares=((rows, 128), F32),
        inv_ref=((rows, 1), F32),
        query_ref=((seq_count, stacked, HEAD), BF16),
        key_ref=((seq_count, length, HEAD), BF16),
        value_ref=((seq_count, length, HEAD), BF16),
        prob_ref=((seq_count, stacked, length), F32),
        pooled=((members, seq_count, width_all), F32),
        slopes=((dp_count * seq_count, 1, width_all), F32),
        normed_out=((blocks, *block), BF16),
        outer_out=((blocks, *block), BF16),
        grad_in=((blocks, *block), BF16),
        mix_grad=((rows, query_cols), F32),
        row_dots=((mp_count, 1, row_pad), F32),
        gain_part=((1, width_all), F32),
        gain_got=((members, 1, width_all // members), F32),
        pool_ref=((pool_rows, rows), BF16),
        near_send=((2 * SUB, *block), BF16),
        near_got=((2 * SUB, *block), BF16),
        far_send=((SUB, *block), BF16),
        far_got=((SUB, *block), BF16),
        relay_send=((SUB, *block), BF16),
        near_send_b=((2 * SUB, *block), BF16),
        near_got_b=((2 * SUB, *block), BF16),
        far_send_b=((SUB, *block), BF16),
        far_got_b=((SUB, *block), BF16),
        relay_send_b=((SUB, *block), BF16),
    )
    counts = dict(
        load_sem=(4,),
        enter_sem=(blocks,),
        pool_s=(members,),
        pool_r=(members,),
        normed_s=(blocks,),
        normed_r=(dp_count, share),
        outer_s=(blocks,),
        outer_r=(dp_count, share),
        mixture_s=(dp_count,),
        mixture_r=(dp_count,),
        heads_s=(dp_count,),
        heads_r=(dp_count,),
        dots_s=(mp_count,),
        dots_r=(mp_count,),
        gain_s=(members,),
        gain_r=(members,),
        relay_s=(SUB,),
        in_far_s=(SUB,),
        out_far_s=(SUB,),
        in_near_s=(2 * SUB,),
        out_near_s=(2 * SUB,),
        relay_r=(SUB,),
        in_far_r=(SUB,),
        out_far_r=(SUB,),
        in_near_r=(2 * SUB,),
        out_near_r=(2 * SUB,),
        relay_sb=(SUB,),
        in_far_sb=(SUB,),
        out_far_sb=(SUB,),
        in_near_sb=(2 * SUB,),
        out_near_sb=(2 * SUB,),
        relay_rb=(SUB,),
        in_far_rb=(SUB,),
        out_far_rb=(SUB,),
        in_near_rb=(2 * SUB,),
        out_near_rb=(2 * SUB,),
    )
    scratch = Scratch(
        **{name: pltpu.VMEM(*shape) for name, shape in shapes.items()},
        **{name: dma(count) for name, count in counts.items()},
    )
    vmem = pl.BlockSpec(memory_space=pltpu.VMEM)
    smem = pl.BlockSpec(memory_space=pltpu.SMEM)
    hbm = pl.BlockSpec(memory_space=pltpu.HBM)
    return pl.pallas_call(
        step_kernel,
        out_shape=(
            jax.ShapeDtypeStruct((1, WIDTHS), F32),
            jax.ShapeDtypeStruct((1, width_all // members), F32),
            jax.ShapeDtypeStruct((dp_count, share, *block), BF16),
            jax.ShapeDtypeStruct((dp_count, rows, query_cols), BF16),
            jax.ShapeDtypeStruct((dp_count, share, *block), BF16),
            jax.ShapeDtypeStruct((dp_count, rows, head_cols), BF16),
        ),
        in_specs=[smem, smem, hbm, vmem, vmem, hbm, hbm, hbm, hbm],
        out_specs=(vmem,) * 6,
        scratch_shapes=[pltpu.VMEM((blocks, *block), BF16)] + list(scratch),
        compiler_params=pltpu.CompilerParams(
            collective_id=0, has_side_effects=True, vmem_limit_bytes=56 * 1024 * 1024
        ),
        name="step_pass",
    )(lengths, positives, entrance, gain, table, wq, wk, wv, wo)


def local(entrance, lengths, positives, norm_gains, query_proj, key_proj, value_proj, out_proj):
    length = entrance.shape[2]
    width_all = entrance.shape[3]
    query_cols = query_proj.shape[2]
    kv_cols = key_proj.shape[2]
    losses, gain_share, normed, mixture, outer, heads = step_pass(
        lengths,
        positives,
        entrance.reshape(-1, width_all),
        norm_gains,
        jnp.asarray(rotary_constants(length)),
        query_proj[0],
        key_proj[0],
        value_proj[0],
        out_proj[0],
    )
    normed = normed.transpose(0, 2, 1, 3).reshape(heads.shape[0] * heads.shape[1], -1)
    outer = outer.transpose(0, 2, 1, 3).reshape(heads.shape[0] * heads.shape[1], -1)
    heads = heads.reshape(normed.shape[0], -1)
    mixture = mixture.reshape(normed.shape[0], -1)
    return (
        losses,
        gain_share,
        contract_rows(normed, heads[:, :query_cols])[None],
        contract_rows(normed, heads[:, query_cols : query_cols + kv_cols])[None],
        contract_rows(normed, heads[:, query_cols + kv_cols :])[None],
        contract_rows(mixture, outer)[None],
    )


def solution(mesh):
    in_specs = (
        P("dp", None, None, None),
        P("dp", None),
        P(),
        P("section", None),
        P("section", None, "mp"),
        P("section", None, "mp"),
        P("section", None, "mp"),
        P("section", "mp", None),
    )
    out_specs = (
        P("section", None),
        P("section", ("dp", "mp")),
        P("section", "dp", "mp"),
        P("section", "dp", "mp"),
        P("section", "dp", "mp"),
        P("section", "mp", "dp"),
    )
    return jax.shard_map(local, mesh=mesh, in_specs=in_specs, out_specs=out_specs, check_vma=False)
```

```python
from typing import NamedTuple

import jax
import jax.numpy as jnp
import numpy as np
from jax import lax
from jax.experimental import pallas as pl
from jax.experimental.pallas import tpu as pltpu
from jax.sharding import PartitionSpec as P

HEAD = 128
WIDTHS = 7


EPSILON = 1e-05
SOFTMAX_TEMPER = 0.05
ROPE_BASE = 500000.0
MESH = pl.DeviceIdType.MESH
ROW_TILE = 16
SUB = 4
F32 = jnp.float32
BF16 = jnp.bfloat16


def contract_rows(left, right):
    return lax.dot_general(
        left, right, (((0,), (0,)), ((), ())), preferred_element_type=jnp.float32
    )


def contract_last(left, right):
    return lax.dot_general(
        left, right, (((left.ndim - 1,), (1,)), ((), ())), preferred_element_type=jnp.float32
    )


def rotary_constants(length):
    half_size = HEAD // 2
    frequencies = ROPE_BASE ** (-np.arange(half_size, dtype=np.float64) * 2.0 / HEAD)
    angles = np.arange(length, dtype=np.float64)[:, None] * frequencies[None, :]
    cosine = np.concatenate([np.cos(angles), np.cos(angles)], axis=1)
    sine = np.concatenate([-np.sin(angles), np.sin(angles)], axis=1)
    return np.stack([cosine, sine]).astype(np.float32)


def mp_place(me, levels):
    bits = [(me // (1 << level)) % 2 for level in range(levels)]
    partners = [me + (1 - 2 * bits[level]) * (1 << level) for level in range(levels)]
    return bits, partners


def rows_at(start, size):
    return pl.ds(pl.multiple_of(start, ROW_TILE), size)


def lanes_at(start, size):
    return pl.ds(pl.multiple_of(start, 128), size)


class Place:
    def __init__(self, direction):
        self.here = lax.axis_index("section")
        self.count = lax.axis_size("section")
        (self.low, self.high), (self.near, self.far) = mp_place(lax.axis_index("mp"), 2)
        self.direction = direction
        if direction > 0:
            self.has_source, self.has_target = self.here > 0, self.here < self.count - 1
        else:
            self.has_source, self.has_target = self.here < self.count - 1, self.here > 0

    def quarter(self, flip_low, flip_high):
        low = 1 - self.low if flip_low else self.low
        high = 1 - self.high if flip_high else self.high
        return (low * 2 + high) * SUB


def send(source, target, sems, slot, **device):
    return pltpu.make_async_remote_copy(
        src_ref=source,
        dst_ref=target,
        send_sem=sems[0].at[slot],
        recv_sem=sems[1].at[slot],
        device_id=device,
        device_id_type=MESH,
    )


def stream_in(place, buf, relay, far, near, consume):
    def near_copy(slot, block):
        return send(buf.at[block], buf.at[block], near, slot, mp=place.near)

    def far_copy(slot, block):
        return send(buf.at[block], buf.at[block], far, slot, mp=place.far)

    own, other = place.quarter(0, 0), place.quarter(0, 1)
    near_own, near_other = place.quarter(1, 0), place.quarter(1, 1)
    for tick in range(SUB + 2):
        if tick < SUB:
            block = own + tick
            send(buf.at[block], buf.at[block], relay, tick, section=place.here).wait_recv()
            far_copy(tick, block).start()
            near_copy(tick, block).start()
        if 1 <= tick <= SUB:
            block = other + tick - 1
            far_copy(tick - 1, block).wait_recv()
            near_copy(SUB + tick - 1, block).start()
        if tick >= 2:
            step = tick - 2
            near_copy(step, near_own + step).wait_recv()
            near_copy(SUB + step, near_other + step).wait_recv()

            def body(part, carry, step=step):
                consume(part * SUB + step)
                return carry

            lax.fori_loop(0, 4, body, 0)
    for step in range(SUB):
        far_copy(step, own + step).wait_send()
        near_copy(step, own + step).wait_send()
        near_copy(SUB + step, other + step).wait_send()


def stream_out(place, part, finish, dest, bufs, relay, far, near):
    near_send, near_got, far_send, far_got, relay_send, prepare = bufs

    def near_copy(slot):
        return send(near_send.at[slot], near_got.at[slot], near, slot, mp=place.near)

    def far_copy(step):
        return send(far_send.at[step], far_got.at[step], far, step, mp=place.far)

    def relay_copy(step):
        return send(
            relay_send.at[step],
            dest.at[place.quarter(0, 0) + step],
            relay,
            step,
            section=place.here + place.direction,
        )

    for flip in (1, 0):
        base = (1 - place.high if flip else place.high) * SUB
        for step in range(SUB):
            near_send[base + step] = part(place.quarter(1, flip) + step).astype(BF16)
            near_copy(base + step).start()
    base = (1 - place.high) * SUB
    for step in range(SUB):
        value = part(place.quarter(0, 1) + step)
        near_copy(base + step).wait_recv()
        far_send[step] = (value + near_got[base + step].astype(F32)).astype(BF16)
        far_copy(step).start()
    base = place.high * SUB
    if prepare is not None:
        prepare()
    for step in range(SUB):
        value = part(place.quarter(0, 0) + step)
        near_copy(base + step).wait_recv()
        value = value + near_got[base + step].astype(F32)
        far_copy(step).wait_recv()
        value = value + far_got[step].astype(F32)
        relay_send[step] = finish(place.quarter(0, 0) + step, value)
        relay_copy(step).start()
    for step in range(SUB):
        far_copy(step).wait_send()
        relay_copy(step).wait_send()
    for slot in range(2 * SUB):
        near_copy(slot).wait_send()


def rotary(values, table, sign):
    turned = pltpu.roll(values, HEAD // 2, axis=1)
    return values * table[0] + turned * (table[1] * sign)


def fold_lanes(values):
    total = values[:, :128]
    for lane in range(1, values.shape[1] // 128):
        total = total + values[:, lane * 128 : (lane + 1) * 128]
    return total


def lane_sum(values):
    return jnp.sum(fold_lanes(values), axis=1, keepdims=True)


def matryoshka(queries, passages, target):
    pairs, width_all = queries.shape
    widths = [width_all >> level for level in range(WIDTHS)]
    bounds = [0] + widths[::-1]
    lane = lax.broadcasted_iota(jnp.int32, (pairs, 128), 1)

    def segment_sums(product):
        sums = []
        for low, high in zip(bounds[:-1], bounds[1:]):
            if high <= 128:
                inside = jnp.logical_and(lane >= low, lane < high)
                piece = jnp.where(inside, product[:, :128], 0.0)
            else:
                piece = fold_lanes(product[:, low:high])
            sums.append(jnp.sum(piece, axis=1, keepdims=True))
        for index in range(1, len(sums)):
            sums[index] = sums[index] + sums[index - 1]
        return sums[::-1]

    query_squares = segment_sums(queries * queries)
    passage_squares = segment_sums(passages * passages)
    dots = [segment_sums(queries * passages[j : j + 1]) for j in range(pairs)]
    losses = []
    mixed = [[] for _ in range(pairs)]
    query_own, passage_own = [], []
    for level, width in enumerate(widths):
        query_inv = lax.rsqrt(query_squares[level] * (1.0 / width) + 1e-06)
        passage_inv = lax.rsqrt(passage_squares[level] * (1.0 / width) + 1e-06)
        factors = [
            query_inv * passage_inv[j : j + 1] * (1.0 / (width * SOFTMAX_TEMPER))
            for j in range(pairs)
        ]
        logits = [dots[j][level] * factors[j] for j in range(pairs)]
        highest = logits[0]
        for j in range(1, pairs):
            highest = jnp.maximum(highest, logits[j])
        powers = [jnp.exp(logits[j] - highest) for j in range(pairs)]
        total = powers[0]
        picked = logits[0] * target[:, 0:1]
        for j in range(1, pairs):
            total = total + powers[j]
            picked = picked + logits[j] * target[:, j : j + 1]
        gap = jnp.log(total) + highest - picked
        losses.append(jnp.sum(gap, axis=0, keepdims=True) * (1.0 / pairs))
        slopes = [
            (powers[j] / total - target[:, j : j + 1]) * (1.0 / pairs) for j in range(pairs)
        ]
        pulls = [slopes[j] * logits[j] for j in range(pairs)]
        row_pull = pulls[0]
        for j in range(1, pairs):
            row_pull = row_pull + pulls[j]
        column_pull = jnp.concatenate(
            [jnp.sum(pulls[j], axis=0, keepdims=True) for j in range(pairs)], axis=0
        )
        for j in range(pairs):
            mixed[j].append(slopes[j] * factors[j])
        query_own.append(row_pull * query_inv * query_inv * (-1.0 / width))
        passage_own.append(column_pull * passage_inv * passage_inv * (-1.0 / width))
    for series in mixed + [query_own, passage_own]:
        for level in range(1, WIDTHS):
            series[level] = series[level] + series[level - 1]
    turned = [
        [
            jnp.concatenate([mixed[j][level][p : p + 1] for j in range(pairs)], axis=0)
            for level in range(WIDTHS)
        ]
        for p in range(pairs)
    ]

    def spread(own, own_rows, weights, rows):
        pieces = []
        low = 0
        while low < width_all:
            inside = [k for k in range(WIDTHS) if low < bounds[k + 1] and low + 128 > bounds[k]]
            high = max(low + 128, bounds[inside[-1] + 1])

            def coefficient(series, inside=inside):
                value = series[WIDTHS - 1 - inside[-1]]
                for k in reversed(inside[:-1]):
                    value = jnp.where(lane < bounds[k + 1], series[WIDTHS - 1 - k], value)
                return value

            def columns(values, low=low, high=high):
                return values[:, low:high]

            piece = coefficient(own) * columns(own_rows)
            for j in range(pairs):
                piece = piece + coefficient(weights[j]) * columns(rows[j : j + 1])
            pieces.append(piece)
            low = high
        return jnp.concatenate(pieces, axis=1)

    return (
        losses,
        spread(query_own, queries, mixed, passages),
        spread(passage_own, passages, turned, queries),
    )


class Scratch(NamedTuple):
    head_w: object
    out_w: object
    acc: object
    squares: object
    inv_ref: object
    query_ref: object
    key_ref: object
    value_ref: object
    prob_ref: object
    pooled: object
    slopes: object
    normed_out: object
    outer_out: object
    grad_in: object
    mix_grad: object
    row_dots: object
    gain_part: object
    gain_got: object
    pool_ref: object
    near_send: object
    near_got: object
    far_send: object
    far_got: object
    relay_send: object
    near_send_b: object
    near_got_b: object
    far_send_b: object
    far_got_b: object
    relay_send_b: object
    load_sem: object
    enter_sem: object
    relay_s: object
    relay_r: object
    in_far_s: object
    in_far_r: object
    in_near_s: object
    in_near_r: object
    out_far_s: object
    out_far_r: object
    out_near_s: object
    out_near_r: object
    relay_sb: object
    relay_rb: object
    in_far_sb: object
    in_far_rb: object
    in_near_sb: object
    in_near_rb: object
    out_far_sb: object
    out_far_rb: object
    out_near_sb: object
    out_near_rb: object
    pool_s: object
    pool_r: object
    normed_s: object
    normed_r: object
    mixture_s: object
    mixture_r: object
    outer_s: object
    outer_r: object
    heads_s: object
    heads_r: object
    dots_s: object
    dots_r: object
    gain_s: object
    gain_r: object


def step_kernel(
    lengths,
    positives,
    entrance,
    gain,
    table,
    wq,
    wk,
    wv,
    wo,
    losses_out,
    gain_out,
    normed_all,
    mixture_all,
    outer_all,
    heads_all,
    hidden,
    *scratch,
):
    r = Scratch(*scratch)
    head_w, out_w, acc, squares = r.head_w, r.out_w, r.acc, r.squares
    forth, back = Place(1), Place(-1)
    blocks, rows, width = hidden.shape
    width_all = blocks * width
    pair_count = lengths.shape[0]
    seq_count = 2 * pair_count
    length = rows // seq_count
    query_cols, kv_cols = wq.shape[1], wk.shape[1]
    groups = query_cols // HEAD
    dp_me, mp_me = lax.axis_index("dp"), lax.axis_index("mp")
    dp_count, mp_count = lax.axis_size("dp"), lax.axis_size("mp")
    members = dp_count * mp_count
    me = dp_me * mp_count + mp_me
    share = blocks // dp_count
    row_pad = r.row_dots.shape[2]
    normed_sems, outer_sems = (r.normed_s, r.normed_r), (r.outer_s, r.outer_r)
    mixture_sems, heads_sems = (r.mixture_s, r.mixture_r), (r.heads_s, r.heads_r)
    outer_out = r.outer_out

    def peer(shift):
        spot = lax.rem(me + shift, members)
        return spot // mp_count, lax.rem(spot, mp_count), spot

    loads = [
        pltpu.make_async_copy(wq, head_w.at[:, :query_cols], r.load_sem.at[0]),
        pltpu.make_async_copy(
            wk, head_w.at[:, query_cols : query_cols + kv_cols], r.load_sem.at[1]
        ),
        pltpu.make_async_copy(wv, head_w.at[:, query_cols + kv_cols :], r.load_sem.at[2]),
        pltpu.make_async_copy(wo, out_w, r.load_sem.at[3]),
    ]

    def enter(block):
        return pltpu.make_async_copy(
            entrance.at[:, lanes_at(block * width, width)],
            hidden.at[block],
            r.enter_sem.at[block],
        )

    @pl.when(jnp.logical_not(forth.has_source))
    def _():
        for block in range(blocks):
            enter(block).start()

    for load in loads:
        load.start()
    barrier = pltpu.get_barrier_semaphore()
    for shift in range(1, members):
        to_dp, to_mp, _ = peer(shift)
        pl.semaphore_signal(
            barrier, inc=1, device_id={"dp": to_dp, "mp": to_mp}, device_id_type=MESH
        )

    @pl.when(forth.has_source)
    def _():
        pl.semaphore_signal(
            barrier, inc=1, device_id={"section": forth.here - 1}, device_id_type=MESH
        )

    @pl.when(forth.has_target)
    def _():
        pl.semaphore_signal(
            barrier, inc=1, device_id={"section": forth.here + 1}, device_id_type=MESH
        )

    acc[...] = jnp.zeros_like(acc)
    squares[...] = jnp.zeros_like(squares)
    r.mix_grad[...] = jnp.zeros_like(r.mix_grad)
    pool_shape = r.pool_ref.shape
    column = lax.broadcasted_iota(jnp.int32, pool_shape, 1)
    line = lax.broadcasted_iota(jnp.int32, pool_shape, 0)
    picks = jnp.zeros(pool_shape, F32)
    for seq in range(seq_count):
        inside = jnp.logical_and(
            column >= seq * length, column < seq * length + lengths[seq // 2, seq % 2]
        )
        picks = jnp.where(jnp.logical_and(line == seq, inside), 1.0, picks)
    r.pool_ref[...] = picks.astype(BF16)
    expected = (
        members - 1 + forth.has_source.astype(jnp.int32) + forth.has_target.astype(jnp.int32)
    )

    def gain_at(block):
        return gain[:, lanes_at(block * width, width)]

    def consume(block):
        value = hidden[block].astype(F32)
        squares[...] += fold_lanes(value * value)
        acc[...] += jnp.dot(
            (value * gain_at(block)).astype(BF16),
            head_w[rows_at(block * width, width), :],
            preferred_element_type=F32,
        )

    for load in loads[:3]:
        load.wait()

    @pl.when(forth.has_source)
    def _():
        pl.semaphore_wait(barrier, expected)
        stream_in(
            forth,
            hidden,
            (r.relay_s, r.relay_r),
            (r.in_far_s, r.in_far_r),
            (r.in_near_s, r.in_near_r),
            consume,
        )

    @pl.when(jnp.logical_not(forth.has_source))
    def _():
        def body(block, carry):
            enter(block).wait()
            consume(block)
            return carry

        lax.fori_loop(0, blocks, body, 0, unroll=4)
        pl.semaphore_wait(barrier, expected)

    inv_rms = lax.rsqrt(
        jnp.sum(squares[...], axis=1, keepdims=True) * (1.0 / width_all) + EPSILON
    )
    r.inv_ref[...] = inv_rms
    mixture = mixture_all.at[dp_me]
    for seq in range(seq_count):
        span = slice(seq * length, (seq + 1) * length)
        inverse = inv_rms[span]
        query = jnp.concatenate(
            [
                rotary(acc[span, g * HEAD : (g + 1) * HEAD] * inverse, table, 1.0)
                for g in range(groups)
            ],
            axis=0,
        ).astype(BF16)
        key = rotary(acc[span, query_cols : query_cols + kv_cols] * inverse, table, 1.0)
        key = key.astype(BF16)
        value = (acc[span, query_cols + kv_cols :] * inverse).astype(BF16)
        r.query_ref[seq] = query
        r.key_ref[seq] = key
        r.value_ref[seq] = value
        scores = contract_last(query, key) * HEAD ** (-0.5)
        spot = lax.broadcasted_iota(jnp.int32, scores.shape, 0) % length
        scores = jnp.where(spot >= lax.broadcasted_iota(jnp.int32, scores.shape, 1), scores, -1e30)
        weights = jnp.exp(scores - jnp.max(scores, axis=1, keepdims=True))
        weights = weights / jnp.sum(weights, axis=1, keepdims=True)
        r.prob_ref[seq] = weights
        mixed = jnp.dot(weights.astype(BF16), value, preferred_element_type=F32).astype(BF16)
        for g in range(groups):
            mixture[span, g * HEAD : (g + 1) * HEAD] = mixed[g * length : (g + 1) * length]
    loads[3].wait()

    def out_columns(block):
        return out_w[:, lanes_at(block * width, width)]

    @pl.when(forth.has_target)
    def _():
        def part(block):
            return jnp.dot(mixture[...], out_columns(block), preferred_element_type=F32)

        def finish(block, total):
            return (hidden[block].astype(F32) + total).astype(BF16)

        stream_out(
            forth,
            part,
            finish,
            hidden,
            (r.near_send, r.near_got, r.far_send, r.far_got, r.relay_send, None),
            (r.relay_s, r.relay_r),
            (r.out_far_s, r.out_far_r),
            (r.out_near_s, r.out_near_r),
        )

    pool = r.pool_ref[...]
    mixture_sum = jnp.dot(pool, mixture[...], preferred_element_type=F32)
    coarse = mixture_sum.astype(BF16)
    fine = (mixture_sum - coarse.astype(F32)).astype(BF16)
    both = jnp.concatenate([coarse, fine], axis=0)
    first = (mp_me == 0).astype(F32)
    pooled = r.pooled

    def pool_block(block, carry):
        sums = jnp.dot(both, out_columns(block), preferred_element_type=F32)
        sums = sums[: pool_shape[0]] + sums[pool_shape[0] :]
        sums = sums + first * jnp.dot(pool, hidden[block], preferred_element_type=F32)
        lines = [
            sums[seq : seq + 1] / lengths[seq // 2, seq % 2].astype(F32)
            for seq in range(seq_count)
        ]
        pooled[me, :, lanes_at(block * width, width)] = jnp.concatenate(lines, axis=0)
        return carry

    lax.fori_loop(0, blocks, pool_block, 0)

    def pool_copy(shift):
        to_dp, to_mp, _ = peer(shift)
        return pltpu.make_async_remote_copy(
            src_ref=pooled.at[me],
            dst_ref=pooled.at[me],
            send_sem=r.pool_s.at[shift],
            recv_sem=r.pool_r.at[me],
            device_id={"dp": to_dp, "mp": to_mp},
            device_id_type=MESH,
        )

    def pool_arrival(shift):
        from_dp, from_mp, spot = peer(shift)
        return pltpu.make_async_remote_copy(
            src_ref=pooled.at[spot],
            dst_ref=pooled.at[spot],
            send_sem=r.pool_s.at[shift],
            recv_sem=r.pool_r.at[spot],
            device_id={"dp": from_dp, "mp": from_mp},
            device_id_type=MESH,
        )

    for shift in range(1, members):
        pool_copy(shift).start()

    def to_owner(source, target, sems, block):
        return pltpu.make_async_remote_copy(
            src_ref=source.at[block],
            dst_ref=target.at[dp_me, lax.rem(block, share)],
            send_sem=sems[0].at[block],
            recv_sem=sems[1].at[dp_me, lax.rem(block, share)],
            device_id={"dp": block // share},
            device_id_type=MESH,
        )

    def from_member(target, sems, member, step):
        return pltpu.make_async_remote_copy(
            src_ref=target.at[member, step],
            dst_ref=target.at[member, step],
            send_sem=sems[0].at[0],
            recv_sem=sems[1].at[member, step],
            device_id={"dp": member},
            device_id_type=MESH,
        )

    def whole_copy(target, sems, shift):
        return pltpu.make_async_remote_copy(
            src_ref=target.at[dp_me],
            dst_ref=target.at[dp_me],
            send_sem=sems[0].at[shift],
            recv_sem=sems[1].at[dp_me],
            device_id={"dp": lax.rem(dp_me + shift, dp_count)},
            device_id_type=MESH,
        )

    def whole_arrival(target, sems, shift):
        member = lax.rem(dp_me + shift, dp_count)
        return pltpu.make_async_remote_copy(
            src_ref=target.at[member],
            dst_ref=target.at[member],
            send_sem=sems[0].at[shift],
            recv_sem=sems[1].at[member],
            device_id={"dp": member},
            device_id_type=MESH,
        )

    def normed_block(block, carry):
        value = hidden[block].astype(F32) * r.inv_ref[...] * gain_at(block)
        value = value.astype(BF16)
        mine = block // share == dp_me

        @pl.when(mine)
        def _():
            normed_all[dp_me, lax.rem(block, share)] = value

        @pl.when(jnp.logical_not(mine))
        def _():
            r.normed_out[block] = value
            to_owner(r.normed_out, normed_all, normed_sems, block).start()

        return carry

    lax.fori_loop(0, blocks, normed_block, 0)
    for shift in range(1, dp_count):
        whole_copy(mixture_all, mixture_sems, shift).start()

    for shift in range(1, members):
        pool_arrival(shift).wait_recv()
    embedded = []
    for member in range(dp_count):
        total = pooled[member * mp_count]
        for other in range(1, mp_count):
            total = total + pooled[member * mp_count + other]
        embedded.append(total)
    pairs = dp_count * pair_count
    queries = jnp.concatenate(
        [embedded[p // pair_count][2 * (p % pair_count) :][:1] for p in range(pairs)], axis=0
    )
    passages = jnp.concatenate(
        [embedded[p // pair_count][2 * (p % pair_count) + 1 :][:1] for p in range(pairs)], axis=0
    )
    partner = lax.broadcasted_iota(jnp.int32, (pairs, pairs), 1)
    line = lax.broadcasted_iota(jnp.int32, (pairs, pairs), 0)
    target = jnp.zeros((pairs, pairs), F32)
    for p in range(pairs):
        target = jnp.where(jnp.logical_and(line == p, partner == positives[p]), 1.0, target)
    losses, query_slopes, passage_slopes = matryoshka(queries, passages, target)
    lane = lax.broadcasted_iota(jnp.int32, (1, 128), 1)
    packed = jnp.zeros((1, 128), F32)
    for level in range(WIDTHS):
        packed = jnp.where(lane == level, losses[level], packed)
    losses_out[...] = packed[:, :WIDTHS]
    slopes = r.slopes
    for p in range(pairs):
        slopes[2 * p] = query_slopes[p : p + 1]
        slopes[2 * p + 1] = passage_slopes[p : p + 1]

    grad_in, mix_grad = r.grad_in, r.mix_grad
    spot = lax.broadcasted_iota(jnp.int32, (length, 1), 0)
    shares = []
    for seq in range(seq_count):
        count = lengths[seq // 2, seq % 2]
        shares.append(jnp.where(spot < count, 1.0, 0.0) / count.astype(F32))

    def upstream(block):
        tokens = jnp.concatenate(
            [
                shares[seq] * slopes[dp_me * seq_count + seq, :, lanes_at(block * width, width)]
                for seq in range(seq_count)
            ],
            axis=0,
        )
        return tokens + grad_in[block].astype(F32)

    def consume_back(block):
        outer = upstream(block).astype(BF16)
        mine = block // share == dp_me

        @pl.when(mine)
        def _():
            outer_all[dp_me, lax.rem(block, share)] = outer

        @pl.when(jnp.logical_not(mine))
        def _():
            outer_out[block] = outer
            to_owner(outer_out, outer_all, outer_sems, block).start()

        mix_grad[...] += contract_last(outer, out_columns(block))

    @pl.when(back.has_source)
    def _():
        stream_in(
            back,
            grad_in,
            (r.relay_sb, r.relay_rb),
            (r.in_far_sb, r.in_far_rb),
            (r.in_near_sb, r.in_near_rb),
            consume_back,
        )

    @pl.when(jnp.logical_not(back.has_source))
    def _():
        def body(block, carry):
            grad_in[block] = jnp.zeros((rows, width), BF16)
            consume_back(block)
            return carry

        lax.fori_loop(0, blocks, body, 0)

    head_grads = heads_all.at[dp_me]
    row_dot = []
    for seq in range(seq_count):
        span = slice(seq * length, (seq + 1) * length)
        mixed = jnp.concatenate(
            [mix_grad[span, g * HEAD : (g + 1) * HEAD] for g in range(groups)], axis=0
        ).astype(BF16)
        weights = r.prob_ref[seq]
        value_grad = contract_rows(weights.astype(BF16), mixed).astype(BF16)
        pulled = contract_last(mixed, r.value_ref[seq]).astype(BF16).astype(F32)
        score_grad = weights * (pulled - jnp.sum(weights * pulled, axis=1, keepdims=True))
        score_grad = (score_grad * HEAD ** (-0.5)).astype(BF16)
        query_grad = jnp.dot(score_grad, r.key_ref[seq], preferred_element_type=F32)
        query_grad = query_grad.astype(BF16).astype(F32)
        key_grad = contract_rows(score_grad, r.query_ref[seq]).astype(BF16).astype(F32)
        pieces = [
            rotary(query_grad[g * length : (g + 1) * length], table, -1.0).astype(BF16)
            for g in range(groups)
        ]
        pieces = pieces + [rotary(key_grad, table, -1.0).astype(BF16), value_grad]
        joined = jnp.concatenate(pieces, axis=1)
        head_grads[span, :] = joined
        row_dot.append(lane_sum(joined.astype(F32) * acc[span, :]))
    for shift in range(1, dp_count):
        whole_copy(heads_all, heads_sems, shift).start()
    row_dot = jnp.concatenate(row_dot, axis=0)

    def part_back(block):
        value = contract_last(head_grads[...], head_w[rows_at(block * width, width), :])
        scaled = value * (hidden[block].astype(F32) * r.inv_ref[...])
        r.gain_part[:, lanes_at(block * width, width)] = jnp.sum(scaled, axis=0, keepdims=True)
        return value

    row_dots = r.row_dots

    def dots_copy(shift):
        return pltpu.make_async_remote_copy(
            src_ref=row_dots.at[mp_me],
            dst_ref=row_dots.at[mp_me],
            send_sem=r.dots_s.at[shift],
            recv_sem=r.dots_r.at[mp_me],
            device_id={"mp": lax.rem(mp_me + shift, mp_count)},
            device_id_type=MESH,
        )

    def dots_arrival(shift):
        member = lax.rem(mp_me + shift, mp_count)
        return pltpu.make_async_remote_copy(
            src_ref=row_dots.at[member],
            dst_ref=row_dots.at[member],
            send_sem=r.dots_s.at[shift],
            recv_sem=r.dots_r.at[member],
            device_id={"mp": member},
            device_id_type=MESH,
        )

    @pl.when(back.has_target)
    def _():
        diagonal = lax.broadcasted_iota(jnp.int32, (rows, row_pad), 0) == lax.broadcasted_iota(
            jnp.int32, (rows, row_pad), 1
        )
        row_dots[mp_me] = jnp.sum(jnp.where(diagonal, row_dot, 0.0), axis=0, keepdims=True)
        for shift in range(1, mp_count):
            dots_copy(shift).start()

        def prepare():
            for shift in range(1, mp_count):
                dots_arrival(shift).wait_recv()
            total = row_dots[0]
            for member in range(1, mp_count):
                total = total + row_dots[member]
            column = lane_sum(jnp.where(diagonal, total, 0.0))
            inverse = r.inv_ref[...]
            squares[:, :1] = column * inverse * inverse * inverse * (1.0 / width_all)

        def finish(block, total):
            value = upstream(block) + total * gain_at(block) * r.inv_ref[...]
            return (value - hidden[block].astype(F32) * squares[:, :1]).astype(BF16)

        stream_out(
            back,
            part_back,
            finish,
            grad_in,
            (
                r.near_send_b,
                r.near_got_b,
                r.far_send_b,
                r.far_got_b,
                r.relay_send_b,
                prepare,
            ),
            (r.relay_sb, r.relay_rb),
            (r.out_far_sb, r.out_far_rb),
            (r.out_near_sb, r.out_near_rb),
        )
        for shift in range(1, mp_count):
            dots_copy(shift).wait_send()

    @pl.when(jnp.logical_not(back.has_target))
    def _():
        def body(block, carry):
            part_back(block)
            return carry

        lax.fori_loop(0, blocks, body, 0)

    gain_got = r.gain_got
    gain_cols = gain_got.shape[2]

    def gain_copy(shift):
        to_dp, to_mp, spot = peer(shift)
        return pltpu.make_async_remote_copy(
            src_ref=r.gain_part.at[:, lanes_at(spot * gain_cols, gain_cols)],
            dst_ref=gain_got.at[me],
            send_sem=r.gain_s.at[shift],
            recv_sem=r.gain_r.at[me],
            device_id={"dp": to_dp, "mp": to_mp},
            device_id_type=MESH,
        )

    def gain_arrival(shift):
        from_dp, from_mp, spot = peer(shift)
        return pltpu.make_async_remote_copy(
            src_ref=gain_got.at[spot],
            dst_ref=gain_got.at[spot],
            send_sem=r.gain_s.at[shift],
            recv_sem=r.gain_r.at[spot],
            device_id={"dp": from_dp, "mp": from_mp},
            device_id_type=MESH,
        )

    for shift in range(1, members):
        gain_copy(shift).start()
    total = r.gain_part[:, lanes_at(me * gain_cols, gain_cols)]
    for shift in range(1, members):
        gain_arrival(shift).wait_recv()
        total = total + gain_got[lax.rem(me + shift, members)]
    gain_out[...] = total

    for shift in range(1, members):
        pool_copy(shift).wait_send()
        gain_copy(shift).wait_send()
    for shift in range(1, dp_count):
        whole_copy(mixture_all, mixture_sems, shift).wait_send()
        whole_copy(heads_all, heads_sems, shift).wait_send()
        whole_arrival(mixture_all, mixture_sems, shift).wait_recv()
        whole_arrival(heads_all, heads_sems, shift).wait_recv()

    def drain(block, carry):
        @pl.when(block // share != dp_me)
        def _():
            to_owner(r.normed_out, normed_all, normed_sems, block).wait_send()
            to_owner(outer_out, outer_all, outer_sems, block).wait_send()

        return carry

    lax.fori_loop(0, blocks, drain, 0)
    for shift in range(1, dp_count):
        member = lax.rem(dp_me + shift, dp_count)
        for step in range(share):
            from_member(normed_all, normed_sems, member, step).wait_recv()
            from_member(outer_all, outer_sems, member, step).wait_recv()


def step_pass(lengths, positives, entrance, gain, table, wq, wk, wv, wo):
    rows, width_all = entrance.shape
    dp_count, mp_count = lax.axis_size("dp"), lax.axis_size("mp")
    members = dp_count * mp_count
    blocks = mp_count * SUB
    width = width_all // blocks
    share = blocks // dp_count
    seq_count = 2 * lengths.shape[0]
    length = rows // seq_count
    query_cols = wq.shape[1]
    head_cols = query_cols + wk.shape[1] + wv.shape[1]
    stacked = query_cols // HEAD * length
    row_pad = -(-rows // 128) * 128
    pool_rows = -(-seq_count // 16) * 16
    dma = pltpu.SemaphoreType.DMA
    block = (rows, width)
    shapes = dict(
        head_w=((width_all, head_cols), BF16),
        out_w=(wo.shape, BF16),
        acc=((rows, head_cols), F32),
        squares=((rows, 128), F32),
        inv_ref=((rows, 1), F32),
        query_ref=((seq_count, stacked, HEAD), BF16),
        key_ref=((seq_count, length, HEAD), BF16),
        value_ref=((seq_count, length, HEAD), BF16),
        prob_ref=((seq_count, stacked, length), F32),
        pooled=((members, seq_count, width_all), F32),
        slopes=((dp_count * seq_count, 1, width_all), F32),
        normed_out=((blocks, *block), BF16),
        outer_out=((blocks, *block), BF16),
        grad_in=((blocks, *block), BF16),
        mix_grad=((rows, query_cols), F32),
        row_dots=((mp_count, 1, row_pad), F32),
        gain_part=((1, width_all), F32),
        gain_got=((members, 1, width_all // members), F32),
        pool_ref=((pool_rows, rows), BF16),
        near_send=((2 * SUB, *block), BF16),
        near_got=((2 * SUB, *block), BF16),
        far_send=((SUB, *block), BF16),
        far_got=((SUB, *block), BF16),
        relay_send=((SUB, *block), BF16),
        near_send_b=((2 * SUB, *block), BF16),
        near_got_b=((2 * SUB, *block), BF16),
        far_send_b=((SUB, *block), BF16),
        far_got_b=((SUB, *block), BF16),
        relay_send_b=((SUB, *block), BF16),
    )
    counts = dict(
        load_sem=(4,),
        enter_sem=(blocks,),
        pool_s=(members,),
        pool_r=(members,),
        normed_s=(blocks,),
        normed_r=(dp_count, share),
        outer_s=(blocks,),
        outer_r=(dp_count, share),
        mixture_s=(dp_count,),
        mixture_r=(dp_count,),
        heads_s=(dp_count,),
        heads_r=(dp_count,),
        dots_s=(mp_count,),
        dots_r=(mp_count,),
        gain_s=(members,),
        gain_r=(members,),
        relay_s=(SUB,),
        in_far_s=(SUB,),
        out_far_s=(SUB,),
        in_near_s=(2 * SUB,),
        out_near_s=(2 * SUB,),
        relay_r=(SUB,),
        in_far_r=(SUB,),
        out_far_r=(SUB,),
        in_near_r=(2 * SUB,),
        out_near_r=(2 * SUB,),
        relay_sb=(SUB,),
        in_far_sb=(SUB,),
        out_far_sb=(SUB,),
        in_near_sb=(2 * SUB,),
        out_near_sb=(2 * SUB,),
        relay_rb=(SUB,),
        in_far_rb=(SUB,),
        out_far_rb=(SUB,),
        in_near_rb=(2 * SUB,),
        out_near_rb=(2 * SUB,),
    )
    scratch = Scratch(
        **{name: pltpu.VMEM(*shape) for name, shape in shapes.items()},
        **{name: dma(count) for name, count in counts.items()},
    )
    vmem = pl.BlockSpec(memory_space=pltpu.VMEM)
    smem = pl.BlockSpec(memory_space=pltpu.SMEM)
    hbm = pl.BlockSpec(memory_space=pltpu.HBM)
    return pl.pallas_call(
        step_kernel,
        out_shape=(
            jax.ShapeDtypeStruct((1, WIDTHS), F32),
            jax.ShapeDtypeStruct((1, width_all // members), F32),
            jax.ShapeDtypeStruct((dp_count, share, *block), BF16),
            jax.ShapeDtypeStruct((dp_count, rows, query_cols), BF16),
            jax.ShapeDtypeStruct((dp_count, share, *block), BF16),
            jax.ShapeDtypeStruct((dp_count, rows, head_cols), BF16),
        ),
        in_specs=[smem, smem, hbm, vmem, vmem, hbm, hbm, hbm, hbm],
        out_specs=(vmem,) * 6,
        scratch_shapes=[pltpu.VMEM((blocks, *block), BF16)] + list(scratch),
        compiler_params=pltpu.CompilerParams(
            collective_id=0, has_side_effects=True, vmem_limit_bytes=56 * 1024 * 1024
        ),
        name="step_pass",
    )(lengths, positives, entrance, gain, table, wq, wk, wv, wo)


def weight_kernel(
    normed, mixture, outer, heads, query_grad, key_grad, value_grad, out_grad, turned
):
    members, rows = heads.shape[:2]
    query_cols, kv_cols = query_grad.shape[1], key_grad.shape[1]

    @pl.when(pl.program_id(0) == 0)
    def _():
        for member in range(members):
            turned[:, member * rows : (member + 1) * rows] = mixture[member].T

    inputs = jnp.concatenate([normed[member, 0] for member in range(members)], axis=0)
    grads = jnp.concatenate([heads[member] for member in range(members)], axis=0)
    product = contract_rows(inputs, grads)
    query_grad[...] = product[:, :query_cols]
    key_grad[...] = product[:, query_cols : query_cols + kv_cols]
    value_grad[...] = product[:, query_cols + kv_cols :]
    grads = jnp.concatenate([outer[member, 0] for member in range(members)], axis=0)
    out_grad[...] = jnp.dot(turned[...], grads, preferred_element_type=F32)


def weight_grads(normed, mixture, outer, heads, query_cols, kv_cols):
    members, share, rows, width = normed.shape
    columns = share * width
    streamed = pl.BlockSpec((members, 1, rows, width), lambda step: (0, step, 0, 0))
    vmem = pl.BlockSpec(memory_space=pltpu.VMEM)

    def tall(cols):
        return pl.BlockSpec((width, cols), lambda step: (step, 0))

    return pl.pallas_call(
        weight_kernel,
        grid=(share,),
        in_specs=[streamed, vmem, streamed, vmem],
        out_specs=(
            tall(query_cols),
            tall(kv_cols),
            tall(kv_cols),
            pl.BlockSpec((query_cols, width), lambda step: (0, step)),
        ),
        out_shape=(
            jax.ShapeDtypeStruct((columns, query_cols), F32),
            jax.ShapeDtypeStruct((columns, kv_cols), F32),
            jax.ShapeDtypeStruct((columns, kv_cols), F32),
            jax.ShapeDtypeStruct((query_cols, columns), F32),
        ),
        scratch_shapes=[pltpu.VMEM((query_cols, members * rows), BF16)],
        compiler_params=pltpu.CompilerParams(dimension_semantics=("arbitrary",)),
        name="weight_grads",
    )(normed, mixture, outer, heads)


def local(entrance, lengths, positives, norm_gains, query_proj, key_proj, value_proj, out_proj):
    length = entrance.shape[2]
    width_all = entrance.shape[3]
    query_cols = query_proj.shape[2]
    kv_cols = key_proj.shape[2]
    losses, gain_share, normed, mixture, outer, heads = step_pass(
        lengths,
        positives,
        entrance.reshape(-1, width_all),
        norm_gains,
        jnp.asarray(rotary_constants(length)),
        query_proj[0],
        key_proj[0],
        value_proj[0],
        out_proj[0],
    )
    query_grad, key_grad, value_grad, out_grad = weight_grads(
        normed, mixture, outer, heads, query_cols, kv_cols
    )
    return (
        losses,
        gain_share,
        query_grad[None],
        key_grad[None],
        value_grad[None],
        out_grad[None],
    )


def solution(mesh):
    in_specs = (
        P("dp", None, None, None),
        P("dp", None),
        P(),
        P("section", None),
        P("section", None, "mp"),
        P("section", None, "mp"),
        P("section", None, "mp"),
        P("section", "mp", None),
    )
    out_specs = (
        P("section", None),
        P("section", ("dp", "mp")),
        P("section", "dp", "mp"),
        P("section", "dp", "mp"),
        P("section", "dp", "mp"),
        P("section", "mp", "dp"),
    )
    return jax.shard_map(local, mesh=mesh, in_specs=in_specs, out_specs=out_specs, check_vma=False)
```

```python
from typing import NamedTuple

import jax
import jax.numpy as jnp
import numpy as np
from jax import lax
from jax.experimental import pallas as pl
from jax.experimental.pallas import tpu as pltpu
from jax.sharding import PartitionSpec as P

HEAD = 128
WIDTHS = 7


EPSILON = 1e-05
SOFTMAX_TEMPER = 0.05
ROPE_BASE = 500000.0
MESH = pl.DeviceIdType.MESH
ROW_TILE = 16
SUB = 4
RELAY, CROSS, TAKE, ATTEND, NEAR, FAR, NEAR_OWN, OWN, FINISH = range(9)
FORWARD_ORDER = (
    (RELAY, 0, 0, 1, 2, 3), (CROSS, 0, 0, 2, 1), (TAKE, 0, 0), (RELAY, 1, 0), (CROSS, 0, 3),
    (TAKE, 0, 2), (RELAY, 1, 1), (TAKE, 0, 1, 3), (RELAY, 1, 2), (ATTEND, 0, 0), (NEAR, 0, 0, 1),
    (RELAY, 1, 3), (NEAR_OWN, 0, 2, 0), (NEAR, 0, 2), (CROSS, 1, 0), (NEAR, 0, 3), (FAR, 0, 0),
    (NEAR_OWN, 0, 1), (FAR, 0, 1), (OWN, 0, 0), (CROSS, 1, 1), (TAKE, 1, 0), (CROSS, 1, 2),
    (FAR, 0, 2, 3), (OWN, 0, 1), (CROSS, 1, 3), (TAKE, 1, 1, 2), (FINISH, 0, 0), (TAKE, 1, 3),
    (ATTEND, 1, 0), (FINISH, 0, 1), (NEAR, 1, 0), (NEAR_OWN, 0, 3), (OWN, 0, 2), (NEAR, 1, 1),
    (FINISH, 0, 2), (NEAR_OWN, 1, 0), (FAR, 1, 0), (OWN, 0, 3), (FINISH, 0, 3), (NEAR, 1, 2, 3),
    (FAR, 1, 1), (NEAR_OWN, 1, 2), (FAR, 1, 2), (NEAR_OWN, 1, 1), (FAR, 1, 3), (OWN, 1, 0),
    (FINISH, 1, 0), (NEAR_OWN, 1, 3), (OWN, 1, 1), (FINISH, 1, 1), (OWN, 1, 2, 3),
    (FINISH, 1, 2, 3),
)
BACKWARD_ORDER = (
    (RELAY, 0, 0, 1, 2, 3), (CROSS, 0, 0, 1), (TAKE, 0, 0), (CROSS, 0, 2), (TAKE, 0, 1),
    (CROSS, 0, 3), (TAKE, 0, 2, 3), (ATTEND, 0, 0), (NEAR, 0, 0), (NEAR_OWN, 0, 0),
    (NEAR, 0, 1, 2), (FAR, 0, 0), (NEAR, 0, 3), (FAR, 0, 1, 2), (NEAR_OWN, 0, 2, 1), (OWN, 0, 0),
    (FAR, 0, 3), (FINISH, 0, 0), (RELAY, 1, 0), (OWN, 0, 2, 1), (RELAY, 1, 1), (FINISH, 0, 1),
    (NEAR_OWN, 0, 3), (RELAY, 1, 2), (FINISH, 0, 2), (OWN, 0, 3), (RELAY, 1, 3), (FINISH, 0, 3),
    (CROSS, 1, 0, 1), (TAKE, 1, 0), (CROSS, 1, 2), (TAKE, 1, 1), (CROSS, 1, 3), (TAKE, 1, 2, 3),
    (ATTEND, 1, 0), (NEAR, 1, 0, 1), (NEAR_OWN, 1, 0), (NEAR, 1, 3), (FAR, 1, 0), (NEAR, 1, 2),
    (FAR, 1, 1), (OWN, 1, 0), (NEAR_OWN, 1, 1), (FAR, 1, 2, 3), (NEAR_OWN, 1, 2), (FINISH, 1, 0),
    (OWN, 1, 1), (NEAR_OWN, 1, 3), (FINISH, 1, 1), (OWN, 1, 2), (FINISH, 1, 2), (OWN, 1, 3),
    (FINISH, 1, 3),
)
F32 = jnp.float32
BF16 = jnp.bfloat16


def contract_rows(left, right):
    return lax.dot_general(
        left, right, (((0,), (0,)), ((), ())), preferred_element_type=jnp.float32
    )


def contract_last(left, right):
    return lax.dot_general(
        left, right, (((left.ndim - 1,), (1,)), ((), ())), preferred_element_type=jnp.float32
    )


def rotary_constants(length):
    half_size = HEAD // 2
    frequencies = ROPE_BASE ** (-np.arange(half_size, dtype=np.float64) * 2.0 / HEAD)
    angles = np.arange(length, dtype=np.float64)[:, None] * frequencies[None, :]
    cosine = np.concatenate([np.cos(angles), np.cos(angles)], axis=1)
    sine = np.concatenate([-np.sin(angles), np.sin(angles)], axis=1)
    return np.stack([cosine, sine]).astype(np.float32)


def mp_place(me, levels):
    bits = [(me // (1 << level)) % 2 for level in range(levels)]
    partners = [me + (1 - 2 * bits[level]) * (1 << level) for level in range(levels)]
    return bits, partners


def rows_at(start, size):
    return pl.ds(pl.multiple_of(start, ROW_TILE), size)


def lanes_at(start, size):
    return pl.ds(pl.multiple_of(start, 128), size)


class Place:
    def __init__(self, direction):
        self.here = lax.axis_index("section")
        self.count = lax.axis_size("section")
        (self.low, self.high), (self.near, self.far) = mp_place(lax.axis_index("mp"), 2)
        self.direction = direction
        if direction > 0:
            self.has_source, self.has_target = self.here > 0, self.here < self.count - 1
        else:
            self.has_source, self.has_target = self.here < self.count - 1, self.here > 0

    def quarter(self, flip_low, flip_high):
        low = 1 - self.low if flip_low else self.low
        high = 1 - self.high if flip_high else self.high
        return (low * 2 + high) * SUB


def send(source, target, sems, slot, **device):
    return pltpu.make_async_remote_copy(
        src_ref=source,
        dst_ref=target,
        send_sem=sems[0].at[slot],
        recv_sem=sems[1].at[slot],
        device_id=device,
        device_id_type=MESH,
    )


class StreamIn:
    def __init__(self, place, group, buf, relay, far, near):
        self.place, self.buf = place, buf
        self.relay, self.far, self.near = relay, far, near
        self.group = group

    def at(self, block):
        return self.buf.at[self.group * 4 * SUB + block]

    def relay_copy(self, step, block):
        slot = self.group * SUB + step
        return send(self.at(block), self.at(block), self.relay, slot, section=self.place.here)

    def near_copy(self, slot, block):
        slot = self.group * 2 * SUB + slot
        return send(self.at(block), self.at(block), self.near, slot, mp=self.place.near)

    def far_copy(self, step, block):
        slot = self.group * SUB + step
        return send(self.at(block), self.at(block), self.far, slot, mp=self.place.far)

    def relay_step(self, step):
        block = self.place.quarter(0, 0) + step
        self.relay_copy(step, block).wait_recv()
        self.far_copy(step, block).start()
        self.near_copy(step, block).start()

    def cross_step(self, step):
        block = self.place.quarter(0, 1) + step
        self.far_copy(step, block).wait_recv()
        self.near_copy(SUB + step, block).start()

    def settle(self, step):
        self.near_copy(step, self.place.quarter(1, 0) + step).wait_recv()
        self.near_copy(SUB + step, self.place.quarter(1, 1) + step).wait_recv()

    def drain(self):
        own, other = self.place.quarter(0, 0), self.place.quarter(0, 1)
        for step in range(SUB):
            self.far_copy(step, own + step).wait_send()
            self.near_copy(step, own + step).wait_send()
            self.near_copy(SUB + step, other + step).wait_send()


class StreamOut:
    def __init__(self, place, group, part, finish, dest, bufs, relay, far, near):
        self.place, self.group = place, group
        self.part_of, self.finish_of, self.dest = part, finish, dest
        self.near_send, self.near_got, self.far_send, self.far_got, self.relay_send, self.keep = (
            bufs
        )
        self.relay_sems, self.far_sems, self.near_sems = relay, far, near

    def near_copy(self, slot):
        slot = self.group * 2 * SUB + slot
        return send(
            self.near_send.at[slot], self.near_got.at[slot], self.near_sems, slot, mp=self.place.near
        )

    def far_copy(self, step):
        slot = self.group * SUB + step
        return send(
            self.far_send.at[slot], self.far_got.at[slot], self.far_sems, slot, mp=self.place.far
        )

    def relay_copy(self, step):
        slot = self.group * SUB + step
        place = self.place
        return send(
            self.relay_send.at[slot],
            self.dest.at[self.group * 4 * SUB + place.quarter(0, 0) + step],
            self.relay_sems,
            slot,
            section=place.here + place.direction,
        )

    def near(self, flip, step):
        place = self.place
        slot = (1 - place.high if flip else place.high) * SUB + step
        value = self.part_of(self.group, place.quarter(1, flip) + step)
        self.near_send[self.group * 2 * SUB + slot] = value.astype(BF16)
        self.near_copy(slot).start()

    def arrived(self, slot):
        self.near_copy(slot).wait_recv()
        return self.near_got[self.group * 2 * SUB + slot].astype(F32)

    def far(self, step):
        place = self.place
        value = self.part_of(self.group, place.quarter(0, 1) + step)
        value = value + self.arrived((1 - place.high) * SUB + step)
        self.far_send[self.group * SUB + step] = value.astype(BF16)
        self.far_copy(step).start()

    def own(self, step):
        place = self.place
        value = self.part_of(self.group, place.quarter(0, 0) + step)
        self.keep[self.group * SUB + step] = value + self.arrived(place.high * SUB + step)

    def finish(self, step):
        slot = self.group * SUB + step
        block = self.place.quarter(0, 0) + step
        self.far_copy(step).wait_recv()
        value = self.keep[slot] + self.far_got[slot].astype(F32)
        self.relay_send[slot] = self.finish_of(self.group, block, value)
        self.relay_copy(step).start()

    def drain(self):
        for step in range(SUB):
            self.far_copy(step).wait_send()
            self.relay_copy(step).wait_send()
        for slot in range(2 * SUB):
            self.near_copy(slot).wait_send()


def run_pass(order, ins, outs, has_source, has_target, consume, attend, prepare, rest):
    def take(group, step):
        @pl.when(has_source)
        def _():
            ins[group].settle(step)

        for quarter in range(4):
            consume(group, quarter * SUB + step)

    def finish(group, step):
        if step == 0:
            prepare(group)
        outs[group].finish(step)

    receive = {
        RELAY: lambda group, step: ins[group].relay_step(step),
        CROSS: lambda group, step: ins[group].cross_step(step),
    }
    produce = {
        NEAR: lambda group, step: outs[group].near(1, step),
        NEAR_OWN: lambda group, step: outs[group].near(0, step),
        FAR: lambda group, step: outs[group].far(step),
        OWN: lambda group, step: outs[group].own(step),
        FINISH: finish,
    }
    for kind, group, *steps in order:
        if kind == ATTEND:
            attend(group)
            if rest is not None:
                pl.when(jnp.logical_not(has_target))(lambda group=group: rest(group))
        elif kind == TAKE:
            for step in steps:
                take(group, step)
        else:
            action = receive.get(kind) or produce[kind]

            @pl.when(has_source if kind in receive else has_target)
            def _(group=group, steps=steps, action=action):
                for step in steps:
                    action(group, step)


def drain_pass(ins, outs, has_source, has_target):
    @pl.when(has_source)
    def _():
        for flow in ins:
            flow.drain()

    @pl.when(has_target)
    def _():
        for flow in outs:
            flow.drain()


def rotary(values, table, sign):
    turned = pltpu.roll(values, HEAD // 2, axis=1)
    return values * table[0] + turned * (table[1] * sign)


def fold_lanes(values):
    total = values[:, :128]
    for lane in range(1, values.shape[1] // 128):
        total = total + values[:, lane * 128 : (lane + 1) * 128]
    return total


def lane_sum(values):
    return jnp.sum(fold_lanes(values), axis=1, keepdims=True)


def matryoshka(queries, passages, target):
    pairs, width_all = queries.shape
    widths = [width_all >> level for level in range(WIDTHS)]
    bounds = [0] + widths[::-1]
    lane = lax.broadcasted_iota(jnp.int32, (pairs, 128), 1)

    def segment_sums(product):
        sums = []
        for low, high in zip(bounds[:-1], bounds[1:]):
            if high <= 128:
                inside = jnp.logical_and(lane >= low, lane < high)
                piece = jnp.where(inside, product[:, :128], 0.0)
            else:
                piece = fold_lanes(product[:, low:high])
            sums.append(jnp.sum(piece, axis=1, keepdims=True))
        for index in range(1, len(sums)):
            sums[index] = sums[index] + sums[index - 1]
        return sums[::-1]

    query_squares = segment_sums(queries * queries)
    passage_squares = segment_sums(passages * passages)
    dots = [segment_sums(queries * passages[j : j + 1]) for j in range(pairs)]
    losses = []
    mixed = [[] for _ in range(pairs)]
    query_own, passage_own = [], []
    for level, width in enumerate(widths):
        query_inv = lax.rsqrt(query_squares[level] * (1.0 / width) + 1e-06)
        passage_inv = lax.rsqrt(passage_squares[level] * (1.0 / width) + 1e-06)
        factors = [
            query_inv * passage_inv[j : j + 1] * (1.0 / (width * SOFTMAX_TEMPER))
            for j in range(pairs)
        ]
        logits = [dots[j][level] * factors[j] for j in range(pairs)]
        highest = logits[0]
        for j in range(1, pairs):
            highest = jnp.maximum(highest, logits[j])
        powers = [jnp.exp(logits[j] - highest) for j in range(pairs)]
        total = powers[0]
        picked = logits[0] * target[:, 0:1]
        for j in range(1, pairs):
            total = total + powers[j]
            picked = picked + logits[j] * target[:, j : j + 1]
        gap = jnp.log(total) + highest - picked
        losses.append(jnp.sum(gap, axis=0, keepdims=True) * (1.0 / pairs))
        slopes = [
            (powers[j] / total - target[:, j : j + 1]) * (1.0 / pairs) for j in range(pairs)
        ]
        pulls = [slopes[j] * logits[j] for j in range(pairs)]
        row_pull = pulls[0]
        for j in range(1, pairs):
            row_pull = row_pull + pulls[j]
        column_pull = jnp.concatenate(
            [jnp.sum(pulls[j], axis=0, keepdims=True) for j in range(pairs)], axis=0
        )
        for j in range(pairs):
            mixed[j].append(slopes[j] * factors[j])
        query_own.append(row_pull * query_inv * query_inv * (-1.0 / width))
        passage_own.append(column_pull * passage_inv * passage_inv * (-1.0 / width))
    for series in mixed + [query_own, passage_own]:
        for level in range(1, WIDTHS):
            series[level] = series[level] + series[level - 1]
    turned = [
        [
            jnp.concatenate([mixed[j][level][p : p + 1] for j in range(pairs)], axis=0)
            for level in range(WIDTHS)
        ]
        for p in range(pairs)
    ]

    def spread(own, own_rows, weights, rows):
        pieces = []
        low = 0
        while low < width_all:
            inside = [k for k in range(WIDTHS) if low < bounds[k + 1] and low + 128 > bounds[k]]
            high = max(low + 128, bounds[inside[-1] + 1])

            def coefficient(series, inside=inside):
                value = series[WIDTHS - 1 - inside[-1]]
                for k in reversed(inside[:-1]):
                    value = jnp.where(lane < bounds[k + 1], series[WIDTHS - 1 - k], value)
                return value

            def columns(values, low=low, high=high):
                return values[:, low:high]

            piece = coefficient(own) * columns(own_rows)
            for j in range(pairs):
                piece = piece + coefficient(weights[j]) * columns(rows[j : j + 1])
            pieces.append(piece)
            low = high
        return jnp.concatenate(pieces, axis=1)

    return (
        losses,
        spread(query_own, queries, mixed, passages),
        spread(passage_own, passages, turned, queries),
    )


class Scratch(NamedTuple):
    head_w: object
    out_w: object
    acc: object
    squares: object
    inv_ref: object
    query_ref: object
    key_ref: object
    value_ref: object
    prob_ref: object
    pooled: object
    slopes: object
    normed_out: object
    outer_out: object
    grad_in: object
    mix_grad: object
    row_dots: object
    gain_part: object
    hidden_sum: object
    pull_ref: object
    keep: object
    keep_b: object
    gain_got: object
    pool_ref: object
    near_send: object
    near_got: object
    far_send: object
    far_got: object
    relay_send: object
    near_send_b: object
    near_got_b: object
    far_send_b: object
    far_got_b: object
    relay_send_b: object
    load_sem: object
    enter_sem: object
    relay_s: object
    relay_r: object
    in_far_s: object
    in_far_r: object
    in_near_s: object
    in_near_r: object
    out_far_s: object
    out_far_r: object
    out_near_s: object
    out_near_r: object
    relay_sb: object
    relay_rb: object
    in_far_sb: object
    in_far_rb: object
    in_near_sb: object
    in_near_rb: object
    out_far_sb: object
    out_far_rb: object
    out_near_sb: object
    out_near_rb: object
    pool_s: object
    pool_r: object
    normed_s: object
    normed_r: object
    mixture_s: object
    mixture_r: object
    outer_s: object
    outer_r: object
    heads_s: object
    heads_r: object
    dots_s: object
    dots_r: object
    gain_s: object
    gain_r: object


def step_kernel(
    lengths,
    positives,
    entrance,
    gain,
    table,
    wq,
    wk,
    wv,
    wo,
    losses_out,
    gain_out,
    normed_all,
    mixture_all,
    outer_all,
    heads_all,
    hidden,
    *scratch,
):
    r = Scratch(*scratch)
    head_w, out_w, acc, squares = r.head_w, r.out_w, r.acc, r.squares
    forth, back = Place(1), Place(-1)
    rows, width = hidden.shape[1:]
    blocks = hidden.shape[0] // 2
    width_all = blocks * width
    pair_count = lengths.shape[0]
    seq_count = 2 * pair_count
    length = rows // pair_count
    query_cols, kv_cols = wq.shape[1], wk.shape[1]
    groups = query_cols // HEAD
    dp_me, mp_me = lax.axis_index("dp"), lax.axis_index("mp")
    dp_count, mp_count = lax.axis_size("dp"), lax.axis_size("mp")
    members = dp_count * mp_count
    me = dp_me * mp_count + mp_me
    share = blocks // dp_count
    row_pad = r.row_dots.shape[2]
    normed_sems, outer_sems = (r.normed_s, r.normed_r), (r.outer_s, r.outer_r)
    mixture_sems, heads_sems = (r.mixture_s, r.mixture_r), (r.heads_s, r.heads_r)
    outer_out = r.outer_out

    def peer(shift):
        spot = lax.rem(me + shift, members)
        return spot // mp_count, lax.rem(spot, mp_count), spot

    def span_of(group):
        return slice(group * rows, (group + 1) * rows)

    def sequences(group):
        for local_seq in range(pair_count):
            inner = slice(local_seq * length, (local_seq + 1) * length)
            outer = slice(group * rows + inner.start, group * rows + inner.stop)
            yield group * pair_count + local_seq, inner, outer

    def count_of(seq):
        return lengths[seq // 2, seq % 2]

    spot = lax.broadcasted_iota(jnp.int32, (length, 1), 0)

    def valid_of(seq):
        return jnp.where(spot < count_of(seq), 1.0, 0.0)

    loads = [
        pltpu.make_async_copy(wq, head_w.at[:, :query_cols], r.load_sem.at[0]),
        pltpu.make_async_copy(wk, head_w.at[:, query_cols : query_cols + kv_cols], r.load_sem.at[1]),
        pltpu.make_async_copy(wv, head_w.at[:, query_cols + kv_cols :], r.load_sem.at[2]),
        pltpu.make_async_copy(wo, out_w, r.load_sem.at[3]),
    ]

    def enter(group, block):
        slot = group * blocks + block
        return pltpu.make_async_copy(
            entrance.at[pl.ds(group * rows, rows), lanes_at(block * width, width)],
            hidden.at[slot],
            r.enter_sem.at[slot],
        )

    @pl.when(jnp.logical_not(forth.has_source))
    def _():
        for group in range(2):
            for block in range(blocks):
                enter(group, block).start()

    for load in loads:
        load.start()
    barrier = pltpu.get_barrier_semaphore()
    for shift in range(1, members):
        to_dp, to_mp, _ = peer(shift)
        pl.semaphore_signal(
            barrier, inc=1, device_id={"dp": to_dp, "mp": to_mp}, device_id_type=MESH
        )

    @pl.when(forth.has_source)
    def _():
        pl.semaphore_signal(
            barrier, inc=1, device_id={"section": forth.here - 1}, device_id_type=MESH
        )

    @pl.when(forth.has_target)
    def _():
        pl.semaphore_signal(
            barrier, inc=1, device_id={"section": forth.here + 1}, device_id_type=MESH
        )

    acc[...] = jnp.zeros_like(acc)
    squares[...] = jnp.zeros_like(squares)
    r.mix_grad[...] = jnp.zeros_like(r.mix_grad)
    r.gain_part[...] = jnp.zeros_like(r.gain_part)

    @pl.when(jnp.logical_not(back.has_source))
    def _():
        def clear(block, carry):
            r.grad_in[block] = jnp.zeros((rows, width), BF16)
            return carry

        lax.fori_loop(0, 2 * blocks, clear, 0)

    pool_shape = r.pool_ref.shape
    column = lax.broadcasted_iota(jnp.int32, pool_shape, 1)
    line = lax.broadcasted_iota(jnp.int32, pool_shape, 0)
    picks = jnp.zeros(pool_shape, F32)
    for seq in range(seq_count):
        inside = jnp.logical_and(column >= seq * length, column < seq * length + count_of(seq))
        picks = jnp.where(jnp.logical_and(line == seq, inside), 1.0, picks)
    r.pool_ref[...] = picks.astype(BF16)
    for load in loads[:3]:
        load.wait()
    expected = (
        members - 1 + forth.has_source.astype(jnp.int32) + forth.has_target.astype(jnp.int32)
    )

    @pl.when(forth.has_source)
    def _():
        pl.semaphore_wait(barrier, expected)

    def gain_at(block):
        return gain[:, lanes_at(block * width, width)]

    def out_columns(block):
        return out_w[:, lanes_at(block * width, width)]

    def consume(group, block):
        slot = group * blocks + block

        @pl.when(jnp.logical_not(forth.has_source))
        def _():
            enter(group, block).wait()

        value = hidden[slot].astype(F32)
        span = span_of(group)
        squares[span, :] += fold_lanes(value * value)
        for seq, inner, _ in sequences(group):
            r.hidden_sum[seq, :, lanes_at(block * width, width)] = jnp.sum(
                value[inner] * valid_of(seq), axis=0, keepdims=True
            )
        acc[span, :] += jnp.dot(
            (value * gain_at(block)).astype(BF16),
            head_w[rows_at(block * width, width), :],
            preferred_element_type=F32,
        )

    mixture = mixture_all.at[dp_me]

    def attend(group):
        whole = span_of(group)
        inv_rms = lax.rsqrt(
            jnp.sum(squares[whole, :], axis=1, keepdims=True) * (1.0 / width_all) + EPSILON
        )
        r.inv_ref[whole, :] = inv_rms
        for seq, inner, span in sequences(group):
            inverse = inv_rms[inner]
            query = jnp.concatenate(
                [
                    rotary(acc[span, g * HEAD : (g + 1) * HEAD] * inverse, table, 1.0)
                    for g in range(groups)
                ],
                axis=0,
            ).astype(BF16)
            key = rotary(acc[span, query_cols : query_cols + kv_cols] * inverse, table, 1.0)
            key = key.astype(BF16)
            value = (acc[span, query_cols + kv_cols :] * inverse).astype(BF16)
            r.query_ref[seq] = query
            r.key_ref[seq] = key
            r.value_ref[seq] = value
            scores = contract_last(query, key) * HEAD ** (-0.5)
            place = lax.broadcasted_iota(jnp.int32, scores.shape, 0) % length
            scores = jnp.where(
                place >= lax.broadcasted_iota(jnp.int32, scores.shape, 1), scores, -1e30
            )
            weights = jnp.exp(scores - jnp.max(scores, axis=1, keepdims=True))
            weights = weights / jnp.sum(weights, axis=1, keepdims=True)
            r.prob_ref[seq] = weights
            mixed = jnp.dot(weights.astype(BF16), value, preferred_element_type=F32).astype(BF16)
            for g in range(groups):
                mixture[span, g * HEAD : (g + 1) * HEAD] = mixed[g * length : (g + 1) * length]
        if group == 0:

            @pl.when(jnp.logical_not(forth.has_source))
            def _():
                pl.semaphore_wait(barrier, expected)

            loads[3].wait()

    def part(group, block):
        return jnp.dot(mixture[span_of(group), :], out_columns(block), preferred_element_type=F32)

    def finish(group, block, total):
        return (hidden[group * blocks + block].astype(F32) + total).astype(BF16)

    ins = [
        StreamIn(
            forth,
            group,
            hidden,
            (r.relay_s, r.relay_r),
            (r.in_far_s, r.in_far_r),
            (r.in_near_s, r.in_near_r),
        )
        for group in range(2)
    ]
    outs = [
        StreamOut(
            forth,
            group,
            part,
            finish,
            hidden,
            (r.near_send, r.near_got, r.far_send, r.far_got, r.relay_send, r.keep),
            (r.relay_s, r.relay_r),
            (r.out_far_s, r.out_far_r),
            (r.out_near_s, r.out_near_r),
        )
        for group in range(2)
    ]
    run_pass(
        FORWARD_ORDER, ins, outs, forth.has_source, forth.has_target, consume, attend, lambda group: None, None
    )

    mixture_sum = jnp.dot(r.pool_ref[...], mixture[...], preferred_element_type=F32)
    coarse = mixture_sum.astype(BF16)
    fine = (mixture_sum - coarse.astype(F32)).astype(BF16)
    both = jnp.concatenate([coarse, fine], axis=0)
    first = (mp_me == 0).astype(F32)
    pooled = r.pooled

    def pool_block(block, carry):
        sums = jnp.dot(both, out_columns(block), preferred_element_type=F32)
        sums = sums[: pool_shape[0]] + sums[pool_shape[0] :]
        lines = [
            (sums[seq : seq + 1] + first * r.hidden_sum[seq, :, lanes_at(block * width, width)])
            / count_of(seq).astype(F32)
            for seq in range(seq_count)
        ]
        pooled[me, :, lanes_at(block * width, width)] = jnp.concatenate(lines, axis=0)
        return carry

    lax.fori_loop(0, blocks, pool_block, 0, unroll=4)

    def pool_copy(shift):
        to_dp, to_mp, _ = peer(shift)
        return pltpu.make_async_remote_copy(
            src_ref=pooled.at[me],
            dst_ref=pooled.at[me],
            send_sem=r.pool_s.at[shift],
            recv_sem=r.pool_r.at[me],
            device_id={"dp": to_dp, "mp": to_mp},
            device_id_type=MESH,
        )

    def pool_arrival(shift):
        from_dp, from_mp, spot = peer(shift)
        return pltpu.make_async_remote_copy(
            src_ref=pooled.at[spot],
            dst_ref=pooled.at[spot],
            send_sem=r.pool_s.at[shift],
            recv_sem=r.pool_r.at[spot],
            device_id={"dp": from_dp, "mp": from_mp},
            device_id_type=MESH,
        )

    for shift in range(1, members):
        pool_copy(shift).start()

    def to_owner(source, target, sems, group, block):
        step = lax.rem(block, share)
        return pltpu.make_async_remote_copy(
            src_ref=source.at[group * blocks + block],
            dst_ref=target.at[dp_me, step, pl.ds(group * rows, rows)],
            send_sem=sems[0].at[group * blocks + block],
            recv_sem=sems[1].at[dp_me, group * share + step],
            device_id={"dp": block // share},
            device_id_type=MESH,
        )

    def from_member(target, sems, member, group, step):
        piece = target.at[member, step, pl.ds(group * rows, rows)]
        return pltpu.make_async_remote_copy(
            src_ref=piece,
            dst_ref=piece,
            send_sem=sems[0].at[0],
            recv_sem=sems[1].at[member, group * share + step],
            device_id={"dp": member},
            device_id_type=MESH,
        )

    def rows_copy(target, sems, shift, group, own):
        other = lax.rem(dp_me + shift, dp_count)
        member = dp_me if own else other
        piece = target.at[member, pl.ds(group * rows, rows)]
        return pltpu.make_async_remote_copy(
            src_ref=piece,
            dst_ref=piece,
            send_sem=sems[0].at[group * dp_count + shift],
            recv_sem=sems[1].at[group * dp_count + member],
            device_id={"dp": other},
            device_id_type=MESH,
        )

    def hand_out(value, spare, target, sems, group, block):
        mine = block // share == dp_me

        @pl.when(mine)
        def _():
            target[dp_me, lax.rem(block, share), span_of(group), :] = value

        @pl.when(jnp.logical_not(mine))
        def _():
            spare[group * blocks + block] = value
            to_owner(spare, target, sems, group, block).start()

    def hand_out_normed():
        for group in range(2):

            def normed_block(block, carry, group=group):
                value = hidden[group * blocks + block].astype(F32) * r.inv_ref[span_of(group), :]
                value = (value * gain_at(block)).astype(BF16)
                hand_out(value, r.normed_out, normed_all, normed_sems, group, block)
                return carry

            lax.fori_loop(0, blocks, normed_block, 0, unroll=2)
            for shift in range(1, dp_count):
                rows_copy(mixture_all, mixture_sems, shift, group, True).start()

    pl.when(back.has_source)(hand_out_normed)
    for shift in range(1, members):
        pool_arrival(shift).wait_recv()
    embedded = []
    for member in range(dp_count):
        total = pooled[member * mp_count]
        for other in range(1, mp_count):
            total = total + pooled[member * mp_count + other]
        embedded.append(total)
    pairs = dp_count * pair_count
    queries = jnp.concatenate(
        [embedded[p // pair_count][2 * (p % pair_count) :][:1] for p in range(pairs)], axis=0
    )
    passages = jnp.concatenate(
        [embedded[p // pair_count][2 * (p % pair_count) + 1 :][:1] for p in range(pairs)], axis=0
    )
    partner = lax.broadcasted_iota(jnp.int32, (pairs, pairs), 1)
    line = lax.broadcasted_iota(jnp.int32, (pairs, pairs), 0)
    target = jnp.zeros((pairs, pairs), F32)
    for p in range(pairs):
        target = jnp.where(jnp.logical_and(line == p, partner == positives[p]), 1.0, target)
    losses, query_slopes, passage_slopes = matryoshka(queries, passages, target)
    lane = lax.broadcasted_iota(jnp.int32, (1, 128), 1)
    packed = jnp.zeros((1, 128), F32)
    for level in range(WIDTHS):
        packed = jnp.where(lane == level, losses[level], packed)
    losses_out[...] = packed[:, :WIDTHS]
    slopes = r.slopes
    for p in range(pairs):
        slopes[2 * p] = query_slopes[p : p + 1]
        slopes[2 * p + 1] = passage_slopes[p : p + 1]

    grad_in, mix_grad = r.grad_in, r.mix_grad

    def upstream(group, block):
        tokens = [
            valid_of(seq)
            / count_of(seq).astype(F32)
            * slopes[dp_me * seq_count + seq, :, lanes_at(block * width, width)]
            for seq, _, _ in sequences(group)
        ]
        tokens = tokens[0] if pair_count == 1 else jnp.concatenate(tokens, axis=0)
        return tokens + grad_in[group * blocks + block].astype(F32)

    def consume_back(group, block):
        outer = upstream(group, block).astype(BF16)
        hand_out(outer, outer_out, outer_all, outer_sems, group, block)
        mix_grad[span_of(group), :] += contract_last(outer, out_columns(block))

    head_grads = heads_all.at[dp_me]
    row_dots = r.row_dots
    diagonal = lax.broadcasted_iota(jnp.int32, (rows, row_pad), 0) == lax.broadcasted_iota(
        jnp.int32, (rows, row_pad), 1
    )

    def dots_copy(shift, group, own):
        other = lax.rem(mp_me + shift, mp_count)
        member = mp_me if own else other
        piece = row_dots.at[group * mp_count + member]
        return pltpu.make_async_remote_copy(
            src_ref=piece,
            dst_ref=piece,
            send_sem=r.dots_s.at[group * mp_count + shift],
            recv_sem=r.dots_r.at[group * mp_count + member],
            device_id={"mp": other},
            device_id_type=MESH,
        )

    def attend_back(group):
        row_dot = []
        for seq, _, span in sequences(group):
            mixed = jnp.concatenate(
                [mix_grad[span, g * HEAD : (g + 1) * HEAD] for g in range(groups)], axis=0
            ).astype(BF16)
            weights = r.prob_ref[seq]
            value_grad = contract_rows(weights.astype(BF16), mixed).astype(BF16)
            pulled = contract_last(mixed, r.value_ref[seq]).astype(BF16).astype(F32)
            score_grad = weights * (pulled - jnp.sum(weights * pulled, axis=1, keepdims=True))
            score_grad = (score_grad * HEAD ** (-0.5)).astype(BF16)
            query_grad = jnp.dot(score_grad, r.key_ref[seq], preferred_element_type=F32)
            query_grad = query_grad.astype(BF16).astype(F32)
            key_grad = contract_rows(score_grad, r.query_ref[seq]).astype(BF16).astype(F32)
            pieces = [
                rotary(query_grad[g * length : (g + 1) * length], table, -1.0).astype(BF16)
                for g in range(groups)
            ]
            pieces = pieces + [rotary(key_grad, table, -1.0).astype(BF16), value_grad]
            joined = jnp.concatenate(pieces, axis=1)
            head_grads[span, :] = joined
            row_dot.append(lane_sum(joined.astype(F32) * acc[span, :]))
        for shift in range(1, dp_count):
            rows_copy(heads_all, heads_sems, shift, group, True).start()
        row_dot = row_dot[0] if pair_count == 1 else jnp.concatenate(row_dot, axis=0)

        @pl.when(back.has_target)
        def _():
            row_dots[group * mp_count + mp_me] = jnp.sum(
                jnp.where(diagonal, row_dot, 0.0), axis=0, keepdims=True
            )
            for shift in range(1, mp_count):
                dots_copy(shift, group, True).start()

    def part_back(group, block):
        span = span_of(group)
        value = contract_last(head_grads[span, :], head_w[rows_at(block * width, width), :])
        scaled = value * (hidden[group * blocks + block].astype(F32) * r.inv_ref[span, :])
        r.gain_part[:, lanes_at(block * width, width)] += jnp.sum(scaled, axis=0, keepdims=True)
        return value

    def prepare(group):
        for shift in range(1, mp_count):
            dots_copy(shift, group, False).wait_recv()
        total = row_dots[group * mp_count]
        for member in range(1, mp_count):
            total = total + row_dots[group * mp_count + member]
        inverse = r.inv_ref[span_of(group), :]
        r.pull_ref[span_of(group), :] = (
            lane_sum(jnp.where(diagonal, total, 0.0))
            * inverse
            * inverse
            * inverse
            * (1.0 / width_all)
        )

    def finish_back(group, block, total):
        span = span_of(group)
        value = upstream(group, block) + total * gain_at(block) * r.inv_ref[span, :]
        pulled = hidden[group * blocks + block].astype(F32) * r.pull_ref[span, :]
        return (value - pulled).astype(BF16)

    def gain_only(group):
        def body(block, carry):
            part_back(group, block)
            return carry

        lax.fori_loop(0, blocks, body, 0, unroll=2)

    ins_back = [
        StreamIn(
            back,
            group,
            grad_in,
            (r.relay_sb, r.relay_rb),
            (r.in_far_sb, r.in_far_rb),
            (r.in_near_sb, r.in_near_rb),
        )
        for group in range(2)
    ]
    outs_back = [
        StreamOut(
            back,
            group,
            part_back,
            finish_back,
            grad_in,
            (r.near_send_b, r.near_got_b, r.far_send_b, r.far_got_b, r.relay_send_b, r.keep_b),
            (r.relay_sb, r.relay_rb),
            (r.out_far_sb, r.out_far_rb),
            (r.out_near_sb, r.out_near_rb),
        )
        for group in range(2)
    ]
    run_pass(
        BACKWARD_ORDER,
        ins_back,
        outs_back,
        back.has_source,
        back.has_target,
        consume_back,
        attend_back,
        prepare,
        gain_only,
    )

    pl.when(jnp.logical_not(back.has_source))(hand_out_normed)

    gain_got = r.gain_got
    gain_cols = gain_got.shape[2]

    def gain_copy(shift):
        to_dp, to_mp, spot = peer(shift)
        return pltpu.make_async_remote_copy(
            src_ref=r.gain_part.at[:, lanes_at(spot * gain_cols, gain_cols)],
            dst_ref=gain_got.at[me],
            send_sem=r.gain_s.at[shift],
            recv_sem=r.gain_r.at[me],
            device_id={"dp": to_dp, "mp": to_mp},
            device_id_type=MESH,
        )

    def gain_arrival(shift):
        from_dp, from_mp, spot = peer(shift)
        return pltpu.make_async_remote_copy(
            src_ref=gain_got.at[spot],
            dst_ref=gain_got.at[spot],
            send_sem=r.gain_s.at[shift],
            recv_sem=r.gain_r.at[spot],
            device_id={"dp": from_dp, "mp": from_mp},
            device_id_type=MESH,
        )

    for shift in range(1, members):
        gain_copy(shift).start()
    drain_pass(ins, outs, forth.has_source, forth.has_target)
    drain_pass(ins_back, outs_back, back.has_source, back.has_target)

    @pl.when(back.has_target)
    def _():
        for group in range(2):
            for shift in range(1, mp_count):
                dots_copy(shift, group, True).wait_send()

    total = r.gain_part[:, lanes_at(me * gain_cols, gain_cols)]
    for shift in range(1, members):
        gain_arrival(shift).wait_recv()
        total = total + gain_got[lax.rem(me + shift, members)]
    gain_out[...] = total

    for shift in range(1, members):
        pool_copy(shift).wait_send()
        gain_copy(shift).wait_send()
    for group in range(2):
        for shift in range(1, dp_count):
            rows_copy(mixture_all, mixture_sems, shift, group, True).wait_send()
            rows_copy(heads_all, heads_sems, shift, group, True).wait_send()
            rows_copy(mixture_all, mixture_sems, shift, group, False).wait_recv()
            rows_copy(heads_all, heads_sems, shift, group, False).wait_recv()

        def drain(block, carry, group=group):
            @pl.when(block // share != dp_me)
            def _():
                to_owner(r.normed_out, normed_all, normed_sems, group, block).wait_send()
                to_owner(outer_out, outer_all, outer_sems, group, block).wait_send()

            return carry

        lax.fori_loop(0, blocks, drain, 0)
        for shift in range(1, dp_count):
            member = lax.rem(dp_me + shift, dp_count)
            for step in range(share):
                from_member(normed_all, normed_sems, member, group, step).wait_recv()
                from_member(outer_all, outer_sems, member, group, step).wait_recv()


def step_pass(lengths, positives, entrance, gain, table, wq, wk, wv, wo):
    rows, width_all = entrance.shape
    dp_count, mp_count = lax.axis_size("dp"), lax.axis_size("mp")
    members = dp_count * mp_count
    blocks = mp_count * SUB
    width = width_all // blocks
    share = blocks // dp_count
    seq_count = 2 * lengths.shape[0]
    length = rows // seq_count
    query_cols = wq.shape[1]
    head_cols = query_cols + wk.shape[1] + wv.shape[1]
    stacked = query_cols // HEAD * length
    row_pad = -(-(rows // 2) // 128) * 128
    pool_rows = -(-seq_count // 16) * 16
    dma = pltpu.SemaphoreType.DMA
    block = (rows // 2, width)
    shapes = dict(
        head_w=((width_all, head_cols), BF16),
        out_w=(wo.shape, BF16),
        acc=((rows, head_cols), F32),
        squares=((rows, 128), F32),
        inv_ref=((rows, 1), F32),
        pull_ref=((rows, 1), F32),
        query_ref=((seq_count, stacked, HEAD), BF16),
        key_ref=((seq_count, length, HEAD), BF16),
        value_ref=((seq_count, length, HEAD), BF16),
        prob_ref=((seq_count, stacked, length), F32),
        pooled=((members, seq_count, width_all), F32),
        hidden_sum=((seq_count, 1, width_all), F32),
        slopes=((dp_count * seq_count, 1, width_all), F32),
        normed_out=((2 * blocks, *block), BF16),
        outer_out=((2 * blocks, *block), BF16),
        grad_in=((2 * blocks, *block), BF16),
        mix_grad=((rows, query_cols), F32),
        row_dots=((2 * mp_count, 1, row_pad), F32),
        gain_part=((1, width_all), F32),
        gain_got=((members, 1, width_all // members), F32),
        pool_ref=((pool_rows, rows), BF16),
        near_send=((4 * SUB, *block), BF16),
        near_got=((4 * SUB, *block), BF16),
        far_send=((2 * SUB, *block), BF16),
        far_got=((2 * SUB, *block), BF16),
        relay_send=((2 * SUB, *block), BF16),
        keep=((2 * SUB, *block), F32),
        near_send_b=((4 * SUB, *block), BF16),
        near_got_b=((4 * SUB, *block), BF16),
        far_send_b=((2 * SUB, *block), BF16),
        far_got_b=((2 * SUB, *block), BF16),
        relay_send_b=((2 * SUB, *block), BF16),
        keep_b=((2 * SUB, *block), F32),
    )
    counts = dict(
        load_sem=(4,),
        enter_sem=(2 * blocks,),
        pool_s=(members,),
        pool_r=(members,),
        normed_s=(2 * blocks,),
        normed_r=(dp_count, 2 * share),
        outer_s=(2 * blocks,),
        outer_r=(dp_count, 2 * share),
        mixture_s=(2 * dp_count,),
        mixture_r=(2 * dp_count,),
        heads_s=(2 * dp_count,),
        heads_r=(2 * dp_count,),
        dots_s=(2 * mp_count,),
        dots_r=(2 * mp_count,),
        gain_s=(members,),
        gain_r=(members,),
        relay_s=(2 * SUB,),
        in_far_s=(2 * SUB,),
        out_far_s=(2 * SUB,),
        in_near_s=(4 * SUB,),
        out_near_s=(4 * SUB,),
        relay_r=(2 * SUB,),
        in_far_r=(2 * SUB,),
        out_far_r=(2 * SUB,),
        in_near_r=(4 * SUB,),
        out_near_r=(4 * SUB,),
        relay_sb=(2 * SUB,),
        in_far_sb=(2 * SUB,),
        out_far_sb=(2 * SUB,),
        in_near_sb=(4 * SUB,),
        out_near_sb=(4 * SUB,),
        relay_rb=(2 * SUB,),
        in_far_rb=(2 * SUB,),
        out_far_rb=(2 * SUB,),
        in_near_rb=(4 * SUB,),
        out_near_rb=(4 * SUB,),
    )
    scratch = Scratch(
        **{name: pltpu.VMEM(*shape) for name, shape in shapes.items()},
        **{name: dma(count) for name, count in counts.items()},
    )
    vmem = pl.BlockSpec(memory_space=pltpu.VMEM)
    smem = pl.BlockSpec(memory_space=pltpu.SMEM)
    hbm = pl.BlockSpec(memory_space=pltpu.HBM)
    return pl.pallas_call(
        step_kernel,
        out_shape=(
            jax.ShapeDtypeStruct((1, WIDTHS), F32),
            jax.ShapeDtypeStruct((1, width_all // members), F32),
            jax.ShapeDtypeStruct((dp_count, share, rows, width), BF16),
            jax.ShapeDtypeStruct((dp_count, rows, query_cols), BF16),
            jax.ShapeDtypeStruct((dp_count, share, rows, width), BF16),
            jax.ShapeDtypeStruct((dp_count, rows, head_cols), BF16),
        ),
        in_specs=[smem, smem, hbm, vmem, vmem, hbm, hbm, hbm, hbm],
        out_specs=(vmem,) * 6,
        scratch_shapes=[pltpu.VMEM((2 * blocks, *block), BF16)] + list(scratch),
        compiler_params=pltpu.CompilerParams(
            collective_id=0, has_side_effects=True, vmem_limit_bytes=56 * 1024 * 1024
        ),
        name="step_pass",
    )(lengths, positives, entrance, gain, table, wq, wk, wv, wo)


def weight_kernel(
    normed, mixture, outer, heads, query_grad, key_grad, value_grad, out_grad, turned
):
    members, rows = heads.shape[:2]
    query_cols, kv_cols = query_grad.shape[1], key_grad.shape[1]

    @pl.when(pl.program_id(0) == 0)
    def _():
        for member in range(members):
            turned[:, member * rows : (member + 1) * rows] = mixture[member].T

    inputs = jnp.concatenate([normed[member, 0] for member in range(members)], axis=0)
    grads = jnp.concatenate([heads[member] for member in range(members)], axis=0)
    product = contract_rows(inputs, grads)
    query_grad[...] = product[:, :query_cols]
    key_grad[...] = product[:, query_cols : query_cols + kv_cols]
    value_grad[...] = product[:, query_cols + kv_cols :]
    grads = jnp.concatenate([outer[member, 0] for member in range(members)], axis=0)
    out_grad[...] = jnp.dot(turned[...], grads, preferred_element_type=F32)


def weight_grads(normed, mixture, outer, heads, query_cols, kv_cols):
    members, share, rows, width = normed.shape
    columns = share * width
    streamed = pl.BlockSpec((members, 1, rows, width), lambda step: (0, step, 0, 0))
    vmem = pl.BlockSpec(memory_space=pltpu.VMEM)

    def tall(cols):
        return pl.BlockSpec((width, cols), lambda step: (step, 0))

    return pl.pallas_call(
        weight_kernel,
        grid=(share,),
        in_specs=[streamed, vmem, streamed, vmem],
        out_specs=(
            tall(query_cols),
            tall(kv_cols),
            tall(kv_cols),
            pl.BlockSpec((query_cols, width), lambda step: (0, step)),
        ),
        out_shape=(
            pltpu.HBM((columns, query_cols), F32),
            pltpu.HBM((columns, kv_cols), F32),
            pltpu.HBM((columns, kv_cols), F32),
            pltpu.HBM((query_cols, columns), F32),
        ),
        scratch_shapes=[pltpu.VMEM((query_cols, members * rows), BF16)],
        compiler_params=pltpu.CompilerParams(dimension_semantics=("arbitrary",)),
        name="weight_grads",
    )(normed, mixture, outer, heads)


def local(entrance, lengths, positives, norm_gains, query_proj, key_proj, value_proj, out_proj):
    length = entrance.shape[2]
    width_all = entrance.shape[3]
    query_cols = query_proj.shape[2]
    kv_cols = key_proj.shape[2]
    losses, gain_share, normed, mixture, outer, heads = step_pass(
        lengths,
        positives,
        entrance.reshape(-1, width_all),
        norm_gains,
        jnp.asarray(rotary_constants(length)),
        query_proj[0],
        key_proj[0],
        value_proj[0],
        out_proj[0],
    )
    query_grad, key_grad, value_grad, out_grad = weight_grads(
        normed, mixture, outer, heads, query_cols, kv_cols
    )
    return (
        losses,
        gain_share,
        query_grad[None],
        key_grad[None],
        value_grad[None],
        out_grad[None],
    )


def solution(mesh):
    in_specs = (
        P("dp", None, None, None),
        P("dp", None),
        P(),
        P("section", None),
        P("section", None, "mp"),
        P("section", None, "mp"),
        P("section", None, "mp"),
        P("section", "mp", None),
    )
    out_specs = (
        P("section", None),
        P("section", ("dp", "mp")),
        P("section", "dp", "mp"),
        P("section", "dp", "mp"),
        P("section", "dp", "mp"),
        P("section", "mp", "dp"),
    )
    return jax.shard_map(local, mesh=mesh, in_specs=in_specs, out_specs=out_specs, check_vma=False)
```

```python
from typing import NamedTuple

import jax
import jax.numpy as jnp
import numpy as np
from jax import lax
from jax.experimental import pallas as pl
from jax.experimental.pallas import tpu as pltpu
from jax.sharding import PartitionSpec as P

HEAD = 128
WIDTHS = 7


EPSILON = 1e-05
SOFTMAX_TEMPER = 0.05
ROPE_BASE = 500000.0
MESH = pl.DeviceIdType.MESH
ROW_TILE = 16
SUB = 4
RELAY, CROSS, TAKE, ATTEND, NEAR, FAR, NEAR_OWN, OWN, FINISH = range(9)
FORWARD_ORDER = (
    (RELAY, 0, 0, 1, 2, 3), (CROSS, 0, 0, 2, 1), (TAKE, 0, 0), (RELAY, 1, 0), (CROSS, 0, 3),
    (TAKE, 0, 2), (RELAY, 1, 1), (TAKE, 0, 1, 3), (RELAY, 1, 2), (ATTEND, 0, 0), (NEAR, 0, 0, 1),
    (RELAY, 1, 3), (NEAR_OWN, 0, 2, 0), (NEAR, 0, 2), (CROSS, 1, 0), (NEAR, 0, 3), (FAR, 0, 0),
    (NEAR_OWN, 0, 1), (FAR, 0, 1), (OWN, 0, 0), (CROSS, 1, 1), (TAKE, 1, 0), (CROSS, 1, 2),
    (FAR, 0, 2, 3), (OWN, 0, 1), (CROSS, 1, 3), (TAKE, 1, 1, 2), (FINISH, 0, 0), (TAKE, 1, 3),
    (ATTEND, 1, 0), (FINISH, 0, 1), (NEAR, 1, 0), (NEAR_OWN, 0, 3), (OWN, 0, 2), (NEAR, 1, 1),
    (FINISH, 0, 2), (NEAR_OWN, 1, 0), (FAR, 1, 0), (OWN, 0, 3), (FINISH, 0, 3), (NEAR, 1, 2, 3),
    (FAR, 1, 1), (NEAR_OWN, 1, 2), (FAR, 1, 2), (NEAR_OWN, 1, 1), (FAR, 1, 3), (OWN, 1, 0),
    (FINISH, 1, 0), (NEAR_OWN, 1, 3), (OWN, 1, 1), (FINISH, 1, 1), (OWN, 1, 2, 3),
    (FINISH, 1, 2, 3),
)
BACKWARD_ORDER = (
    (RELAY, 0, 0, 1, 2, 3), (CROSS, 0, 0, 1), (TAKE, 0, 0), (CROSS, 0, 2), (TAKE, 0, 1),
    (CROSS, 0, 3), (TAKE, 0, 2, 3), (ATTEND, 0, 0), (NEAR, 0, 0), (NEAR_OWN, 0, 0),
    (NEAR, 0, 1, 2), (FAR, 0, 0), (NEAR, 0, 3), (FAR, 0, 1, 2), (NEAR_OWN, 0, 2, 1), (OWN, 0, 0),
    (FAR, 0, 3), (FINISH, 0, 0), (RELAY, 1, 0), (OWN, 0, 2, 1), (RELAY, 1, 1), (FINISH, 0, 1),
    (NEAR_OWN, 0, 3), (RELAY, 1, 2), (FINISH, 0, 2), (OWN, 0, 3), (RELAY, 1, 3), (FINISH, 0, 3),
    (CROSS, 1, 0, 1), (TAKE, 1, 0), (CROSS, 1, 2), (TAKE, 1, 1), (CROSS, 1, 3), (TAKE, 1, 2, 3),
    (ATTEND, 1, 0), (NEAR, 1, 0, 1), (NEAR_OWN, 1, 0), (NEAR, 1, 3), (FAR, 1, 0), (NEAR, 1, 2),
    (FAR, 1, 1), (OWN, 1, 0), (NEAR_OWN, 1, 1), (FAR, 1, 2, 3), (NEAR_OWN, 1, 2), (FINISH, 1, 0),
    (OWN, 1, 1), (NEAR_OWN, 1, 3), (FINISH, 1, 1), (OWN, 1, 2), (FINISH, 1, 2), (OWN, 1, 3),
    (FINISH, 1, 3),
)
F32 = jnp.float32
BF16 = jnp.bfloat16


def contract_rows(left, right):
    return lax.dot_general(
        left, right, (((0,), (0,)), ((), ())), preferred_element_type=jnp.float32
    )


def contract_last(left, right):
    return lax.dot_general(
        left, right, (((left.ndim - 1,), (1,)), ((), ())), preferred_element_type=jnp.float32
    )


def rotary_constants(length):
    half_size = HEAD // 2
    frequencies = ROPE_BASE ** (-np.arange(half_size, dtype=np.float64) * 2.0 / HEAD)
    angles = np.arange(length, dtype=np.float64)[:, None] * frequencies[None, :]
    cosine = np.concatenate([np.cos(angles), np.cos(angles)], axis=1)
    sine = np.concatenate([-np.sin(angles), np.sin(angles)], axis=1)
    return np.stack([cosine, sine]).astype(np.float32)


def mp_place(me, levels):
    bits = [(me // (1 << level)) % 2 for level in range(levels)]
    partners = [me + (1 - 2 * bits[level]) * (1 << level) for level in range(levels)]
    return bits, partners


def rows_at(start, size):
    return pl.ds(pl.multiple_of(start, ROW_TILE), size)


def lanes_at(start, size):
    return pl.ds(pl.multiple_of(start, 128), size)


class Place:
    def __init__(self, direction):
        self.here = lax.axis_index("section")
        self.count = lax.axis_size("section")
        (self.low, self.high), (self.near, self.far) = mp_place(lax.axis_index("mp"), 2)
        self.direction = direction
        if direction > 0:
            self.has_source, self.has_target = self.here > 0, self.here < self.count - 1
        else:
            self.has_source, self.has_target = self.here < self.count - 1, self.here > 0

    def quarter(self, flip_low, flip_high):
        low = 1 - self.low if flip_low else self.low
        high = 1 - self.high if flip_high else self.high
        return (low * 2 + high) * SUB


def send(source, target, sems, slot, **device):
    return pltpu.make_async_remote_copy(
        src_ref=source,
        dst_ref=target,
        send_sem=sems[0].at[slot],
        recv_sem=sems[1].at[slot],
        device_id=device,
        device_id_type=MESH,
    )


class StreamIn:
    def __init__(self, place, group, buf, relay, far, near):
        self.place, self.buf = place, buf
        self.relay, self.far, self.near = relay, far, near
        self.group = group

    def at(self, block):
        return self.buf.at[self.group * 4 * SUB + block]

    def relay_copy(self, step, block):
        slot = self.group * SUB + step
        return send(self.at(block), self.at(block), self.relay, slot, section=self.place.here)

    def near_copy(self, slot, block):
        slot = self.group * 2 * SUB + slot
        return send(self.at(block), self.at(block), self.near, slot, mp=self.place.near)

    def far_copy(self, step, block):
        slot = self.group * SUB + step
        return send(self.at(block), self.at(block), self.far, slot, mp=self.place.far)

    def relay_step(self, step):
        block = self.place.quarter(0, 0) + step
        self.relay_copy(step, block).wait_recv()
        self.far_copy(step, block).start()
        self.near_copy(step, block).start()

    def cross_step(self, step):
        block = self.place.quarter(0, 1) + step
        self.far_copy(step, block).wait_recv()
        self.near_copy(SUB + step, block).start()

    def settle(self, step):
        self.near_copy(step, self.place.quarter(1, 0) + step).wait_recv()
        self.near_copy(SUB + step, self.place.quarter(1, 1) + step).wait_recv()

    def drain(self):
        own, other = self.place.quarter(0, 0), self.place.quarter(0, 1)
        for step in range(SUB):
            self.far_copy(step, own + step).wait_send()
            self.near_copy(step, own + step).wait_send()
            self.near_copy(SUB + step, other + step).wait_send()


class StreamOut:
    def __init__(self, place, group, part, finish, dest, bufs, relay, far, near):
        self.place, self.group = place, group
        self.part_of, self.finish_of, self.dest = part, finish, dest
        self.near_send, self.near_got, self.far_send, self.far_got, self.relay_send, self.keep = (
            bufs
        )
        self.relay_sems, self.far_sems, self.near_sems = relay, far, near

    def near_copy(self, slot):
        slot = self.group * 2 * SUB + slot
        return send(
            self.near_send.at[slot], self.near_got.at[slot], self.near_sems, slot, mp=self.place.near
        )

    def far_copy(self, step):
        slot = self.group * SUB + step
        return send(
            self.far_send.at[slot], self.far_got.at[slot], self.far_sems, slot, mp=self.place.far
        )

    def relay_copy(self, step):
        slot = self.group * SUB + step
        place = self.place
        return send(
            self.relay_send.at[slot],
            self.dest.at[self.group * 4 * SUB + place.quarter(0, 0) + step],
            self.relay_sems,
            slot,
            section=place.here + place.direction,
        )

    def near(self, flip, step):
        place = self.place
        slot = (1 - place.high if flip else place.high) * SUB + step
        value = self.part_of(self.group, place.quarter(1, flip) + step)
        self.near_send[self.group * 2 * SUB + slot] = value.astype(BF16)
        self.near_copy(slot).start()

    def arrived(self, slot):
        self.near_copy(slot).wait_recv()
        return self.near_got[self.group * 2 * SUB + slot].astype(F32)

    def far(self, step):
        place = self.place
        value = self.part_of(self.group, place.quarter(0, 1) + step)
        value = value + self.arrived((1 - place.high) * SUB + step)
        self.far_send[self.group * SUB + step] = value.astype(BF16)
        self.far_copy(step).start()

    def own(self, step):
        place = self.place
        value = self.part_of(self.group, place.quarter(0, 0) + step)
        self.keep[self.group * SUB + step] = value + self.arrived(place.high * SUB + step)

    def finish(self, step):
        slot = self.group * SUB + step
        block = self.place.quarter(0, 0) + step
        self.far_copy(step).wait_recv()
        value = self.keep[slot] + self.far_got[slot].astype(F32)
        self.relay_send[slot] = self.finish_of(self.group, block, value)
        self.relay_copy(step).start()

    def drain(self):
        for step in range(SUB):
            self.far_copy(step).wait_send()
            self.relay_copy(step).wait_send()
        for slot in range(2 * SUB):
            self.near_copy(slot).wait_send()


def run_pass(order, ins, outs, has_source, has_target, consume, attend, prepare, rest):
    def take(group, step):
        @pl.when(has_source)
        def _():
            ins[group].settle(step)

        for quarter in range(4):
            consume(group, quarter * SUB + step)

    def finish(group, step):
        if step == 0:
            prepare(group)
        outs[group].finish(step)

    receive = {
        RELAY: lambda group, step: ins[group].relay_step(step),
        CROSS: lambda group, step: ins[group].cross_step(step),
    }
    produce = {
        NEAR: lambda group, step: outs[group].near(1, step),
        NEAR_OWN: lambda group, step: outs[group].near(0, step),
        FAR: lambda group, step: outs[group].far(step),
        OWN: lambda group, step: outs[group].own(step),
        FINISH: finish,
    }
    for kind, group, *steps in order:
        if kind == ATTEND:
            attend(group)
            if rest is not None:
                pl.when(jnp.logical_not(has_target))(lambda group=group: rest(group))
        elif kind == TAKE:
            for step in steps:
                take(group, step)
        else:
            action = receive.get(kind) or produce[kind]

            @pl.when(has_source if kind in receive else has_target)
            def _(group=group, steps=steps, action=action):
                for step in steps:
                    action(group, step)


def drain_pass(ins, outs, has_source, has_target):
    @pl.when(has_source)
    def _():
        for flow in ins:
            flow.drain()

    @pl.when(has_target)
    def _():
        for flow in outs:
            flow.drain()


def rotary(values, table, sign):
    turned = pltpu.roll(values, HEAD // 2, axis=1)
    return values * table[0] + turned * (table[1] * sign)


def fold_lanes(values):
    total = values[:, :128]
    for lane in range(1, values.shape[1] // 128):
        total = total + values[:, lane * 128 : (lane + 1) * 128]
    return total


def lane_sum(values):
    return jnp.sum(fold_lanes(values), axis=1, keepdims=True)


def matryoshka(queries, passages, target):
    pairs, width_all = queries.shape
    widths = [width_all >> level for level in range(WIDTHS)]
    bounds = [0] + widths[::-1]
    lane = lax.broadcasted_iota(jnp.int32, (pairs, 128), 1)

    def segment_sums(product):
        sums = []
        for low, high in zip(bounds[:-1], bounds[1:]):
            if high <= 128:
                inside = jnp.logical_and(lane >= low, lane < high)
                piece = jnp.where(inside, product[:, :128], 0.0)
            else:
                piece = fold_lanes(product[:, low:high])
            sums.append(jnp.sum(piece, axis=1, keepdims=True))
        for index in range(1, len(sums)):
            sums[index] = sums[index] + sums[index - 1]
        return sums[::-1]

    query_squares = segment_sums(queries * queries)
    passage_squares = segment_sums(passages * passages)
    dots = [segment_sums(queries * passages[j : j + 1]) for j in range(pairs)]
    losses = []
    mixed = [[] for _ in range(pairs)]
    query_own, passage_own = [], []
    for level, width in enumerate(widths):
        query_inv = lax.rsqrt(query_squares[level] * (1.0 / width) + 1e-06)
        passage_inv = lax.rsqrt(passage_squares[level] * (1.0 / width) + 1e-06)
        factors = [
            query_inv * passage_inv[j : j + 1] * (1.0 / (width * SOFTMAX_TEMPER))
            for j in range(pairs)
        ]
        logits = [dots[j][level] * factors[j] for j in range(pairs)]
        highest = logits[0]
        for j in range(1, pairs):
            highest = jnp.maximum(highest, logits[j])
        powers = [jnp.exp(logits[j] - highest) for j in range(pairs)]
        total = powers[0]
        picked = logits[0] * target[:, 0:1]
        for j in range(1, pairs):
            total = total + powers[j]
            picked = picked + logits[j] * target[:, j : j + 1]
        gap = jnp.log(total) + highest - picked
        losses.append(jnp.sum(gap, axis=0, keepdims=True) * (1.0 / pairs))
        slopes = [
            (powers[j] / total - target[:, j : j + 1]) * (1.0 / pairs) for j in range(pairs)
        ]
        pulls = [slopes[j] * logits[j] for j in range(pairs)]
        row_pull = pulls[0]
        for j in range(1, pairs):
            row_pull = row_pull + pulls[j]
        column_pull = jnp.concatenate(
            [jnp.sum(pulls[j], axis=0, keepdims=True) for j in range(pairs)], axis=0
        )
        for j in range(pairs):
            mixed[j].append(slopes[j] * factors[j])
        query_own.append(row_pull * query_inv * query_inv * (-1.0 / width))
        passage_own.append(column_pull * passage_inv * passage_inv * (-1.0 / width))
    for series in mixed + [query_own, passage_own]:
        for level in range(1, WIDTHS):
            series[level] = series[level] + series[level - 1]
    turned = [
        [
            jnp.concatenate([mixed[j][level][p : p + 1] for j in range(pairs)], axis=0)
            for level in range(WIDTHS)
        ]
        for p in range(pairs)
    ]

    def spread(own, own_rows, weights, rows):
        pieces = []
        low = 0
        while low < width_all:
            inside = [k for k in range(WIDTHS) if low < bounds[k + 1] and low + 128 > bounds[k]]
            high = max(low + 128, bounds[inside[-1] + 1])

            def coefficient(series, inside=inside):
                value = series[WIDTHS - 1 - inside[-1]]
                for k in reversed(inside[:-1]):
                    value = jnp.where(lane < bounds[k + 1], series[WIDTHS - 1 - k], value)
                return value

            def columns(values, low=low, high=high):
                return values[:, low:high]

            piece = coefficient(own) * columns(own_rows)
            for j in range(pairs):
                piece = piece + coefficient(weights[j]) * columns(rows[j : j + 1])
            pieces.append(piece)
            low = high
        return jnp.concatenate(pieces, axis=1)

    return (
        losses,
        spread(query_own, queries, mixed, passages),
        spread(passage_own, passages, turned, queries),
    )


class Scratch(NamedTuple):
    head_w: object
    out_w: object
    acc: object
    squares: object
    inv_ref: object
    query_ref: object
    key_ref: object
    value_ref: object
    prob_ref: object
    pooled: object
    slopes: object
    normed_out: object
    outer_out: object
    grad_in: object
    mix_grad: object
    row_dots: object
    gain_part: object
    hidden_sum: object
    pull_ref: object
    keep: object
    keep_b: object
    gain_got: object
    pool_ref: object
    near_send: object
    near_got: object
    far_send: object
    far_got: object
    relay_send: object
    near_send_b: object
    near_got_b: object
    far_send_b: object
    far_got_b: object
    relay_send_b: object
    load_sem: object
    enter_sem: object
    relay_s: object
    relay_r: object
    in_far_s: object
    in_far_r: object
    in_near_s: object
    in_near_r: object
    out_far_s: object
    out_far_r: object
    out_near_s: object
    out_near_r: object
    relay_sb: object
    relay_rb: object
    in_far_sb: object
    in_far_rb: object
    in_near_sb: object
    in_near_rb: object
    out_far_sb: object
    out_far_rb: object
    out_near_sb: object
    out_near_rb: object
    pool_s: object
    pool_r: object
    normed_s: object
    normed_r: object
    mixture_s: object
    mixture_r: object
    outer_s: object
    outer_r: object
    heads_s: object
    heads_r: object
    dots_s: object
    dots_r: object
    pass_s: object
    pass_r: object
    gain_s: object
    gain_r: object


def step_kernel(
    lengths,
    positives,
    entrance,
    gain,
    table,
    wq,
    wk,
    wv,
    wo,
    losses_out,
    gain_out,
    normed_all,
    mixture_all,
    outer_all,
    heads_all,
    hidden,
    *scratch,
):
    r = Scratch(*scratch)
    head_w, out_w, acc, squares = r.head_w, r.out_w, r.acc, r.squares
    forth, back = Place(1), Place(-1)
    rows, width = hidden.shape[1:]
    blocks = hidden.shape[0] // 2
    width_all = blocks * width
    pair_count = lengths.shape[0]
    seq_count = 2 * pair_count
    length = rows // pair_count
    query_cols, kv_cols = wq.shape[1], wk.shape[1]
    groups = query_cols // HEAD
    dp_me, mp_me = lax.axis_index("dp"), lax.axis_index("mp")
    dp_count, mp_count = lax.axis_size("dp"), lax.axis_size("mp")
    members = dp_count * mp_count
    me = dp_me * mp_count + mp_me
    share = blocks // dp_count
    row_pad = r.row_dots.shape[2]
    normed_sems, outer_sems = (r.normed_s, r.normed_r), (r.outer_s, r.outer_r)
    mixture_sems, heads_sems = (r.mixture_s, r.mixture_r), (r.heads_s, r.heads_r)
    outer_out = r.outer_out

    def peer(shift):
        spot = lax.rem(me + shift, members)
        return spot // mp_count, lax.rem(spot, mp_count), spot

    def span_of(group):
        return slice(group * rows, (group + 1) * rows)

    def member_rows(member, group):
        return rows_at((member * 2 + group) * rows, rows)

    def sequences(group):
        for local_seq in range(pair_count):
            inner = slice(local_seq * length, (local_seq + 1) * length)
            outer = slice(group * rows + inner.start, group * rows + inner.stop)
            yield group * pair_count + local_seq, inner, outer

    def count_of(seq):
        return lengths[seq // 2, seq % 2]

    spot = lax.broadcasted_iota(jnp.int32, (length, 1), 0)

    def valid_of(seq):
        return jnp.where(spot < count_of(seq), 1.0, 0.0)

    loads = [
        pltpu.make_async_copy(wq, head_w.at[:, :query_cols], r.load_sem.at[0]),
        pltpu.make_async_copy(wk, head_w.at[:, query_cols : query_cols + kv_cols], r.load_sem.at[1]),
        pltpu.make_async_copy(wv, head_w.at[:, query_cols + kv_cols :], r.load_sem.at[2]),
        pltpu.make_async_copy(wo, out_w, r.load_sem.at[3]),
    ]

    def enter(group, block):
        slot = group * blocks + block
        return pltpu.make_async_copy(
            entrance.at[pl.ds(group * rows, rows), lanes_at(block * width, width)],
            hidden.at[slot],
            r.enter_sem.at[slot],
        )

    @pl.when(jnp.logical_not(forth.has_source))
    def _():
        for group in range(2):
            for block in range(blocks):
                enter(group, block).start()

    for load in loads:
        load.start()
    barrier = pltpu.get_barrier_semaphore()
    for shift in range(1, members):
        to_dp, to_mp, _ = peer(shift)
        pl.semaphore_signal(
            barrier, inc=1, device_id={"dp": to_dp, "mp": to_mp}, device_id_type=MESH
        )

    @pl.when(forth.has_source)
    def _():
        pl.semaphore_signal(
            barrier, inc=1, device_id={"section": forth.here - 1}, device_id_type=MESH
        )

    @pl.when(forth.has_target)
    def _():
        pl.semaphore_signal(
            barrier, inc=1, device_id={"section": forth.here + 1}, device_id_type=MESH
        )

    acc[...] = jnp.zeros_like(acc)
    squares[...] = jnp.zeros_like(squares)
    r.mix_grad[...] = jnp.zeros_like(r.mix_grad)
    r.gain_part[...] = jnp.zeros_like(r.gain_part)

    @pl.when(jnp.logical_not(back.has_source))
    def _():
        def clear(block, carry):
            r.grad_in[block] = jnp.zeros((rows, width), BF16)
            return carry

        lax.fori_loop(0, 2 * blocks, clear, 0)

    pool_shape = r.pool_ref.shape
    column = lax.broadcasted_iota(jnp.int32, pool_shape, 1)
    line = lax.broadcasted_iota(jnp.int32, pool_shape, 0)
    picks = jnp.zeros(pool_shape, F32)
    for seq in range(seq_count):
        inside = jnp.logical_and(column >= seq * length, column < seq * length + count_of(seq))
        picks = jnp.where(jnp.logical_and(line == seq % pair_count, inside), 1.0, picks)
    r.pool_ref[...] = picks.astype(BF16)
    for load in loads[:3]:
        load.wait()
    expected = (
        members - 1 + forth.has_source.astype(jnp.int32) + forth.has_target.astype(jnp.int32)
    )

    @pl.when(forth.has_source)
    def _():
        pl.semaphore_wait(barrier, expected)

    def gain_at(block):
        return gain[:, lanes_at(block * width, width)]

    def out_columns(block):
        return out_w[:, lanes_at(block * width, width)]

    def consume(group, block):
        slot = group * blocks + block

        @pl.when(jnp.logical_not(forth.has_source))
        def _():
            enter(group, block).wait()

        value = hidden[slot].astype(F32)
        span = span_of(group)
        squares[span, :] += fold_lanes(value * value)
        for seq, inner, _ in sequences(group):
            r.hidden_sum[seq, :, lanes_at(block * width, width)] = jnp.sum(
                value[inner] * valid_of(seq), axis=0, keepdims=True
            )
        acc[span, :] += jnp.dot(
            (value * gain_at(block)).astype(BF16),
            head_w[rows_at(block * width, width), :],
            preferred_element_type=F32,
        )

    mixture = mixture_all.at[pl.ds(pl.multiple_of(dp_me * 2 * rows, ROW_TILE), 2 * rows)]

    def attend(group):
        whole = span_of(group)
        inv_rms = lax.rsqrt(
            jnp.sum(squares[whole, :], axis=1, keepdims=True) * (1.0 / width_all) + EPSILON
        )
        r.inv_ref[whole, :] = inv_rms
        for seq, inner, span in sequences(group):
            inverse = inv_rms[inner]
            query = jnp.concatenate(
                [
                    rotary(acc[span, g * HEAD : (g + 1) * HEAD] * inverse, table, 1.0)
                    for g in range(groups)
                ],
                axis=0,
            ).astype(BF16)
            key = rotary(acc[span, query_cols : query_cols + kv_cols] * inverse, table, 1.0)
            key = key.astype(BF16)
            value = (acc[span, query_cols + kv_cols :] * inverse).astype(BF16)
            r.query_ref[seq] = query
            r.key_ref[seq] = key
            r.value_ref[seq] = value
            scores = contract_last(query, key) * HEAD ** (-0.5)
            place = lax.broadcasted_iota(jnp.int32, scores.shape, 0) % length
            scores = jnp.where(
                place >= lax.broadcasted_iota(jnp.int32, scores.shape, 1), scores, -1e30
            )
            weights = jnp.exp(scores - jnp.max(scores, axis=1, keepdims=True))
            weights = weights / jnp.sum(weights, axis=1, keepdims=True)
            r.prob_ref[seq] = weights
            mixed = jnp.dot(weights.astype(BF16), value, preferred_element_type=F32).astype(BF16)
            for g in range(groups):
                mixture[span, g * HEAD : (g + 1) * HEAD] = mixed[g * length : (g + 1) * length]
        if group == 0:

            @pl.when(jnp.logical_not(forth.has_source))
            def _():
                pl.semaphore_wait(barrier, expected)

            loads[3].wait()

    first = (mp_me == 0).astype(F32)
    pooled = r.pooled

    def pool_copy(group, shift, own):
        other_dp, other_mp, spot = peer(shift)
        member = group * members + (me if own else spot)
        return pltpu.make_async_remote_copy(
            src_ref=pooled.at[member],
            dst_ref=pooled.at[member],
            send_sem=r.pool_s.at[group * members + shift],
            recv_sem=r.pool_r.at[member],
            device_id={"dp": other_dp, "mp": other_mp},
            device_id_type=MESH,
        )

    def send_pooled(group):
        span = span_of(group)
        mixture_sum = jnp.dot(r.pool_ref[:, span], mixture[span, :], preferred_element_type=F32)
        coarse = mixture_sum.astype(BF16)
        fine = (mixture_sum - coarse.astype(F32)).astype(BF16)
        both = jnp.concatenate([coarse, fine], axis=0)

        def pool_block(block, carry):
            sums = jnp.dot(both, out_columns(block), preferred_element_type=F32)
            sums = sums[: pool_shape[0]] + sums[pool_shape[0] :]
            lines = [
                (sums[line : line + 1] + first * r.hidden_sum[seq, :, lanes_at(block * width, width)])
                / count_of(seq).astype(F32)
                for line, (seq, _, _) in enumerate(sequences(group))
            ]
            lines = lines[0] if pair_count == 1 else jnp.concatenate(lines, axis=0)
            pooled[group * members + me, :, lanes_at(block * width, width)] = lines
            return carry

        lax.fori_loop(0, blocks, pool_block, 0, unroll=4)
        for shift in range(1, members):
            pool_copy(group, shift, True).start()

    def part(group, block):
        return jnp.dot(mixture[span_of(group), :], out_columns(block), preferred_element_type=F32)

    def finish(group, block, total):
        return (hidden[group * blocks + block].astype(F32) + total).astype(BF16)

    ins = [
        StreamIn(
            forth,
            group,
            hidden,
            (r.relay_s, r.relay_r),
            (r.in_far_s, r.in_far_r),
            (r.in_near_s, r.in_near_r),
        )
        for group in range(2)
    ]
    outs = [
        StreamOut(
            forth,
            group,
            part,
            finish,
            hidden,
            (r.near_send, r.near_got, r.far_send, r.far_got, r.relay_send, r.keep),
            (r.relay_s, r.relay_r),
            (r.out_far_s, r.out_far_r),
            (r.out_near_s, r.out_near_r),
        )
        for group in range(2)
    ]
    run_pass(
        FORWARD_ORDER, ins, outs, forth.has_source, forth.has_target, consume, attend, lambda group: None, send_pooled
    )

    @pl.when(forth.has_target)
    def _():
        for group in range(2):
            send_pooled(group)

    def to_owner(source, target, sems, group, block):
        step = lax.rem(block, share)
        return pltpu.make_async_remote_copy(
            src_ref=source.at[group * blocks + block],
            dst_ref=target.at[step, member_rows(dp_me, group)],
            send_sem=sems[0].at[group * blocks + block],
            recv_sem=sems[1].at[dp_me, group * share + step],
            device_id={"dp": block // share},
            device_id_type=MESH,
        )

    def from_member(target, sems, member, group, step):
        piece = target.at[step, member_rows(member, group)]
        return pltpu.make_async_remote_copy(
            src_ref=piece,
            dst_ref=piece,
            send_sem=sems[0].at[0],
            recv_sem=sems[1].at[member, group * share + step],
            device_id={"dp": member},
            device_id_type=MESH,
        )

    def rows_copy(target, sems, shift, group, own):
        other = lax.rem(dp_me + shift, dp_count)
        member = dp_me if own else other
        piece = target.at[member_rows(member, group)]
        return pltpu.make_async_remote_copy(
            src_ref=piece,
            dst_ref=piece,
            send_sem=sems[0].at[group * dp_count + shift],
            recv_sem=sems[1].at[group * dp_count + member],
            device_id={"dp": other},
            device_id_type=MESH,
        )

    def hand_out(value, spare, target, sems, group, block, passes=None):
        mine = block // share == dp_me

        @pl.when(mine)
        def _():
            target[lax.rem(block, share), member_rows(dp_me, group), :] = value

        sends = jnp.logical_not(mine)
        if passes is not None:
            sends = jnp.logical_and(sends, passes)

        @pl.when(sends)
        def _():
            spare[group * blocks + block] = value
            to_owner(spare, target, sems, group, block).start()

    def hand_out_normed():
        for group in range(2):

            def normed_block(block, carry, group=group):
                value = hidden[group * blocks + block].astype(F32) * r.inv_ref[span_of(group), :]
                value = (value * gain_at(block)).astype(BF16)
                hand_out(value, r.normed_out, normed_all, normed_sems, group, block)
                return carry

            lax.fori_loop(0, blocks, normed_block, 0, unroll=2)
            for shift in range(1, dp_count):
                rows_copy(mixture_all, mixture_sems, shift, group, True).start()

    pl.when(back.has_source)(hand_out_normed)
    for group in range(2):
        for shift in range(1, members):
            pool_copy(group, shift, False).wait_recv()
    embedded = []
    for group in range(2):
        for member in range(dp_count):
            start = group * members + member * mp_count
            total = pooled[start]
            for other in range(1, mp_count):
                total = total + pooled[start + other]
            embedded.append(total)
    pairs = dp_count * pair_count

    def embedding(seq):
        member, inner = seq // seq_count, seq % seq_count
        block = embedded[inner // pair_count * dp_count + member]
        return block[inner % pair_count :][:1]

    queries = jnp.concatenate([embedding(2 * p) for p in range(pairs)], axis=0)
    passages = jnp.concatenate([embedding(2 * p + 1) for p in range(pairs)], axis=0)
    partner = lax.broadcasted_iota(jnp.int32, (pairs, pairs), 1)
    line = lax.broadcasted_iota(jnp.int32, (pairs, pairs), 0)
    target = jnp.zeros((pairs, pairs), F32)
    for p in range(pairs):
        target = jnp.where(jnp.logical_and(line == p, partner == positives[p]), 1.0, target)
    losses, query_slopes, passage_slopes = matryoshka(queries, passages, target)
    lane = lax.broadcasted_iota(jnp.int32, (1, 128), 1)
    packed = jnp.zeros((1, 128), F32)
    for level in range(WIDTHS):
        packed = jnp.where(lane == level, losses[level], packed)
    losses_out[...] = packed[:, :WIDTHS]
    slopes = r.slopes
    for p in range(pairs):
        slopes[2 * p] = query_slopes[p : p + 1]
        slopes[2 * p + 1] = passage_slopes[p : p + 1]

    grad_in, mix_grad = r.grad_in, r.mix_grad

    def upstream(group, block):
        tokens = [
            valid_of(seq)
            / count_of(seq).astype(F32)
            * slopes[dp_me * seq_count + seq, :, lanes_at(block * width, width)]
            for seq, _, _ in sequences(group)
        ]
        tokens = tokens[0] if pair_count == 1 else jnp.concatenate(tokens, axis=0)
        return tokens + grad_in[group * blocks + block].astype(F32)

    def consume_back(group, block):
        outer = upstream(group, block).astype(BF16)
        passes = lax.rem(block, 2) == forth.low
        hand_out(outer, outer_out, outer_all, outer_sems, group, block, passes)
        mix_grad[span_of(group), :] += contract_last(outer, out_columns(block))

    head_grads = heads_all.at[pl.ds(pl.multiple_of(dp_me * 2 * rows, ROW_TILE), 2 * rows)]
    row_dots = r.row_dots
    diagonal = lax.broadcasted_iota(jnp.int32, (rows, row_pad), 0) == lax.broadcasted_iota(
        jnp.int32, (rows, row_pad), 1
    )

    def dots_copy(shift, group, own):
        other = lax.rem(mp_me + shift, mp_count)
        member = mp_me if own else other
        piece = row_dots.at[group * mp_count + member]
        return pltpu.make_async_remote_copy(
            src_ref=piece,
            dst_ref=piece,
            send_sem=r.dots_s.at[group * mp_count + shift],
            recv_sem=r.dots_r.at[group * mp_count + member],
            device_id={"mp": other},
            device_id_type=MESH,
        )

    def attend_back(group):
        row_dot = []
        for seq, _, span in sequences(group):
            mixed = jnp.concatenate(
                [mix_grad[span, g * HEAD : (g + 1) * HEAD] for g in range(groups)], axis=0
            ).astype(BF16)
            weights = r.prob_ref[seq]
            value_grad = contract_rows(weights.astype(BF16), mixed).astype(BF16)
            pulled = contract_last(mixed, r.value_ref[seq]).astype(BF16).astype(F32)
            score_grad = weights * (pulled - jnp.sum(weights * pulled, axis=1, keepdims=True))
            score_grad = (score_grad * HEAD ** (-0.5)).astype(BF16)
            query_grad = jnp.dot(score_grad, r.key_ref[seq], preferred_element_type=F32)
            query_grad = query_grad.astype(BF16).astype(F32)
            key_grad = contract_rows(score_grad, r.query_ref[seq]).astype(BF16).astype(F32)
            pieces = [
                rotary(query_grad[g * length : (g + 1) * length], table, -1.0).astype(BF16)
                for g in range(groups)
            ]
            pieces = pieces + [rotary(key_grad, table, -1.0).astype(BF16), value_grad]
            joined = jnp.concatenate(pieces, axis=1)
            head_grads[span, :] = joined
            row_dot.append(lane_sum(joined.astype(F32) * acc[span, :]))
        for shift in range(1, dp_count):
            rows_copy(heads_all, heads_sems, shift, group, True).start()
        row_dot = row_dot[0] if pair_count == 1 else jnp.concatenate(row_dot, axis=0)

        @pl.when(back.has_target)
        def _():
            row_dots[group * mp_count + mp_me] = jnp.sum(
                jnp.where(diagonal, row_dot, 0.0), axis=0, keepdims=True
            )
            for shift in range(1, mp_count):
                dots_copy(shift, group, True).start()

    def part_back(group, block):
        span = span_of(group)
        value = contract_last(head_grads[span, :], head_w[rows_at(block * width, width), :])
        scaled = value * (hidden[group * blocks + block].astype(F32) * r.inv_ref[span, :])
        r.gain_part[:, lanes_at(block * width, width)] += jnp.sum(scaled, axis=0, keepdims=True)
        return value

    def prepare(group):
        for shift in range(1, mp_count):
            dots_copy(shift, group, False).wait_recv()
        total = row_dots[group * mp_count]
        for member in range(1, mp_count):
            total = total + row_dots[group * mp_count + member]
        inverse = r.inv_ref[span_of(group), :]
        r.pull_ref[span_of(group), :] = (
            lane_sum(jnp.where(diagonal, total, 0.0))
            * inverse
            * inverse
            * inverse
            * (1.0 / width_all)
        )

    def finish_back(group, block, total):
        span = span_of(group)
        value = upstream(group, block) + total * gain_at(block) * r.inv_ref[span, :]
        pulled = hidden[group * blocks + block].astype(F32) * r.pull_ref[span, :]
        return (value - pulled).astype(BF16)

    def gain_only(group):
        def body(block, carry):
            part_back(group, block)
            return carry

        lax.fori_loop(0, blocks, body, 0, unroll=2)

    ins_back = [
        StreamIn(
            back,
            group,
            grad_in,
            (r.relay_sb, r.relay_rb),
            (r.in_far_sb, r.in_far_rb),
            (r.in_near_sb, r.in_near_rb),
        )
        for group in range(2)
    ]
    outs_back = [
        StreamOut(
            back,
            group,
            part_back,
            finish_back,
            grad_in,
            (r.near_send_b, r.near_got_b, r.far_send_b, r.far_got_b, r.relay_send_b, r.keep_b),
            (r.relay_sb, r.relay_rb),
            (r.out_far_sb, r.out_far_rb),
            (r.out_near_sb, r.out_near_rb),
        )
        for group in range(2)
    ]
    run_pass(
        BACKWARD_ORDER,
        ins_back,
        outs_back,
        back.has_source,
        back.has_target,
        consume_back,
        attend_back,
        prepare,
        gain_only,
    )

    pl.when(jnp.logical_not(back.has_source))(hand_out_normed)

    def pass_on(member, group, step):
        piece = outer_all.at[step, member_rows(member, group)]
        return pltpu.make_async_remote_copy(
            src_ref=piece,
            dst_ref=piece,
            send_sem=r.pass_s.at[member, group * share + step],
            recv_sem=r.pass_r.at[member, group * share + step],
            device_id={"mp": forth.near},
            device_id_type=MESH,
        )

    gain_got = r.gain_got
    gain_cols = gain_got.shape[2]

    def gain_copy(shift):
        to_dp, to_mp, spot = peer(shift)
        return pltpu.make_async_remote_copy(
            src_ref=r.gain_part.at[:, lanes_at(spot * gain_cols, gain_cols)],
            dst_ref=gain_got.at[me],
            send_sem=r.gain_s.at[shift],
            recv_sem=r.gain_r.at[me],
            device_id={"dp": to_dp, "mp": to_mp},
            device_id_type=MESH,
        )

    def gain_arrival(shift):
        from_dp, from_mp, spot = peer(shift)
        return pltpu.make_async_remote_copy(
            src_ref=gain_got.at[spot],
            dst_ref=gain_got.at[spot],
            send_sem=r.gain_s.at[shift],
            recv_sem=r.gain_r.at[spot],
            device_id={"dp": from_dp, "mp": from_mp},
            device_id_type=MESH,
        )

    for shift in range(1, members):
        gain_copy(shift).start()
    for group in range(2):
        for shift in range(1, dp_count):
            member = lax.rem(dp_me + shift, dp_count)
            for pair in range(share // 2):
                step = 2 * pair + forth.low
                from_member(outer_all, outer_sems, member, group, step).wait_recv()
                pass_on(member, group, step).start()
    drain_pass(ins, outs, forth.has_source, forth.has_target)
    for group in range(2):
        for shift in range(1, dp_count):
            member = lax.rem(dp_me + shift, dp_count)
            for pair in range(share // 2):
                pass_on(member, group, 2 * pair + 1 - forth.low).wait_recv()
    drain_pass(ins_back, outs_back, back.has_source, back.has_target)

    @pl.when(back.has_target)
    def _():
        for group in range(2):
            for shift in range(1, mp_count):
                dots_copy(shift, group, True).wait_send()

    total = r.gain_part[:, lanes_at(me * gain_cols, gain_cols)]
    for shift in range(1, members):
        gain_arrival(shift).wait_recv()
        total = total + gain_got[lax.rem(me + shift, members)]
    gain_out[...] = total

    for shift in range(1, members):
        for group in range(2):
            pool_copy(group, shift, True).wait_send()
        gain_copy(shift).wait_send()
    for group in range(2):
        for shift in range(1, dp_count):
            rows_copy(mixture_all, mixture_sems, shift, group, True).wait_send()
            rows_copy(heads_all, heads_sems, shift, group, True).wait_send()
            rows_copy(mixture_all, mixture_sems, shift, group, False).wait_recv()
            rows_copy(heads_all, heads_sems, shift, group, False).wait_recv()

        def drain(block, carry, group=group):
            away = block // share != dp_me

            @pl.when(away)
            def _():
                to_owner(r.normed_out, normed_all, normed_sems, group, block).wait_send()

            @pl.when(jnp.logical_and(away, lax.rem(block, 2) == forth.low))
            def _():
                to_owner(outer_out, outer_all, outer_sems, group, block).wait_send()

            return carry

        lax.fori_loop(0, blocks, drain, 0)
        for shift in range(1, dp_count):
            member = lax.rem(dp_me + shift, dp_count)
            for step in range(share):
                from_member(normed_all, normed_sems, member, group, step).wait_recv()
            for pair in range(share // 2):
                pass_on(member, group, 2 * pair + forth.low).wait_send()


def step_pass(lengths, positives, entrance, gain, table, wq, wk, wv, wo):
    rows, width_all = entrance.shape
    dp_count, mp_count = lax.axis_size("dp"), lax.axis_size("mp")
    members = dp_count * mp_count
    blocks = mp_count * SUB
    width = width_all // blocks
    share = blocks // dp_count
    seq_count = 2 * lengths.shape[0]
    length = rows // seq_count
    query_cols = wq.shape[1]
    head_cols = query_cols + wk.shape[1] + wv.shape[1]
    stacked = query_cols // HEAD * length
    row_pad = -(-(rows // 2) // 128) * 128
    pool_rows = -(-seq_count // 16) * 16
    dma = pltpu.SemaphoreType.DMA
    block = (rows // 2, width)
    shapes = dict(
        head_w=((width_all, head_cols), BF16),
        out_w=(wo.shape, BF16),
        acc=((rows, head_cols), F32),
        squares=((rows, 128), F32),
        inv_ref=((rows, 1), F32),
        pull_ref=((rows, 1), F32),
        query_ref=((seq_count, stacked, HEAD), BF16),
        key_ref=((seq_count, length, HEAD), BF16),
        value_ref=((seq_count, length, HEAD), BF16),
        prob_ref=((seq_count, stacked, length), F32),
        pooled=((2 * members, seq_count // 2, width_all), F32),
        hidden_sum=((seq_count, 1, width_all), F32),
        slopes=((dp_count * seq_count, 1, width_all), F32),
        normed_out=((2 * blocks, *block), BF16),
        outer_out=((2 * blocks, *block), BF16),
        grad_in=((2 * blocks, *block), BF16),
        mix_grad=((rows, query_cols), F32),
        row_dots=((2 * mp_count, 1, row_pad), F32),
        gain_part=((1, width_all), F32),
        gain_got=((members, 1, width_all // members), F32),
        pool_ref=((pool_rows, rows), BF16),
        near_send=((4 * SUB, *block), BF16),
        near_got=((4 * SUB, *block), BF16),
        far_send=((2 * SUB, *block), BF16),
        far_got=((2 * SUB, *block), BF16),
        relay_send=((2 * SUB, *block), BF16),
        keep=((2 * SUB, *block), F32),
        near_send_b=((4 * SUB, *block), BF16),
        near_got_b=((4 * SUB, *block), BF16),
        far_send_b=((2 * SUB, *block), BF16),
        far_got_b=((2 * SUB, *block), BF16),
        relay_send_b=((2 * SUB, *block), BF16),
        keep_b=((2 * SUB, *block), F32),
    )
    counts = dict(
        load_sem=(4,),
        enter_sem=(2 * blocks,),
        pool_s=(2 * members,),
        pool_r=(2 * members,),
        normed_s=(2 * blocks,),
        normed_r=(dp_count, 2 * share),
        outer_s=(2 * blocks,),
        outer_r=(dp_count, 2 * share),
        mixture_s=(2 * dp_count,),
        mixture_r=(2 * dp_count,),
        pass_s=(dp_count, 2 * share),
        pass_r=(dp_count, 2 * share),
        heads_s=(2 * dp_count,),
        heads_r=(2 * dp_count,),
        dots_s=(2 * mp_count,),
        dots_r=(2 * mp_count,),
        gain_s=(members,),
        gain_r=(members,),
        relay_s=(2 * SUB,),
        in_far_s=(2 * SUB,),
        out_far_s=(2 * SUB,),
        in_near_s=(4 * SUB,),
        out_near_s=(4 * SUB,),
        relay_r=(2 * SUB,),
        in_far_r=(2 * SUB,),
        out_far_r=(2 * SUB,),
        in_near_r=(4 * SUB,),
        out_near_r=(4 * SUB,),
        relay_sb=(2 * SUB,),
        in_far_sb=(2 * SUB,),
        out_far_sb=(2 * SUB,),
        in_near_sb=(4 * SUB,),
        out_near_sb=(4 * SUB,),
        relay_rb=(2 * SUB,),
        in_far_rb=(2 * SUB,),
        out_far_rb=(2 * SUB,),
        in_near_rb=(4 * SUB,),
        out_near_rb=(4 * SUB,),
    )
    scratch = Scratch(
        **{name: pltpu.VMEM(*shape) for name, shape in shapes.items()},
        **{name: dma(count) for name, count in counts.items()},
    )
    vmem = pl.BlockSpec(memory_space=pltpu.VMEM)
    smem = pl.BlockSpec(memory_space=pltpu.SMEM)
    hbm = pl.BlockSpec(memory_space=pltpu.HBM)
    return pl.pallas_call(
        step_kernel,
        out_shape=(
            jax.ShapeDtypeStruct((1, WIDTHS), F32),
            jax.ShapeDtypeStruct((1, width_all // members), F32),
            jax.ShapeDtypeStruct((share, dp_count * rows, width), BF16),
            jax.ShapeDtypeStruct((dp_count * rows, query_cols), BF16),
            jax.ShapeDtypeStruct((share, dp_count * rows, width), BF16),
            jax.ShapeDtypeStruct((dp_count * rows, head_cols), BF16),
        ),
        in_specs=[smem, smem, hbm, vmem, vmem, hbm, hbm, hbm, hbm],
        out_specs=(vmem,) * 6,
        scratch_shapes=[pltpu.VMEM((2 * blocks, *block), BF16)] + list(scratch),
        compiler_params=pltpu.CompilerParams(
            collective_id=0, has_side_effects=True, vmem_limit_bytes=36 * 1024 * 1024
        ),
        name="step_pass",
    )(lengths, positives, entrance, gain, table, wq, wk, wv, wo)


def weight_kernel(
    normed,
    mixture,
    outer,
    heads,
    losses,
    gain_share,
    query_grad,
    key_grad,
    value_grad,
    out_grad,
    losses_out,
    gain_out,
    turned,
):
    query_cols, kv_cols = query_grad.shape[1], key_grad.shape[1]

    @pl.when(pl.program_id(0) == 0)
    def _():
        turned[...] = mixture[...].T
        losses_out[...] = losses[...]
        gain_out[...] = gain_share[...]

    step = pl.program_id(0)
    product = contract_rows(normed[step], heads[...])
    query_grad[...] = product[:, :query_cols]
    key_grad[...] = product[:, query_cols : query_cols + kv_cols]
    value_grad[...] = product[:, query_cols + kv_cols :]
    out_grad[...] = jnp.dot(turned[...], outer[step], preferred_element_type=F32)


def weight_grads(normed, mixture, outer, heads, losses, gain_share, query_cols, kv_cols):
    share, rows, width = normed.shape
    columns = share * width
    vmem = pl.BlockSpec(memory_space=pltpu.VMEM)

    def tall(cols):
        return pl.BlockSpec((width, cols), lambda step: (step, 0))

    return pl.pallas_call(
        weight_kernel,
        grid=(share,),
        in_specs=[vmem] * 6,
        out_specs=(
            tall(query_cols),
            tall(kv_cols),
            tall(kv_cols),
            pl.BlockSpec((query_cols, width), lambda step: (0, step)),
            vmem,
            vmem,
        ),
        out_shape=(
            pltpu.HBM((columns, query_cols), F32),
            pltpu.HBM((columns, kv_cols), F32),
            pltpu.HBM((columns, kv_cols), F32),
            pltpu.HBM((query_cols, columns), F32),
            jax.ShapeDtypeStruct(losses.shape, F32),
            jax.ShapeDtypeStruct(gain_share.shape, F32),
        ),
        scratch_shapes=[pltpu.VMEM((query_cols, rows), BF16)],
        compiler_params=pltpu.CompilerParams(
            dimension_semantics=("arbitrary",), vmem_limit_bytes=16 * 1024 * 1024
        ),
        name="weight_grads",
    )(normed, mixture, outer, heads, losses, gain_share)


def local(entrance, lengths, positives, norm_gains, query_proj, key_proj, value_proj, out_proj):
    length = entrance.shape[2]
    width_all = entrance.shape[3]
    query_cols = query_proj.shape[2]
    kv_cols = key_proj.shape[2]
    losses, gain_share, normed, mixture, outer, heads = step_pass(
        lengths,
        positives,
        entrance.reshape(-1, width_all),
        norm_gains,
        jnp.asarray(rotary_constants(length)),
        query_proj[0],
        key_proj[0],
        value_proj[0],
        out_proj[0],
    )
    query_grad, key_grad, value_grad, out_grad, losses, gain_share = weight_grads(
        normed, mixture, outer, heads, losses, gain_share, query_cols, kv_cols
    )
    return (
        losses,
        gain_share,
        query_grad[None],
        key_grad[None],
        value_grad[None],
        out_grad[None],
    )


def solution(mesh):
    in_specs = (
        P("dp", None, None, None),
        P("dp", None),
        P(),
        P("section", None),
        P("section", None, "mp"),
        P("section", None, "mp"),
        P("section", None, "mp"),
        P("section", "mp", None),
    )
    out_specs = (
        P("section", None),
        P("section", ("dp", "mp")),
        P("section", "dp", "mp"),
        P("section", "dp", "mp"),
        P("section", "dp", "mp"),
        P("section", "mp", "dp"),
    )
    return jax.shard_map(local, mesh=mesh, in_specs=in_specs, out_specs=out_specs, check_vma=False)
```

```python
from typing import NamedTuple

import jax
import jax.numpy as jnp
import numpy as np
from jax import lax
from jax.experimental import pallas as pl
from jax.experimental.pallas import tpu as pltpu
from jax.sharding import PartitionSpec as P

HEAD = 128
WIDTHS = 7


EPSILON = 1e-05
SOFTMAX_TEMPER = 0.05
ROPE_BASE = 500000.0
MESH = pl.DeviceIdType.MESH
ROW_TILE = 16
SUB = 4
RELAY, CROSS, TAKE, ATTEND, NEAR, FAR, NEAR_OWN, OWN, FINISH = range(9)
FORWARD_ORDER = (
    (RELAY, 0, 0, 1, 2, 3), (CROSS, 0, 0, 2, 1), (TAKE, 0, 0), (RELAY, 1, 0), (CROSS, 0, 3),
    (TAKE, 0, 2), (RELAY, 1, 1), (TAKE, 0, 1, 3), (RELAY, 1, 2), (ATTEND, 0, 0), (NEAR, 0, 0, 1),
    (RELAY, 1, 3), (NEAR_OWN, 0, 2, 0), (NEAR, 0, 2), (CROSS, 1, 0), (NEAR, 0, 3), (FAR, 0, 0),
    (NEAR_OWN, 0, 1), (FAR, 0, 1), (OWN, 0, 0), (CROSS, 1, 1), (TAKE, 1, 0), (CROSS, 1, 2),
    (FAR, 0, 2, 3), (OWN, 0, 1), (CROSS, 1, 3), (TAKE, 1, 1, 2), (FINISH, 0, 0), (TAKE, 1, 3),
    (ATTEND, 1, 0), (FINISH, 0, 1), (NEAR, 1, 0), (NEAR_OWN, 0, 3), (OWN, 0, 2), (NEAR, 1, 1),
    (FINISH, 0, 2), (NEAR_OWN, 1, 0), (FAR, 1, 0), (OWN, 0, 3), (FINISH, 0, 3), (NEAR, 1, 2, 3),
    (FAR, 1, 1), (NEAR_OWN, 1, 2), (FAR, 1, 2), (NEAR_OWN, 1, 1), (FAR, 1, 3), (OWN, 1, 0),
    (FINISH, 1, 0), (NEAR_OWN, 1, 3), (OWN, 1, 1), (FINISH, 1, 1), (OWN, 1, 2, 3),
    (FINISH, 1, 2, 3),
)
BACKWARD_ORDER = (
    (RELAY, 0, 0, 1, 2, 3), (CROSS, 0, 0, 1), (TAKE, 0, 0), (CROSS, 0, 2), (TAKE, 0, 1),
    (CROSS, 0, 3), (TAKE, 0, 2, 3), (ATTEND, 0, 0), (NEAR, 0, 0), (NEAR_OWN, 0, 0),
    (NEAR, 0, 1, 2), (FAR, 0, 0), (NEAR, 0, 3), (FAR, 0, 1, 2), (NEAR_OWN, 0, 2, 1), (OWN, 0, 0),
    (FAR, 0, 3), (FINISH, 0, 0), (RELAY, 1, 0), (OWN, 0, 2, 1), (RELAY, 1, 1), (FINISH, 0, 1),
    (NEAR_OWN, 0, 3), (RELAY, 1, 2), (FINISH, 0, 2), (OWN, 0, 3), (RELAY, 1, 3), (FINISH, 0, 3),
    (CROSS, 1, 0, 1), (TAKE, 1, 0), (CROSS, 1, 2), (TAKE, 1, 1), (CROSS, 1, 3), (TAKE, 1, 2, 3),
    (ATTEND, 1, 0), (NEAR, 1, 0, 1), (NEAR_OWN, 1, 0), (NEAR, 1, 3), (FAR, 1, 0), (NEAR, 1, 2),
    (FAR, 1, 1), (OWN, 1, 0), (NEAR_OWN, 1, 1), (FAR, 1, 2, 3), (NEAR_OWN, 1, 2), (FINISH, 1, 0),
    (OWN, 1, 1), (NEAR_OWN, 1, 3), (FINISH, 1, 1), (OWN, 1, 2), (FINISH, 1, 2), (OWN, 1, 3),
    (FINISH, 1, 3),
)
F32 = jnp.float32
BF16 = jnp.bfloat16


def contract_rows(left, right):
    return lax.dot_general(
        left, right, (((0,), (0,)), ((), ())), preferred_element_type=jnp.float32
    )


def contract_last(left, right):
    return lax.dot_general(
        left, right, (((left.ndim - 1,), (1,)), ((), ())), preferred_element_type=jnp.float32
    )


def rotary_constants(length):
    half_size = HEAD // 2
    frequencies = ROPE_BASE ** (-np.arange(half_size, dtype=np.float64) * 2.0 / HEAD)
    angles = np.arange(length, dtype=np.float64)[:, None] * frequencies[None, :]
    cosine = np.concatenate([np.cos(angles), np.cos(angles)], axis=1)
    sine = np.concatenate([-np.sin(angles), np.sin(angles)], axis=1)
    return np.stack([cosine, sine]).astype(np.float32)


def mp_place(me, levels):
    bits = [(me // (1 << level)) % 2 for level in range(levels)]
    partners = [me + (1 - 2 * bits[level]) * (1 << level) for level in range(levels)]
    return bits, partners


def rows_at(start, size):
    return pl.ds(pl.multiple_of(start, ROW_TILE), size)


def lanes_at(start, size):
    return pl.ds(pl.multiple_of(start, 128), size)


class Place:
    def __init__(self, direction):
        self.here = lax.axis_index("section")
        self.count = lax.axis_size("section")
        (self.low, self.high), (self.near, self.far) = mp_place(lax.axis_index("mp"), 2)
        self.direction = direction
        if direction > 0:
            self.has_source, self.has_target = self.here > 0, self.here < self.count - 1
        else:
            self.has_source, self.has_target = self.here < self.count - 1, self.here > 0

    def quarter(self, flip_low, flip_high):
        low = 1 - self.low if flip_low else self.low
        high = 1 - self.high if flip_high else self.high
        return (low * 2 + high) * SUB


def send(source, target, sems, slot, **device):
    return pltpu.make_async_remote_copy(
        src_ref=source,
        dst_ref=target,
        send_sem=sems[0].at[slot],
        recv_sem=sems[1].at[slot],
        device_id=device,
        device_id_type=MESH,
    )


class StreamIn:
    def __init__(self, place, group, buf, relay, far, near):
        self.place, self.buf = place, buf
        self.relay, self.far, self.near = relay, far, near
        self.group = group

    def at(self, block):
        return self.buf.at[self.group * 4 * SUB + block]

    def relay_copy(self, step, block):
        slot = self.group * SUB + step
        return send(self.at(block), self.at(block), self.relay, slot, section=self.place.here)

    def near_copy(self, slot, block):
        slot = self.group * 2 * SUB + slot
        return send(self.at(block), self.at(block), self.near, slot, mp=self.place.near)

    def far_copy(self, step, block):
        slot = self.group * SUB + step
        return send(self.at(block), self.at(block), self.far, slot, mp=self.place.far)

    def relay_step(self, step):
        block = self.place.quarter(0, 0) + step
        self.relay_copy(step, block).wait_recv()
        self.far_copy(step, block).start()
        self.near_copy(step, block).start()

    def cross_step(self, step):
        block = self.place.quarter(0, 1) + step
        self.far_copy(step, block).wait_recv()
        self.near_copy(SUB + step, block).start()

    def settle(self, step):
        self.near_copy(step, self.place.quarter(1, 0) + step).wait_recv()
        self.near_copy(SUB + step, self.place.quarter(1, 1) + step).wait_recv()

    def drain(self):
        own, other = self.place.quarter(0, 0), self.place.quarter(0, 1)
        for step in range(SUB):
            self.far_copy(step, own + step).wait_send()
            self.near_copy(step, own + step).wait_send()
            self.near_copy(SUB + step, other + step).wait_send()


class StreamOut:
    def __init__(self, place, group, part, finish, dest, bufs, relay, far, near):
        self.place, self.group = place, group
        self.part_of, self.finish_of, self.dest = part, finish, dest
        self.near_send, self.near_got, self.far_send, self.far_got, self.relay_send, self.keep = (
            bufs
        )
        self.relay_sems, self.far_sems, self.near_sems = relay, far, near

    def near_copy(self, slot):
        slot = self.group * 2 * SUB + slot
        return send(
            self.near_send.at[slot], self.near_got.at[slot], self.near_sems, slot, mp=self.place.near
        )

    def far_copy(self, step):
        slot = self.group * SUB + step
        return send(
            self.far_send.at[slot], self.far_got.at[slot], self.far_sems, slot, mp=self.place.far
        )

    def relay_copy(self, step):
        slot = self.group * SUB + step
        place = self.place
        return send(
            self.relay_send.at[slot],
            self.dest.at[self.group * 4 * SUB + place.quarter(0, 0) + step],
            self.relay_sems,
            slot,
            section=place.here + place.direction,
        )

    def near(self, flip, step):
        place = self.place
        slot = (1 - place.high if flip else place.high) * SUB + step
        value = self.part_of(self.group, place.quarter(1, flip) + step)
        self.near_send[self.group * 2 * SUB + slot] = value.astype(BF16)
        self.near_copy(slot).start()

    def arrived(self, slot):
        self.near_copy(slot).wait_recv()
        return self.near_got[self.group * 2 * SUB + slot].astype(F32)

    def far(self, step):
        place = self.place
        value = self.part_of(self.group, place.quarter(0, 1) + step)
        value = value + self.arrived((1 - place.high) * SUB + step)
        self.far_send[self.group * SUB + step] = value.astype(BF16)
        self.far_copy(step).start()

    def own(self, step):
        place = self.place
        value = self.part_of(self.group, place.quarter(0, 0) + step)
        self.keep[self.group * SUB + step] = value + self.arrived(place.high * SUB + step)

    def finish(self, step):
        slot = self.group * SUB + step
        block = self.place.quarter(0, 0) + step
        self.far_copy(step).wait_recv()
        value = self.keep[slot] + self.far_got[slot].astype(F32)
        self.relay_send[slot] = self.finish_of(self.group, block, value)
        self.relay_copy(step).start()

    def drain(self):
        for step in range(SUB):
            self.far_copy(step).wait_send()
            self.relay_copy(step).wait_send()
        for slot in range(2 * SUB):
            self.near_copy(slot).wait_send()


def run_pass(order, ins, outs, has_source, has_target, consume, attend, prepare, rest):
    def take(group, step):
        @pl.when(has_source)
        def _():
            ins[group].settle(step)

        for quarter in range(4):
            consume(group, quarter * SUB + step)

    def finish(group, step):
        if step == 0:
            prepare(group)
        outs[group].finish(step)

    receive = {
        RELAY: lambda group, step: ins[group].relay_step(step),
        CROSS: lambda group, step: ins[group].cross_step(step),
    }
    produce = {
        NEAR: lambda group, step: outs[group].near(1, step),
        NEAR_OWN: lambda group, step: outs[group].near(0, step),
        FAR: lambda group, step: outs[group].far(step),
        OWN: lambda group, step: outs[group].own(step),
        FINISH: finish,
    }
    for kind, group, *steps in order:
        if kind == ATTEND:
            attend(group)
            if rest is not None:
                pl.when(jnp.logical_not(has_target))(lambda group=group: rest(group))
        elif kind == TAKE:
            for step in steps:
                take(group, step)
        else:
            action = receive.get(kind) or produce[kind]

            @pl.when(has_source if kind in receive else has_target)
            def _(group=group, steps=steps, action=action):
                for step in steps:
                    action(group, step)


def drain_pass(ins, outs, has_source, has_target):
    @pl.when(has_source)
    def _():
        for flow in ins:
            flow.drain()

    @pl.when(has_target)
    def _():
        for flow in outs:
            flow.drain()


def rotary(values, table, sign):
    turned = pltpu.roll(values, HEAD // 2, axis=1)
    return values * table[0] + turned * (table[1] * sign)


def fold_lanes(values):
    total = values[:, :128]
    for lane in range(1, values.shape[1] // 128):
        total = total + values[:, lane * 128 : (lane + 1) * 128]
    return total


def lane_sum(values):
    return jnp.sum(fold_lanes(values), axis=1, keepdims=True)


def matryoshka(queries, passages, target):
    pairs, width_all = queries.shape
    widths = [width_all >> level for level in range(WIDTHS)]
    bounds = [0] + widths[::-1]
    lane = lax.broadcasted_iota(jnp.int32, (pairs, 128), 1)

    def segment_sums(product):
        sums = []
        for low, high in zip(bounds[:-1], bounds[1:]):
            if high <= 128:
                inside = jnp.logical_and(lane >= low, lane < high)
                piece = jnp.where(inside, product[:, :128], 0.0)
            else:
                piece = fold_lanes(product[:, low:high])
            sums.append(jnp.sum(piece, axis=1, keepdims=True))
        for index in range(1, len(sums)):
            sums[index] = sums[index] + sums[index - 1]
        return sums[::-1]

    query_squares = segment_sums(queries * queries)
    passage_squares = segment_sums(passages * passages)
    dots = [segment_sums(queries * passages[j : j + 1]) for j in range(pairs)]
    losses = []
    mixed = [[] for _ in range(pairs)]
    query_own, passage_own = [], []
    for level, width in enumerate(widths):
        query_inv = lax.rsqrt(query_squares[level] * (1.0 / width) + 1e-06)
        passage_inv = lax.rsqrt(passage_squares[level] * (1.0 / width) + 1e-06)
        factors = [
            query_inv * passage_inv[j : j + 1] * (1.0 / (width * SOFTMAX_TEMPER))
            for j in range(pairs)
        ]
        logits = [dots[j][level] * factors[j] for j in range(pairs)]
        highest = logits[0]
        for j in range(1, pairs):
            highest = jnp.maximum(highest, logits[j])
        powers = [jnp.exp(logits[j] - highest) for j in range(pairs)]
        total = powers[0]
        picked = logits[0] * target[:, 0:1]
        for j in range(1, pairs):
            total = total + powers[j]
            picked = picked + logits[j] * target[:, j : j + 1]
        gap = jnp.log(total) + highest - picked
        losses.append(jnp.sum(gap, axis=0, keepdims=True) * (1.0 / pairs))
        slopes = [
            (powers[j] / total - target[:, j : j + 1]) * (1.0 / pairs) for j in range(pairs)
        ]
        pulls = [slopes[j] * logits[j] for j in range(pairs)]
        row_pull = pulls[0]
        for j in range(1, pairs):
            row_pull = row_pull + pulls[j]
        column_pull = jnp.concatenate(
            [jnp.sum(pulls[j], axis=0, keepdims=True) for j in range(pairs)], axis=0
        )
        for j in range(pairs):
            mixed[j].append(slopes[j] * factors[j])
        query_own.append(row_pull * query_inv * query_inv * (-1.0 / width))
        passage_own.append(column_pull * passage_inv * passage_inv * (-1.0 / width))
    for series in mixed + [query_own, passage_own]:
        for level in range(1, WIDTHS):
            series[level] = series[level] + series[level - 1]
    turned = [
        [
            jnp.concatenate([mixed[j][level][p : p + 1] for j in range(pairs)], axis=0)
            for level in range(WIDTHS)
        ]
        for p in range(pairs)
    ]

    def spread(own, own_rows, weights, rows):
        pieces = []
        low = 0
        while low < width_all:
            inside = [k for k in range(WIDTHS) if low < bounds[k + 1] and low + 128 > bounds[k]]
            high = max(low + 128, bounds[inside[-1] + 1])

            def coefficient(series, inside=inside):
                value = series[WIDTHS - 1 - inside[-1]]
                for k in reversed(inside[:-1]):
                    value = jnp.where(lane < bounds[k + 1], series[WIDTHS - 1 - k], value)
                return value

            def columns(values, low=low, high=high):
                return values[:, low:high]

            piece = coefficient(own) * columns(own_rows)
            for j in range(pairs):
                piece = piece + coefficient(weights[j]) * columns(rows[j : j + 1])
            pieces.append(piece)
            low = high
        return jnp.concatenate(pieces, axis=1)

    return (
        losses,
        spread(query_own, queries, mixed, passages),
        spread(passage_own, passages, turned, queries),
    )


class Scratch(NamedTuple):
    head_w: object
    out_w: object
    acc: object
    squares: object
    inv_ref: object
    query_ref: object
    key_ref: object
    value_ref: object
    prob_ref: object
    pooled: object
    slopes: object
    normed_out: object
    outer_out: object
    grad_in: object
    mix_grad: object
    row_dots: object
    gain_part: object
    hidden_sum: object
    pull_ref: object
    keep: object
    keep_b: object
    gain_got: object
    pool_ref: object
    near_send: object
    near_got: object
    far_send: object
    far_got: object
    relay_send: object
    near_send_b: object
    near_got_b: object
    far_send_b: object
    far_got_b: object
    relay_send_b: object
    load_sem: object
    enter_sem: object
    relay_s: object
    relay_r: object
    in_far_s: object
    in_far_r: object
    in_near_s: object
    in_near_r: object
    out_far_s: object
    out_far_r: object
    out_near_s: object
    out_near_r: object
    relay_sb: object
    relay_rb: object
    in_far_sb: object
    in_far_rb: object
    in_near_sb: object
    in_near_rb: object
    out_far_sb: object
    out_far_rb: object
    out_near_sb: object
    out_near_rb: object
    pool_s: object
    pool_r: object
    normed_s: object
    normed_r: object
    mixture_s: object
    mixture_r: object
    outer_s: object
    outer_r: object
    heads_s: object
    heads_r: object
    dots_s: object
    dots_r: object
    pass_s: object
    pass_r: object
    gain_s: object
    gain_r: object


def step_kernel(
    lengths,
    positives,
    entrance,
    gain,
    table,
    wq,
    wk,
    wv,
    wo,
    losses_out,
    gain_out,
    normed_all,
    mixture_all,
    outer_all,
    heads_all,
    hidden,
    *scratch,
):
    r = Scratch(*scratch)
    head_w, out_w, acc, squares = r.head_w, r.out_w, r.acc, r.squares
    forth, back = Place(1), Place(-1)
    rows, width = hidden.shape[1:]
    blocks = hidden.shape[0] // 2
    width_all = blocks * width
    pair_count = lengths.shape[0]
    seq_count = 2 * pair_count
    length = rows // pair_count
    query_cols, kv_cols = wq.shape[1], wk.shape[1]
    groups = query_cols // HEAD
    dp_me, mp_me = lax.axis_index("dp"), lax.axis_index("mp")
    dp_count, mp_count = lax.axis_size("dp"), lax.axis_size("mp")
    members = dp_count * mp_count
    me = dp_me * mp_count + mp_me
    share = blocks // dp_count
    row_pad = r.row_dots.shape[2]
    normed_sems, outer_sems = (r.normed_s, r.normed_r), (r.outer_s, r.outer_r)
    mixture_sems, heads_sems = (r.mixture_s, r.mixture_r), (r.heads_s, r.heads_r)
    outer_out = r.outer_out

    def peer(shift):
        spot = lax.rem(me + shift, members)
        return spot // mp_count, lax.rem(spot, mp_count), spot

    def span_of(group):
        return slice(group * rows, (group + 1) * rows)

    def member_rows(member, group):
        return rows_at((member * 2 + group) * rows, rows)

    def sequences(group):
        for local_seq in range(pair_count):
            inner = slice(local_seq * length, (local_seq + 1) * length)
            outer = slice(group * rows + inner.start, group * rows + inner.stop)
            yield group * pair_count + local_seq, inner, outer

    def count_of(seq):
        return lengths[seq // 2, seq % 2]

    spot = lax.broadcasted_iota(jnp.int32, (length, 1), 0)

    def valid_of(seq):
        return jnp.where(spot < count_of(seq), 1.0, 0.0)

    loads = [
        pltpu.make_async_copy(wq, head_w.at[:, :query_cols], r.load_sem.at[0]),
        pltpu.make_async_copy(wk, head_w.at[:, query_cols : query_cols + kv_cols], r.load_sem.at[1]),
        pltpu.make_async_copy(wv, head_w.at[:, query_cols + kv_cols :], r.load_sem.at[2]),
        pltpu.make_async_copy(wo, out_w, r.load_sem.at[3]),
    ]

    def enter(group, block):
        slot = group * blocks + block
        return pltpu.make_async_copy(
            entrance.at[pl.ds(group * rows, rows), lanes_at(block * width, width)],
            hidden.at[slot],
            r.enter_sem.at[slot],
        )

    @pl.when(jnp.logical_not(forth.has_source))
    def _():
        for group in range(2):
            for block in range(blocks):
                enter(group, block).start()

    for load in loads:
        load.start()
    barrier = pltpu.get_barrier_semaphore()
    for shift in range(1, members):
        to_dp, to_mp, _ = peer(shift)
        pl.semaphore_signal(
            barrier, inc=1, device_id={"dp": to_dp, "mp": to_mp}, device_id_type=MESH
        )

    @pl.when(forth.has_source)
    def _():
        pl.semaphore_signal(
            barrier, inc=1, device_id={"section": forth.here - 1}, device_id_type=MESH
        )

    @pl.when(forth.has_target)
    def _():
        pl.semaphore_signal(
            barrier, inc=1, device_id={"section": forth.here + 1}, device_id_type=MESH
        )

    acc[...] = jnp.zeros_like(acc)
    squares[...] = jnp.zeros_like(squares)
    r.mix_grad[...] = jnp.zeros_like(r.mix_grad)
    r.gain_part[...] = jnp.zeros_like(r.gain_part)

    @pl.when(jnp.logical_not(back.has_source))
    def _():
        def clear(block, carry):
            r.grad_in[block] = jnp.zeros((rows, width), BF16)
            return carry

        lax.fori_loop(0, 2 * blocks, clear, 0)

    pool_shape = r.pool_ref.shape
    column = lax.broadcasted_iota(jnp.int32, pool_shape, 1)
    line = lax.broadcasted_iota(jnp.int32, pool_shape, 0)
    picks = jnp.zeros(pool_shape, F32)
    for seq in range(seq_count):
        inside = jnp.logical_and(column >= seq * length, column < seq * length + count_of(seq))
        picks = jnp.where(jnp.logical_and(line == seq % pair_count, inside), 1.0, picks)
    r.pool_ref[...] = picks.astype(BF16)
    for load in loads[:3]:
        load.wait()
    expected = (
        members - 1 + forth.has_source.astype(jnp.int32) + forth.has_target.astype(jnp.int32)
    )

    @pl.when(forth.has_source)
    def _():
        pl.semaphore_wait(barrier, expected)

    def gain_at(block):
        return gain[:, lanes_at(block * width, width)]

    def out_columns(block):
        return out_w[:, lanes_at(block * width, width)]

    def consume(group, block):
        slot = group * blocks + block

        @pl.when(jnp.logical_not(forth.has_source))
        def _():
            enter(group, block).wait()

        value = hidden[slot].astype(F32)
        span = span_of(group)
        squares[span, :] += fold_lanes(value * value)
        for seq, inner, _ in sequences(group):
            r.hidden_sum[seq, :, lanes_at(block * width, width)] = jnp.sum(
                value[inner] * valid_of(seq), axis=0, keepdims=True
            )
        acc[span, :] += jnp.dot(
            (value * gain_at(block)).astype(BF16),
            head_w[rows_at(block * width, width), :],
            preferred_element_type=F32,
        )

    mixture = mixture_all.at[pl.ds(pl.multiple_of(dp_me * 2 * rows, ROW_TILE), 2 * rows)]

    def attend(group):
        whole = span_of(group)
        inv_rms = lax.rsqrt(
            jnp.sum(squares[whole, :], axis=1, keepdims=True) * (1.0 / width_all) + EPSILON
        )
        r.inv_ref[whole, :] = inv_rms
        for seq, inner, span in sequences(group):
            inverse = inv_rms[inner]
            query = jnp.concatenate(
                [
                    rotary(acc[span, g * HEAD : (g + 1) * HEAD] * inverse, table, 1.0)
                    for g in range(groups)
                ],
                axis=0,
            ).astype(BF16)
            key = rotary(acc[span, query_cols : query_cols + kv_cols] * inverse, table, 1.0)
            key = key.astype(BF16)
            value = (acc[span, query_cols + kv_cols :] * inverse).astype(BF16)
            r.query_ref[seq] = query
            r.key_ref[seq] = key
            r.value_ref[seq] = value
            scores = contract_last(query, key) * HEAD ** (-0.5)
            place = lax.broadcasted_iota(jnp.int32, scores.shape, 0) % length
            scores = jnp.where(
                place >= lax.broadcasted_iota(jnp.int32, scores.shape, 1), scores, -1e30
            )
            weights = jnp.exp(scores - jnp.max(scores, axis=1, keepdims=True))
            weights = weights / jnp.sum(weights, axis=1, keepdims=True)
            r.prob_ref[seq] = weights
            mixed = jnp.dot(weights.astype(BF16), value, preferred_element_type=F32).astype(BF16)
            for g in range(groups):
                mixture[span, g * HEAD : (g + 1) * HEAD] = mixed[g * length : (g + 1) * length]
        if group == 0:

            @pl.when(jnp.logical_not(forth.has_source))
            def _():
                pl.semaphore_wait(barrier, expected)

            loads[3].wait()

    first = (mp_me == 0).astype(F32)
    pooled = r.pooled

    def pool_copy(group, shift, own):
        other_dp, other_mp, spot = peer(shift)
        member = group * members + (me if own else spot)
        return pltpu.make_async_remote_copy(
            src_ref=pooled.at[member],
            dst_ref=pooled.at[member],
            send_sem=r.pool_s.at[group * members + shift],
            recv_sem=r.pool_r.at[member],
            device_id={"dp": other_dp, "mp": other_mp},
            device_id_type=MESH,
        )

    def send_pooled(group):
        span = span_of(group)
        mixture_sum = jnp.dot(r.pool_ref[:, span], mixture[span, :], preferred_element_type=F32)
        coarse = mixture_sum.astype(BF16)
        fine = (mixture_sum - coarse.astype(F32)).astype(BF16)
        both = jnp.concatenate([coarse, fine], axis=0)

        def pool_block(block, carry):
            sums = jnp.dot(both, out_columns(block), preferred_element_type=F32)
            sums = sums[: pool_shape[0]] + sums[pool_shape[0] :]
            lines = [
                (sums[line : line + 1] + first * r.hidden_sum[seq, :, lanes_at(block * width, width)])
                / count_of(seq).astype(F32)
                for line, (seq, _, _) in enumerate(sequences(group))
            ]
            lines = lines[0] if pair_count == 1 else jnp.concatenate(lines, axis=0)
            pooled[group * members + me, :, lanes_at(block * width, width)] = lines
            return carry

        lax.fori_loop(0, blocks, pool_block, 0, unroll=4)
        for shift in range(1, members):
            pool_copy(group, shift, True).start()

    def part(group, block):
        return jnp.dot(mixture[span_of(group), :], out_columns(block), preferred_element_type=F32)

    def finish(group, block, total):
        return (hidden[group * blocks + block].astype(F32) + total).astype(BF16)

    ins = [
        StreamIn(
            forth,
            group,
            hidden,
            (r.relay_s, r.relay_r),
            (r.in_far_s, r.in_far_r),
            (r.in_near_s, r.in_near_r),
        )
        for group in range(2)
    ]
    outs = [
        StreamOut(
            forth,
            group,
            part,
            finish,
            hidden,
            (r.near_send, r.near_got, r.far_send, r.far_got, r.relay_send, r.keep),
            (r.relay_s, r.relay_r),
            (r.out_far_s, r.out_far_r),
            (r.out_near_s, r.out_near_r),
        )
        for group in range(2)
    ]
    run_pass(
        FORWARD_ORDER, ins, outs, forth.has_source, forth.has_target, consume, attend, lambda group: None, send_pooled
    )

    @pl.when(forth.has_target)
    def _():
        for group in range(2):
            send_pooled(group)

    def to_owner(source, target, sems, group, block):
        step = lax.rem(block, share)
        return pltpu.make_async_remote_copy(
            src_ref=source.at[group * blocks + block],
            dst_ref=target.at[step, member_rows(dp_me, group)],
            send_sem=sems[0].at[group * blocks + block],
            recv_sem=sems[1].at[dp_me, group * share + step],
            device_id={"dp": block // share},
            device_id_type=MESH,
        )

    def from_member(target, sems, member, group, step):
        piece = target.at[step, member_rows(member, group)]
        return pltpu.make_async_remote_copy(
            src_ref=piece,
            dst_ref=piece,
            send_sem=sems[0].at[0],
            recv_sem=sems[1].at[member, group * share + step],
            device_id={"dp": member},
            device_id_type=MESH,
        )

    def rows_copy(target, sems, shift, group, own):
        other = lax.rem(dp_me + shift, dp_count)
        member = dp_me if own else other
        piece = target.at[member_rows(member, group)]
        return pltpu.make_async_remote_copy(
            src_ref=piece,
            dst_ref=piece,
            send_sem=sems[0].at[group * dp_count + shift],
            recv_sem=sems[1].at[group * dp_count + member],
            device_id={"dp": other},
            device_id_type=MESH,
        )

    def hand_out(value, spare, target, sems, group, block, passes=None):
        mine = block // share == dp_me

        @pl.when(mine)
        def _():
            target[lax.rem(block, share), member_rows(dp_me, group), :] = value

        sends = jnp.logical_not(mine)
        if passes is not None:
            sends = jnp.logical_and(sends, passes)

        @pl.when(sends)
        def _():
            spare[group * blocks + block] = value
            to_owner(spare, target, sems, group, block).start()

    def hand_out_normed():
        for group in range(2):

            def normed_block(block, carry, group=group):
                value = hidden[group * blocks + block].astype(F32) * r.inv_ref[span_of(group), :]
                value = (value * gain_at(block)).astype(BF16)
                hand_out(value, r.normed_out, normed_all, normed_sems, group, block)
                return carry

            lax.fori_loop(0, blocks, normed_block, 0, unroll=2)
            for shift in range(1, dp_count):
                rows_copy(mixture_all, mixture_sems, shift, group, True).start()

    pl.when(back.has_source)(hand_out_normed)
    for group in range(2):
        for shift in range(1, members):
            pool_copy(group, shift, False).wait_recv()
    embedded = []
    for group in range(2):
        for member in range(dp_count):
            start = group * members + member * mp_count
            total = pooled[start]
            for other in range(1, mp_count):
                total = total + pooled[start + other]
            embedded.append(total)
    pairs = dp_count * pair_count

    def embedding(seq):
        member, inner = seq // seq_count, seq % seq_count
        block = embedded[inner // pair_count * dp_count + member]
        return block[inner % pair_count :][:1]

    queries = jnp.concatenate([embedding(2 * p) for p in range(pairs)], axis=0)
    passages = jnp.concatenate([embedding(2 * p + 1) for p in range(pairs)], axis=0)
    partner = lax.broadcasted_iota(jnp.int32, (pairs, pairs), 1)
    line = lax.broadcasted_iota(jnp.int32, (pairs, pairs), 0)
    target = jnp.zeros((pairs, pairs), F32)
    for p in range(pairs):
        target = jnp.where(jnp.logical_and(line == p, partner == positives[p]), 1.0, target)
    losses, query_slopes, passage_slopes = matryoshka(queries, passages, target)
    lane = lax.broadcasted_iota(jnp.int32, (1, 128), 1)
    packed = jnp.zeros((1, 128), F32)
    for level in range(WIDTHS):
        packed = jnp.where(lane == level, losses[level], packed)
    losses_out[...] = packed[:, :WIDTHS]
    slopes = r.slopes
    for p in range(pairs):
        slopes[2 * p] = query_slopes[p : p + 1]
        slopes[2 * p + 1] = passage_slopes[p : p + 1]

    grad_in, mix_grad = r.grad_in, r.mix_grad

    def upstream(group, block):
        tokens = [
            valid_of(seq)
            / count_of(seq).astype(F32)
            * slopes[dp_me * seq_count + seq, :, lanes_at(block * width, width)]
            for seq, _, _ in sequences(group)
        ]
        tokens = tokens[0] if pair_count == 1 else jnp.concatenate(tokens, axis=0)
        return tokens + grad_in[group * blocks + block].astype(F32)

    def consume_back(group, block):
        outer = upstream(group, block).astype(BF16)
        passes = lax.rem(block, 2) == forth.low
        hand_out(outer, outer_out, outer_all, outer_sems, group, block, passes)
        mix_grad[span_of(group), :] += contract_last(outer, out_columns(block))

    head_grads = heads_all.at[pl.ds(pl.multiple_of(dp_me * 2 * rows, ROW_TILE), 2 * rows)]
    row_dots = r.row_dots
    diagonal = lax.broadcasted_iota(jnp.int32, (rows, row_pad), 0) == lax.broadcasted_iota(
        jnp.int32, (rows, row_pad), 1
    )

    def dots_copy(shift, group, own):
        other = lax.rem(mp_me + shift, mp_count)
        member = mp_me if own else other
        piece = row_dots.at[group * mp_count + member]
        return pltpu.make_async_remote_copy(
            src_ref=piece,
            dst_ref=piece,
            send_sem=r.dots_s.at[group * mp_count + shift],
            recv_sem=r.dots_r.at[group * mp_count + member],
            device_id={"mp": other},
            device_id_type=MESH,
        )

    def attend_back(group):
        row_dot = []
        for seq, _, span in sequences(group):
            mixed = jnp.concatenate(
                [mix_grad[span, g * HEAD : (g + 1) * HEAD] for g in range(groups)], axis=0
            ).astype(BF16)
            weights = r.prob_ref[seq]
            value_grad = contract_rows(weights.astype(BF16), mixed).astype(BF16)
            pulled = contract_last(mixed, r.value_ref[seq]).astype(BF16).astype(F32)
            score_grad = weights * (pulled - jnp.sum(weights * pulled, axis=1, keepdims=True))
            score_grad = (score_grad * HEAD ** (-0.5)).astype(BF16)
            query_grad = jnp.dot(score_grad, r.key_ref[seq], preferred_element_type=F32)
            query_grad = query_grad.astype(BF16).astype(F32)
            key_grad = contract_rows(score_grad, r.query_ref[seq]).astype(BF16).astype(F32)
            pieces = [
                rotary(query_grad[g * length : (g + 1) * length], table, -1.0).astype(BF16)
                for g in range(groups)
            ]
            pieces = pieces + [rotary(key_grad, table, -1.0).astype(BF16), value_grad]
            joined = jnp.concatenate(pieces, axis=1)
            head_grads[span, :] = joined
            row_dot.append(lane_sum(joined.astype(F32) * acc[span, :]))
        for shift in range(1, dp_count):
            rows_copy(heads_all, heads_sems, shift, group, True).start()
        row_dot = row_dot[0] if pair_count == 1 else jnp.concatenate(row_dot, axis=0)

        @pl.when(back.has_target)
        def _():
            row_dots[group * mp_count + mp_me] = jnp.sum(
                jnp.where(diagonal, row_dot, 0.0), axis=0, keepdims=True
            )
            for shift in range(1, mp_count):
                dots_copy(shift, group, True).start()

    def part_back(group, block):
        span = span_of(group)
        value = contract_last(head_grads[span, :], head_w[rows_at(block * width, width), :])
        scaled = value * (hidden[group * blocks + block].astype(F32) * r.inv_ref[span, :])
        r.gain_part[:, lanes_at(block * width, width)] += jnp.sum(scaled, axis=0, keepdims=True)
        return value

    def prepare(group):
        for shift in range(1, mp_count):
            dots_copy(shift, group, False).wait_recv()
        total = row_dots[group * mp_count]
        for member in range(1, mp_count):
            total = total + row_dots[group * mp_count + member]
        inverse = r.inv_ref[span_of(group), :]
        r.pull_ref[span_of(group), :] = (
            lane_sum(jnp.where(diagonal, total, 0.0))
            * inverse
            * inverse
            * inverse
            * (1.0 / width_all)
        )

    def finish_back(group, block, total):
        span = span_of(group)
        value = upstream(group, block) + total * gain_at(block) * r.inv_ref[span, :]
        pulled = hidden[group * blocks + block].astype(F32) * r.pull_ref[span, :]
        return (value - pulled).astype(BF16)

    def gain_only(group):
        def body(block, carry):
            part_back(group, block)
            return carry

        lax.fori_loop(0, blocks, body, 0, unroll=2)

    ins_back = [
        StreamIn(
            back,
            group,
            grad_in,
            (r.relay_sb, r.relay_rb),
            (r.in_far_sb, r.in_far_rb),
            (r.in_near_sb, r.in_near_rb),
        )
        for group in range(2)
    ]
    outs_back = [
        StreamOut(
            back,
            group,
            part_back,
            finish_back,
            grad_in,
            (r.near_send_b, r.near_got_b, r.far_send_b, r.far_got_b, r.relay_send_b, r.keep_b),
            (r.relay_sb, r.relay_rb),
            (r.out_far_sb, r.out_far_rb),
            (r.out_near_sb, r.out_near_rb),
        )
        for group in range(2)
    ]
    run_pass(
        BACKWARD_ORDER,
        ins_back,
        outs_back,
        back.has_source,
        back.has_target,
        consume_back,
        attend_back,
        prepare,
        gain_only,
    )

    pl.when(jnp.logical_not(back.has_source))(hand_out_normed)

    def pass_on(member, group, step):
        piece = outer_all.at[step, member_rows(member, group)]
        return pltpu.make_async_remote_copy(
            src_ref=piece,
            dst_ref=piece,
            send_sem=r.pass_s.at[member, group * share + step],
            recv_sem=r.pass_r.at[member, group * share + step],
            device_id={"mp": forth.near},
            device_id_type=MESH,
        )

    gain_got = r.gain_got
    gain_cols = gain_got.shape[2]

    def gain_copy(shift):
        to_dp, to_mp, spot = peer(shift)
        return pltpu.make_async_remote_copy(
            src_ref=r.gain_part.at[:, lanes_at(spot * gain_cols, gain_cols)],
            dst_ref=gain_got.at[me],
            send_sem=r.gain_s.at[shift],
            recv_sem=r.gain_r.at[me],
            device_id={"dp": to_dp, "mp": to_mp},
            device_id_type=MESH,
        )

    def gain_arrival(shift):
        from_dp, from_mp, spot = peer(shift)
        return pltpu.make_async_remote_copy(
            src_ref=gain_got.at[spot],
            dst_ref=gain_got.at[spot],
            send_sem=r.gain_s.at[shift],
            recv_sem=r.gain_r.at[spot],
            device_id={"dp": from_dp, "mp": from_mp},
            device_id_type=MESH,
        )

    for shift in range(1, members):
        gain_copy(shift).start()
    for group in range(2):
        for shift in range(1, dp_count):
            member = lax.rem(dp_me + shift, dp_count)
            for pair in range(share // 2):
                step = 2 * pair + forth.low
                from_member(outer_all, outer_sems, member, group, step).wait_recv()
                pass_on(member, group, step).start()
    drain_pass(ins, outs, forth.has_source, forth.has_target)
    for group in range(2):
        for shift in range(1, dp_count):
            member = lax.rem(dp_me + shift, dp_count)
            for pair in range(share // 2):
                pass_on(member, group, 2 * pair + 1 - forth.low).wait_recv()
    drain_pass(ins_back, outs_back, back.has_source, back.has_target)

    @pl.when(back.has_target)
    def _():
        for group in range(2):
            for shift in range(1, mp_count):
                dots_copy(shift, group, True).wait_send()

    total = r.gain_part[:, lanes_at(me * gain_cols, gain_cols)]
    for shift in range(1, members):
        gain_arrival(shift).wait_recv()
        total = total + gain_got[lax.rem(me + shift, members)]
    gain_out[...] = total

    for shift in range(1, members):
        for group in range(2):
            pool_copy(group, shift, True).wait_send()
        gain_copy(shift).wait_send()
    for group in range(2):
        for shift in range(1, dp_count):
            rows_copy(mixture_all, mixture_sems, shift, group, True).wait_send()
            rows_copy(heads_all, heads_sems, shift, group, True).wait_send()
            rows_copy(mixture_all, mixture_sems, shift, group, False).wait_recv()
            rows_copy(heads_all, heads_sems, shift, group, False).wait_recv()

        def drain(block, carry, group=group):
            away = block // share != dp_me

            @pl.when(away)
            def _():
                to_owner(r.normed_out, normed_all, normed_sems, group, block).wait_send()

            @pl.when(jnp.logical_and(away, lax.rem(block, 2) == forth.low))
            def _():
                to_owner(outer_out, outer_all, outer_sems, group, block).wait_send()

            return carry

        lax.fori_loop(0, blocks, drain, 0)
        for shift in range(1, dp_count):
            member = lax.rem(dp_me + shift, dp_count)
            for step in range(share):
                from_member(normed_all, normed_sems, member, group, step).wait_recv()
            for pair in range(share // 2):
                pass_on(member, group, 2 * pair + forth.low).wait_send()


def step_pass(lengths, positives, entrance, gain, table, wq, wk, wv, wo):
    rows, width_all = entrance.shape
    dp_count, mp_count = lax.axis_size("dp"), lax.axis_size("mp")
    members = dp_count * mp_count
    blocks = mp_count * SUB
    width = width_all // blocks
    share = blocks // dp_count
    seq_count = 2 * lengths.shape[0]
    length = rows // seq_count
    query_cols = wq.shape[1]
    head_cols = query_cols + wk.shape[1] + wv.shape[1]
    stacked = query_cols // HEAD * length
    row_pad = -(-(rows // 2) // 128) * 128
    pool_rows = -(-seq_count // 16) * 16
    dma = pltpu.SemaphoreType.DMA
    block = (rows // 2, width)
    shapes = dict(
        head_w=((width_all, head_cols), BF16),
        out_w=(wo.shape, BF16),
        acc=((rows, head_cols), F32),
        squares=((rows, 128), F32),
        inv_ref=((rows, 1), F32),
        pull_ref=((rows, 1), F32),
        query_ref=((seq_count, stacked, HEAD), BF16),
        key_ref=((seq_count, length, HEAD), BF16),
        value_ref=((seq_count, length, HEAD), BF16),
        prob_ref=((seq_count, stacked, length), F32),
        pooled=((2 * members, seq_count // 2, width_all), F32),
        hidden_sum=((seq_count, 1, width_all), F32),
        slopes=((dp_count * seq_count, 1, width_all), F32),
        normed_out=((2 * blocks, *block), BF16),
        outer_out=((2 * blocks, *block), BF16),
        grad_in=((2 * blocks, *block), BF16),
        mix_grad=((rows, query_cols), F32),
        row_dots=((2 * mp_count, 1, row_pad), F32),
        gain_part=((1, width_all), F32),
        gain_got=((members, 1, width_all // members), F32),
        pool_ref=((pool_rows, rows), BF16),
        near_send=((4 * SUB, *block), BF16),
        near_got=((4 * SUB, *block), BF16),
        far_send=((2 * SUB, *block), BF16),
        far_got=((2 * SUB, *block), BF16),
        relay_send=((2 * SUB, *block), BF16),
        keep=((2 * SUB, *block), F32),
        near_send_b=((4 * SUB, *block), BF16),
        near_got_b=((4 * SUB, *block), BF16),
        far_send_b=((2 * SUB, *block), BF16),
        far_got_b=((2 * SUB, *block), BF16),
        relay_send_b=((2 * SUB, *block), BF16),
        keep_b=((2 * SUB, *block), F32),
    )
    counts = dict(
        load_sem=(4,),
        enter_sem=(2 * blocks,),
        pool_s=(2 * members,),
        pool_r=(2 * members,),
        normed_s=(2 * blocks,),
        normed_r=(dp_count, 2 * share),
        outer_s=(2 * blocks,),
        outer_r=(dp_count, 2 * share),
        mixture_s=(2 * dp_count,),
        mixture_r=(2 * dp_count,),
        pass_s=(dp_count, 2 * share),
        pass_r=(dp_count, 2 * share),
        heads_s=(2 * dp_count,),
        heads_r=(2 * dp_count,),
        dots_s=(2 * mp_count,),
        dots_r=(2 * mp_count,),
        gain_s=(members,),
        gain_r=(members,),
        relay_s=(2 * SUB,),
        in_far_s=(2 * SUB,),
        out_far_s=(2 * SUB,),
        in_near_s=(4 * SUB,),
        out_near_s=(4 * SUB,),
        relay_r=(2 * SUB,),
        in_far_r=(2 * SUB,),
        out_far_r=(2 * SUB,),
        in_near_r=(4 * SUB,),
        out_near_r=(4 * SUB,),
        relay_sb=(2 * SUB,),
        in_far_sb=(2 * SUB,),
        out_far_sb=(2 * SUB,),
        in_near_sb=(4 * SUB,),
        out_near_sb=(4 * SUB,),
        relay_rb=(2 * SUB,),
        in_far_rb=(2 * SUB,),
        out_far_rb=(2 * SUB,),
        in_near_rb=(4 * SUB,),
        out_near_rb=(4 * SUB,),
    )
    scratch = Scratch(
        **{name: pltpu.VMEM(*shape) for name, shape in shapes.items()},
        **{name: dma(count) for name, count in counts.items()},
    )
    vmem = pl.BlockSpec(memory_space=pltpu.VMEM)
    smem = pl.BlockSpec(memory_space=pltpu.SMEM)
    hbm = pl.BlockSpec(memory_space=pltpu.HBM)
    return pl.pallas_call(
        step_kernel,
        out_shape=(
            jax.ShapeDtypeStruct((1, WIDTHS), F32),
            jax.ShapeDtypeStruct((1, width_all // members), F32),
            jax.ShapeDtypeStruct((share, dp_count * rows, width), BF16),
            jax.ShapeDtypeStruct((dp_count * rows, query_cols), BF16),
            jax.ShapeDtypeStruct((share, dp_count * rows, width), BF16),
            jax.ShapeDtypeStruct((dp_count * rows, head_cols), BF16),
        ),
        in_specs=[smem, smem, hbm, vmem, vmem, hbm, hbm, hbm, hbm],
        out_specs=(vmem,) * 6,
        scratch_shapes=[pltpu.VMEM((2 * blocks, *block), BF16)] + list(scratch),
        compiler_params=pltpu.CompilerParams(
            collective_id=0, has_side_effects=True, vmem_limit_bytes=36 * 1024 * 1024
        ),
        name="step_pass",
    )(
        *[
            pltpu.with_memory_space_constraint(array, pltpu.HBM)
            for array in (lengths, positives, entrance, gain, table, wq, wk, wv, wo)
        ]
    )


def weight_kernel(
    normed,
    mixture,
    outer,
    heads,
    losses,
    gain_share,
    query_grad,
    key_grad,
    value_grad,
    out_grad,
    losses_out,
    gain_out,
    turned,
):
    query_cols, kv_cols = query_grad.shape[1], key_grad.shape[1]

    @pl.when(pl.program_id(0) == 0)
    def _():
        turned[...] = mixture[...].T
        losses_out[...] = losses[...]
        gain_out[...] = gain_share[...]

    step = pl.program_id(0)
    product = contract_rows(normed[step], heads[...])
    query_grad[...] = product[:, :query_cols]
    key_grad[...] = product[:, query_cols : query_cols + kv_cols]
    value_grad[...] = product[:, query_cols + kv_cols :]
    out_grad[...] = jnp.dot(turned[...], outer[step], preferred_element_type=F32)


def weight_grads(normed, mixture, outer, heads, losses, gain_share, query_cols, kv_cols):
    share, rows, width = normed.shape
    columns = share * width
    vmem = pl.BlockSpec(memory_space=pltpu.VMEM)

    def tall(cols):
        return pl.BlockSpec((width, cols), lambda step: (step, 0))

    return pl.pallas_call(
        weight_kernel,
        grid=(share,),
        in_specs=[vmem] * 6,
        out_specs=(
            tall(query_cols),
            tall(kv_cols),
            tall(kv_cols),
            pl.BlockSpec((query_cols, width), lambda step: (0, step)),
            vmem,
            vmem,
        ),
        out_shape=(
            pltpu.HBM((columns, query_cols), F32),
            pltpu.HBM((columns, kv_cols), F32),
            pltpu.HBM((columns, kv_cols), F32),
            pltpu.HBM((query_cols, columns), F32),
            jax.ShapeDtypeStruct(losses.shape, F32),
            jax.ShapeDtypeStruct(gain_share.shape, F32),
        ),
        scratch_shapes=[pltpu.VMEM((query_cols, rows), BF16)],
        compiler_params=pltpu.CompilerParams(
            dimension_semantics=("arbitrary",), vmem_limit_bytes=16 * 1024 * 1024
        ),
        name="weight_grads",
    )(normed, mixture, outer, heads, losses, gain_share)


def local(entrance, lengths, positives, norm_gains, query_proj, key_proj, value_proj, out_proj):
    length = entrance.shape[2]
    width_all = entrance.shape[3]
    query_cols = query_proj.shape[2]
    kv_cols = key_proj.shape[2]
    losses, gain_share, normed, mixture, outer, heads = step_pass(
        lengths,
        positives,
        entrance.reshape(-1, width_all),
        norm_gains,
        jnp.asarray(rotary_constants(length)),
        query_proj[0],
        key_proj[0],
        value_proj[0],
        out_proj[0],
    )
    query_grad, key_grad, value_grad, out_grad, losses, gain_share = weight_grads(
        normed, mixture, outer, heads, losses, gain_share, query_cols, kv_cols
    )
    return (
        losses,
        gain_share,
        query_grad[None],
        key_grad[None],
        value_grad[None],
        out_grad[None],
    )


def solution(mesh):
    in_specs = (
        P("dp", None, None, None),
        P("dp", None),
        P(),
        P("section", None),
        P("section", None, "mp"),
        P("section", None, "mp"),
        P("section", None, "mp"),
        P("section", "mp", None),
    )
    out_specs = (
        P("section", None),
        P("section", ("dp", "mp")),
        P("section", "dp", "mp"),
        P("section", "dp", "mp"),
        P("section", "dp", "mp"),
        P("section", "mp", "dp"),
    )
    return jax.shard_map(local, mesh=mesh, in_specs=in_specs, out_specs=out_specs, check_vma=False)
```

```python
from typing import NamedTuple

import jax
import jax.numpy as jnp
import numpy as np
from jax import lax
from jax.experimental import pallas as pl
from jax.experimental.pallas import tpu as pltpu
from jax.sharding import PartitionSpec as P

HEAD = 128
WIDTHS = 7


EPSILON = 1e-05
SOFTMAX_TEMPER = 0.05
ROPE_BASE = 500000.0
MESH = pl.DeviceIdType.MESH
ROW_TILE = 16
SUB = 4
PIECES = 2
RELAY, CROSS, TAKE, ATTEND, NEAR, FAR, NEAR_OWN, OWN, FINISH = range(9)
FORWARD_ORDER = (
    (RELAY, 0, 0, 1, 2, 3, 4, 5, 6, 7), (CROSS, 0, 0, 1, 4, 5, 2, 3), (TAKE, 0, 0),
    (RELAY, 1, 0, 1), (CROSS, 0, 6, 7), (TAKE, 0, 2), (RELAY, 1, 2, 3), (TAKE, 0, 1, 3),
    (RELAY, 1, 4, 5), (ATTEND, 0, 0), (NEAR, 0, 0, 1), (RELAY, 1, 6, 7), (NEAR_OWN, 0, 2, 0),
    (NEAR, 0, 2), (CROSS, 1, 0, 1), (NEAR, 0, 3), (FAR, 0, 0), (NEAR_OWN, 0, 1), (FAR, 0, 1),
    (OWN, 0, 0), (CROSS, 1, 2, 3), (TAKE, 1, 0), (CROSS, 1, 4, 5), (FAR, 0, 2, 3), (OWN, 0, 1),
    (CROSS, 1, 6, 7), (TAKE, 1, 1, 2), (FINISH, 0, 0, 1), (TAKE, 1, 3), (ATTEND, 1, 0),
    (FINISH, 0, 2, 3), (NEAR, 1, 0), (NEAR_OWN, 0, 3), (OWN, 0, 2), (NEAR, 1, 1),
    (FINISH, 0, 4, 5), (NEAR_OWN, 1, 0), (FAR, 1, 0), (OWN, 0, 3), (FINISH, 0, 6, 7),
    (NEAR, 1, 2, 3), (FAR, 1, 1), (NEAR_OWN, 1, 2), (FAR, 1, 2), (NEAR_OWN, 1, 1), (FAR, 1, 3),
    (OWN, 1, 0), (FINISH, 1, 0, 1), (NEAR_OWN, 1, 3), (OWN, 1, 1), (FINISH, 1, 2, 3),
    (OWN, 1, 2, 3), (FINISH, 1, 4, 5, 6, 7),
)
BACKWARD_ORDER = (
    (RELAY, 0, 0, 1, 2, 3, 4, 5, 6, 7), (CROSS, 0, 0, 1, 2, 3), (TAKE, 0, 0), (CROSS, 0, 4, 5),
    (TAKE, 0, 1), (CROSS, 0, 6, 7), (TAKE, 0, 2, 3), (ATTEND, 0, 0), (NEAR, 0, 0),
    (NEAR_OWN, 0, 0), (NEAR, 0, 1, 2), (FAR, 0, 0), (NEAR, 0, 3), (FAR, 0, 1, 2),
    (NEAR_OWN, 0, 2, 1), (OWN, 0, 0), (FAR, 0, 3), (FINISH, 0, 0, 1), (RELAY, 1, 0, 1),
    (OWN, 0, 2, 1), (RELAY, 1, 2, 3), (FINISH, 0, 2, 3), (NEAR_OWN, 0, 3), (RELAY, 1, 4, 5),
    (FINISH, 0, 4, 5), (OWN, 0, 3), (RELAY, 1, 6, 7), (FINISH, 0, 6, 7), (CROSS, 1, 0, 1, 2, 3),
    (TAKE, 1, 0), (CROSS, 1, 4, 5), (TAKE, 1, 1), (CROSS, 1, 6, 7), (TAKE, 1, 2, 3),
    (ATTEND, 1, 0), (NEAR, 1, 0, 1), (NEAR_OWN, 1, 0), (NEAR, 1, 3), (FAR, 1, 0), (NEAR, 1, 2),
    (FAR, 1, 1), (OWN, 1, 0), (NEAR_OWN, 1, 1), (FAR, 1, 2, 3), (NEAR_OWN, 1, 2),
    (FINISH, 1, 0, 1), (OWN, 1, 1), (NEAR_OWN, 1, 3), (FINISH, 1, 2, 3), (OWN, 1, 2),
    (FINISH, 1, 4, 5), (OWN, 1, 3), (FINISH, 1, 6, 7),
)
F32 = jnp.float32
BF16 = jnp.bfloat16


def contract_rows(left, right):
    return lax.dot_general(
        left, right, (((0,), (0,)), ((), ())), preferred_element_type=jnp.float32
    )


def contract_last(left, right):
    return lax.dot_general(
        left, right, (((left.ndim - 1,), (1,)), ((), ())), preferred_element_type=jnp.float32
    )


def rotary_constants(length):
    half_size = HEAD // 2
    frequencies = ROPE_BASE ** (-np.arange(half_size, dtype=np.float64) * 2.0 / HEAD)
    angles = np.arange(length, dtype=np.float64)[:, None] * frequencies[None, :]
    cosine = np.concatenate([np.cos(angles), np.cos(angles)], axis=1)
    sine = np.concatenate([-np.sin(angles), np.sin(angles)], axis=1)
    return np.stack([cosine, sine]).astype(np.float32)


def mp_place(me, levels):
    bits = [(me // (1 << level)) % 2 for level in range(levels)]
    partners = [me + (1 - 2 * bits[level]) * (1 << level) for level in range(levels)]
    return bits, partners


def rows_at(start, size):
    return pl.ds(pl.multiple_of(start, ROW_TILE), size)


def lanes_at(start, size):
    return pl.ds(pl.multiple_of(start, 128), size)


class Place:
    def __init__(self, direction):
        self.here = lax.axis_index("section")
        self.count = lax.axis_size("section")
        (self.low, self.high), (self.near, self.far) = mp_place(lax.axis_index("mp"), 2)
        self.direction = direction
        if direction > 0:
            self.has_source, self.has_target = self.here > 0, self.here < self.count - 1
        else:
            self.has_source, self.has_target = self.here < self.count - 1, self.here > 0

    def quarter(self, flip_low, flip_high):
        low = 1 - self.low if flip_low else self.low
        high = 1 - self.high if flip_high else self.high
        return (low * 2 + high) * SUB


def send(source, target, sems, slot, **device):
    return pltpu.make_async_remote_copy(
        src_ref=source,
        dst_ref=target,
        send_sem=sems[0].at[slot],
        recv_sem=sems[1].at[slot],
        device_id=device,
        device_id_type=MESH,
    )


class StreamIn:
    def __init__(self, place, group, buf, relay, far, near):
        self.place, self.buf = place, buf
        self.relay, self.far, self.near = relay, far, near
        self.group = group

    def copy(self, sems, first, step, block, **device):
        rows = self.buf.shape[1] // PIECES
        slot = self.group * 4 * SUB + block + step // PIECES
        piece = self.buf.at[slot, pl.ds(step % PIECES * rows, rows)]
        return send(piece, piece, sems, first * SUB * PIECES + step, **device)

    def relay_copy(self, step):
        own = self.place.quarter(0, 0)
        return self.copy(self.relay, self.group, step, own, section=self.place.here)

    def far_copy(self, step, flip):
        block = self.place.quarter(0, flip)
        return self.copy(self.far, self.group, step, block, mp=self.place.far)

    def near_copy(self, step, low, high):
        block = self.place.quarter(low, high)
        return self.copy(self.near, self.group * 2 + high, step, block, mp=self.place.near)

    def relay_step(self, step):
        self.relay_copy(step).wait_recv()
        self.far_copy(step, 0).start()
        self.near_copy(step, 0, 0).start()

    def cross_step(self, step):
        self.far_copy(step, 1).wait_recv()
        self.near_copy(step, 0, 1).start()

    def settle(self, block):
        for step in range(block * PIECES, (block + 1) * PIECES):
            self.near_copy(step, 1, 0).wait_recv()
            self.near_copy(step, 1, 1).wait_recv()

    def drain(self):
        for step in range(SUB * PIECES):
            self.far_copy(step, 0).wait_send()
            self.near_copy(step, 0, 0).wait_send()
            self.near_copy(step, 0, 1).wait_send()


class StreamOut:
    def __init__(self, place, group, part, finish, dest, bufs, relay, far, near):
        self.place, self.group = place, group
        self.part_of, self.finish_of, self.dest = part, finish, dest
        self.near_send, self.near_got, self.far_send, self.far_got, self.relay_send, self.keep = (
            bufs
        )
        self.relay_sems, self.far_sems, self.near_sems = relay, far, near

    def copy(self, source, target, sems, slot, piece, **device):
        rows = source.shape[1] // PIECES
        span = pl.ds(piece * rows, rows)
        return send(
            source.at[slot, span], target[0].at[target[1], span], sems, slot * PIECES + piece, **device
        )

    def near_copies(self, slot):
        slot = self.group * 2 * SUB + slot
        target = (self.near_got, slot)
        return [
            self.copy(self.near_send, target, self.near_sems, slot, piece, mp=self.place.near)
            for piece in range(PIECES)
        ]

    def far_copy(self, step):
        slot = self.group * SUB + step // PIECES
        target = (self.far_got, slot)
        return self.copy(
            self.far_send, target, self.far_sems, slot, step % PIECES, mp=self.place.far
        )

    def relay_copy(self, step):
        place = self.place
        slot = self.group * SUB + step // PIECES
        target = (self.dest, self.group * 4 * SUB + place.quarter(0, 0) + step // PIECES)
        return self.copy(
            self.relay_send,
            target,
            self.relay_sems,
            slot,
            step % PIECES,
            section=place.here + place.direction,
        )

    def part(self, kind, step):
        flips = {NEAR: (1, 1), NEAR_OWN: (1, 0), FAR: (0, 1), OWN: (0, 0)}[kind]
        return self.part_of(self.group, self.place.quarter(*flips) + step)

    def near(self, flip, step, value):
        slot = (1 - self.place.high if flip else self.place.high) * SUB + step
        self.near_send[self.group * 2 * SUB + slot] = value.astype(BF16)
        for copy in self.near_copies(slot):
            copy.start()

    def arrived(self, slot):
        for copy in self.near_copies(slot):
            copy.wait_recv()
        return self.near_got[self.group * 2 * SUB + slot].astype(F32)

    def far(self, step, value):
        value = value + self.arrived((1 - self.place.high) * SUB + step)
        self.far_send[self.group * SUB + step] = value.astype(BF16)
        for piece in range(PIECES):
            self.far_copy(step * PIECES + piece).start()

    def own(self, step, value):
        value = value + self.arrived(self.place.high * SUB + step)
        self.keep[self.group * SUB + step] = value

    def finish(self, step):
        slot = self.group * SUB + step // PIECES
        block = self.place.quarter(0, 0) + step // PIECES
        rows = self.keep.shape[1] // PIECES
        inner = slice(step % PIECES * rows, (step % PIECES + 1) * rows)
        self.far_copy(step).wait_recv()
        value = self.keep[slot, inner, :] + self.far_got[slot, inner, :].astype(F32)
        self.relay_send[slot, inner, :] = self.finish_of(self.group, block, value, inner)
        self.relay_copy(step).start()

    def drain(self):
        for step in range(SUB * PIECES):
            self.far_copy(step).wait_send()
            self.relay_copy(step).wait_send()
        for slot in range(2 * SUB):
            for copy in self.near_copies(slot):
                copy.wait_send()


def run_pass(order, ins, outs, has_source, has_target, consume, attend, prepare, rest):
    def take(group, step):
        @pl.when(has_source)
        def _():
            ins[group].settle(step)

        for quarter in range(4):
            consume(group, quarter * SUB + step)

    prepared = set()

    def finish(group, step):
        if group not in prepared:
            prepare(group)
            prepared.add(group)
        outs[group].finish(step)

    receive = {
        RELAY: lambda group, step: ins[group].relay_step(step),
        CROSS: lambda group, step: ins[group].cross_step(step),
    }
    produce = {
        NEAR: lambda group, step, value: outs[group].near(1, step, value),
        NEAR_OWN: lambda group, step, value: outs[group].near(0, step, value),
        FAR: lambda group, step, value: outs[group].far(step, value),
        OWN: lambda group, step, value: outs[group].own(step, value),
    }
    for kind, group, *steps in order:
        if kind == ATTEND:
            attend(group)
            if rest is not None:
                pl.when(jnp.logical_not(has_target))(lambda group=group: rest(group))
        elif kind == TAKE:
            for step in steps:
                take(group, step)
        elif kind in receive:

            @pl.when(has_source)
            def _(group=group, steps=steps, action=receive[kind]):
                for step in steps:
                    action(group, step)

        elif kind == FINISH:

            @pl.when(has_target)
            def _(group=group, steps=steps):
                for step in steps:
                    finish(group, step)

        else:

            @pl.when(has_target)
            def _(group=group, steps=steps, kind=kind):
                for step in steps:
                    produce[kind](group, step, outs[group].part(kind, step))


def drain_pass(ins, outs, has_source, has_target):
    @pl.when(has_source)
    def _():
        for flow in ins:
            flow.drain()

    @pl.when(has_target)
    def _():
        for flow in outs:
            flow.drain()


def rotary(values, table, sign):
    turned = pltpu.roll(values, HEAD // 2, axis=1)
    return values * table[0] + turned * (table[1] * sign)


def fold_lanes(values):
    total = values[:, :128]
    for lane in range(1, values.shape[1] // 128):
        total = total + values[:, lane * 128 : (lane + 1) * 128]
    return total


def lane_sum(values):
    return jnp.sum(fold_lanes(values), axis=1, keepdims=True)


def matryoshka(queries, passages, target):
    pairs, width_all = queries.shape
    widths = [width_all >> level for level in range(WIDTHS)]
    bounds = [0] + widths[::-1]
    lane = lax.broadcasted_iota(jnp.int32, (pairs, 128), 1)

    def segment_sums(product):
        sums = []
        for low, high in zip(bounds[:-1], bounds[1:]):
            if high <= 128:
                inside = jnp.logical_and(lane >= low, lane < high)
                piece = jnp.where(inside, product[:, :128], 0.0)
            else:
                piece = fold_lanes(product[:, low:high])
            sums.append(jnp.sum(piece, axis=1, keepdims=True))
        for index in range(1, len(sums)):
            sums[index] = sums[index] + sums[index - 1]
        return sums[::-1]

    query_squares = segment_sums(queries * queries)
    passage_squares = segment_sums(passages * passages)
    dots = [segment_sums(queries * passages[j : j + 1]) for j in range(pairs)]
    losses = []
    mixed = [[] for _ in range(pairs)]
    query_own, passage_own = [], []
    for level, width in enumerate(widths):
        query_inv = lax.rsqrt(query_squares[level] * (1.0 / width) + 1e-06)
        passage_inv = lax.rsqrt(passage_squares[level] * (1.0 / width) + 1e-06)
        factors = [
            query_inv * passage_inv[j : j + 1] * (1.0 / (width * SOFTMAX_TEMPER))
            for j in range(pairs)
        ]
        logits = [dots[j][level] * factors[j] for j in range(pairs)]
        highest = logits[0]
        for j in range(1, pairs):
            highest = jnp.maximum(highest, logits[j])
        powers = [jnp.exp(logits[j] - highest) for j in range(pairs)]
        total = powers[0]
        picked = logits[0] * target[:, 0:1]
        for j in range(1, pairs):
            total = total + powers[j]
            picked = picked + logits[j] * target[:, j : j + 1]
        gap = jnp.log(total) + highest - picked
        losses.append(jnp.sum(gap, axis=0, keepdims=True) * (1.0 / pairs))
        slopes = [
            (powers[j] / total - target[:, j : j + 1]) * (1.0 / pairs) for j in range(pairs)
        ]
        pulls = [slopes[j] * logits[j] for j in range(pairs)]
        row_pull = pulls[0]
        for j in range(1, pairs):
            row_pull = row_pull + pulls[j]
        column_pull = jnp.concatenate(
            [jnp.sum(pulls[j], axis=0, keepdims=True) for j in range(pairs)], axis=0
        )
        for j in range(pairs):
            mixed[j].append(slopes[j] * factors[j])
        query_own.append(row_pull * query_inv * query_inv * (-1.0 / width))
        passage_own.append(column_pull * passage_inv * passage_inv * (-1.0 / width))
    for series in mixed + [query_own, passage_own]:
        for level in range(1, WIDTHS):
            series[level] = series[level] + series[level - 1]
    turned = [
        [
            jnp.concatenate([mixed[j][level][p : p + 1] for j in range(pairs)], axis=0)
            for level in range(WIDTHS)
        ]
        for p in range(pairs)
    ]

    def spread(own, own_rows, weights, rows):
        pieces = []
        low = 0
        while low < width_all:
            inside = [k for k in range(WIDTHS) if low < bounds[k + 1] and low + 128 > bounds[k]]
            high = max(low + 128, bounds[inside[-1] + 1])

            def coefficient(series, inside=inside):
                value = series[WIDTHS - 1 - inside[-1]]
                for k in reversed(inside[:-1]):
                    value = jnp.where(lane < bounds[k + 1], series[WIDTHS - 1 - k], value)
                return value

            def columns(values, low=low, high=high):
                return values[:, low:high]

            piece = coefficient(own) * columns(own_rows)
            for j in range(pairs):
                piece = piece + coefficient(weights[j]) * columns(rows[j : j + 1])
            pieces.append(piece)
            low = high
        return jnp.concatenate(pieces, axis=1)

    return (
        losses,
        spread(query_own, queries, mixed, passages),
        spread(passage_own, passages, turned, queries),
    )


class Scratch(NamedTuple):
    head_w: object
    out_w: object
    acc: object
    squares: object
    inv_ref: object
    query_ref: object
    key_ref: object
    value_ref: object
    prob_ref: object
    pooled: object
    slopes: object
    normed_out: object
    outer_out: object
    grad_in: object
    mix_grad: object
    row_dots: object
    gain_part: object
    hidden_sum: object
    pull_ref: object
    keep: object
    keep_b: object
    gain_got: object
    pool_ref: object
    near_send: object
    near_got: object
    far_send: object
    far_got: object
    relay_send: object
    near_send_b: object
    near_got_b: object
    far_send_b: object
    far_got_b: object
    relay_send_b: object
    load_sem: object
    enter_sem: object
    relay_s: object
    relay_r: object
    in_far_s: object
    in_far_r: object
    in_near_s: object
    in_near_r: object
    out_far_s: object
    out_far_r: object
    out_near_s: object
    out_near_r: object
    relay_sb: object
    relay_rb: object
    in_far_sb: object
    in_far_rb: object
    in_near_sb: object
    in_near_rb: object
    out_far_sb: object
    out_far_rb: object
    out_near_sb: object
    out_near_rb: object
    pool_s: object
    pool_r: object
    normed_s: object
    normed_r: object
    mixture_s: object
    mixture_r: object
    outer_s: object
    outer_r: object
    heads_s: object
    heads_r: object
    dots_s: object
    dots_r: object
    pass_s: object
    pass_r: object
    gain_s: object
    gain_r: object


def step_kernel(
    lengths,
    positives,
    entrance,
    gain,
    table,
    wq,
    wk,
    wv,
    wo,
    losses_out,
    gain_out,
    normed_turned,
    mixture_turned,
    outer_all,
    heads_all,
    hidden,
    normed_all,
    mixture_all,
    *scratch,
):
    r = Scratch(*scratch)
    head_w, out_w, acc, squares = r.head_w, r.out_w, r.acc, r.squares
    forth, back = Place(1), Place(-1)
    rows, width = hidden.shape[1:]
    blocks = hidden.shape[0] // 2
    width_all = blocks * width
    pair_count = lengths.shape[0]
    seq_count = 2 * pair_count
    length = rows // pair_count
    query_cols, kv_cols = wq.shape[3], wk.shape[3]
    groups = query_cols // HEAD
    dp_me, mp_me = lax.axis_index("dp"), lax.axis_index("mp")
    dp_count, mp_count = lax.axis_size("dp"), lax.axis_size("mp")
    members = dp_count * mp_count
    me = dp_me * mp_count + mp_me
    share = blocks // dp_count
    row_pad = r.row_dots.shape[2]
    normed_sems, outer_sems = (r.normed_s, r.normed_r), (r.outer_s, r.outer_r)
    mixture_sems, heads_sems = (r.mixture_s, r.mixture_r), (r.heads_s, r.heads_r)
    outer_out = r.outer_out

    def peer(shift):
        spot = lax.rem(me + shift, members)
        return spot // mp_count, lax.rem(spot, mp_count), spot

    def span_of(group):
        return slice(group * rows, (group + 1) * rows)

    def member_rows(member, group):
        return rows_at((member * 2 + group) * rows, rows)

    def sequences(group):
        for local_seq in range(pair_count):
            inner = slice(local_seq * length, (local_seq + 1) * length)
            outer = slice(group * rows + inner.start, group * rows + inner.stop)
            yield group * pair_count + local_seq, inner, outer

    def count_of(seq):
        return lengths[seq // 2, seq % 2]

    spot = lax.broadcasted_iota(jnp.int32, (length, 1), 0)

    def valid_of(seq):
        return jnp.where(spot < count_of(seq), 1.0, 0.0)

    def load(chunk):
        copies, start = [], 0
        for index, weight in enumerate((wq, wk, wv)):
            columns = pl.ds(start, weight.shape[3])
            copies.append(
                pltpu.make_async_copy(
                    weight.at[:, chunk],
                    head_w.at[:, chunk, :, columns],
                    r.load_sem.at[3 * chunk + index],
                )
            )
            start += weight.shape[3]
        return copies

    load_out = pltpu.make_async_copy(wo, out_w, r.load_sem.at[3 * SUB])

    def enter(group, block):
        slot = group * blocks + block
        return pltpu.make_async_copy(
            entrance.at[pl.ds(group * rows, rows), lanes_at(block * width, width)],
            hidden.at[slot],
            r.enter_sem.at[slot],
        )

    for chunk in range(SUB):
        for copy in load(chunk):
            copy.start()

    @pl.when(jnp.logical_not(forth.has_source))
    def _():
        for group in range(2):
            for block in range(blocks):
                enter(group, block).start()

    load_out.start()
    barrier = pltpu.get_barrier_semaphore()
    for shift in range(1, members):
        to_dp, to_mp, _ = peer(shift)
        pl.semaphore_signal(
            barrier, inc=1, device_id={"dp": to_dp, "mp": to_mp}, device_id_type=MESH
        )

    @pl.when(forth.has_source)
    def _():
        pl.semaphore_signal(
            barrier, inc=1, device_id={"section": forth.here - 1}, device_id_type=MESH
        )

    @pl.when(forth.has_target)
    def _():
        pl.semaphore_signal(
            barrier, inc=1, device_id={"section": forth.here + 1}, device_id_type=MESH
        )

    acc[...] = jnp.zeros_like(acc)
    squares[...] = jnp.zeros_like(squares)
    r.mix_grad[...] = jnp.zeros_like(r.mix_grad)
    r.gain_part[...] = jnp.zeros_like(r.gain_part)

    @pl.when(jnp.logical_not(back.has_source))
    def _():
        def clear(block, carry):
            r.grad_in[block] = jnp.zeros((rows, width), BF16)
            return carry

        lax.fori_loop(0, 2 * blocks, clear, 0)

    pool_shape = r.pool_ref.shape
    column = lax.broadcasted_iota(jnp.int32, pool_shape, 1)
    line = lax.broadcasted_iota(jnp.int32, pool_shape, 0)
    picks = jnp.zeros(pool_shape, F32)
    for seq in range(seq_count):
        inside = jnp.logical_and(column >= seq * length, column < seq * length + count_of(seq))
        picks = jnp.where(jnp.logical_and(line == seq % pair_count, inside), 1.0, picks)
    r.pool_ref[...] = picks.astype(BF16)
    expected = (
        members - 1 + forth.has_source.astype(jnp.int32) + forth.has_target.astype(jnp.int32)
    )

    @pl.when(forth.has_source)
    def _():
        for chunk in range(SUB):
            for copy in load(chunk):
                copy.wait()
        pl.semaphore_wait(barrier, expected)

    def gain_at(block):
        return gain[:, lanes_at(block * width, width)]

    def out_columns(block):
        return out_w[:, lanes_at(block * width, width)]

    def consume(group, block):
        slot = group * blocks + block

        @pl.when(jnp.logical_not(forth.has_source))
        def _():
            enter(group, block).wait()
            if group == 0 and block < SUB:
                for copy in load(block):
                    copy.wait()

        value = hidden[slot].astype(F32)
        span = span_of(group)
        squares[span, :] += fold_lanes(value * value)
        for seq, inner, _ in sequences(group):
            r.hidden_sum[seq, :, lanes_at(block * width, width)] = jnp.sum(
                value[inner] * valid_of(seq), axis=0, keepdims=True
            )
        acc[span, :] += jnp.dot(
            (value * gain_at(block)).astype(BF16),
            head_w[block // SUB, block % SUB],
            preferred_element_type=F32,
        )

    mixture = mixture_all.at[pl.ds(pl.multiple_of(dp_me * 2 * rows, ROW_TILE), 2 * rows)]

    def attend(group):
        whole = span_of(group)
        inv_rms = lax.rsqrt(
            jnp.sum(squares[whole, :], axis=1, keepdims=True) * (1.0 / width_all) + EPSILON
        )
        r.inv_ref[whole, :] = inv_rms
        for seq, inner, span in sequences(group):
            inverse = inv_rms[inner]
            query = jnp.concatenate(
                [
                    rotary(acc[span, g * HEAD : (g + 1) * HEAD] * inverse, table, 1.0)
                    for g in range(groups)
                ],
                axis=0,
            ).astype(BF16)
            key = rotary(acc[span, query_cols : query_cols + kv_cols] * inverse, table, 1.0)
            key = key.astype(BF16)
            value = (acc[span, query_cols + kv_cols :] * inverse).astype(BF16)
            r.query_ref[seq] = query
            r.key_ref[seq] = key
            r.value_ref[seq] = value
            scores = contract_last(query, key) * HEAD ** (-0.5)
            place = lax.broadcasted_iota(jnp.int32, scores.shape, 0) % length
            scores = jnp.where(
                place >= lax.broadcasted_iota(jnp.int32, scores.shape, 1), scores, -1e30
            )
            weights = jnp.exp(scores - jnp.max(scores, axis=1, keepdims=True))
            weights = weights / jnp.sum(weights, axis=1, keepdims=True)
            r.prob_ref[seq] = weights
            mixed = jnp.dot(weights.astype(BF16), value, preferred_element_type=F32).astype(BF16)
            for g in range(groups):
                mixture[span, g * HEAD : (g + 1) * HEAD] = mixed[g * length : (g + 1) * length]
        if group == 0:

            @pl.when(jnp.logical_not(forth.has_source))
            def _():
                pl.semaphore_wait(barrier, expected)

            load_out.wait()

    first = (mp_me == 0).astype(F32)
    pooled = r.pooled

    def pool_copy(group, shift, own):
        other_dp, other_mp, spot = peer(shift)
        member = group * members + (me if own else spot)
        return pltpu.make_async_remote_copy(
            src_ref=pooled.at[member],
            dst_ref=pooled.at[member],
            send_sem=r.pool_s.at[group * members + shift],
            recv_sem=r.pool_r.at[member],
            device_id={"dp": other_dp, "mp": other_mp},
            device_id_type=MESH,
        )

    def send_pooled(group):
        span = span_of(group)
        mixture_sum = jnp.dot(r.pool_ref[:, span], mixture[span, :], preferred_element_type=F32)
        coarse = mixture_sum.astype(BF16)
        fine = (mixture_sum - coarse.astype(F32)).astype(BF16)
        both = jnp.concatenate([coarse, fine], axis=0)

        def pool_block(block, carry):
            sums = jnp.dot(both, out_columns(block), preferred_element_type=F32)
            sums = sums[: pool_shape[0]] + sums[pool_shape[0] :]
            lines = [
                (sums[line : line + 1] + first * r.hidden_sum[seq, :, lanes_at(block * width, width)])
                / count_of(seq).astype(F32)
                for line, (seq, _, _) in enumerate(sequences(group))
            ]
            lines = lines[0] if pair_count == 1 else jnp.concatenate(lines, axis=0)
            pooled[group * members + me, :, lanes_at(block * width, width)] = lines
            return carry

        lax.fori_loop(0, blocks, pool_block, 0, unroll=4)
        for shift in range(1, members):
            pool_copy(group, shift, True).start()

    def part(group, block):
        return jnp.dot(mixture[span_of(group), :], out_columns(block), preferred_element_type=F32)

    def finish(group, block, total, inner):
        return (hidden[group * blocks + block, inner, :].astype(F32) + total).astype(BF16)

    ins = [
        StreamIn(
            forth,
            group,
            hidden,
            (r.relay_s, r.relay_r),
            (r.in_far_s, r.in_far_r),
            (r.in_near_s, r.in_near_r),
        )
        for group in range(2)
    ]
    outs = [
        StreamOut(
            forth,
            group,
            part,
            finish,
            hidden,
            (r.near_send, r.near_got, r.far_send, r.far_got, r.relay_send, r.keep),
            (r.relay_s, r.relay_r),
            (r.out_far_s, r.out_far_r),
            (r.out_near_s, r.out_near_r),
        )
        for group in range(2)
    ]
    run_pass(
        FORWARD_ORDER,
        ins,
        outs,
        forth.has_source,
        forth.has_target,
        consume,
        attend,
        lambda group: None,
        send_pooled,
    )

    @pl.when(forth.has_target)
    def _():
        for group in range(2):
            send_pooled(group)

    def to_owner(source, target, sems, group, block):
        step = lax.rem(block, share)
        return pltpu.make_async_remote_copy(
            src_ref=source.at[group * blocks + block],
            dst_ref=target.at[step, member_rows(dp_me, group)],
            send_sem=sems[0].at[group * blocks + block],
            recv_sem=sems[1].at[dp_me, group * share + step],
            device_id={"dp": block // share},
            device_id_type=MESH,
        )

    def from_member(target, sems, member, group, step):
        piece = target.at[step, member_rows(member, group)]
        return pltpu.make_async_remote_copy(
            src_ref=piece,
            dst_ref=piece,
            send_sem=sems[0].at[0],
            recv_sem=sems[1].at[member, group * share + step],
            device_id={"dp": member},
            device_id_type=MESH,
        )

    def rows_copy(target, sems, shift, group, own):
        other = lax.rem(dp_me + shift, dp_count)
        member = dp_me if own else other
        piece = target.at[member_rows(member, group)]
        return pltpu.make_async_remote_copy(
            src_ref=piece,
            dst_ref=piece,
            send_sem=sems[0].at[group * dp_count + shift],
            recv_sem=sems[1].at[group * dp_count + member],
            device_id={"dp": other},
            device_id_type=MESH,
        )

    def hand_out(value, spare, target, sems, group, block, passes=None):
        mine = block // share == dp_me

        @pl.when(mine)
        def _():
            target[lax.rem(block, share), member_rows(dp_me, group), :] = value

        sends = jnp.logical_not(mine)
        if passes is not None:
            sends = jnp.logical_and(sends, passes)

        @pl.when(sends)
        def _():
            spare[group * blocks + block] = value
            to_owner(spare, target, sems, group, block).start()

    def hand_out_normed():
        for group in range(2):

            def normed_block(block, carry, group=group):
                value = hidden[group * blocks + block].astype(F32) * r.inv_ref[span_of(group), :]
                value = (value * gain_at(block)).astype(BF16)
                hand_out(value, r.normed_out, normed_all, normed_sems, group, block)
                return carry

            lax.fori_loop(0, blocks, normed_block, 0, unroll=2)
            for shift in range(1, dp_count):
                rows_copy(mixture_all, mixture_sems, shift, group, True).start()

    def turn_over():
        for group in range(2):
            for shift in range(1, dp_count):
                member = lax.rem(dp_me + shift, dp_count)
                rows_copy(mixture_all, mixture_sems, shift, group, False).wait_recv()
                for step in range(share):
                    from_member(normed_all, normed_sems, member, group, step).wait_recv()

        def turn(step, carry):
            normed_turned[step] = normed_all[step].T
            return carry

        lax.fori_loop(0, share, turn, 0)
        mixture_turned[...] = mixture_all[...].T

    pl.when(back.has_source)(hand_out_normed)
    for group in range(2):
        for shift in range(1, members):
            pool_copy(group, shift, False).wait_recv()
    embedded = []
    for group in range(2):
        for member in range(dp_count):
            start = group * members + member * mp_count
            total = pooled[start]
            for other in range(1, mp_count):
                total = total + pooled[start + other]
            embedded.append(total)
    pairs = dp_count * pair_count

    def embedding(seq):
        member, inner = seq // seq_count, seq % seq_count
        block = embedded[inner // pair_count * dp_count + member]
        return block[inner % pair_count :][:1]

    queries = jnp.concatenate([embedding(2 * p) for p in range(pairs)], axis=0)
    passages = jnp.concatenate([embedding(2 * p + 1) for p in range(pairs)], axis=0)
    partner = lax.broadcasted_iota(jnp.int32, (pairs, pairs), 1)
    line = lax.broadcasted_iota(jnp.int32, (pairs, pairs), 0)
    target = jnp.zeros((pairs, pairs), F32)
    for p in range(pairs):
        target = jnp.where(jnp.logical_and(line == p, partner == positives[p]), 1.0, target)
    losses, query_slopes, passage_slopes = matryoshka(queries, passages, target)
    lane = lax.broadcasted_iota(jnp.int32, (1, 128), 1)
    packed = jnp.zeros((1, 128), F32)
    for level in range(WIDTHS):
        packed = jnp.where(lane == level, losses[level], packed)
    losses_out[...] = packed[:, :WIDTHS]
    slopes = r.slopes
    for p in range(pairs):
        slopes[2 * p] = query_slopes[p : p + 1]
        slopes[2 * p + 1] = passage_slopes[p : p + 1]

    waits_long = back.here < back.count - 2
    pl.when(waits_long)(turn_over)

    grad_in, mix_grad = r.grad_in, r.mix_grad

    def upstream(group, block):
        tokens = [
            valid_of(seq)
            / count_of(seq).astype(F32)
            * slopes[dp_me * seq_count + seq, :, lanes_at(block * width, width)]
            for seq, _, _ in sequences(group)
        ]
        tokens = tokens[0] if pair_count == 1 else jnp.concatenate(tokens, axis=0)
        return tokens + grad_in[group * blocks + block].astype(F32)

    def consume_back(group, block):
        outer = upstream(group, block).astype(BF16)
        passes = lax.rem(block, 2) == forth.low
        hand_out(outer, outer_out, outer_all, outer_sems, group, block, passes)
        mix_grad[span_of(group), :] += contract_last(outer, out_columns(block))

    head_grads = heads_all.at[pl.ds(pl.multiple_of(dp_me * 2 * rows, ROW_TILE), 2 * rows)]
    row_dots = r.row_dots
    diagonal = lax.broadcasted_iota(jnp.int32, (rows, row_pad), 0) == lax.broadcasted_iota(
        jnp.int32, (rows, row_pad), 1
    )

    def dots_copy(shift, group, own):
        other = lax.rem(mp_me + shift, mp_count)
        member = mp_me if own else other
        piece = row_dots.at[group * mp_count + member]
        return pltpu.make_async_remote_copy(
            src_ref=piece,
            dst_ref=piece,
            send_sem=r.dots_s.at[group * mp_count + shift],
            recv_sem=r.dots_r.at[group * mp_count + member],
            device_id={"mp": other},
            device_id_type=MESH,
        )

    def attend_back(group):
        row_dot = []
        for seq, _, span in sequences(group):
            mixed = jnp.concatenate(
                [mix_grad[span, g * HEAD : (g + 1) * HEAD] for g in range(groups)], axis=0
            ).astype(BF16)
            weights = r.prob_ref[seq]
            value_grad = contract_rows(weights.astype(BF16), mixed).astype(BF16)
            pulled = contract_last(mixed, r.value_ref[seq]).astype(BF16).astype(F32)
            score_grad = weights * (pulled - jnp.sum(weights * pulled, axis=1, keepdims=True))
            score_grad = (score_grad * HEAD ** (-0.5)).astype(BF16)
            query_grad = jnp.dot(score_grad, r.key_ref[seq], preferred_element_type=F32)
            query_grad = query_grad.astype(BF16).astype(F32)
            key_grad = contract_rows(score_grad, r.query_ref[seq]).astype(BF16).astype(F32)
            pieces = [
                rotary(query_grad[g * length : (g + 1) * length], table, -1.0).astype(BF16)
                for g in range(groups)
            ]
            pieces = pieces + [rotary(key_grad, table, -1.0).astype(BF16), value_grad]
            joined = jnp.concatenate(pieces, axis=1)
            head_grads[span, :] = joined
            row_dot.append(lane_sum(joined.astype(F32) * acc[span, :]))
        for shift in range(1, dp_count):
            rows_copy(heads_all, heads_sems, shift, group, True).start()
        row_dot = row_dot[0] if pair_count == 1 else jnp.concatenate(row_dot, axis=0)

        @pl.when(back.has_target)
        def _():
            row_dots[group * mp_count + mp_me] = jnp.sum(
                jnp.where(diagonal, row_dot, 0.0), axis=0, keepdims=True
            )
            for shift in range(1, mp_count):
                dots_copy(shift, group, True).start()

    def part_back(group, block):
        span = span_of(group)
        value = contract_last(head_grads[span, :], head_w[block // SUB, lax.rem(block, SUB)])
        scaled = value * (hidden[group * blocks + block].astype(F32) * r.inv_ref[span, :])
        r.gain_part[:, lanes_at(block * width, width)] += jnp.sum(scaled, axis=0, keepdims=True)
        return value

    def prepare(group):
        for shift in range(1, mp_count):
            dots_copy(shift, group, False).wait_recv()
        total = row_dots[group * mp_count]
        for member in range(1, mp_count):
            total = total + row_dots[group * mp_count + member]
        inverse = r.inv_ref[span_of(group), :]
        r.pull_ref[span_of(group), :] = (
            lane_sum(jnp.where(diagonal, total, 0.0))
            * inverse
            * inverse
            * inverse
            * (1.0 / width_all)
        )

    def finish_back(group, block, total, inner):
        span = slice(group * rows + inner.start, group * rows + inner.stop)
        value = upstream(group, block)[inner] + total * gain_at(block) * r.inv_ref[span, :]
        pulled = hidden[group * blocks + block, inner, :].astype(F32) * r.pull_ref[span, :]
        return (value - pulled).astype(BF16)

    def gain_only(group):
        def body(block, carry):
            part_back(group, block)
            return carry

        lax.fori_loop(0, blocks, body, 0, unroll=4)

    ins_back = [
        StreamIn(
            back,
            group,
            grad_in,
            (r.relay_sb, r.relay_rb),
            (r.in_far_sb, r.in_far_rb),
            (r.in_near_sb, r.in_near_rb),
        )
        for group in range(2)
    ]
    outs_back = [
        StreamOut(
            back,
            group,
            part_back,
            finish_back,
            grad_in,
            (r.near_send_b, r.near_got_b, r.far_send_b, r.far_got_b, r.relay_send_b, r.keep_b),
            (r.relay_sb, r.relay_rb),
            (r.out_far_sb, r.out_far_rb),
            (r.out_near_sb, r.out_near_rb),
        )
        for group in range(2)
    ]
    run_pass(
        BACKWARD_ORDER,
        ins_back,
        outs_back,
        back.has_source,
        back.has_target,
        consume_back,
        attend_back,
        prepare,
        gain_only,
    )

    pl.when(jnp.logical_not(back.has_source))(hand_out_normed)
    pl.when(jnp.logical_not(waits_long))(turn_over)

    def pass_on(member, group, step):
        piece = outer_all.at[step, member_rows(member, group)]
        return pltpu.make_async_remote_copy(
            src_ref=piece,
            dst_ref=piece,
            send_sem=r.pass_s.at[member, group * share + step],
            recv_sem=r.pass_r.at[member, group * share + step],
            device_id={"mp": forth.near},
            device_id_type=MESH,
        )

    gain_got = r.gain_got
    gain_cols = gain_got.shape[2]

    def gain_copy(shift):
        to_dp, to_mp, spot = peer(shift)
        return pltpu.make_async_remote_copy(
            src_ref=r.gain_part.at[:, lanes_at(spot * gain_cols, gain_cols)],
            dst_ref=gain_got.at[me],
            send_sem=r.gain_s.at[shift],
            recv_sem=r.gain_r.at[me],
            device_id={"dp": to_dp, "mp": to_mp},
            device_id_type=MESH,
        )

    def gain_arrival(shift):
        from_dp, from_mp, spot = peer(shift)
        return pltpu.make_async_remote_copy(
            src_ref=gain_got.at[spot],
            dst_ref=gain_got.at[spot],
            send_sem=r.gain_s.at[shift],
            recv_sem=r.gain_r.at[spot],
            device_id={"dp": from_dp, "mp": from_mp},
            device_id_type=MESH,
        )

    for shift in range(1, members):
        gain_copy(shift).start()
    for group in range(2):
        for shift in range(1, dp_count):
            member = lax.rem(dp_me + shift, dp_count)
            for pair in range(share // 2):
                step = 2 * pair + forth.low
                from_member(outer_all, outer_sems, member, group, step).wait_recv()
                pass_on(member, group, step).start()
    drain_pass(ins, outs, forth.has_source, forth.has_target)
    for group in range(2):
        for shift in range(1, dp_count):
            member = lax.rem(dp_me + shift, dp_count)
            for pair in range(share // 2):
                pass_on(member, group, 2 * pair + 1 - forth.low).wait_recv()
    drain_pass(ins_back, outs_back, back.has_source, back.has_target)

    @pl.when(back.has_target)
    def _():
        for group in range(2):
            for shift in range(1, mp_count):
                dots_copy(shift, group, True).wait_send()

    total = r.gain_part[:, lanes_at(me * gain_cols, gain_cols)]
    for shift in range(1, members):
        gain_arrival(shift).wait_recv()
        total = total + gain_got[lax.rem(me + shift, members)]
    gain_out[...] = total

    for shift in range(1, members):
        for group in range(2):
            pool_copy(group, shift, True).wait_send()
        gain_copy(shift).wait_send()
    for group in range(2):
        for shift in range(1, dp_count):
            rows_copy(mixture_all, mixture_sems, shift, group, True).wait_send()
            rows_copy(heads_all, heads_sems, shift, group, True).wait_send()
            rows_copy(heads_all, heads_sems, shift, group, False).wait_recv()

        def drain(block, carry, group=group):
            away = block // share != dp_me

            @pl.when(away)
            def _():
                to_owner(r.normed_out, normed_all, normed_sems, group, block).wait_send()

            @pl.when(jnp.logical_and(away, lax.rem(block, 2) == forth.low))
            def _():
                to_owner(outer_out, outer_all, outer_sems, group, block).wait_send()

            return carry

        lax.fori_loop(0, blocks, drain, 0)
        for shift in range(1, dp_count):
            member = lax.rem(dp_me + shift, dp_count)
            for pair in range(share // 2):
                pass_on(member, group, 2 * pair + forth.low).wait_send()


def step_pass(lengths, positives, entrance, gain, table, wq, wk, wv, wo):
    rows, width_all = entrance.shape
    dp_count, mp_count = lax.axis_size("dp"), lax.axis_size("mp")
    members = dp_count * mp_count
    blocks = mp_count * SUB
    width = width_all // blocks
    share = blocks // dp_count
    seq_count = 2 * lengths.shape[0]
    length = rows // seq_count
    query_cols = wq.shape[1]
    head_cols = query_cols + wk.shape[1] + wv.shape[1]
    stacked = query_cols // HEAD * length
    row_pad = -(-(rows // 2) // 128) * 128
    pool_rows = -(-seq_count // 16) * 16
    head_weights = [weight.reshape(mp_count, SUB, width, -1) for weight in (wq, wk, wv)]
    dma = pltpu.SemaphoreType.DMA
    block = (rows // 2, width)
    shapes = dict(
        head_w=((mp_count, SUB, width, head_cols), BF16),
        out_w=(wo.shape, BF16),
        acc=((rows, head_cols), F32),
        squares=((rows, 128), F32),
        inv_ref=((rows, 1), F32),
        pull_ref=((rows, 1), F32),
        query_ref=((seq_count, stacked, HEAD), BF16),
        key_ref=((seq_count, length, HEAD), BF16),
        value_ref=((seq_count, length, HEAD), BF16),
        prob_ref=((seq_count, stacked, length), F32),
        pooled=((2 * members, seq_count // 2, width_all), F32),
        hidden_sum=((seq_count, 1, width_all), F32),
        slopes=((dp_count * seq_count, 1, width_all), F32),
        normed_out=((2 * blocks, *block), BF16),
        outer_out=((2 * blocks, *block), BF16),
        grad_in=((2 * blocks, *block), BF16),
        mix_grad=((rows, query_cols), F32),
        row_dots=((2 * mp_count, 1, row_pad), F32),
        gain_part=((1, width_all), F32),
        gain_got=((members, 1, width_all // members), F32),
        pool_ref=((pool_rows, rows), BF16),
        near_send=((4 * SUB, *block), BF16),
        near_got=((4 * SUB, *block), BF16),
        far_send=((2 * SUB, *block), BF16),
        far_got=((2 * SUB, *block), BF16),
        relay_send=((2 * SUB, *block), BF16),
        keep=((2 * SUB, *block), F32),
        near_send_b=((4 * SUB, *block), BF16),
        near_got_b=((4 * SUB, *block), BF16),
        far_send_b=((2 * SUB, *block), BF16),
        far_got_b=((2 * SUB, *block), BF16),
        relay_send_b=((2 * SUB, *block), BF16),
        keep_b=((2 * SUB, *block), F32),
    )
    counts = dict(
        load_sem=(3 * SUB + 1,),
        enter_sem=(2 * blocks,),
        pool_s=(2 * members,),
        pool_r=(2 * members,),
        normed_s=(2 * blocks,),
        normed_r=(dp_count, 2 * share),
        outer_s=(2 * blocks,),
        outer_r=(dp_count, 2 * share),
        mixture_s=(2 * dp_count,),
        mixture_r=(2 * dp_count,),
        pass_s=(dp_count, 2 * share),
        pass_r=(dp_count, 2 * share),
        heads_s=(2 * dp_count,),
        heads_r=(2 * dp_count,),
        dots_s=(2 * mp_count,),
        dots_r=(2 * mp_count,),
        gain_s=(members,),
        gain_r=(members,),
        relay_s=(2 * SUB * PIECES,),
        in_far_s=(2 * SUB * PIECES,),
        out_far_s=(2 * SUB * PIECES,),
        in_near_s=(4 * SUB * PIECES,),
        out_near_s=(4 * SUB * PIECES,),
        relay_r=(2 * SUB * PIECES,),
        in_far_r=(2 * SUB * PIECES,),
        out_far_r=(2 * SUB * PIECES,),
        in_near_r=(4 * SUB * PIECES,),
        out_near_r=(4 * SUB * PIECES,),
        relay_sb=(2 * SUB * PIECES,),
        in_far_sb=(2 * SUB * PIECES,),
        out_far_sb=(2 * SUB * PIECES,),
        in_near_sb=(4 * SUB * PIECES,),
        out_near_sb=(4 * SUB * PIECES,),
        relay_rb=(2 * SUB * PIECES,),
        in_far_rb=(2 * SUB * PIECES,),
        out_far_rb=(2 * SUB * PIECES,),
        in_near_rb=(4 * SUB * PIECES,),
        out_near_rb=(4 * SUB * PIECES,),
    )
    scratch = Scratch(
        **{name: pltpu.VMEM(*shape) for name, shape in shapes.items()},
        **{name: dma(count) for name, count in counts.items()},
    )
    vmem = pl.BlockSpec(memory_space=pltpu.VMEM)
    smem = pl.BlockSpec(memory_space=pltpu.SMEM)
    hbm = pl.BlockSpec(memory_space=pltpu.HBM)
    return pl.pallas_call(
        step_kernel,
        out_shape=(
            jax.ShapeDtypeStruct((1, WIDTHS), F32),
            jax.ShapeDtypeStruct((1, width_all // members), F32),
            jax.ShapeDtypeStruct((share, width, dp_count * rows), BF16),
            jax.ShapeDtypeStruct((query_cols, dp_count * rows), BF16),
            jax.ShapeDtypeStruct((share, dp_count * rows, width), BF16),
            jax.ShapeDtypeStruct((dp_count * rows, head_cols), BF16),
        ),
        in_specs=[smem, smem, hbm, vmem, vmem, hbm, hbm, hbm, hbm],
        out_specs=(vmem,) * 6,
        scratch_shapes=[
            pltpu.VMEM((2 * blocks, *block), BF16),
            pltpu.VMEM((share, dp_count * rows, width), BF16),
            pltpu.VMEM((dp_count * rows, query_cols), BF16),
            *scratch,
        ],
        compiler_params=pltpu.CompilerParams(
            collective_id=0, has_side_effects=True, vmem_limit_bytes=36 * 1024 * 1024
        ),
        name="step_pass",
    )(
        *[
            pltpu.with_memory_space_constraint(array, pltpu.HBM)
            for array in (lengths, positives, entrance, gain, table, *head_weights, wo)
        ]
    )


def weight_kernel(
    normed,
    mixture,
    outer,
    heads,
    losses,
    gain_share,
    query_grad,
    key_grad,
    value_grad,
    out_grad,
    losses_out,
    gain_out,
):
    query_cols, kv_cols = query_grad.shape[1], key_grad.shape[1]

    @pl.when(pl.program_id(0) == 0)
    def _():
        losses_out[...] = losses[...]
        gain_out[...] = gain_share[...]

    step = pl.program_id(0)
    product = jnp.dot(normed[step], heads[...], preferred_element_type=F32)
    query_grad[...] = product[:, :query_cols]
    key_grad[...] = product[:, query_cols : query_cols + kv_cols]
    value_grad[...] = product[:, query_cols + kv_cols :]
    out_grad[...] = jnp.dot(mixture[...], outer[step], preferred_element_type=F32)


def weight_grads(normed, mixture, outer, heads, losses, gain_share, query_cols, kv_cols):
    share, width, _ = normed.shape
    columns = share * width
    vmem = pl.BlockSpec(memory_space=pltpu.VMEM)

    def tall(cols):
        return pl.BlockSpec((width, cols), lambda step: (step, 0))

    return pl.pallas_call(
        weight_kernel,
        grid=(share,),
        in_specs=[vmem] * 6,
        out_specs=(
            tall(query_cols),
            tall(kv_cols),
            tall(kv_cols),
            pl.BlockSpec((query_cols, width), lambda step: (0, step)),
            vmem,
            vmem,
        ),
        out_shape=(
            pltpu.HBM((columns, query_cols), F32),
            pltpu.HBM((columns, kv_cols), F32),
            pltpu.HBM((columns, kv_cols), F32),
            pltpu.HBM((query_cols, columns), F32),
            jax.ShapeDtypeStruct(losses.shape, F32),
            jax.ShapeDtypeStruct(gain_share.shape, F32),
        ),
        compiler_params=pltpu.CompilerParams(
            dimension_semantics=("arbitrary",), vmem_limit_bytes=16 * 1024 * 1024
        ),
        name="weight_grads",
    )(normed, mixture, outer, heads, losses, gain_share)


def local(entrance, lengths, positives, norm_gains, query_proj, key_proj, value_proj, out_proj):
    length = entrance.shape[2]
    width_all = entrance.shape[3]
    query_cols = query_proj.shape[2]
    kv_cols = key_proj.shape[2]
    losses, gain_share, normed, mixture, outer, heads = step_pass(
        lengths,
        positives,
        entrance.reshape(-1, width_all),
        norm_gains,
        jnp.asarray(rotary_constants(length)),
        query_proj[0],
        key_proj[0],
        value_proj[0],
        out_proj[0],
    )
    query_grad, key_grad, value_grad, out_grad, losses, gain_share = weight_grads(
        normed, mixture, outer, heads, losses, gain_share, query_cols, kv_cols
    )
    return (
        losses,
        gain_share,
        query_grad[None],
        key_grad[None],
        value_grad[None],
        out_grad[None],
    )


def solution(mesh):
    in_specs = (
        P("dp", None, None, None),
        P("dp", None),
        P(),
        P("section", None),
        P("section", None, "mp"),
        P("section", None, "mp"),
        P("section", None, "mp"),
        P("section", "mp", None),
    )
    out_specs = (
        P("section", None),
        P("section", ("dp", "mp")),
        P("section", "dp", "mp"),
        P("section", "dp", "mp"),
        P("section", "dp", "mp"),
        P("section", "mp", "dp"),
    )
    return jax.shard_map(local, mesh=mesh, in_specs=in_specs, out_specs=out_specs, check_vma=False)
```

```python
from typing import NamedTuple

import jax
import jax.numpy as jnp
import numpy as np
from jax import lax
from jax.experimental import pallas as pl
from jax.experimental.pallas import tpu as pltpu
from jax.sharding import PartitionSpec as P

HEAD = 128
WIDTHS = 7


EPSILON = 1e-05
SOFTMAX_TEMPER = 0.05
ROPE_BASE = 500000.0
MESH = pl.DeviceIdType.MESH
ROW_TILE = 16
SUB = 4
PIECES = 2
RELAY, CROSS, TAKE, ATTEND, NEAR, FAR, NEAR_OWN, OWN, FINISH = range(9)
FORWARD_ORDER = (
    (RELAY, 0, 0, 1, 2, 3, 4, 5, 6, 7), (CROSS, 0, 0, 1, 4, 5, 2, 3), (TAKE, 0, 0),
    (RELAY, 1, 0, 1), (CROSS, 0, 6, 7), (TAKE, 0, 2), (RELAY, 1, 2, 3), (TAKE, 0, 1, 3),
    (RELAY, 1, 4, 5), (ATTEND, 0, 0), (NEAR, 0, 0, 1), (RELAY, 1, 6, 7), (NEAR_OWN, 0, 2, 0),
    (NEAR, 0, 2), (CROSS, 1, 0, 1), (NEAR, 0, 3), (FAR, 0, 0), (NEAR_OWN, 0, 1), (FAR, 0, 1),
    (OWN, 0, 0), (CROSS, 1, 2, 3), (TAKE, 1, 0), (CROSS, 1, 4, 5), (FAR, 0, 2, 3), (OWN, 0, 1),
    (CROSS, 1, 6, 7), (TAKE, 1, 1, 2), (FINISH, 0, 0, 1), (TAKE, 1, 3), (ATTEND, 1, 0),
    (FINISH, 0, 2, 3), (NEAR, 1, 0), (NEAR_OWN, 0, 3), (OWN, 0, 2), (NEAR, 1, 1),
    (FINISH, 0, 4, 5), (NEAR_OWN, 1, 0), (FAR, 1, 0), (OWN, 0, 3), (FINISH, 0, 6, 7),
    (NEAR, 1, 2, 3), (FAR, 1, 1), (NEAR_OWN, 1, 2), (FAR, 1, 2), (NEAR_OWN, 1, 1), (FAR, 1, 3),
    (OWN, 1, 0), (FINISH, 1, 0, 1), (NEAR_OWN, 1, 3), (OWN, 1, 1), (FINISH, 1, 2, 3),
    (OWN, 1, 2, 3), (FINISH, 1, 4, 5, 6, 7),
)
BACKWARD_ORDER = (
    (RELAY, 0, 0, 1, 2, 3, 4, 5, 6, 7), (CROSS, 0, 0, 1, 2, 3), (TAKE, 0, 0), (CROSS, 0, 4, 5),
    (TAKE, 0, 1), (CROSS, 0, 6, 7), (TAKE, 0, 2, 3), (ATTEND, 0, 0), (NEAR, 0, 0),
    (NEAR_OWN, 0, 0), (NEAR, 0, 1, 2), (FAR, 0, 0), (NEAR, 0, 3), (FAR, 0, 1, 2),
    (NEAR_OWN, 0, 2, 1), (OWN, 0, 0), (FAR, 0, 3), (FINISH, 0, 0, 1), (RELAY, 1, 0, 1),
    (OWN, 0, 2, 1), (RELAY, 1, 2, 3), (FINISH, 0, 2, 3), (NEAR_OWN, 0, 3), (RELAY, 1, 4, 5),
    (FINISH, 0, 4, 5), (OWN, 0, 3), (RELAY, 1, 6, 7), (FINISH, 0, 6, 7), (CROSS, 1, 0, 1, 2, 3),
    (TAKE, 1, 0), (CROSS, 1, 4, 5), (TAKE, 1, 1), (CROSS, 1, 6, 7), (TAKE, 1, 2, 3),
    (ATTEND, 1, 0), (NEAR, 1, 0, 1), (NEAR_OWN, 1, 0), (NEAR, 1, 3), (FAR, 1, 0), (NEAR, 1, 2),
    (FAR, 1, 1), (OWN, 1, 0), (NEAR_OWN, 1, 1), (FAR, 1, 2, 3), (NEAR_OWN, 1, 2),
    (FINISH, 1, 0, 1), (OWN, 1, 1), (NEAR_OWN, 1, 3), (FINISH, 1, 2, 3), (OWN, 1, 2),
    (FINISH, 1, 4, 5), (OWN, 1, 3), (FINISH, 1, 6, 7),
)
F32 = jnp.float32
BF16 = jnp.bfloat16


def contract_rows(left, right):
    return lax.dot_general(
        left, right, (((0,), (0,)), ((), ())), preferred_element_type=jnp.float32
    )


def contract_last(left, right):
    return lax.dot_general(
        left, right, (((left.ndim - 1,), (1,)), ((), ())), preferred_element_type=jnp.float32
    )


def rotary_constants(length):
    half_size = HEAD // 2
    frequencies = ROPE_BASE ** (-np.arange(half_size, dtype=np.float64) * 2.0 / HEAD)
    angles = np.arange(length, dtype=np.float64)[:, None] * frequencies[None, :]
    cosine = np.concatenate([np.cos(angles), np.cos(angles)], axis=1)
    sine = np.concatenate([-np.sin(angles), np.sin(angles)], axis=1)
    return np.stack([cosine, sine]).astype(np.float32)


def mp_place(me, levels):
    bits = [(me // (1 << level)) % 2 for level in range(levels)]
    partners = [me + (1 - 2 * bits[level]) * (1 << level) for level in range(levels)]
    return bits, partners


def rows_at(start, size):
    return pl.ds(pl.multiple_of(start, ROW_TILE), size)


def lanes_at(start, size):
    return pl.ds(pl.multiple_of(start, 128), size)


class Place:
    def __init__(self, direction):
        self.here = lax.axis_index("section")
        self.count = lax.axis_size("section")
        (self.low, self.high), (self.near, self.far) = mp_place(lax.axis_index("mp"), 2)
        self.direction = direction
        if direction > 0:
            self.has_source, self.has_target = self.here > 0, self.here < self.count - 1
        else:
            self.has_source, self.has_target = self.here < self.count - 1, self.here > 0

    def quarter(self, flip_low, flip_high):
        low = 1 - self.low if flip_low else self.low
        high = 1 - self.high if flip_high else self.high
        return (low * 2 + high) * SUB


def send(source, target, sems, slot, **device):
    return pltpu.make_async_remote_copy(
        src_ref=source,
        dst_ref=target,
        send_sem=sems[0].at[slot],
        recv_sem=sems[1].at[slot],
        device_id=device,
        device_id_type=MESH,
    )


class StreamIn:
    def __init__(self, place, group, buf, relay, far, near):
        self.place, self.buf = place, buf
        self.relay, self.far, self.near = relay, far, near
        self.group = group

    def copy(self, sems, first, step, block, **device):
        rows = self.buf.shape[1] // PIECES
        slot = self.group * 4 * SUB + block + step // PIECES
        piece = self.buf.at[slot, pl.ds(step % PIECES * rows, rows)]
        return send(piece, piece, sems, first * SUB * PIECES + step, **device)

    def relay_copy(self, step):
        own = self.place.quarter(0, 0)
        return self.copy(self.relay, self.group, step, own, section=self.place.here)

    def far_copy(self, step, flip):
        block = self.place.quarter(0, flip)
        return self.copy(self.far, self.group, step, block, mp=self.place.far)

    def near_copy(self, step, low, high):
        block = self.place.quarter(low, high)
        return self.copy(self.near, self.group * 2 + high, step, block, mp=self.place.near)

    def relay_step(self, step):
        self.relay_copy(step).wait_recv()
        self.far_copy(step, 0).start()
        self.near_copy(step, 0, 0).start()

    def cross_step(self, step):
        self.far_copy(step, 1).wait_recv()
        self.near_copy(step, 0, 1).start()

    def settle(self, block):
        for step in range(block * PIECES, (block + 1) * PIECES):
            self.near_copy(step, 1, 0).wait_recv()
            self.near_copy(step, 1, 1).wait_recv()

    def drain(self):
        for step in range(SUB * PIECES):
            self.far_copy(step, 0).wait_send()
            self.near_copy(step, 0, 0).wait_send()
            self.near_copy(step, 0, 1).wait_send()


class StreamOut:
    def __init__(self, place, group, part, finish, dest, bufs, relay, far, near):
        self.place, self.group = place, group
        self.part_of, self.finish_of, self.dest = part, finish, dest
        self.near_send, self.near_got, self.far_send, self.far_got, self.relay_send, self.keep = (
            bufs
        )
        self.relay_sems, self.far_sems, self.near_sems = relay, far, near

    def copy(self, source, target, sems, slot, piece, **device):
        rows = source.shape[1] // PIECES
        span = pl.ds(piece * rows, rows)
        return send(
            source.at[slot, span], target[0].at[target[1], span], sems, slot * PIECES + piece, **device
        )

    def near_copies(self, slot):
        slot = self.group * 2 * SUB + slot
        target = (self.near_got, slot)
        return [
            self.copy(self.near_send, target, self.near_sems, slot, piece, mp=self.place.near)
            for piece in range(PIECES)
        ]

    def far_copy(self, step):
        slot = self.group * SUB + step // PIECES
        target = (self.far_got, slot)
        return self.copy(
            self.far_send, target, self.far_sems, slot, step % PIECES, mp=self.place.far
        )

    def relay_copy(self, step):
        place = self.place
        slot = self.group * SUB + step // PIECES
        target = (self.dest, self.group * 4 * SUB + place.quarter(0, 0) + step // PIECES)
        return self.copy(
            self.relay_send,
            target,
            self.relay_sems,
            slot,
            step % PIECES,
            section=place.here + place.direction,
        )

    def part(self, kind, step):
        flips = {NEAR: (1, 1), NEAR_OWN: (1, 0), FAR: (0, 1), OWN: (0, 0)}[kind]
        return self.part_of(self.group, self.place.quarter(*flips) + step)

    def near(self, flip, step, value):
        slot = (1 - self.place.high if flip else self.place.high) * SUB + step
        self.near_send[self.group * 2 * SUB + slot] = value.astype(BF16)
        for copy in self.near_copies(slot):
            copy.start()

    def arrived(self, slot):
        for copy in self.near_copies(slot):
            copy.wait_recv()
        return self.near_got[self.group * 2 * SUB + slot].astype(F32)

    def far(self, step, value):
        value = value + self.arrived((1 - self.place.high) * SUB + step)
        self.far_send[self.group * SUB + step] = value.astype(BF16)
        for piece in range(PIECES):
            self.far_copy(step * PIECES + piece).start()

    def own(self, step, value):
        value = value + self.arrived(self.place.high * SUB + step)
        self.keep[self.group * SUB + step] = value

    def finish(self, step):
        slot = self.group * SUB + step // PIECES
        block = self.place.quarter(0, 0) + step // PIECES
        rows = self.keep.shape[1] // PIECES
        inner = slice(step % PIECES * rows, (step % PIECES + 1) * rows)
        self.far_copy(step).wait_recv()
        value = self.keep[slot, inner, :] + self.far_got[slot, inner, :].astype(F32)
        self.relay_send[slot, inner, :] = self.finish_of(self.group, block, value, inner)
        self.relay_copy(step).start()

    def drain(self):
        for step in range(SUB * PIECES):
            self.far_copy(step).wait_send()
            self.relay_copy(step).wait_send()
        for slot in range(2 * SUB):
            for copy in self.near_copies(slot):
                copy.wait_send()


def run_pass(order, ins, outs, has_source, has_target, consume, attend, prepare, rest):
    def take(group, step):
        @pl.when(has_source)
        def _():
            ins[group].settle(step)

        for quarter in range(4):
            consume(group, quarter * SUB + step)

    prepared = set()

    def finish(group, step):
        if group not in prepared:
            prepare(group)
            prepared.add(group)
        outs[group].finish(step)

    receive = {
        RELAY: lambda group, step: ins[group].relay_step(step),
        CROSS: lambda group, step: ins[group].cross_step(step),
    }
    produce = {
        NEAR: lambda group, step, value: outs[group].near(1, step, value),
        NEAR_OWN: lambda group, step, value: outs[group].near(0, step, value),
        FAR: lambda group, step, value: outs[group].far(step, value),
        OWN: lambda group, step, value: outs[group].own(step, value),
    }
    for kind, group, *steps in order:
        if kind == ATTEND:
            attend(group)
            if rest is not None:
                pl.when(jnp.logical_not(has_target))(lambda group=group: rest(group))
        elif kind == TAKE:
            for step in steps:
                take(group, step)
        elif kind in receive:

            @pl.when(has_source)
            def _(group=group, steps=steps, action=receive[kind]):
                for step in steps:
                    action(group, step)

        elif kind == FINISH:

            @pl.when(has_target)
            def _(group=group, steps=steps):
                for step in steps:
                    finish(group, step)

        else:

            @pl.when(has_target)
            def _(group=group, steps=steps, kind=kind):
                for step in steps:
                    produce[kind](group, step, outs[group].part(kind, step))


def drain_pass(ins, outs, has_source, has_target):
    @pl.when(has_source)
    def _():
        for flow in ins:
            flow.drain()

    @pl.when(has_target)
    def _():
        for flow in outs:
            flow.drain()


def rotary(values, table, sign):
    turned = pltpu.roll(values, HEAD // 2, axis=1)
    return values * table[0] + turned * (table[1] * sign)


def fold_lanes(values):
    total = values[:, :128]
    for lane in range(1, values.shape[1] // 128):
        total = total + values[:, lane * 128 : (lane + 1) * 128]
    return total


def lane_sum(values):
    return jnp.sum(fold_lanes(values), axis=1, keepdims=True)


def matryoshka(queries, passages, target):
    pairs, width_all = queries.shape
    widths = [width_all >> level for level in range(WIDTHS)]
    bounds = [0] + widths[::-1]
    lane = lax.broadcasted_iota(jnp.int32, (pairs, 128), 1)

    def segment_sums(product):
        sums = []
        for low, high in zip(bounds[:-1], bounds[1:]):
            if high <= 128:
                inside = jnp.logical_and(lane >= low, lane < high)
                piece = jnp.where(inside, product[:, :128], 0.0)
            else:
                piece = fold_lanes(product[:, low:high])
            sums.append(jnp.sum(piece, axis=1, keepdims=True))
        for index in range(1, len(sums)):
            sums[index] = sums[index] + sums[index - 1]
        return sums[::-1]

    query_squares = segment_sums(queries * queries)
    passage_squares = segment_sums(passages * passages)
    dots = [segment_sums(queries * passages[j : j + 1]) for j in range(pairs)]
    losses = []
    mixed = [[] for _ in range(pairs)]
    query_own, passage_own = [], []
    for level, width in enumerate(widths):
        query_inv = lax.rsqrt(query_squares[level] * (1.0 / width) + 1e-06)
        passage_inv = lax.rsqrt(passage_squares[level] * (1.0 / width) + 1e-06)
        factors = [
            query_inv * passage_inv[j : j + 1] * (1.0 / (width * SOFTMAX_TEMPER))
            for j in range(pairs)
        ]
        logits = [dots[j][level] * factors[j] for j in range(pairs)]
        highest = logits[0]
        for j in range(1, pairs):
            highest = jnp.maximum(highest, logits[j])
        powers = [jnp.exp(logits[j] - highest) for j in range(pairs)]
        total = powers[0]
        picked = logits[0] * target[:, 0:1]
        for j in range(1, pairs):
            total = total + powers[j]
            picked = picked + logits[j] * target[:, j : j + 1]
        gap = jnp.log(total) + highest - picked
        losses.append(jnp.sum(gap, axis=0, keepdims=True) * (1.0 / pairs))
        slopes = [
            (powers[j] / total - target[:, j : j + 1]) * (1.0 / pairs) for j in range(pairs)
        ]
        pulls = [slopes[j] * logits[j] for j in range(pairs)]
        row_pull = pulls[0]
        for j in range(1, pairs):
            row_pull = row_pull + pulls[j]
        column_pull = jnp.concatenate(
            [jnp.sum(pulls[j], axis=0, keepdims=True) for j in range(pairs)], axis=0
        )
        for j in range(pairs):
            mixed[j].append(slopes[j] * factors[j])
        query_own.append(row_pull * query_inv * query_inv * (-1.0 / width))
        passage_own.append(column_pull * passage_inv * passage_inv * (-1.0 / width))
    for series in mixed + [query_own, passage_own]:
        for level in range(1, WIDTHS):
            series[level] = series[level] + series[level - 1]
    turned = [
        [
            jnp.concatenate([mixed[j][level][p : p + 1] for j in range(pairs)], axis=0)
            for level in range(WIDTHS)
        ]
        for p in range(pairs)
    ]

    def spread(own, own_rows, weights, rows):
        pieces = []
        low = 0
        while low < width_all:
            inside = [k for k in range(WIDTHS) if low < bounds[k + 1] and low + 128 > bounds[k]]
            high = max(low + 128, bounds[inside[-1] + 1])

            def coefficient(series, inside=inside):
                value = series[WIDTHS - 1 - inside[-1]]
                for k in reversed(inside[:-1]):
                    value = jnp.where(lane < bounds[k + 1], series[WIDTHS - 1 - k], value)
                return value

            def columns(values, low=low, high=high):
                return values[:, low:high]

            piece = coefficient(own) * columns(own_rows)
            for j in range(pairs):
                piece = piece + coefficient(weights[j]) * columns(rows[j : j + 1])
            pieces.append(piece)
            low = high
        return jnp.concatenate(pieces, axis=1)

    return (
        losses,
        spread(query_own, queries, mixed, passages),
        spread(passage_own, passages, turned, queries),
    )


class Scratch(NamedTuple):
    head_w: object
    out_w: object
    acc: object
    squares: object
    inv_ref: object
    query_ref: object
    key_ref: object
    value_ref: object
    prob_ref: object
    pooled: object
    slopes: object
    normed_out: object
    outer_out: object
    grad_in: object
    mix_grad: object
    row_dots: object
    gain_part: object
    hidden_sum: object
    pull_ref: object
    keep: object
    keep_b: object
    gain_got: object
    pool_ref: object
    near_send: object
    near_got: object
    far_send: object
    far_got: object
    relay_send: object
    near_send_b: object
    near_got_b: object
    far_send_b: object
    far_got_b: object
    relay_send_b: object
    load_sem: object
    enter_sem: object
    relay_s: object
    relay_r: object
    in_far_s: object
    in_far_r: object
    in_near_s: object
    in_near_r: object
    out_far_s: object
    out_far_r: object
    out_near_s: object
    out_near_r: object
    relay_sb: object
    relay_rb: object
    in_far_sb: object
    in_far_rb: object
    in_near_sb: object
    in_near_rb: object
    out_far_sb: object
    out_far_rb: object
    out_near_sb: object
    out_near_rb: object
    pool_s: object
    pool_r: object
    normed_s: object
    normed_r: object
    mixture_s: object
    mixture_r: object
    outer_s: object
    outer_r: object
    heads_s: object
    heads_r: object
    dots_s: object
    dots_r: object
    pass_s: object
    pass_r: object
    gain_s: object
    gain_r: object


def step_kernel(
    lengths,
    positives,
    entrance,
    gain,
    table,
    wq,
    wk,
    wv,
    wo,
    losses_out,
    gain_out,
    normed_turned,
    mixture_turned,
    outer_all,
    heads_all,
    hidden,
    normed_all,
    mixture_all,
    *scratch,
):
    r = Scratch(*scratch)
    head_w, out_w, acc, squares = r.head_w, r.out_w, r.acc, r.squares
    forth, back = Place(1), Place(-1)
    rows, width = hidden.shape[1:]
    blocks = hidden.shape[0] // 2
    width_all = blocks * width
    pair_count = lengths.shape[0]
    seq_count = 2 * pair_count
    length = rows // pair_count
    query_cols, kv_cols = wq.shape[3], wk.shape[3]
    groups = query_cols // HEAD
    dp_me, mp_me = lax.axis_index("dp"), lax.axis_index("mp")
    dp_count, mp_count = lax.axis_size("dp"), lax.axis_size("mp")
    members = dp_count * mp_count
    me = dp_me * mp_count + mp_me
    share = blocks // dp_count
    row_pad = r.row_dots.shape[2]
    normed_sems, outer_sems = (r.normed_s, r.normed_r), (r.outer_s, r.outer_r)
    mixture_sems, heads_sems = (r.mixture_s, r.mixture_r), (r.heads_s, r.heads_r)
    outer_out = r.outer_out

    def peer(shift):
        spot = lax.rem(me + shift, members)
        return spot // mp_count, lax.rem(spot, mp_count), spot

    def span_of(group):
        return slice(group * rows, (group + 1) * rows)

    def member_rows(member, group):
        return rows_at((member * 2 + group) * rows, rows)

    def sequences(group):
        for local_seq in range(pair_count):
            inner = slice(local_seq * length, (local_seq + 1) * length)
            outer = slice(group * rows + inner.start, group * rows + inner.stop)
            yield group * pair_count + local_seq, inner, outer

    def count_of(seq):
        return lengths[seq // 2, seq % 2]

    spot = lax.broadcasted_iota(jnp.int32, (length, 1), 0)

    def valid_of(seq):
        return jnp.where(spot < count_of(seq), 1.0, 0.0)

    def load(chunk):
        copies, start = [], 0
        for index, weight in enumerate((wq, wk, wv)):
            columns = pl.ds(start, weight.shape[3])
            copies.append(
                pltpu.make_async_copy(
                    weight.at[:, chunk],
                    head_w.at[:, chunk, :, columns],
                    r.load_sem.at[3 * chunk + index],
                )
            )
            start += weight.shape[3]
        return copies

    load_out = pltpu.make_async_copy(wo, out_w, r.load_sem.at[3 * SUB])

    def enter(group, block):
        slot = group * blocks + block
        return pltpu.make_async_copy(
            entrance.at[pl.ds(group * rows, rows), lanes_at(block * width, width)],
            hidden.at[slot],
            r.enter_sem.at[slot],
        )

    for chunk in range(SUB):
        for copy in load(chunk):
            copy.start()

    @pl.when(jnp.logical_not(forth.has_source))
    def _():
        for group in range(2):
            for block in range(blocks):
                enter(group, block).start()

    load_out.start()
    barrier = pltpu.get_barrier_semaphore()
    for shift in range(1, members):
        to_dp, to_mp, _ = peer(shift)
        pl.semaphore_signal(
            barrier, inc=1, device_id={"dp": to_dp, "mp": to_mp}, device_id_type=MESH
        )

    @pl.when(forth.has_source)
    def _():
        pl.semaphore_signal(
            barrier, inc=1, device_id={"section": forth.here - 1}, device_id_type=MESH
        )

    @pl.when(forth.has_target)
    def _():
        pl.semaphore_signal(
            barrier, inc=1, device_id={"section": forth.here + 1}, device_id_type=MESH
        )

    acc[...] = jnp.zeros_like(acc)
    squares[...] = jnp.zeros_like(squares)
    r.mix_grad[...] = jnp.zeros_like(r.mix_grad)
    r.gain_part[...] = jnp.zeros_like(r.gain_part)

    @pl.when(jnp.logical_not(back.has_source))
    def _():
        def clear(block, carry):
            r.grad_in[block] = jnp.zeros((rows, width), BF16)
            return carry

        lax.fori_loop(0, 2 * blocks, clear, 0)

    pool_shape = r.pool_ref.shape
    column = lax.broadcasted_iota(jnp.int32, pool_shape, 1)
    line = lax.broadcasted_iota(jnp.int32, pool_shape, 0)
    picks = jnp.zeros(pool_shape, F32)
    for seq in range(seq_count):
        inside = jnp.logical_and(column >= seq * length, column < seq * length + count_of(seq))
        picks = jnp.where(jnp.logical_and(line == seq % pair_count, inside), 1.0, picks)
    r.pool_ref[...] = picks.astype(BF16)
    expected = (
        members - 1 + forth.has_source.astype(jnp.int32) + forth.has_target.astype(jnp.int32)
    )

    @pl.when(forth.has_source)
    def _():
        for chunk in range(SUB):
            for copy in load(chunk):
                copy.wait()
        pl.semaphore_wait(barrier, expected)

    def gain_at(block):
        return gain[:, lanes_at(block * width, width)]

    def out_columns(block):
        return out_w[:, lanes_at(block * width, width)]

    def consume(group, block):
        slot = group * blocks + block

        @pl.when(jnp.logical_not(forth.has_source))
        def _():
            enter(group, block).wait()
            if group == 0 and block < SUB:
                for copy in load(block):
                    copy.wait()

        value = hidden[slot].astype(F32)
        span = span_of(group)
        squares[span, :] += fold_lanes(value * value)
        for seq, inner, _ in sequences(group):
            r.hidden_sum[seq, :, lanes_at(block * width, width)] = jnp.sum(
                value[inner] * valid_of(seq), axis=0, keepdims=True
            )
        acc[span, :] += jnp.dot(
            (value * gain_at(block)).astype(BF16),
            head_w[block // SUB, block % SUB],
            preferred_element_type=F32,
        )

    mixture = mixture_all.at[pl.ds(pl.multiple_of(dp_me * 2 * rows, ROW_TILE), 2 * rows)]

    def attend(group):
        whole = span_of(group)
        inv_rms = lax.rsqrt(
            jnp.sum(squares[whole, :], axis=1, keepdims=True) * (1.0 / width_all) + EPSILON
        )
        r.inv_ref[whole, :] = inv_rms
        for seq, inner, span in sequences(group):
            inverse = inv_rms[inner]
            query = jnp.concatenate(
                [
                    rotary(acc[span, g * HEAD : (g + 1) * HEAD] * inverse, table, 1.0)
                    for g in range(groups)
                ],
                axis=0,
            ).astype(BF16)
            key = rotary(acc[span, query_cols : query_cols + kv_cols] * inverse, table, 1.0)
            key = key.astype(BF16)
            value = (acc[span, query_cols + kv_cols :] * inverse).astype(BF16)
            r.query_ref[seq] = query
            r.key_ref[seq] = key
            r.value_ref[seq] = value
            scores = contract_last(query, key) * HEAD ** (-0.5)
            place = lax.broadcasted_iota(jnp.int32, scores.shape, 0) % length
            scores = jnp.where(
                place >= lax.broadcasted_iota(jnp.int32, scores.shape, 1), scores, -1e30
            )
            weights = jnp.exp(scores - jnp.max(scores, axis=1, keepdims=True))
            weights = weights / jnp.sum(weights, axis=1, keepdims=True)
            r.prob_ref[seq] = weights
            mixed = jnp.dot(weights.astype(BF16), value, preferred_element_type=F32).astype(BF16)
            for g in range(groups):
                mixture[span, g * HEAD : (g + 1) * HEAD] = mixed[g * length : (g + 1) * length]
        if group == 0:

            @pl.when(jnp.logical_not(forth.has_source))
            def _():
                pl.semaphore_wait(barrier, expected)

            load_out.wait()

    first = (mp_me == 0).astype(F32)
    pooled = r.pooled

    def pool_copy(group, shift, own):
        other_dp, other_mp, spot = peer(shift)
        member = group * members + (me if own else spot)
        return pltpu.make_async_remote_copy(
            src_ref=pooled.at[member],
            dst_ref=pooled.at[member],
            send_sem=r.pool_s.at[group * members + shift],
            recv_sem=r.pool_r.at[member],
            device_id={"dp": other_dp, "mp": other_mp},
            device_id_type=MESH,
        )

    def send_pooled(group):
        span = span_of(group)
        mixture_sum = jnp.dot(r.pool_ref[:, span], mixture[span, :], preferred_element_type=F32)
        coarse = mixture_sum.astype(BF16)
        fine = (mixture_sum - coarse.astype(F32)).astype(BF16)
        both = jnp.concatenate([coarse, fine], axis=0)

        def pool_block(block, carry):
            sums = jnp.dot(both, out_columns(block), preferred_element_type=F32)
            sums = sums[: pool_shape[0]] + sums[pool_shape[0] :]
            lines = [
                (sums[line : line + 1] + first * r.hidden_sum[seq, :, lanes_at(block * width, width)])
                / count_of(seq).astype(F32)
                for line, (seq, _, _) in enumerate(sequences(group))
            ]
            lines = lines[0] if pair_count == 1 else jnp.concatenate(lines, axis=0)
            pooled[group * members + me, :, lanes_at(block * width, width)] = lines
            return carry

        lax.fori_loop(0, blocks, pool_block, 0, unroll=4)
        for shift in range(1, members):
            pool_copy(group, shift, True).start()

    def part(group, block):
        return jnp.dot(mixture[span_of(group), :], out_columns(block), preferred_element_type=F32)

    def finish(group, block, total, inner):
        return (hidden[group * blocks + block, inner, :].astype(F32) + total).astype(BF16)

    ins = [
        StreamIn(
            forth,
            group,
            hidden,
            (r.relay_s, r.relay_r),
            (r.in_far_s, r.in_far_r),
            (r.in_near_s, r.in_near_r),
        )
        for group in range(2)
    ]
    outs = [
        StreamOut(
            forth,
            group,
            part,
            finish,
            hidden,
            (r.near_send, r.near_got, r.far_send, r.far_got, r.relay_send, r.keep),
            (r.relay_s, r.relay_r),
            (r.out_far_s, r.out_far_r),
            (r.out_near_s, r.out_near_r),
        )
        for group in range(2)
    ]
    run_pass(
        FORWARD_ORDER,
        ins,
        outs,
        forth.has_source,
        forth.has_target,
        consume,
        attend,
        lambda group: None,
        send_pooled,
    )

    @pl.when(forth.has_target)
    def _():
        for group in range(2):
            send_pooled(group)

    def to_owner(source, target, sems, group, block):
        step = lax.rem(block, share)
        return pltpu.make_async_remote_copy(
            src_ref=source.at[group * blocks + block],
            dst_ref=target.at[step, member_rows(dp_me, group)],
            send_sem=sems[0].at[group * blocks + block],
            recv_sem=sems[1].at[dp_me, group * share + step],
            device_id={"dp": block // share},
            device_id_type=MESH,
        )

    def from_member(target, sems, member, group, step):
        piece = target.at[step, member_rows(member, group)]
        return pltpu.make_async_remote_copy(
            src_ref=piece,
            dst_ref=piece,
            send_sem=sems[0].at[0],
            recv_sem=sems[1].at[member, group * share + step],
            device_id={"dp": member},
            device_id_type=MESH,
        )

    def rows_copy(target, sems, shift, group, own):
        other = lax.rem(dp_me + shift, dp_count)
        member = dp_me if own else other
        piece = target.at[member_rows(member, group)]
        return pltpu.make_async_remote_copy(
            src_ref=piece,
            dst_ref=piece,
            send_sem=sems[0].at[group * dp_count + shift],
            recv_sem=sems[1].at[group * dp_count + member],
            device_id={"dp": other},
            device_id_type=MESH,
        )

    def hand_out(value, spare, target, sems, group, block, passes=None):
        mine = block // share == dp_me

        @pl.when(mine)
        def _():
            target[lax.rem(block, share), member_rows(dp_me, group), :] = value

        sends = jnp.logical_not(mine)
        if passes is not None:
            sends = jnp.logical_and(sends, passes)

        @pl.when(sends)
        def _():
            spare[group * blocks + block] = value
            to_owner(spare, target, sems, group, block).start()

    def hand_out_normed():
        for group in range(2):

            def normed_block(block, carry, group=group):
                value = hidden[group * blocks + block].astype(F32) * r.inv_ref[span_of(group), :]
                value = (value * gain_at(block)).astype(BF16)
                hand_out(value, r.normed_out, normed_all, normed_sems, group, block)
                return carry

            lax.fori_loop(0, blocks, normed_block, 0, unroll=2)
            for shift in range(1, dp_count):
                rows_copy(mixture_all, mixture_sems, shift, group, True).start()

    def turn_over():
        for group in range(2):
            for shift in range(1, dp_count):
                member = lax.rem(dp_me + shift, dp_count)
                rows_copy(mixture_all, mixture_sems, shift, group, False).wait_recv()
                for step in range(share):
                    from_member(normed_all, normed_sems, member, group, step).wait_recv()

        def turn(step, carry):
            normed_turned[step] = normed_all[step].T
            return carry

        lax.fori_loop(0, share, turn, 0)
        mixture_turned[...] = mixture_all[...].T

    pl.when(back.has_source)(hand_out_normed)
    for group in range(2):
        for shift in range(1, members):
            pool_copy(group, shift, False).wait_recv()
    embedded = []
    for group in range(2):
        for member in range(dp_count):
            start = group * members + member * mp_count
            total = pooled[start]
            for other in range(1, mp_count):
                total = total + pooled[start + other]
            embedded.append(total)
    pairs = dp_count * pair_count

    def embedding(seq):
        member, inner = seq // seq_count, seq % seq_count
        block = embedded[inner // pair_count * dp_count + member]
        return block[inner % pair_count :][:1]

    queries = jnp.concatenate([embedding(2 * p) for p in range(pairs)], axis=0)
    passages = jnp.concatenate([embedding(2 * p + 1) for p in range(pairs)], axis=0)
    partner = lax.broadcasted_iota(jnp.int32, (pairs, pairs), 1)
    line = lax.broadcasted_iota(jnp.int32, (pairs, pairs), 0)
    target = jnp.zeros((pairs, pairs), F32)
    for p in range(pairs):
        target = jnp.where(jnp.logical_and(line == p, partner == positives[p]), 1.0, target)
    losses, query_slopes, passage_slopes = matryoshka(queries, passages, target)
    lane = lax.broadcasted_iota(jnp.int32, (1, 128), 1)
    packed = jnp.zeros((1, 128), F32)
    for level in range(WIDTHS):
        packed = jnp.where(lane == level, losses[level], packed)
    losses_out[...] = packed[:, :WIDTHS]
    slopes = r.slopes
    for p in range(pairs):
        slopes[2 * p] = query_slopes[p : p + 1]
        slopes[2 * p + 1] = passage_slopes[p : p + 1]

    waits_long = back.here < back.count - 2
    pl.when(waits_long)(turn_over)

    grad_in, mix_grad = r.grad_in, r.mix_grad

    def upstream(group, block):
        tokens = [
            valid_of(seq)
            / count_of(seq).astype(F32)
            * slopes[dp_me * seq_count + seq, :, lanes_at(block * width, width)]
            for seq, _, _ in sequences(group)
        ]
        tokens = tokens[0] if pair_count == 1 else jnp.concatenate(tokens, axis=0)
        return tokens + grad_in[group * blocks + block].astype(F32)

    def consume_back(group, block):
        outer = upstream(group, block).astype(BF16)
        passes = lax.rem(block, 2) == forth.low
        hand_out(outer, outer_out, outer_all, outer_sems, group, block, passes)
        mix_grad[span_of(group), :] += contract_last(outer, out_columns(block))

    head_grads = heads_all.at[pl.ds(pl.multiple_of(dp_me * 2 * rows, ROW_TILE), 2 * rows)]
    row_dots = r.row_dots
    diagonal = lax.broadcasted_iota(jnp.int32, (rows, row_pad), 0) == lax.broadcasted_iota(
        jnp.int32, (rows, row_pad), 1
    )

    def dots_copy(shift, group, own):
        other = lax.rem(mp_me + shift, mp_count)
        member = mp_me if own else other
        piece = row_dots.at[group * mp_count + member]
        return pltpu.make_async_remote_copy(
            src_ref=piece,
            dst_ref=piece,
            send_sem=r.dots_s.at[group * mp_count + shift],
            recv_sem=r.dots_r.at[group * mp_count + member],
            device_id={"mp": other},
            device_id_type=MESH,
        )

    def attend_back(group):
        row_dot = []
        for seq, _, span in sequences(group):
            mixed = jnp.concatenate(
                [mix_grad[span, g * HEAD : (g + 1) * HEAD] for g in range(groups)], axis=0
            ).astype(BF16)
            weights = r.prob_ref[seq]
            value_grad = contract_rows(weights.astype(BF16), mixed).astype(BF16)
            pulled = contract_last(mixed, r.value_ref[seq]).astype(BF16).astype(F32)
            score_grad = weights * (pulled - jnp.sum(weights * pulled, axis=1, keepdims=True))
            score_grad = (score_grad * HEAD ** (-0.5)).astype(BF16)
            query_grad = jnp.dot(score_grad, r.key_ref[seq], preferred_element_type=F32)
            query_grad = query_grad.astype(BF16).astype(F32)
            key_grad = contract_rows(score_grad, r.query_ref[seq]).astype(BF16).astype(F32)
            pieces = [
                rotary(query_grad[g * length : (g + 1) * length], table, -1.0).astype(BF16)
                for g in range(groups)
            ]
            pieces = pieces + [rotary(key_grad, table, -1.0).astype(BF16), value_grad]
            joined = jnp.concatenate(pieces, axis=1)
            head_grads[span, :] = joined
            row_dot.append(lane_sum(joined.astype(F32) * acc[span, :]))
        for shift in range(1, dp_count):
            rows_copy(heads_all, heads_sems, shift, group, True).start()
        row_dot = row_dot[0] if pair_count == 1 else jnp.concatenate(row_dot, axis=0)

        @pl.when(back.has_target)
        def _():
            row_dots[group * mp_count + mp_me] = jnp.sum(
                jnp.where(diagonal, row_dot, 0.0), axis=0, keepdims=True
            )
            for shift in range(1, mp_count):
                dots_copy(shift, group, True).start()

    def part_back(group, block):
        span = span_of(group)
        value = contract_last(head_grads[span, :], head_w[block // SUB, lax.rem(block, SUB)])
        scaled = value * (hidden[group * blocks + block].astype(F32) * r.inv_ref[span, :])
        r.gain_part[:, lanes_at(block * width, width)] += jnp.sum(scaled, axis=0, keepdims=True)
        return value

    def prepare(group):
        for shift in range(1, mp_count):
            dots_copy(shift, group, False).wait_recv()
        total = row_dots[group * mp_count]
        for member in range(1, mp_count):
            total = total + row_dots[group * mp_count + member]
        inverse = r.inv_ref[span_of(group), :]
        r.pull_ref[span_of(group), :] = (
            lane_sum(jnp.where(diagonal, total, 0.0))
            * inverse
            * inverse
            * inverse
            * (1.0 / width_all)
        )

    def finish_back(group, block, total, inner):
        span = slice(group * rows + inner.start, group * rows + inner.stop)
        value = upstream(group, block)[inner] + total * gain_at(block) * r.inv_ref[span, :]
        pulled = hidden[group * blocks + block, inner, :].astype(F32) * r.pull_ref[span, :]
        return (value - pulled).astype(BF16)

    def gain_only(group):
        def body(block, carry):
            part_back(group, block)
            return carry

        lax.fori_loop(0, blocks, body, 0, unroll=4)

    ins_back = [
        StreamIn(
            back,
            group,
            grad_in,
            (r.relay_sb, r.relay_rb),
            (r.in_far_sb, r.in_far_rb),
            (r.in_near_sb, r.in_near_rb),
        )
        for group in range(2)
    ]
    outs_back = [
        StreamOut(
            back,
            group,
            part_back,
            finish_back,
            grad_in,
            (r.near_send_b, r.near_got_b, r.far_send_b, r.far_got_b, r.relay_send_b, r.keep_b),
            (r.relay_sb, r.relay_rb),
            (r.out_far_sb, r.out_far_rb),
            (r.out_near_sb, r.out_near_rb),
        )
        for group in range(2)
    ]
    run_pass(
        BACKWARD_ORDER,
        ins_back,
        outs_back,
        back.has_source,
        back.has_target,
        consume_back,
        attend_back,
        prepare,
        gain_only,
    )

    pl.when(jnp.logical_not(back.has_source))(hand_out_normed)
    pl.when(jnp.logical_not(waits_long))(turn_over)

    def pass_on(member, group, step):
        piece = outer_all.at[step, member_rows(member, group)]
        return pltpu.make_async_remote_copy(
            src_ref=piece,
            dst_ref=piece,
            send_sem=r.pass_s.at[member, group * share + step],
            recv_sem=r.pass_r.at[member, group * share + step],
            device_id={"mp": forth.near},
            device_id_type=MESH,
        )

    gain_got = r.gain_got
    gain_cols = gain_got.shape[2]

    def gain_copy(shift):
        to_dp, to_mp, spot = peer(shift)
        return pltpu.make_async_remote_copy(
            src_ref=r.gain_part.at[:, lanes_at(spot * gain_cols, gain_cols)],
            dst_ref=gain_got.at[me],
            send_sem=r.gain_s.at[shift],
            recv_sem=r.gain_r.at[me],
            device_id={"dp": to_dp, "mp": to_mp},
            device_id_type=MESH,
        )

    def gain_arrival(shift):
        from_dp, from_mp, spot = peer(shift)
        return pltpu.make_async_remote_copy(
            src_ref=gain_got.at[spot],
            dst_ref=gain_got.at[spot],
            send_sem=r.gain_s.at[shift],
            recv_sem=r.gain_r.at[spot],
            device_id={"dp": from_dp, "mp": from_mp},
            device_id_type=MESH,
        )

    for shift in range(1, members):
        gain_copy(shift).start()
    for group in range(2):
        for shift in range(1, dp_count):
            member = lax.rem(dp_me + shift, dp_count)
            for pair in range(share // 2):
                step = 2 * pair + forth.low
                from_member(outer_all, outer_sems, member, group, step).wait_recv()
                pass_on(member, group, step).start()
    drain_pass(ins, outs, forth.has_source, forth.has_target)
    for group in range(2):
        for shift in range(1, dp_count):
            member = lax.rem(dp_me + shift, dp_count)
            for pair in range(share // 2):
                pass_on(member, group, 2 * pair + 1 - forth.low).wait_recv()
    drain_pass(ins_back, outs_back, back.has_source, back.has_target)

    @pl.when(back.has_target)
    def _():
        for group in range(2):
            for shift in range(1, mp_count):
                dots_copy(shift, group, True).wait_send()

    total = r.gain_part[:, lanes_at(me * gain_cols, gain_cols)]
    for shift in range(1, members):
        gain_arrival(shift).wait_recv()
        total = total + gain_got[lax.rem(me + shift, members)]
    gain_out[...] = total

    for shift in range(1, members):
        for group in range(2):
            pool_copy(group, shift, True).wait_send()
        gain_copy(shift).wait_send()
    for group in range(2):
        for shift in range(1, dp_count):
            rows_copy(mixture_all, mixture_sems, shift, group, True).wait_send()
            rows_copy(heads_all, heads_sems, shift, group, True).wait_send()
            rows_copy(heads_all, heads_sems, shift, group, False).wait_recv()

        def drain(block, carry, group=group):
            away = block // share != dp_me

            @pl.when(away)
            def _():
                to_owner(r.normed_out, normed_all, normed_sems, group, block).wait_send()

            @pl.when(jnp.logical_and(away, lax.rem(block, 2) == forth.low))
            def _():
                to_owner(outer_out, outer_all, outer_sems, group, block).wait_send()

            return carry

        lax.fori_loop(0, blocks, drain, 0)
        for shift in range(1, dp_count):
            member = lax.rem(dp_me + shift, dp_count)
            for pair in range(share // 2):
                pass_on(member, group, 2 * pair + forth.low).wait_send()


def step_pass(lengths, positives, entrance, gain, table, wq, wk, wv, wo):
    rows, width_all = entrance.shape
    dp_count, mp_count = lax.axis_size("dp"), lax.axis_size("mp")
    members = dp_count * mp_count
    blocks = mp_count * SUB
    width = width_all // blocks
    share = blocks // dp_count
    seq_count = 2 * lengths.shape[0]
    length = rows // seq_count
    query_cols = wq.shape[1]
    head_cols = query_cols + wk.shape[1] + wv.shape[1]
    stacked = query_cols // HEAD * length
    row_pad = -(-(rows // 2) // 128) * 128
    pool_rows = -(-seq_count // 16) * 16
    head_weights = [weight.reshape(mp_count, SUB, width, -1) for weight in (wq, wk, wv)]
    dma = pltpu.SemaphoreType.DMA
    block = (rows // 2, width)
    shapes = dict(
        head_w=((mp_count, SUB, width, head_cols), BF16),
        out_w=(wo.shape, BF16),
        acc=((rows, head_cols), F32),
        squares=((rows, 128), F32),
        inv_ref=((rows, 1), F32),
        pull_ref=((rows, 1), F32),
        query_ref=((seq_count, stacked, HEAD), BF16),
        key_ref=((seq_count, length, HEAD), BF16),
        value_ref=((seq_count, length, HEAD), BF16),
        prob_ref=((seq_count, stacked, length), F32),
        pooled=((2 * members, seq_count // 2, width_all), F32),
        hidden_sum=((seq_count, 1, width_all), F32),
        slopes=((dp_count * seq_count, 1, width_all), F32),
        normed_out=((2 * blocks, *block), BF16),
        outer_out=((2 * blocks, *block), BF16),
        grad_in=((2 * blocks, *block), BF16),
        mix_grad=((rows, query_cols), F32),
        row_dots=((2 * mp_count, 1, row_pad), F32),
        gain_part=((1, width_all), F32),
        gain_got=((members, 1, width_all // members), F32),
        pool_ref=((pool_rows, rows), BF16),
        near_send=((4 * SUB, *block), BF16),
        near_got=((4 * SUB, *block), BF16),
        far_send=((2 * SUB, *block), BF16),
        far_got=((2 * SUB, *block), BF16),
        relay_send=((2 * SUB, *block), BF16),
        keep=((2 * SUB, *block), F32),
        near_send_b=((4 * SUB, *block), BF16),
        near_got_b=((4 * SUB, *block), BF16),
        far_send_b=((2 * SUB, *block), BF16),
        far_got_b=((2 * SUB, *block), BF16),
        relay_send_b=((2 * SUB, *block), BF16),
        keep_b=((2 * SUB, *block), F32),
    )
    counts = dict(
        load_sem=(3 * SUB + 1,),
        enter_sem=(2 * blocks,),
        pool_s=(2 * members,),
        pool_r=(2 * members,),
        normed_s=(2 * blocks,),
        normed_r=(dp_count, 2 * share),
        outer_s=(2 * blocks,),
        outer_r=(dp_count, 2 * share),
        mixture_s=(2 * dp_count,),
        mixture_r=(2 * dp_count,),
        pass_s=(dp_count, 2 * share),
        pass_r=(dp_count, 2 * share),
        heads_s=(2 * dp_count,),
        heads_r=(2 * dp_count,),
        dots_s=(2 * mp_count,),
        dots_r=(2 * mp_count,),
        gain_s=(members,),
        gain_r=(members,),
        relay_s=(2 * SUB * PIECES,),
        in_far_s=(2 * SUB * PIECES,),
        out_far_s=(2 * SUB * PIECES,),
        in_near_s=(4 * SUB * PIECES,),
        out_near_s=(4 * SUB * PIECES,),
        relay_r=(2 * SUB * PIECES,),
        in_far_r=(2 * SUB * PIECES,),
        out_far_r=(2 * SUB * PIECES,),
        in_near_r=(4 * SUB * PIECES,),
        out_near_r=(4 * SUB * PIECES,),
        relay_sb=(2 * SUB * PIECES,),
        in_far_sb=(2 * SUB * PIECES,),
        out_far_sb=(2 * SUB * PIECES,),
        in_near_sb=(4 * SUB * PIECES,),
        out_near_sb=(4 * SUB * PIECES,),
        relay_rb=(2 * SUB * PIECES,),
        in_far_rb=(2 * SUB * PIECES,),
        out_far_rb=(2 * SUB * PIECES,),
        in_near_rb=(4 * SUB * PIECES,),
        out_near_rb=(4 * SUB * PIECES,),
    )
    scratch = Scratch(
        **{name: pltpu.VMEM(*shape) for name, shape in shapes.items()},
        **{name: dma(count) for name, count in counts.items()},
    )
    vmem = pl.BlockSpec(memory_space=pltpu.VMEM)
    smem = pl.BlockSpec(memory_space=pltpu.SMEM)
    hbm = pl.BlockSpec(memory_space=pltpu.HBM)
    return pl.pallas_call(
        step_kernel,
        out_shape=(
            jax.ShapeDtypeStruct((1, WIDTHS), F32),
            jax.ShapeDtypeStruct((1, width_all // members), F32),
            jax.ShapeDtypeStruct((share, width, dp_count * rows), BF16),
            jax.ShapeDtypeStruct((query_cols, dp_count * rows), BF16),
            jax.ShapeDtypeStruct((share, dp_count * rows, width), BF16),
            jax.ShapeDtypeStruct((dp_count * rows, head_cols), BF16),
        ),
        in_specs=[smem, smem, hbm, vmem, vmem, hbm, hbm, hbm, hbm],
        out_specs=(vmem,) * 6,
        scratch_shapes=[
            pltpu.VMEM((2 * blocks, *block), BF16),
            pltpu.VMEM((share, dp_count * rows, width), BF16),
            pltpu.VMEM((dp_count * rows, query_cols), BF16),
            *scratch,
        ],
        compiler_params=pltpu.CompilerParams(
            collective_id=0, has_side_effects=True, vmem_limit_bytes=36 * 1024 * 1024
        ),
        name="step_pass",
    )(
        *[
            pltpu.with_memory_space_constraint(array, pltpu.HBM)
            for array in (lengths, positives, entrance, gain, table, *head_weights, wo)
        ]
    )


def weight_kernel(
    normed,
    mixture,
    outer,
    heads,
    losses,
    gain_share,
    query_grad,
    key_grad,
    value_grad,
    out_grad,
    losses_out,
    gain_out,
):
    query_cols, kv_cols = query_grad.shape[1], key_grad.shape[1]

    @pl.when(pl.program_id(0) == 0)
    def _():
        losses_out[...] = losses[...]
        gain_out[...] = gain_share[...]

    width = normed.shape[1]
    for half in range(2):
        step = pl.program_id(0) * 2 + half
        span = slice(half * width, (half + 1) * width)
        product = jnp.dot(normed[step], heads[...], preferred_element_type=F32)
        query_grad[span, :] = product[:, :query_cols]
        key_grad[span, :] = product[:, query_cols : query_cols + kv_cols]
        value_grad[span, :] = product[:, query_cols + kv_cols :]
        out_grad[:, span] = jnp.dot(mixture[...], outer[step], preferred_element_type=F32)


def weight_grads(normed, mixture, outer, heads, losses, gain_share, query_cols, kv_cols):
    share, width, _ = normed.shape
    columns = share * width
    vmem = pl.BlockSpec(memory_space=pltpu.VMEM)

    def tall(cols):
        return pl.BlockSpec((2 * width, cols), lambda step: (step, 0))

    return pl.pallas_call(
        weight_kernel,
        grid=(share // 2,),
        in_specs=[vmem] * 6,
        out_specs=(
            tall(query_cols),
            tall(kv_cols),
            tall(kv_cols),
            pl.BlockSpec((query_cols, 2 * width), lambda step: (0, step)),
            vmem,
            vmem,
        ),
        out_shape=(
            pltpu.HBM((columns, query_cols), F32),
            pltpu.HBM((columns, kv_cols), F32),
            pltpu.HBM((columns, kv_cols), F32),
            pltpu.HBM((query_cols, columns), F32),
            jax.ShapeDtypeStruct(losses.shape, F32),
            jax.ShapeDtypeStruct(gain_share.shape, F32),
        ),
        compiler_params=pltpu.CompilerParams(
            dimension_semantics=("arbitrary",), vmem_limit_bytes=16 * 1024 * 1024
        ),
        name="weight_grads",
    )(normed, mixture, outer, heads, losses, gain_share)


def local(entrance, lengths, positives, norm_gains, query_proj, key_proj, value_proj, out_proj):
    length = entrance.shape[2]
    width_all = entrance.shape[3]
    query_cols = query_proj.shape[2]
    kv_cols = key_proj.shape[2]
    losses, gain_share, normed, mixture, outer, heads = step_pass(
        lengths,
        positives,
        entrance.reshape(-1, width_all),
        norm_gains,
        jnp.asarray(rotary_constants(length)),
        query_proj[0],
        key_proj[0],
        value_proj[0],
        out_proj[0],
    )
    query_grad, key_grad, value_grad, out_grad, losses, gain_share = weight_grads(
        normed, mixture, outer, heads, losses, gain_share, query_cols, kv_cols
    )
    return (
        losses,
        gain_share,
        query_grad[None],
        key_grad[None],
        value_grad[None],
        out_grad[None],
    )


def solution(mesh):
    in_specs = (
        P("dp", None, None, None),
        P("dp", None),
        P(),
        P("section", None),
        P("section", None, "mp"),
        P("section", None, "mp"),
        P("section", None, "mp"),
        P("section", "mp", None),
    )
    out_specs = (
        P("section", None),
        P("section", ("dp", "mp")),
        P("section", "dp", "mp"),
        P("section", "dp", "mp"),
        P("section", "dp", "mp"),
        P("section", "mp", "dp"),
    )
    return jax.shard_map(local, mesh=mesh, in_specs=in_specs, out_specs=out_specs, check_vma=False)
```
